32 devices in a mesh: batch: 2 (over y), seq: 4 (over x, core), mp: 4 (over z).
Axes of the slice: x: 2, y: 2, z: 4, core: 2. Of those that a mesh axis runs over, the one named last changes fastest.
Arguments:
- tokens: bfloat16 [4096, 2048], P(('batch', 'seq')), may hold values from -6 to 6
- segment_ids: int32 [2, 2048], P('batch'), may hold values from 0 to 3, never falling along the last dimension, each value on 1 to 1024 neighbouring positions
- attn_gain: float32 [2048], replicated, may hold values from 0.5 to 1.5
- w_query: bfloat16 [2048, 2048], P(None, 'mp'), may hold values from -1 to 1
- w_key: bfloat16 [2048, 512], P(None, 'mp'), may hold values from -1 to 1
- w_value: bfloat16 [2048, 512], P(None, 'mp'), may hold values from -0.125 to 0.125
- w_output: bfloat16 [2048, 2048], P('mp'), may hold values from -1 to 1
- mlp_gain: float32 [2048], replicated, may hold values from 0.5 to 1.5
- w_gate: bfloat16 [2048, 8192], P(None, 'mp'), may hold values from -0.125 to 0.125
- w_up: bfloat16 [2048, 8192], P(None, 'mp'), may hold values from -0.125 to 0.125
- w_down: bfloat16 [8192, 2048], P('mp'), may hold values from -0.0625 to 0.0625
- cotangent: bfloat16 [4096, 2048], P(('batch', 'seq')), may hold values from -6 to 6
Outputs:
- output: bfloat16 [4096, 2048], P(('batch', 'seq'))
- grad_tokens: bfloat16 [4096, 2048], P(('batch', 'seq'))
- grad_attn_gain: float32 [2048], P(('batch', 'seq'))
- grad_query: float32 [2048, 2048], P(('batch', 'seq'), 'mp')
- grad_key: float32 [2048, 512], P(('batch', 'seq'), 'mp')
- grad_value: float32 [2048, 512], P(('batch', 'seq'), 'mp')
- grad_output: float32 [2048, 2048], P('mp', ('batch', 'seq'))
- grad_mlp_gain: float32 [2048], P(('batch', 'seq'))
- grad_gate: float32 [2048, 8192], P(('batch', 'seq'), 'mp')
- grad_up: float32 [2048, 8192], P(('batch', 'seq'), 'mp')
- grad_down: float32 [8192, 2048], P('mp', ('batch', 'seq'))
The draws below stay inside these ranges and needn't reach their ends.
Inputs may be any that keep to these rules, and one draw needn't show every extreme that they name: `segment_ids`: within a row the ids never fall; a document (a run of one id) has 1 to 1024 tokens, and some document has exactly 1024.
All inputs are finite; a program needn't handle non-finite values.
Results may differ from the reference program's by a relative error of at most 0.025.
Values may be sent and summed in bfloat16 or wider, within the bound.
A program may use at most 256 MiB of HBM per device.

```python
import math
import jax
import jax.numpy as jnp
import numpy as np
from jax import lax

D = 2048
HQ = 32
KV = 8
HS = 64
FF = 8192
QH = 2
COPIES = 2
L = 2048
SEQS = 2
TOKENS = 4096


def draw_projections(key):
    query_w = jnp.clip(jax.random.normal(jax.random.fold_in(key, 71), (D, HQ * HS), jnp.float32), -6.0, 6.0) * D ** (-0.5)
    key_w = jnp.clip(jax.random.normal(jax.random.fold_in(key, 72), (D, KV * HS), jnp.float32), -6.0, 6.0) * D ** (-0.5)
    return (jnp.clip(query_w, -1.0, 1.0), jnp.clip(key_w, -1.0, 1.0))


def draw_w_query(key, part):
    return draw_projections(key)[0].astype(jnp.bfloat16)


def draw_w_key(key, part):
    return draw_projections(key)[1].astype(jnp.bfloat16)


def with_spikes(drawn, rng, source, target, parts, factor):
    def block_of(dim):
        return (jnp.arange(drawn.shape[dim]) // (drawn.shape[dim] // parts)).reshape((-1,) + (1,) * (drawn.ndim - 1 - dim))

    first = jax.random.permutation(rng, parts)[block_of(target)]
    other_side = (block_of(target) + parts // 2) % parts
    return jnp.where((block_of(source) == first) | (block_of(source) == other_side), factor * drawn, drawn)


def level_of(key, extent, cuts, smallest, top_value):
    def one(axis_at, blocks):
        steps = jax.random.uniform(jax.random.fold_in(jax.random.fold_in(key, 6), axis_at), (blocks,), jnp.float32, smallest / len(cuts), top_value / len(cuts))
        return jnp.repeat(jnp.exp(steps), extent[axis_at] // blocks).reshape((-1,) + (1,) * (len(extent) - axis_at - 1))

    gain = one(*cuts[0])
    for cut in cuts[1:]:
        gain = gain * one(*cut)
    return gain


def length_profile(number_of, total, most, slope):
    loads = [(1 << 20) // math.isqrt(grade ** slope) + 1 for grade in range(2, number_of + 1)]
    surplus, given = total - most - (number_of - 1), [1] * (number_of - 1)
    while surplus > 0:
        free = [i for i in range(number_of - 1) if given[i] < most]
        pool, remaining = sum([loads[i] for i in free]), surplus
        for i in free:
            addition = min(most - given[i], max(1, remaining * loads[i] // pool), surplus)
            given[i] = given[i] + addition
            surplus = surplus - addition
    return np.array([most] + given)


def ragged_sizes(own_key, number_of, total, limit, lean):
    if number_of == 2:
        one = jax.random.randint(own_key, (), max(1, total - limit), min(limit, total - 1) + 1)
        return jnp.stack([one, total - one])
    lengths = jnp.asarray(length_profile(number_of, total, limit, lean), jnp.int32)
    couples = (number_of - 1) // 2
    source_of, taker = lengths[1:1 + 2 * couples:2], lengths[2:2 + 2 * couples:2]
    room = jnp.minimum(source_of - 1, limit - taker)
    shifted = jax.random.randint(jax.random.fold_in(own_key, 1), (couples,), 0, 1 << 20) % (room + 1)
    lengths = lengths.at[1:1 + 2 * couples:2].set(source_of - shifted).at[2:2 + 2 * couples:2].set(taker + shifted)
    return lengths[jax.random.permutation(jax.random.fold_in(own_key, 2), number_of)]


def normal_values(rng, extent, scale, most, shards=(), kind=jnp.bfloat16):
    loudness = level_of(rng, extent, shards, -0.22, 0.18) if shards else 1.0
    entries = jax.random.normal(rng, extent, jnp.float32) * scale * loudness
    return jnp.minimum(jnp.maximum(entries, -most), most).astype(kind)


def bell_draw_with(own_key, dims, deviation, bound, split, heavy, held_as=jnp.bfloat16):
    values = deviation * jax.random.normal(own_key, dims, jnp.float32)
    if split:
        values = values * level_of(own_key, dims, split, -0.22, 0.18)
    return jnp.clip(with_spikes(values, jax.random.fold_in(own_key, 3), *heavy), -bound, bound).astype(held_as)


def setup_inputs(seed: int = 0) -> dict:
    key_of = jax.random.split(jax.random.key(seed), 13)
    return {
        "tokens": bell_draw_with(key_of[0], (TOKENS, D), 1.0, 6.0, ((0, 8),), (0, 1, 8, 2.0)),
        "segment_ids": jax.vmap(lambda own: jnp.searchsorted(jnp.cumsum(ragged_sizes(own, 4, L, L // 2, 0)), jnp.arange(L), side="right"))(jax.random.split(key_of[1], SEQS)).reshape((SEQS, L)).astype(jnp.int32),
        "attn_gain": jnp.clip(1.0 + 0.1 * jax.random.normal(key_of[2], (D,), jnp.float32), 0.5, 1.5),
        "w_query": draw_w_query(jax.random.fold_in(key_of[12], 71), 0),
        "w_key": draw_w_key(jax.random.fold_in(key_of[12], 71), 0),
        "w_value": normal_values(key_of[5], (D, KV * HS), D ** -0.5, 0.125, ((1, 4),)),
        "w_output": normal_values(key_of[6], (HQ * HS, D), (HQ * HS // 64) ** -0.5, 1.0, ((0, 4),)),
        "mlp_gain": jnp.clip(1.0 + 0.1 * jax.random.normal(key_of[7], (D,), jnp.float32), 0.5, 1.5),
        "w_gate": normal_values(key_of[8], (D, FF), D ** -0.5, 0.125, ((1, 4),)),
        "w_up": normal_values(key_of[9], (D, FF), D ** -0.5, 0.125, ((1, 4),)),
        "w_down": normal_values(key_of[10], (FF, D), FF ** -0.5, 0.0625, ((0, 4),)),
        "cotangent": normal_values(key_of[11], (TOKENS, D), 1.0, 6.0, ((0, 8),)),
    }


highest = lax.Precision.HIGHEST
rope_base = 500000.0
epsilon = 1e-05
masked_score = -1e+30

@jax.custom_vjp
def low(v):
    return lax.optimization_barrier(v.astype(jnp.bfloat16)).astype(jnp.float32)

@jax.custom_vjp
def low_back(v):
    return v

def low_keep(v):
    return (low(v), None)

def low_pass(kept, grad):
    return (grad,)

def back_keep(v):
    return (v, None)

def back_low(kept, grad):
    return (low(grad),)
low.defvjp(low_keep, low_pass)
low_back.defvjp(back_keep, back_low)

def tables(seq_ids):
    positions = jnp.arange(seq_ids.shape[0], dtype=jnp.int32)
    before = jnp.concatenate([seq_ids[:1] - 1, seq_ids[:-1]])
    doc_start = lax.cummax(jnp.where(seq_ids != before, positions, 0), axis=0)
    doc_place = (positions - doc_start).astype(jnp.float32)
    half_width = HS // 2
    frequency = jnp.exp(jnp.arange(half_width, dtype=jnp.float32) * (-2.0 * math.log(rope_base) / HS))
    angles = doc_place[:, None] * frequency[None, :]
    angles = jnp.concatenate([angles, angles], axis=1)
    return (jnp.cos(angles), jnp.sin(angles))

def rotate_half(values):
    half_width = values.shape[-1] // 2
    return jnp.concatenate([-values[..., half_width:], values[..., :half_width]], axis=-1)

def rope_apply(values, cos_table, sin_table):
    return values * cos_table + rotate_half(values) * sin_table

def matmul(left_side, right_side):
    return jnp.dot(left_side, right_side, precision=highest, preferred_element_type=jnp.float32)

def rms_norm(values, gain_vec):
    inv_rms = lax.rsqrt(lax.optimization_barrier(jnp.mean(values * values, axis=-1, keepdims=True)) + epsilon)
    return values * inv_rms * gain_vec

def attend_group(query_in, key_in, value_in, allowed):
    scores = low_back(jnp.einsum('qhd,kd->hqk', query_in, key_in, precision=highest) * HS ** (-0.5))
    scores = jnp.where(allowed[None], scores, masked_score)
    row_max = lax.optimization_barrier(jnp.max(scores, axis=-1, keepdims=True))
    powers = jnp.exp(scores - row_max)
    shares = powers / lax.optimization_barrier(jnp.sum(powers, axis=-1, keepdims=True))
    return jnp.einsum('hqk,kd->qhd', low(shares), value_in, precision=highest)

def block_forward(tokens, weights, cos_table, sin_table, allowed):
    attn_gain, w_query, w_key, w_value, w_output, mlp_gain, w_gate, w_up, w_down = weights
    seq_length = tokens.shape[0]
    normed = low(rms_norm(tokens, attn_gain))
    query_pre = matmul(normed, w_query).reshape(seq_length, HQ, HS)
    key_pre = low_back(matmul(normed, w_key)).reshape(seq_length, KV, HS)
    value_pre = low_back(matmul(normed, w_value)).reshape(seq_length, KV, HS)
    cos_rows = cos_table[:, None, :]
    sin_rows = sin_table[:, None, :]
    queries = low(rope_apply(low_back(query_pre), cos_rows, sin_rows))
    key_copies = low(rope_apply(low_back(jnp.repeat(key_pre, COPIES, axis=1)), cos_rows, sin_rows))
    value_copies = low(low_back(jnp.repeat(value_pre, COPIES, axis=1)))
    group_count = KV * COPIES

    def one_group(group_items):
        return attend_group(group_items[0], group_items[1], group_items[2], allowed)
    mixed_out = lax.map(jax.checkpoint(one_group), (jnp.moveaxis(queries.reshape(seq_length, group_count, QH, HS), 1, 0), jnp.moveaxis(key_copies, 1, 0), jnp.moveaxis(value_copies, 1, 0)))
    mixed_out = jnp.moveaxis(mixed_out, 0, 1).reshape(seq_length, HQ * HS)
    mixed_out = low_back(low(mixed_out))
    branch = low_back(matmul(mixed_out, w_output))
    middle = tokens + branch
    normed_two = low(rms_norm(middle, mlp_gain))
    gate_pre = low_back(matmul(normed_two, w_gate))
    up_pre = low_back(matmul(normed_two, w_up))
    active = low(jax.nn.silu(gate_pre) * up_pre)
    return middle + low_back(matmul(active, w_down))

def reference(tokens, segment_ids, attn_gain, w_query, w_key, w_value, w_output, mlp_gain, w_gate, w_up, w_down, cotangent):
    params = (attn_gain.astype(jnp.float32), w_query.astype(jnp.float32), w_key.astype(jnp.float32), w_value.astype(jnp.float32), w_output.astype(jnp.float32), mlp_gain.astype(jnp.float32), w_gate.astype(jnp.float32), w_up.astype(jnp.float32), w_down.astype(jnp.float32))
    token_rows = tokens.astype(jnp.float32).reshape(SEQS, L, D)
    cot_rows = cotangent.astype(jnp.float32).reshape(SEQS, L, D)
    positions = jnp.arange(L, dtype=jnp.int32)

    def scan_step(running, inputs):
        seq_tokens, seq_ids, seq_cot = inputs
        cos_table, sin_table = tables(seq_ids)
        allowed = (seq_ids[:, None] == seq_ids[None, :]) & (positions[None, :] <= positions[:, None])

        def forward(values_in, weights):
            return block_forward(values_in, weights, cos_table, sin_table, allowed)
        result, pullback = jax.vjp(forward, seq_tokens, params)
        grad_in, grad_weights = pullback(seq_cot)
        running = tuple((summed + addend for summed, addend in zip(running, grad_weights)))
        return (running, (result, grad_in))
    zero_grads = tuple((jnp.zeros_like(weight) for weight in params))
    totals, (results, grad_rows) = lax.scan(scan_step, zero_grads, (token_rows, segment_ids, cot_rows))
    output = results.reshape(TOKENS, D).astype(jnp.bfloat16)
    grad_tokens = grad_rows.reshape(TOKENS, D).astype(jnp.bfloat16)
    return (output, grad_tokens, totals[0], totals[1], totals[2], totals[3], totals[4], totals[5], totals[6], totals[7], totals[8])
```

```python
import functools
import math

import jax
import jax.numpy as jnp
from jax import lax
from jax.experimental import pallas as pl
from jax.experimental.pallas import tpu as pltpu
from jax.sharding import PartitionSpec as P

HS = 64
PAIR = 2 * HS
LONGEST = 1024
rope_base = 500000.0
epsilon = 1e-05
masked_score = -1e30
MESH = pl.DeviceIdType.MESH
F32 = jnp.float32
BF16 = jnp.bfloat16


def dot_nn(left, right):
    return lax.dot_general(left, right, (((1,), (0,)), ((), ())), preferred_element_type=F32)


def dot_nt(left, right):
    return lax.dot_general(left, right, (((1,), (1,)), ((), ())), preferred_element_type=F32)


def dot_tn(left, right):
    return lax.dot_general(left, right, (((0,), (0,)), ((), ())), preferred_element_type=F32)


def lanes_of(values):
    return lax.broadcasted_iota(jnp.int32, values.shape, 1)


def swap_halves(values):
    ahead = pltpu.roll(values, PAIR - HS // 2, 1)
    behind = pltpu.roll(values, HS // 2, 1)
    return jnp.where(lanes_of(values) % HS < HS // 2, ahead, behind)


def rope_tables(segments, first_row, rows):
    row_segment = lax.dynamic_slice_in_dim(segments, first_row, rows, 0)
    doc_start = jnp.sum((segments[None, :] < row_segment[:, None]).astype(jnp.int32), axis=1)
    place = (first_row + jnp.arange(rows, dtype=jnp.int32) - doc_start).astype(F32)
    lane = jnp.arange(PAIR, dtype=jnp.int32)
    frequency = jnp.exp((lane % (HS // 2)).astype(F32) * (-2.0 * math.log(rope_base) / HS))
    angles = place[:, None] * frequency[None, :]
    sign = jnp.where(lane % HS < HS // 2, -1.0, 1.0)
    return jnp.cos(angles), jnp.sin(angles) * sign[None, :]


def project_kernel(x_ref, gain_ref, wq_ref, wk_ref, wv_ref, cos_ref, sin_ref, n_ref, q_ref, kv_ref):
    wide = x_ref[...].astype(F32)
    scale = lax.rsqrt(jnp.mean(wide * wide, axis=-1, keepdims=True) + epsilon)
    normed = (wide * scale * gain_ref[...]).astype(BF16)
    n_ref[...] = normed
    cos, sin = cos_ref[...], sin_ref[...]
    queries = dot_nn(normed, wq_ref[...])
    for start in range(0, queries.shape[1], PAIR):
        part = queries[:, start : start + PAIR]
        q_ref[:, start : start + PAIR] = (part * cos + swap_halves(part) * sin).astype(BF16)
    keys = dot_nn(normed, wk_ref[...])
    keys = keys * cos + swap_halves(keys) * sin
    values = dot_nn(normed, wv_ref[...])
    low_half = lanes_of(keys) < HS
    kv_ref[:, :PAIR] = jnp.where(low_half, keys, pltpu.roll(values, HS, 1)).astype(BF16)
    kv_ref[:, PAIR:] = jnp.where(low_half, pltpu.roll(keys, HS, 1), values).astype(BF16)


def project(tokens, gain, w_query, w_key, w_value, cos, sin):
    rows, width = tokens.shape
    block = rows // 2
    full = lambda array: pl.BlockSpec(array.shape, lambda i: (0, 0))
    tile = lambda columns: pl.BlockSpec((block, columns), lambda i: (i, 0))
    return pl.pallas_call(
        project_kernel,
        grid=(rows // block,),
        in_specs=[
            tile(width),
            full(gain),
            full(w_query),
            full(w_key),
            full(w_value),
            tile(PAIR),
            tile(PAIR),
        ],
        out_specs=[tile(width), tile(w_query.shape[1]), tile(2 * PAIR)],
        out_shape=[
            jax.ShapeDtypeStruct((rows, width), BF16),
            jax.ShapeDtypeStruct((rows, w_query.shape[1]), BF16),
            jax.ShapeDtypeStruct((rows, 2 * PAIR), BF16),
        ],
        cost_estimate=pl.CostEstimate(
            flops=2 * rows * width * (w_query.shape[1] + 2 * PAIR),
            bytes_accessed=8 << 20,
            transcendentals=0,
        ),
        name="project",
    )(tokens, gain, w_query, w_key, w_value, cos, sin)


def write_bias(bias_ref, key_ref, row_ref):
    keys, rows = bias_ref.shape
    key_place = lax.broadcasted_iota(jnp.int32, (keys, rows), 0) - (keys - rows)
    row_place = lax.broadcasted_iota(jnp.int32, (keys, rows), 1)
    allowed = (key_ref[...] == row_ref[...]) & (key_place <= row_place)
    bias_ref[...] = jnp.where(allowed, 0.0, masked_score)


def attend_kernel(q_ref, far_ref, near_ref, own_ref, key_ref, row_ref, out_ref, log_ref, bias_ref, kv_ref):
    @pl.when(pl.program_id(0) == 0)
    def _():
        write_bias(bias_ref, key_ref, row_ref)

    rows = q_ref.shape[0]
    for at, ref in enumerate((far_ref, near_ref, own_ref)):
        kv_ref[at * rows : (at + 1) * rows, :] = ref[...]
    key_value = kv_ref[...]
    flipped = key_value.T
    q_flipped = (q_ref[...].astype(F32) * HS ** (-0.5)).astype(BF16).T
    outs = []
    for head in range(2):
        scores = dot_nn(key_value[:, :HS], q_flipped[head * HS : (head + 1) * HS, :]) + bias_ref[...]
        top = jnp.max(scores, axis=0, keepdims=True)
        powers = jnp.exp(scores - top)
        total = jnp.sum(powers, axis=0, keepdims=True)
        mixed = dot_nn(flipped[HS:, :], powers.astype(BF16))
        outs.append(mixed / total)
        log_ref[0, head : head + 1, :] = top + jnp.log(total)
    out_ref[...] = jnp.concatenate(outs, axis=0).T.astype(BF16)


def attend(queries, far, near, own, key_segment, row_segment):
    rows, width = queries.shape
    pairs = width // PAIR
    per_group = pairs // 2
    pair_tile = pl.BlockSpec((rows, PAIR), lambda p: (0, p))
    kv_tile = pl.BlockSpec((rows, PAIR), lambda p: (0, p // per_group))
    return pl.pallas_call(
        attend_kernel,
        grid=(pairs,),
        in_specs=[
            pair_tile,
            kv_tile,
            kv_tile,
            kv_tile,
            pl.BlockSpec(key_segment.shape, lambda p: (0, 0)),
            pl.BlockSpec(row_segment.shape, lambda p: (0, 0)),
        ],
        out_specs=[pair_tile, pl.BlockSpec((1, 2, rows), lambda p: (p, 0, 0))],
        out_shape=[
            jax.ShapeDtypeStruct((rows, width), BF16),
            jax.ShapeDtypeStruct((pairs, 2, rows), F32),
        ],
        scratch_shapes=[pltpu.VMEM((3 * rows, rows), F32), pltpu.VMEM((3 * rows, PAIR), BF16)],
        cost_estimate=pl.CostEstimate(
            flops=16 << 30, bytes_accessed=4 << 20, transcendentals=3 * rows * rows * 2 * pairs
        ),
        name="attend",
    )(queries, far, near, own, key_segment, row_segment)


def attend_back_kernel(
    q_ref, far_ref, near_ref, own_ref, key_ref, row_ref, out_ref, grad_ref, log_ref, cos_ref, sin_ref,
    dq_ref, dfar_ref, dnear_ref, down_ref, bias_ref, kv_ref, dkv_ref, per_group,
):
    step = pl.program_id(0)

    @pl.when(step == 0)
    def _():
        write_bias(bias_ref, key_ref, row_ref)

    rows = q_ref.shape[0]
    for at, ref in enumerate((far_ref, near_ref, own_ref)):
        kv_ref[at * rows : (at + 1) * rows, :] = ref[...]
    key_value = kv_ref[...]
    flipped = key_value[:, :].T
    scaled = (q_ref[...].astype(F32) * HS ** (-0.5)).astype(BF16)
    q_flipped = scaled.T
    grad = grad_ref[...]
    grad_flipped = grad.T
    product = (out_ref[...].astype(F32) * grad.astype(F32)).T
    dqs, dkey, dvalue = [], None, None
    for head in range(2):
        here = slice(head * HS, (head + 1) * HS)
        scores = dot_nn(key_value[:, :HS], q_flipped[here, :]) + bias_ref[...]
        shares = jnp.exp(scores - log_ref[0, head : head + 1, :])
        grad_shares = dot_nn(key_value[:, HS:], grad_flipped[here, :])
        delta = jnp.sum(product[here, :], axis=0, keepdims=True)
        grad_scores = (shares * (grad_shares - delta)).astype(BF16)
        value_part = dot_nn(shares.astype(BF16), grad[:, here])
        key_part = dot_nn(grad_scores, scaled[:, here])
        dvalue = value_part if dvalue is None else dvalue + value_part
        dkey = key_part if dkey is None else dkey + key_part
        dqs.append(dot_nn(flipped[:HS, :], grad_scores))
    dq = jnp.concatenate(dqs, axis=0).T * HS ** (-0.5)
    dq_ref[...] = (dq * cos_ref[...] - swap_halves(dq) * sin_ref[...]).astype(BF16)
    both = jnp.concatenate([dkey, dvalue], axis=1)

    @pl.when(step % per_group == 0)
    def _():
        dkv_ref[...] = both

    @pl.when(step % per_group != 0)
    def _():
        dkv_ref[...] += both

    @pl.when(step % per_group == per_group - 1)
    def _():
        dfar_ref[...] = dkv_ref[:rows, :].astype(BF16)
        dnear_ref[...] = dkv_ref[rows : 2 * rows, :].astype(BF16)
        down_ref[...] = dkv_ref[2 * rows :, :]


def attend_back(queries, far, near, own, key_segment, row_segment, mixed, grad, logs, cos, sin):
    rows, width = queries.shape
    pairs = width // PAIR
    per_group = pairs // 2
    pair_tile = pl.BlockSpec((rows, PAIR), lambda p: (0, p))
    kv_tile = pl.BlockSpec((rows, PAIR), lambda p: (0, p // per_group))
    full = lambda array: pl.BlockSpec(array.shape, lambda p: (0, 0))
    return pl.pallas_call(
        functools.partial(attend_back_kernel, per_group=per_group),
        grid=(pairs,),
        in_specs=[
            pair_tile,
            kv_tile,
            kv_tile,
            kv_tile,
            full(key_segment),
            full(row_segment),
            pair_tile,
            pair_tile,
            pl.BlockSpec((1, 2, rows), lambda p: (p, 0, 0)),
            full(cos),
            full(sin),
        ],
        out_specs=[pair_tile, kv_tile, kv_tile, kv_tile],
        out_shape=[
            jax.ShapeDtypeStruct((rows, width), BF16),
            jax.ShapeDtypeStruct((rows, 2 * PAIR), BF16),
            jax.ShapeDtypeStruct((rows, 2 * PAIR), BF16),
            jax.ShapeDtypeStruct((rows, 2 * PAIR), F32),
        ],
        scratch_shapes=[
            pltpu.VMEM((3 * rows, rows), F32),
            pltpu.VMEM((3 * rows, PAIR), BF16),
            pltpu.VMEM((3 * rows, PAIR), F32),
        ],
        cost_estimate=pl.CostEstimate(
            flops=40 << 30, bytes_accessed=6 << 20, transcendentals=3 * rows * rows * 2 * pairs
        ),
        name="attend_back",
    )(queries, far, near, own, key_segment, row_segment, mixed, grad, logs, cos, sin)


def line_sum_kernel(modes, chunks, *refs):
    count = len(modes)
    a_refs, w_refs, out_ref = refs[:count], refs[count : 2 * count], refs[2 * count]
    rest = refs[2 * count + 1 :]
    w_bufs = rest[:count]
    part, first, second, total, w_sem, send_sem, recv_sem = rest[count:]
    width = part.shape[2]
    place = lax.axis_index("mp")
    pair = place + 1 - 2 * lax.rem(place, 2)
    across = 3 - place
    is_mid = (place == 1) | (place == 2)
    is_end = (place == 0) | (place == 3)

    def weight(at, c):
        if modes[at] == "nt":
            source = w_refs[at].at[pl.ds(pl.multiple_of(c * width, width), width), :]
        else:
            source = w_refs[at].at[:, pl.ds(pl.multiple_of(c * width, width), width)]
        return pltpu.make_async_copy(source, w_bufs[at].at[c], w_sem.at[at, c])

    def remote(kind, source, target, c, device):
        return pltpu.make_async_remote_copy(
            src_ref=source.at[c],
            dst_ref=target.at[c],
            send_sem=send_sem.at[kind, c],
            recv_sem=recv_sem.at[kind, c],
            device_id={"mp": device},
            device_id_type=MESH,
        )

    def up(c):
        return remote(0, part, first, c, pair)

    def over(c):
        return remote(1, part, second, c, across)

    def down(c):
        return remote(2, total, total, c, pair)

    def start_weights(c, carry):
        for at in range(count):
            weight(at, c).start()
        return carry

    lax.fori_loop(0, chunks, start_weights, 0)
    barrier = pltpu.get_barrier_semaphore()
    pl.semaphore_signal(barrier, inc=1, device_id={"mp": pair}, device_id_type=MESH)

    @pl.when(is_mid)
    def _():
        pl.semaphore_signal(barrier, inc=1, device_id={"mp": across}, device_id_type=MESH)
        pl.semaphore_wait(barrier, 2)

    @pl.when(is_end)
    def _():
        pl.semaphore_wait(barrier, 1)

    def step(t, carry):
        @pl.when(t < chunks)
        def _():
            value = None
            for at in range(count):
                weight(at, t).wait()
                dot = dot_nt if modes[at] == "nt" else dot_nn
                term = dot(a_refs[at][...], w_bufs[at][t])
                value = term if value is None else value + term
            part[t] = value.astype(BF16)

            @pl.when(is_end)
            def _():
                up(t).start()

        @pl.when(is_mid & (t >= 1) & (t < chunks + 1))
        def _():
            c = t - 1
            up(c).wait_recv()
            part[c] = (part[c].astype(F32) + first[c].astype(F32)).astype(BF16)
            over(c).start()

        @pl.when(is_mid & (t >= 2))
        def _():
            c = t - 2
            over(c).wait_recv()
            total[c] = (part[c].astype(F32) + second[c].astype(F32)).astype(BF16)
            down(c).start()

        return carry

    lax.fori_loop(0, chunks + 2, step, 0)

    def finish(c, carry):
        @pl.when(is_end)
        def _():
            up(c).wait_send()
            down(c).wait_recv()

        @pl.when(is_mid)
        def _():
            over(c).wait_send()
            down(c).wait_send()

        out_ref[:, pl.ds(pl.multiple_of(c * width, width), width)] = total[c]
        return carry

    lax.fori_loop(0, chunks, finish, 0)


def line_sum(pairs, call_id, chunks=8):
    lefts = [left for left, _, _ in pairs]
    rights = [right for _, right, _ in pairs]
    modes = tuple(mode for _, _, mode in pairs)
    rows = lefts[0].shape[0]
    columns = rights[0].shape[0] if modes[0] == "nt" else rights[0].shape[1]
    width = columns // chunks
    count = len(pairs)
    bufs = [
        pltpu.VMEM((chunks, width, left.shape[1]) if mode == "nt" else (chunks, left.shape[1], width), BF16)
        for left, _, mode in pairs
    ]
    flops = sum(2 * rows * columns * left.shape[1] for left in lefts)
    moved = sum(right.size * 2 for right in rights)
    block = pltpu.VMEM((chunks, rows, width), BF16)
    return pl.pallas_call(
        functools.partial(line_sum_kernel, modes, chunks),
        out_shape=jax.ShapeDtypeStruct((rows, columns), BF16),
        in_specs=[pl.BlockSpec(memory_space=pltpu.VMEM)] * count
        + [pl.BlockSpec(memory_space=pl.ANY)] * count,
        out_specs=pl.BlockSpec(memory_space=pltpu.VMEM),
        scratch_shapes=bufs
        + [
            block,
            block,
            block,
            block,
            pltpu.SemaphoreType.DMA((count, chunks)),
            pltpu.SemaphoreType.DMA((3, chunks)),
            pltpu.SemaphoreType.DMA((3, chunks)),
        ],
        compiler_params=pltpu.CompilerParams(collective_id=call_id, has_side_effects=True),
        cost_estimate=pl.CostEstimate(
            flops=flops + (40 << 30), bytes_accessed=moved, transcendentals=0
        ),
        name=f"line_sum_{call_id}",
    )(*lefts, *rights)


def scatter_sum(left, right):
    rows, depth = left.shape
    columns = right.shape[1]
    batch_count = lax.axis_size("batch")
    seq_index = lax.axis_index("seq")
    core, chip = seq_index % 2, seq_index // 2
    block = depth // (4 * batch_count)
    split = left.reshape(rows, batch_count, 2, 2, block)
    size = lax.axis_size("seq")

    def product(at):
        taken = lax.dynamic_index_in_dim(split, at, 3, keepdims=False).reshape(rows, depth // 2)
        return dot_tn(taken, right)

    away = product(1 - core).astype(BF16)
    arrived = lax.ppermute(away, "seq", [(s, s ^ 1) for s in range(size)])
    kept = (product(core) + arrived.astype(F32)).astype(BF16)
    kept = kept.reshape(batch_count, 2, block, columns)
    half = columns // 2

    def over_chip(values, axis):
        sent = lax.dynamic_index_in_dim(values, 1 - chip, axis, keepdims=False)
        stay = lax.dynamic_index_in_dim(values, chip, axis, keepdims=False)
        came = lax.ppermute(sent, "seq", [(s, s ^ 2) for s in range(size)])
        return stay.astype(F32) + came.astype(F32)

    def over_batch(values):
        if batch_count == 2:
            here = lax.axis_index("batch")
            sent = lax.dynamic_index_in_dim(values, 1 - here, 0, keepdims=False)
            stay = lax.dynamic_index_in_dim(values, here, 0, keepdims=False)
            came = lax.ppermute(sent, "batch", [(0, 1), (1, 0)])
            return stay.astype(F32) + came.astype(F32)
        return lax.psum_scatter(values, "batch", scatter_dimension=0, tiled=False).astype(F32)

    one = over_batch(over_chip(kept[..., :half], 1).astype(BF16))
    two = over_chip(over_batch(kept[..., half:]).astype(BF16), 0)
    return jnp.concatenate([one, two], axis=1)


def local(
    tokens, segment_ids, attn_gain, w_query, w_key, w_value, w_output, mlp_gain, w_gate, w_up, w_down, cotangent
):
    rows, width = tokens.shape
    seq_count = lax.axis_size("seq")
    seq_index = lax.axis_index("seq")
    segments = segment_ids[0]
    first_row = seq_index * rows
    reach = LONGEST // rows
    cos, sin = rope_tables(segments, first_row, rows)
    row_segment = lax.dynamic_slice_in_dim(segments, first_row, rows, 0)[None, :]
    padded = jnp.concatenate([jnp.full((LONGEST,), -1, jnp.int32), segments])
    key_segment = lax.dynamic_slice_in_dim(padded, first_row, rows + LONGEST, 0)[:, None]

    normed, queries, own = project(tokens, attn_gain[None, :], w_query, w_key, w_value, cos, sin)
    near = lax.ppermute(own, "seq", [(s, s + 1) for s in range(seq_count - 1)])
    far = lax.ppermute(own, "seq", [(s, s + 2) for s in range(seq_count - 2)])
    mixed, logs = attend(queries, far, near, own, key_segment, row_segment)

    branch = line_sum([(mixed, w_output, "nn")], 1).astype(F32)
    wide = tokens.astype(F32)
    middle = wide + branch
    scale_two = lax.rsqrt(jnp.mean(middle * middle, axis=-1, keepdims=True) + epsilon)
    normed_two = (middle * scale_two * mlp_gain).astype(BF16)
    gate_pre = dot_nn(normed_two, w_gate)
    up_pre = dot_nn(normed_two, w_up)
    sigmoid_gate = jax.nn.sigmoid(gate_pre)
    swish = gate_pre * sigmoid_gate
    active = (swish * up_pre).astype(BF16)
    grad_active = dot_nt(cotangent, w_down)
    grad_gate_low = (grad_active * up_pre * sigmoid_gate * (1.0 + gate_pre * (1.0 - sigmoid_gate))).astype(BF16)
    grad_up_low = (grad_active * swish).astype(BF16)
    mlp_out = lax.psum(dot_nn(active, w_down).astype(BF16), "mp").astype(F32)
    output = (middle + mlp_out).astype(BF16)

    grad_normed_two = line_sum([(grad_gate_low, w_gate, "nt"), (grad_up_low, w_up, "nt")], 2).astype(F32)
    scaled_two = grad_normed_two * mlp_gain
    grad_middle = (
        cotangent.astype(F32)
        + scale_two * scaled_two
        - middle
        * (scale_two * scale_two * scale_two)
        * jnp.mean(middle * scaled_two, axis=-1, keepdims=True)
    )
    grad_mlp_gain = jnp.sum(grad_normed_two * middle * scale_two, axis=0)
    grad_branch = grad_middle.astype(BF16)
    grad_mixed = dot_nt(grad_branch, w_output).astype(BF16)
    grad_down = scatter_sum(cotangent, active).T
    grad_gate = scatter_sum(normed_two, grad_gate_low)
    grad_up = scatter_sum(normed_two, grad_up_low)
    grad_output = scatter_sum(grad_branch, mixed).T

    grad_query_pre, dfar, dnear, down = attend_back(
        queries, far, near, own, key_segment, row_segment, mixed, grad_mixed, logs, cos, sin
    )
    from_near = lax.ppermute(dnear, "seq", [(s + 1, s) for s in range(seq_count - 1)])
    from_far = lax.ppermute(dfar, "seq", [(s + 2, s) for s in range(seq_count - 2)])
    grad_pair = down + from_near.astype(F32) + from_far.astype(F32)
    grad_keys = jnp.concatenate([grad_pair[:, :HS], grad_pair[:, PAIR : PAIR + HS]], axis=1)
    grad_values = jnp.concatenate([grad_pair[:, HS:PAIR], grad_pair[:, PAIR + HS :]], axis=1)
    quarter = HS // 2
    swapped = jnp.concatenate(
        [grad_keys[:, (at ^ 1) * quarter : ((at ^ 1) + 1) * quarter] for at in range(4)], axis=1
    )
    grad_key_pre = (grad_keys * cos - swapped * sin).astype(BF16)
    grad_value_pre = grad_values.astype(BF16)

    grad_qkv = scatter_sum(normed, jnp.concatenate([grad_query_pre, grad_key_pre, grad_value_pre], axis=1))
    query_width = grad_query_pre.shape[1]
    grad_normed = line_sum(
        [
            (grad_query_pre, w_query, "nt"),
            (grad_key_pre, w_key, "nt"),
            (grad_value_pre, w_value, "nt"),
        ],
        3,
    ).astype(F32)
    scale_one = lax.rsqrt(jnp.mean(wide * wide, axis=-1, keepdims=True) + epsilon)
    scaled_one = grad_normed * attn_gain
    grad_inputs = (
        grad_middle
        + scale_one * scaled_one
        - wide
        * (scale_one * scale_one * scale_one)
        * jnp.mean(wide * scaled_one, axis=-1, keepdims=True)
    )
    grad_attn_gain = jnp.sum(grad_normed * wide * scale_one, axis=0)
    gains = [
        lax.psum_scatter(value.astype(BF16), ("batch", "seq"), scatter_dimension=0, tiled=True).astype(F32)
        for value in (grad_attn_gain, grad_mlp_gain)
    ]
    return (
        output,
        grad_inputs.astype(BF16),
        gains[0],
        grad_qkv[:, :query_width],
        grad_qkv[:, query_width : query_width + PAIR],
        grad_qkv[:, query_width + PAIR :],
        grad_output,
        gains[1],
        grad_gate,
        grad_up,
        grad_down,
    )


def solution(mesh):
    tokens_spec = P(("batch", "seq"), None)
    in_specs = (
        tokens_spec,
        P("batch", None),
        P(),
        P(None, "mp"),
        P(None, "mp"),
        P(None, "mp"),
        P("mp", None),
        P(),
        P(None, "mp"),
        P(None, "mp"),
        P("mp", None),
        tokens_spec,
    )
    row_split = P(("batch", "seq"), "mp")
    column_split = P("mp", ("batch", "seq"))
    out_specs = (
        tokens_spec,
        tokens_spec,
        P(("batch", "seq")),
        row_split,
        row_split,
        row_split,
        column_split,
        P(("batch", "seq")),
        row_split,
        row_split,
        column_split,
    )
    return jax.shard_map(local, mesh=mesh, in_specs=in_specs, out_specs=out_specs, check_vma=False)
```

```python
import functools
import math

import jax
import jax.numpy as jnp
from jax import lax
from jax.experimental import pallas as pl
from jax.experimental.pallas import tpu as pltpu
from jax.sharding import PartitionSpec as P

HS = 64
PAIR = 2 * HS
LONGEST = 1024
rope_base = 500000.0
epsilon = 1e-05
masked_score = -1e30
MESH = pl.DeviceIdType.MESH
F32 = jnp.float32
BF16 = jnp.bfloat16


def dot_nn(left, right):
    return lax.dot_general(left, right, (((1,), (0,)), ((), ())), preferred_element_type=F32)


def dot_nt(left, right):
    return lax.dot_general(left, right, (((1,), (1,)), ((), ())), preferred_element_type=F32)


def dot_tn(left, right):
    return lax.dot_general(left, right, (((0,), (0,)), ((), ())), preferred_element_type=F32)


def lanes_of(values):
    return lax.broadcasted_iota(jnp.int32, values.shape, 1)


def swap_halves(values):
    ahead = pltpu.roll(values, PAIR - HS // 2, 1)
    behind = pltpu.roll(values, HS // 2, 1)
    return jnp.where(lanes_of(values) % HS < HS // 2, ahead, behind)


def rope_tables(segments, first_row, rows):
    row_segment = lax.dynamic_slice_in_dim(segments, first_row, rows, 0)
    doc_start = jnp.sum((segments[None, :] < row_segment[:, None]).astype(jnp.int32), axis=1)
    place = (first_row + jnp.arange(rows, dtype=jnp.int32) - doc_start).astype(F32)
    lane = jnp.arange(PAIR, dtype=jnp.int32)
    frequency = jnp.exp((lane % (HS // 2)).astype(F32) * (-2.0 * math.log(rope_base) / HS))
    angles = place[:, None] * frequency[None, :]
    sign = jnp.where(lane % HS < HS // 2, -1.0, 1.0)
    return jnp.cos(angles), jnp.sin(angles) * sign[None, :]


def project_kernel(x_ref, gain_ref, wq_ref, wk_ref, wv_ref, cos_ref, sin_ref, n_ref, q_ref, kv_ref):
    wide = x_ref[...].astype(F32)
    scale = lax.rsqrt(jnp.mean(wide * wide, axis=-1, keepdims=True) + epsilon)
    normed = (wide * scale * gain_ref[...]).astype(BF16)
    n_ref[...] = normed
    cos, sin = cos_ref[...], sin_ref[...]
    queries = dot_nn(normed, wq_ref[...])
    for start in range(0, queries.shape[1], PAIR):
        part = queries[:, start : start + PAIR]
        q_ref[:, start : start + PAIR] = (part * cos + swap_halves(part) * sin).astype(BF16)
    keys = dot_nn(normed, wk_ref[...])
    keys = keys * cos + swap_halves(keys) * sin
    values = dot_nn(normed, wv_ref[...])
    low_half = lanes_of(keys) < HS
    kv_ref[:, :PAIR] = jnp.where(low_half, keys, pltpu.roll(values, HS, 1)).astype(BF16)
    kv_ref[:, PAIR:] = jnp.where(low_half, pltpu.roll(keys, HS, 1), values).astype(BF16)


def project(tokens, gain, w_query, w_key, w_value, cos, sin):
    rows, width = tokens.shape
    block = rows // 2
    full = lambda array: pl.BlockSpec(array.shape, lambda i: (0, 0))
    tile = lambda columns: pl.BlockSpec((block, columns), lambda i: (i, 0))
    return pl.pallas_call(
        project_kernel,
        grid=(rows // block,),
        in_specs=[
            tile(width),
            full(gain),
            full(w_query),
            full(w_key),
            full(w_value),
            tile(PAIR),
            tile(PAIR),
        ],
        out_specs=[tile(width), tile(w_query.shape[1]), tile(2 * PAIR)],
        out_shape=[
            jax.ShapeDtypeStruct((rows, width), BF16),
            jax.ShapeDtypeStruct((rows, w_query.shape[1]), BF16),
            jax.ShapeDtypeStruct((rows, 2 * PAIR), BF16),
        ],
        cost_estimate=pl.CostEstimate(
            flops=2 * rows * width * (w_query.shape[1] + 2 * PAIR),
            bytes_accessed=8 << 20,
            transcendentals=0,
        ),
        name="project",
    )(tokens, gain, w_query, w_key, w_value, cos, sin)


def write_bias(bias_ref, key_ref, row_ref):
    keys, rows = bias_ref.shape
    key_place = lax.broadcasted_iota(jnp.int32, (keys, rows), 0) - (keys - rows)
    row_place = lax.broadcasted_iota(jnp.int32, (keys, rows), 1)
    allowed = (key_ref[...] == row_ref[...]) & (key_place <= row_place)
    bias_ref[...] = jnp.where(allowed, 0.0, masked_score)


def attend_kernel(q_ref, far_ref, near_ref, own_ref, key_ref, row_ref, out_ref, log_ref, bias_ref, kv_ref):
    @pl.when(pl.program_id(0) == 0)
    def _():
        write_bias(bias_ref, key_ref, row_ref)

    rows = q_ref.shape[0]
    for at, ref in enumerate((far_ref, near_ref, own_ref)):
        kv_ref[at * rows : (at + 1) * rows, :] = ref[...]
    key_value = kv_ref[...]
    flipped = key_value.T
    q_flipped = (q_ref[...].astype(F32) * HS ** (-0.5)).astype(BF16).T
    outs = []
    for head in range(2):
        scores = dot_nn(key_value[:, :HS], q_flipped[head * HS : (head + 1) * HS, :]) + bias_ref[...]
        top = jnp.max(scores, axis=0, keepdims=True)
        powers = jnp.exp(scores - top)
        total = jnp.sum(powers, axis=0, keepdims=True)
        mixed = dot_nn(flipped[HS:, :], powers.astype(BF16))
        outs.append(mixed / total)
        log_ref[0, head : head + 1, :] = top + jnp.log(total)
    out_ref[...] = jnp.concatenate(outs, axis=0).T.astype(BF16)


def attend(queries, far, near, own, key_segment, row_segment):
    rows, width = queries.shape
    pairs = width // PAIR
    per_group = pairs // 2
    pair_tile = pl.BlockSpec((rows, PAIR), lambda p: (0, p))
    kv_tile = pl.BlockSpec((rows, PAIR), lambda p: (0, p // per_group))
    return pl.pallas_call(
        attend_kernel,
        grid=(pairs,),
        in_specs=[
            pair_tile,
            kv_tile,
            kv_tile,
            kv_tile,
            pl.BlockSpec(key_segment.shape, lambda p: (0, 0)),
            pl.BlockSpec(row_segment.shape, lambda p: (0, 0)),
        ],
        out_specs=[pair_tile, pl.BlockSpec((1, 2, rows), lambda p: (p, 0, 0))],
        out_shape=[
            jax.ShapeDtypeStruct((rows, width), BF16),
            jax.ShapeDtypeStruct((pairs, 2, rows), F32),
        ],
        scratch_shapes=[pltpu.VMEM((3 * rows, rows), F32), pltpu.VMEM((3 * rows, PAIR), BF16)],
        cost_estimate=pl.CostEstimate(
            flops=16 << 30, bytes_accessed=4 << 20, transcendentals=3 * rows * rows * 2 * pairs
        ),
        name="attend",
    )(queries, far, near, own, key_segment, row_segment)


def attend_back_kernel(
    q_ref, far_ref, near_ref, own_ref, key_ref, row_ref, out_ref, grad_ref, log_ref, cos_ref, sin_ref,
    dq_ref, dfar_ref, dnear_ref, down_ref, bias_ref, kv_ref, dkv_ref, per_group,
):
    step = pl.program_id(0)

    @pl.when(step == 0)
    def _():
        write_bias(bias_ref, key_ref, row_ref)

    rows = q_ref.shape[0]
    for at, ref in enumerate((far_ref, near_ref, own_ref)):
        kv_ref[at * rows : (at + 1) * rows, :] = ref[...]
    key_value = kv_ref[...]
    flipped = key_value[:, :].T
    scaled = (q_ref[...].astype(F32) * HS ** (-0.5)).astype(BF16)
    q_flipped = scaled.T
    grad = grad_ref[...]
    grad_flipped = grad.T
    product = (out_ref[...].astype(F32) * grad.astype(F32)).T
    dqs, dkey, dvalue = [], None, None
    for head in range(2):
        here = slice(head * HS, (head + 1) * HS)
        scores = dot_nn(key_value[:, :HS], q_flipped[here, :]) + bias_ref[...]
        shares = jnp.exp(scores - log_ref[0, head : head + 1, :])
        grad_shares = dot_nn(key_value[:, HS:], grad_flipped[here, :])
        delta = jnp.sum(product[here, :], axis=0, keepdims=True)
        grad_scores = (shares * (grad_shares - delta)).astype(BF16)
        value_part = dot_nn(shares.astype(BF16), grad[:, here])
        key_part = dot_nn(grad_scores, scaled[:, here])
        dvalue = value_part if dvalue is None else dvalue + value_part
        dkey = key_part if dkey is None else dkey + key_part
        dqs.append(dot_nn(flipped[:HS, :], grad_scores))
    dq = jnp.concatenate(dqs, axis=0).T * HS ** (-0.5)
    dq_ref[...] = (dq * cos_ref[...] - swap_halves(dq) * sin_ref[...]).astype(BF16)
    both = jnp.concatenate([dkey, dvalue], axis=1)

    @pl.when(step % per_group == 0)
    def _():
        dkv_ref[...] = both

    @pl.when(step % per_group != 0)
    def _():
        dkv_ref[...] += both

    @pl.when(step % per_group == per_group - 1)
    def _():
        dfar_ref[...] = dkv_ref[:rows, :].astype(BF16)
        dnear_ref[...] = dkv_ref[rows : 2 * rows, :].astype(BF16)
        down_ref[...] = dkv_ref[2 * rows :, :]


def attend_back(queries, far, near, own, key_segment, row_segment, mixed, grad, logs, cos, sin):
    rows, width = queries.shape
    pairs = width // PAIR
    per_group = pairs // 2
    pair_tile = pl.BlockSpec((rows, PAIR), lambda p: (0, p))
    kv_tile = pl.BlockSpec((rows, PAIR), lambda p: (0, p // per_group))
    full = lambda array: pl.BlockSpec(array.shape, lambda p: (0, 0))
    return pl.pallas_call(
        functools.partial(attend_back_kernel, per_group=per_group),
        grid=(pairs,),
        in_specs=[
            pair_tile,
            kv_tile,
            kv_tile,
            kv_tile,
            full(key_segment),
            full(row_segment),
            pair_tile,
            pair_tile,
            pl.BlockSpec((1, 2, rows), lambda p: (p, 0, 0)),
            full(cos),
            full(sin),
        ],
        out_specs=[pair_tile, kv_tile, kv_tile, kv_tile],
        out_shape=[
            jax.ShapeDtypeStruct((rows, width), BF16),
            jax.ShapeDtypeStruct((rows, 2 * PAIR), BF16),
            jax.ShapeDtypeStruct((rows, 2 * PAIR), BF16),
            jax.ShapeDtypeStruct((rows, 2 * PAIR), F32),
        ],
        scratch_shapes=[
            pltpu.VMEM((3 * rows, rows), F32),
            pltpu.VMEM((3 * rows, PAIR), BF16),
            pltpu.VMEM((3 * rows, PAIR), F32),
        ],
        cost_estimate=pl.CostEstimate(
            flops=40 << 30, bytes_accessed=6 << 20, transcendentals=3 * rows * rows * 2 * pairs
        ),
        name="attend_back",
    )(queries, far, near, own, key_segment, row_segment, mixed, grad, logs, cos, sin)


def line_sum_kernel(modes, chunks, *refs):
    count = len(modes)
    a_refs, w_refs, out_ref = refs[:count], refs[count : 2 * count], refs[2 * count]
    rest = refs[2 * count + 1 :]
    w_bufs = rest[:count]
    part, first, second, total, w_sem, send_sem, recv_sem = rest[count:]
    width = part.shape[2]
    place = lax.axis_index("mp")
    pair = place + 1 - 2 * lax.rem(place, 2)
    across = 3 - place
    is_mid = (place == 1) | (place == 2)
    is_end = (place == 0) | (place == 3)

    def weight(at, c):
        if modes[at] == "nt":
            source = w_refs[at].at[pl.ds(pl.multiple_of(c * width, width), width), :]
        else:
            source = w_refs[at].at[:, pl.ds(pl.multiple_of(c * width, width), width)]
        return pltpu.make_async_copy(source, w_bufs[at].at[c], w_sem.at[at, c])

    def remote(kind, source, target, c, device):
        return pltpu.make_async_remote_copy(
            src_ref=source.at[c],
            dst_ref=target.at[c],
            send_sem=send_sem.at[kind, c],
            recv_sem=recv_sem.at[kind, c],
            device_id={"mp": device},
            device_id_type=MESH,
        )

    def up(c):
        return remote(0, part, first, c, pair)

    def over(c):
        return remote(1, part, second, c, across)

    def down(c):
        return remote(2, total, total, c, pair)

    def start_weights(c, carry):
        for at in range(count):
            weight(at, c).start()
        return carry

    lax.fori_loop(0, chunks, start_weights, 0)
    barrier = pltpu.get_barrier_semaphore()
    pl.semaphore_signal(barrier, inc=1, device_id={"mp": pair}, device_id_type=MESH)

    @pl.when(is_mid)
    def _():
        pl.semaphore_signal(barrier, inc=1, device_id={"mp": across}, device_id_type=MESH)
        pl.semaphore_wait(barrier, 2)

    @pl.when(is_end)
    def _():
        pl.semaphore_wait(barrier, 1)

    def step(t, carry):
        @pl.when(t < chunks)
        def _():
            value = None
            for at in range(count):
                weight(at, t).wait()
                dot = dot_nt if modes[at] == "nt" else dot_nn
                term = dot(a_refs[at][...], w_bufs[at][t])
                value = term if value is None else value + term
            part[t] = value.astype(BF16)

            @pl.when(is_end)
            def _():
                up(t).start()

        @pl.when(is_mid & (t >= 1) & (t < chunks + 1))
        def _():
            c = t - 1
            up(c).wait_recv()
            part[c] = (part[c].astype(F32) + first[c].astype(F32)).astype(BF16)
            over(c).start()

        @pl.when(is_mid & (t >= 2))
        def _():
            c = t - 2
            over(c).wait_recv()
            total[c] = (part[c].astype(F32) + second[c].astype(F32)).astype(BF16)
            down(c).start()

        return carry

    lax.fori_loop(0, chunks + 2, step, 0)

    def finish(c, carry):
        @pl.when(is_end)
        def _():
            up(c).wait_send()
            down(c).wait_recv()

        @pl.when(is_mid)
        def _():
            over(c).wait_send()
            down(c).wait_send()

        out_ref[:, pl.ds(pl.multiple_of(c * width, width), width)] = total[c]
        return carry

    lax.fori_loop(0, chunks, finish, 0)


def line_sum(pairs, call_id, chunks=8):
    lefts = [left for left, _, _ in pairs]
    rights = [right for _, right, _ in pairs]
    modes = tuple(mode for _, _, mode in pairs)
    rows = lefts[0].shape[0]
    columns = rights[0].shape[0] if modes[0] == "nt" else rights[0].shape[1]
    width = columns // chunks
    count = len(pairs)
    bufs = [
        pltpu.VMEM((chunks, width, left.shape[1]) if mode == "nt" else (chunks, left.shape[1], width), BF16)
        for left, _, mode in pairs
    ]
    flops = sum(2 * rows * columns * left.shape[1] for left in lefts)
    moved = sum(right.size * 2 for right in rights)
    block = pltpu.VMEM((chunks, rows, width), BF16)
    return pl.pallas_call(
        functools.partial(line_sum_kernel, modes, chunks),
        out_shape=jax.ShapeDtypeStruct((rows, columns), BF16),
        in_specs=[pl.BlockSpec(memory_space=pltpu.VMEM)] * count
        + [pl.BlockSpec(memory_space=pl.ANY)] * count,
        out_specs=pl.BlockSpec(memory_space=pltpu.VMEM),
        scratch_shapes=bufs
        + [
            block,
            block,
            block,
            block,
            pltpu.SemaphoreType.DMA((count, chunks)),
            pltpu.SemaphoreType.DMA((3, chunks)),
            pltpu.SemaphoreType.DMA((3, chunks)),
        ],
        compiler_params=pltpu.CompilerParams(collective_id=call_id, has_side_effects=True),
        cost_estimate=pl.CostEstimate(
            flops=flops + (40 << 30), bytes_accessed=moved, transcendentals=0
        ),
        name=f"line_sum_{call_id}",
    )(*lefts, *rights)

LAG = 2


def exchange_kernel(plan, *refs):
    left_count, right_spans, sum_spans, flips_before, flipped_units, out_spans, units, chunks = plan
    refs = list(refs)

    def take(n):
        got = refs[:n]
        del refs[:n]
        return got

    left_refs, right_refs, w_refs = take(left_count), take(len(right_spans)), take(len(sum_spans))
    (out_ref,) = take(1)
    grad_refs = take(len(out_spans))
    stage, flip, right_all = take(3)
    w_bufs = take(len(sum_spans))
    part, first, second, total, away, come_one, come_two, come_three, plain, turned = take(10)
    in_sem, right_sem, w_sem, ar_send, ar_recv, core_send, core_recv, two_send, two_recv, three_send, three_recv, out_sem = refs
    width = part.shape[2]
    block = come_three.shape[1]
    place = lax.axis_index("mp")
    seq, batch = lax.axis_index("seq"), lax.axis_index("batch")
    core, chip = lax.rem(seq, 2), lax.div(seq, 2)
    sibling = seq + 1 - 2 * core
    beside = seq + 2 - 4 * chip
    pair = place + 1 - 2 * lax.rem(place, 2)
    across = 3 - place
    is_mid = (place == 1) | (place == 2)
    is_end = (place == 0) | (place == 3)

    def weight(at, c):
        source = w_refs[at].at[pl.ds(pl.multiple_of(c * width, width), width), :]
        slot = lax.rem(c, 3)
        return pltpu.make_async_copy(source, w_bufs[at].at[slot], w_sem.at[at, slot])

    def remote(source, target, send, recv, device):
        return pltpu.make_async_remote_copy(
            src_ref=source, dst_ref=target, send_sem=send, recv_sem=recv, device_id=device, device_id_type=MESH
        )

    def line(kind, source, target, c, device):
        return remote(source.at[c], target.at[c], ar_send.at[kind, c], ar_recv.at[kind, c], {"mp": device})

    def up(c):
        return line(0, part, first, c, pair)

    def over(c):
        return line(1, part, second, c, across)

    def down(c):
        return line(2, total, total, c, pair)

    def to_core(u):
        return remote(away.at[lax.rem(u, 2)], come_one.at[u], core_send.at[u], core_recv.at[u], {"seq": sibling})

    def chip_first(u):
        return 1 - lax.rem(u, 2)

    def sent_at(u, k):
        x_first = chip_first(u)
        return x_first * (2 * k + 1 - chip) + (1 - x_first) * (2 * (1 - batch) + k)

    def kept_at(u, k):
        x_first = chip_first(u)
        return x_first * (2 * k + chip) + (1 - x_first) * (2 * batch + k)

    def own_at(u):
        x_first = chip_first(u)
        return x_first * batch + (1 - x_first) * chip

    def device_of(x_way):
        return {
            "seq": x_way * beside + (1 - x_way) * seq,
            "batch": x_way * batch + (1 - x_way) * (1 - batch),
        }

    def second_hop(u, k):
        return remote(
            come_one.at[u, sent_at(u, k)], come_two.at[u, k], two_send.at[k, u], two_recv.at[k, u], device_of(chip_first(u))
        )

    def third_hop(u):
        return remote(
            come_two.at[u, 1 - own_at(u)], come_three.at[u], three_send.at[u], three_recv.at[u], device_of(1 - chip_first(u))
        )

    def left_copy(at):
        return pltpu.make_async_copy(left_refs[at], stage.at[at], in_sem.at[at])

    def right_copy(at):
        start, size = right_spans[at]
        return pltpu.make_async_copy(right_refs[at], right_all.at[:, start : start + size], right_sem.at[at])

    for at in range(len(sum_spans)):
        weight(at, 0).start()
        weight(at, 1).start()
    for at in range(len(right_spans)):
        right_copy(at).start()
    for at in range(left_count):
        left_copy(at).start()

    barrier = pltpu.get_barrier_semaphore()
    for device in ({"mp": pair}, {"seq": sibling}, {"seq": beside}, {"batch": 1 - batch}):
        pl.semaphore_signal(barrier, inc=1, device_id=device, device_id_type=MESH)

    @pl.when(is_mid)
    def _():
        pl.semaphore_signal(barrier, inc=1, device_id={"mp": across}, device_id_type=MESH)
        pl.semaphore_wait(barrier, 5)

    @pl.when(is_end)
    def _():
        pl.semaphore_wait(barrier, 4)

    for at in range(len(right_spans)):
        right_copy(at).wait()

    def left_of(u):
        index = 0
        for at in range(1, left_count):
            index = index + (u >= flips_before[at]).astype(jnp.int32)
        return index

    def product(u, at, side):
        row = pl.multiple_of((2 * at + side) * block, block)
        column = pl.multiple_of(u * block, block)
        return dot_nn(flip[left_of(u), pl.ds(row, block), :], right_all[:, pl.ds(column, block)])

    def step(t, carry):
        @pl.when(t < chunks)
        def _():
            value = None
            for at, (start, size) in enumerate(sum_spans):
                weight(at, t).wait()
                term = dot_nt(right_all[:, start : start + size], w_bufs[at][lax.rem(t, 3)])
                value = term if value is None else value + term
            part[t] = value.astype(BF16)

            @pl.when(is_end)
            def _():
                up(t).start()

            @pl.when(t + 2 < chunks)
            def _():
                for at in range(len(sum_spans)):
                    weight(at, t + 2).start()

        @pl.when(is_mid & (t >= LAG) & (t < chunks + LAG))
        def _():
            c = t - LAG
            up(c).wait_recv()
            part[c] = (part[c].astype(F32) + first[c].astype(F32)).astype(BF16)
            over(c).start()

        @pl.when(is_mid & (t >= 2 * LAG) & (t < chunks + 2 * LAG))
        def _():
            c = t - 2 * LAG
            over(c).wait_recv()
            total[c] = (part[c].astype(F32) + second[c].astype(F32)).astype(BF16)
            down(c).start()

        for at in range(left_count):

            @pl.when(t == max(flips_before[at] - 2, 0))
            def _():
                left_copy(at).wait()

                def turn(k, carry):
                    here = pl.ds(pl.multiple_of(k * block, block), block)
                    flip[at, here, :] = stage[at, :, here].T
                    return carry

                lax.fori_loop(0, flip.shape[1] // block, turn, 0)

        @pl.when(t < units)
        def _():
            @pl.when(t >= 2)
            def _():
                to_core(t - 2).wait_send()

            for at in range(4):
                away[lax.rem(t, 2), at] = product(t, at, 1 - core).astype(BF16)
            to_core(t).start()

        @pl.when((t >= 1) & (t < units + 1))
        def _():
            u = t - 1
            to_core(u).wait_recv()
            for at in range(4):
                come_one[u, at] = (product(u, at, core) + come_one[u, at].astype(F32)).astype(BF16)
            for k in range(2):
                second_hop(u, k).start()

        @pl.when((t >= 1 + LAG) & (t < units + 1 + LAG))
        def _():
            u = t - 1 - LAG
            for k in range(2):
                second_hop(u, k).wait_recv()
            sent = 1 - own_at(u)
            come_two[u, sent] = (come_two[u, sent].astype(F32) + come_one[u, kept_at(u, sent)].astype(F32)).astype(BF16)
            third_hop(u).start()

        @pl.when((t >= 1 + 2 * LAG) & (t < units + 1 + 2 * LAG))
        def _():
            u = t - 1 - 2 * LAG
            third_hop(u).wait_recv()
            own = own_at(u)
            result = (
                come_three[u].astype(F32) + come_two[u, own].astype(F32) + come_one[u, kept_at(u, own)].astype(F32)
            )
            if flipped_units:

                @pl.when(u < flipped_units)
                def _():
                    turned[pl.ds(pl.multiple_of(u * block, block), block), :] = result.T

                @pl.when(u >= flipped_units)
                def _():
                    plain[:, pl.ds(pl.multiple_of((u - flipped_units) * block, block), block)] = result

            else:
                plain[:, pl.ds(pl.multiple_of(u * block, block), block)] = result

        return carry

    lax.fori_loop(0, max(units + 1, chunks) + 2 * LAG, step, 0)

    def out_copy(at):
        kind, start, size = out_spans[at]
        source = turned.at[start : start + size, :] if kind == "turned" else plain.at[:, start : start + size]
        return pltpu.make_async_copy(source, grad_refs[at], out_sem.at[at])

    for at in range(len(out_spans)):
        out_copy(at).start()

    def finish(c, carry):
        @pl.when(is_end)
        def _():
            up(c).wait_send()
            down(c).wait_recv()

        @pl.when(is_mid)
        def _():
            over(c).wait_send()
            down(c).wait_send()

        out_ref[:, pl.ds(pl.multiple_of(c * width, width), width)] = total[c]
        return carry

    lax.fori_loop(0, chunks, finish, 0)

    def settle(u, carry):
        for k in range(2):
            second_hop(u, k).wait_send()
        third_hop(u).wait_send()
        return carry

    lax.fori_loop(0, units, settle, 0)
    for u in (units - 2, units - 1):
        to_core(u).wait_send()
    for at in range(len(out_spans)):
        out_copy(at).wait()


def exchange(lefts, rights, weights, sums_from, flips_before, flipped_units, outs, call_id, chunks=16):
    rows, depth = lefts[0].shape
    block = depth // 8
    spans, at = [], 0
    for right in rights:
        spans.append((at, right.shape[1]))
        at += right.shape[1]
    units = at // block
    columns = weights[0].shape[0]
    width = columns // chunks
    sum_spans = [spans[i] for i in sums_from]
    plan = (len(lefts), spans, sum_spans, flips_before, flipped_units, outs, units, chunks)
    any_space = pl.BlockSpec(memory_space=pl.ANY)
    grad_shapes = [
        jax.ShapeDtypeStruct((size, block) if kind == "turned" else (block, size), F32) for kind, _, size in outs
    ]
    line_block = pltpu.VMEM((chunks, rows, width), BF16)
    dma = pltpu.SemaphoreType.DMA
    plain_units = max(units - flipped_units, 1)
    flops = 2 * rows * columns * sum(size for _, size in sum_spans) + 2 * rows * depth * at
    return pl.pallas_call(
        functools.partial(exchange_kernel, plan),
        out_shape=[jax.ShapeDtypeStruct((rows, columns), BF16)] + grad_shapes,
        in_specs=[any_space] * (len(lefts) + len(rights) + len(weights)),
        out_specs=[pl.BlockSpec(memory_space=pltpu.VMEM)] + [any_space] * len(outs),
        scratch_shapes=[
            pltpu.VMEM((len(lefts), rows, depth), BF16),
            pltpu.VMEM((len(lefts), depth, rows), BF16),
            pltpu.VMEM((rows, at), BF16),
        ]
        + [pltpu.VMEM((3, width, size), BF16) for _, size in sum_spans]
        + [
            line_block,
            line_block,
            line_block,
            line_block,
            pltpu.VMEM((2, 4, block, block), BF16),
            pltpu.VMEM((units, 4, block, block), BF16),
            pltpu.VMEM((units, 2, block, block), BF16),
            pltpu.VMEM((units, block, block), BF16),
            pltpu.VMEM((block, plain_units * block), F32),
            pltpu.VMEM((max(flipped_units, 1) * block, block), F32),
            dma((len(lefts),)),
            dma((len(rights),)),
            dma((len(weights), 3)),
            dma((3, chunks)),
            dma((3, chunks)),
            dma((units,)),
            dma((units,)),
            dma((2, units)),
            dma((2, units)),
            dma((units,)),
            dma((units,)),
            dma((len(outs),)),
        ],
        compiler_params=pltpu.CompilerParams(
            collective_id=call_id, has_side_effects=True, vmem_limit_bytes=62 << 20
        ),
        cost_estimate=pl.CostEstimate(flops=flops + (50 << 30), bytes_accessed=20 << 20, transcendentals=0),
        name=f"exchange_{call_id}",
    )(*lefts, *rights, *weights)


def final_kernel(gn_ref, x_ref, gm_ref, gain_ref, mlp_ref, out_ref, gains_ref, acc, parts, come, send_sem, recv_sem):
    seq, batch = lax.axis_index("seq"), lax.axis_index("batch")
    seq_count = lax.axis_size("seq")
    peers = parts.shape[0]
    block = parts.shape[2]
    me = batch * seq_count + seq

    def peer(k):
        there = lax.rem(me + k, peers)
        return there, {"batch": lax.div(there, seq_count), "seq": lax.rem(there, seq_count)}

    def copy(k):
        there, device = peer(k)
        return pltpu.make_async_remote_copy(
            src_ref=parts.at[there],
            dst_ref=come.at[k],
            send_sem=send_sem.at[k],
            recv_sem=recv_sem.at[k],
            device_id=device,
            device_id_type=MESH,
        )

    barrier = pltpu.get_barrier_semaphore()
    for k in range(1, peers):
        pl.semaphore_signal(barrier, inc=1, device_id=peer(k)[1], device_id_type=MESH)
    rows = x_ref.shape[0]
    tile = rows // 8
    gain = gain_ref[...]
    acc[...] = jnp.zeros_like(acc)

    def rows_step(i, carry):
        here = pl.ds(pl.multiple_of(i * tile, tile), tile)
        wide = x_ref[here, :].astype(F32)
        grad = gn_ref[here, :].astype(F32)
        scale = lax.rsqrt(jnp.mean(wide * wide, axis=-1, keepdims=True) + epsilon)
        scaled = grad * gain
        mean = jnp.mean(wide * scaled, axis=-1, keepdims=True)
        result = gm_ref[here, :] + scale * scaled - wide * (scale * scale * scale) * mean
        out_ref[here, :] = result.astype(BF16)
        acc[...] += jnp.sum(grad * wide * scale, axis=0, keepdims=True)
        return carry

    lax.fori_loop(0, 8, rows_step, 0)
    for k in range(peers):
        here = slice(k * block, (k + 1) * block)
        parts[k, 0:1, :] = acc[:, here]
        parts[k, 1:2, :] = mlp_ref[:, here]
    pl.semaphore_wait(barrier, peers - 1)
    for k in range(1, peers):
        copy(k).start()
    total = parts[me]
    for k in range(1, peers):
        copy(k).wait_recv()
        total = total + come[k]
    gains_ref[...] = total
    for k in range(1, peers):
        copy(k).wait_send()


def final(grad_normed, tokens, grad_middle, gain, mlp_part, call_id):
    rows, width = tokens.shape
    peers = lax.axis_size("batch") * lax.axis_size("seq")
    block = width // peers
    vmem = pl.BlockSpec(memory_space=pltpu.VMEM)
    return pl.pallas_call(
        final_kernel,
        out_shape=[jax.ShapeDtypeStruct((rows, width), BF16), jax.ShapeDtypeStruct((2, block), F32)],
        in_specs=[vmem] * 5,
        out_specs=[vmem, vmem],
        scratch_shapes=[
            pltpu.VMEM((1, width), F32),
            pltpu.VMEM((peers, 2, block), F32),
            pltpu.VMEM((peers, 2, block), F32),
            pltpu.SemaphoreType.DMA((peers,)),
            pltpu.SemaphoreType.DMA((peers,)),
        ],
        compiler_params=pltpu.CompilerParams(collective_id=call_id, has_side_effects=True),
        name="final",
    )(grad_normed, tokens, grad_middle, gain, mlp_part)


def scatter_sum(left, right):
    rows, depth = left.shape
    columns = right.shape[1]
    batch_count = lax.axis_size("batch")
    seq_index = lax.axis_index("seq")
    core, chip = seq_index % 2, seq_index // 2
    block = depth // (4 * batch_count)
    split = left.reshape(rows, batch_count, 2, 2, block)
    size = lax.axis_size("seq")

    def product(at):
        taken = lax.dynamic_index_in_dim(split, at, 3, keepdims=False).reshape(rows, depth // 2)
        return dot_tn(taken, right)

    away = product(1 - core).astype(BF16)
    arrived = lax.ppermute(away, "seq", [(s, s ^ 1) for s in range(size)])
    kept = (product(core) + arrived.astype(F32)).astype(BF16)
    kept = kept.reshape(batch_count, 2, block, columns)
    half = columns // 2

    def over_chip(values, axis):
        sent = lax.dynamic_index_in_dim(values, 1 - chip, axis, keepdims=False)
        stay = lax.dynamic_index_in_dim(values, chip, axis, keepdims=False)
        came = lax.ppermute(sent, "seq", [(s, s ^ 2) for s in range(size)])
        return stay.astype(F32) + came.astype(F32)

    def over_batch(values):
        if batch_count == 2:
            here = lax.axis_index("batch")
            sent = lax.dynamic_index_in_dim(values, 1 - here, 0, keepdims=False)
            stay = lax.dynamic_index_in_dim(values, here, 0, keepdims=False)
            came = lax.ppermute(sent, "batch", [(0, 1), (1, 0)])
            return stay.astype(F32) + came.astype(F32)
        return lax.psum_scatter(values, "batch", scatter_dimension=0, tiled=False).astype(F32)

    one = over_batch(over_chip(kept[..., :half], 1).astype(BF16))
    two = over_chip(over_batch(kept[..., half:]).astype(BF16), 0)
    return jnp.concatenate([one, two], axis=1)


def local(
    tokens, segment_ids, attn_gain, w_query, w_key, w_value, w_output, mlp_gain, w_gate, w_up, w_down, cotangent
):
    rows, width = tokens.shape
    seq_count = lax.axis_size("seq")
    seq_index = lax.axis_index("seq")
    segments = segment_ids[0]
    first_row = seq_index * rows
    reach = LONGEST // rows
    cos, sin = rope_tables(segments, first_row, rows)
    row_segment = lax.dynamic_slice_in_dim(segments, first_row, rows, 0)[None, :]
    padded = jnp.concatenate([jnp.full((LONGEST,), -1, jnp.int32), segments])
    key_segment = lax.dynamic_slice_in_dim(padded, first_row, rows + LONGEST, 0)[:, None]

    normed, queries, own = project(tokens, attn_gain[None, :], w_query, w_key, w_value, cos, sin)
    near = lax.ppermute(own, "seq", [(s, s + 1) for s in range(seq_count - 1)])
    far = lax.ppermute(own, "seq", [(s, s + 2) for s in range(seq_count - 2)])
    mixed, logs = attend(queries, far, near, own, key_segment, row_segment)

    branch = line_sum([(mixed, w_output, "nn")], 1).astype(F32)
    wide = tokens.astype(F32)
    middle = wide + branch
    scale_two = lax.rsqrt(jnp.mean(middle * middle, axis=-1, keepdims=True) + epsilon)
    normed_two = (middle * scale_two * mlp_gain).astype(BF16)
    gate_pre = dot_nn(normed_two, w_gate)
    up_pre = dot_nn(normed_two, w_up)
    sigmoid_gate = jax.nn.sigmoid(gate_pre)
    swish = gate_pre * sigmoid_gate
    active = (swish * up_pre).astype(BF16)
    grad_active = dot_nt(cotangent, w_down)
    grad_gate_low = (grad_active * up_pre * sigmoid_gate * (1.0 + gate_pre * (1.0 - sigmoid_gate))).astype(BF16)
    grad_up_low = (grad_active * swish).astype(BF16)
    mlp_out = lax.psum(dot_nn(active, w_down).astype(BF16), "mp").astype(F32)
    output = (middle + mlp_out).astype(BF16)

    fused = lax.axis_size("batch") == 2
    if fused:
        grad_normed_two, grad_gate, grad_up = exchange(
            [normed_two],
            [grad_gate_low, grad_up_low],
            [w_gate, w_up],
            (0, 1),
            (0,),
            0,
            (("plain", 0, w_gate.shape[1]), ("plain", w_gate.shape[1], w_up.shape[1])),
            2,
        )
    else:
        grad_normed_two = line_sum([(grad_gate_low, w_gate, "nt"), (grad_up_low, w_up, "nt")], 2)
        grad_gate = scatter_sum(normed_two, grad_gate_low)
        grad_up = scatter_sum(normed_two, grad_up_low)
    grad_normed_two = grad_normed_two.astype(F32)
    scaled_two = grad_normed_two * mlp_gain
    grad_middle = (
        cotangent.astype(F32)
        + scale_two * scaled_two
        - middle
        * (scale_two * scale_two * scale_two)
        * jnp.mean(middle * scaled_two, axis=-1, keepdims=True)
    )
    grad_mlp_gain = jnp.sum(grad_normed_two * middle * scale_two, axis=0)
    grad_branch = grad_middle.astype(BF16)
    grad_mixed = dot_nt(grad_branch, w_output).astype(BF16)
    grad_query_pre, dfar, dnear, down = attend_back(
        queries, far, near, own, key_segment, row_segment, mixed, grad_mixed, logs, cos, sin
    )
    from_near = lax.ppermute(dnear, "seq", [(s + 1, s) for s in range(seq_count - 1)])
    from_far = lax.ppermute(dfar, "seq", [(s + 2, s) for s in range(seq_count - 2)])
    grad_pair = down + from_near.astype(F32) + from_far.astype(F32)
    grad_keys = jnp.concatenate([grad_pair[:, :HS], grad_pair[:, PAIR : PAIR + HS]], axis=1)
    grad_values = jnp.concatenate([grad_pair[:, HS:PAIR], grad_pair[:, PAIR + HS :]], axis=1)
    quarter = HS // 2
    swapped = jnp.concatenate(
        [grad_keys[:, (at ^ 1) * quarter : ((at ^ 1) + 1) * quarter] for at in range(4)], axis=1
    )
    grad_key_pre = (grad_keys * cos - swapped * sin).astype(BF16)
    grad_value_pre = grad_values.astype(BF16)

    query_width = grad_query_pre.shape[1]
    if fused:
        units_down = active.shape[1] // (width // 8)
        units_output = mixed.shape[1] // (width // 8)
        grad_normed, grad_down, grad_output, grad_query, grad_key, grad_value = exchange(
            [cotangent, grad_branch, normed],
            [active, mixed, grad_query_pre, grad_key_pre, grad_value_pre],
            [w_query, w_key, w_value],
            (2, 3, 4),
            (0, units_down, units_down + units_output),
            units_down + units_output,
            (
                ("turned", 0, active.shape[1]),
                ("turned", active.shape[1], mixed.shape[1]),
                ("plain", 0, query_width),
                ("plain", query_width, PAIR),
                ("plain", query_width + PAIR, PAIR),
            ),
            3,
        )
    else:
        grad_down = scatter_sum(cotangent, active).T
        grad_output = scatter_sum(grad_branch, mixed).T
        grad_qkv = scatter_sum(normed, jnp.concatenate([grad_query_pre, grad_key_pre, grad_value_pre], axis=1))
        grad_query = grad_qkv[:, :query_width]
        grad_key = grad_qkv[:, query_width : query_width + PAIR]
        grad_value = grad_qkv[:, query_width + PAIR :]
        grad_normed = line_sum(
            [(grad_query_pre, w_query, "nt"), (grad_key_pre, w_key, "nt"), (grad_value_pre, w_value, "nt")], 3
        )
    grad_tokens, gains = final(
        grad_normed, tokens, grad_middle, attn_gain[None, :], grad_mlp_gain[None, :], 4
    )
    return (
        output,
        grad_tokens,
        gains[0],
        grad_query,
        grad_key,
        grad_value,
        grad_output,
        gains[1],
        grad_gate,
        grad_up,
        grad_down,
    )


def solution(mesh):
    tokens_spec = P(("batch", "seq"), None)
    in_specs = (
        tokens_spec,
        P("batch", None),
        P(),
        P(None, "mp"),
        P(None, "mp"),
        P(None, "mp"),
        P("mp", None),
        P(),
        P(None, "mp"),
        P(None, "mp"),
        P("mp", None),
        tokens_spec,
    )
    row_split = P(("batch", "seq"), "mp")
    column_split = P("mp", ("batch", "seq"))
    out_specs = (
        tokens_spec,
        tokens_spec,
        P(("batch", "seq")),
        row_split,
        row_split,
        row_split,
        column_split,
        P(("batch", "seq")),
        row_split,
        row_split,
        column_split,
    )
    return jax.shard_map(local, mesh=mesh, in_specs=in_specs, out_specs=out_specs, check_vma=False)
```

```python
import functools
import math

import jax
import jax.numpy as jnp
from jax import lax
from jax.experimental import pallas as pl
from jax.experimental.pallas import tpu as pltpu
from jax.sharding import PartitionSpec as P

HS = 64
PAIR = 2 * HS
LONGEST = 1024
rope_base = 500000.0
epsilon = 1e-05
masked_score = -1e30
MESH = pl.DeviceIdType.MESH
F32 = jnp.float32
BF16 = jnp.bfloat16


def dot_nn(left, right):
    return lax.dot_general(left, right, (((1,), (0,)), ((), ())), preferred_element_type=F32)


def dot_nt(left, right):
    return lax.dot_general(left, right, (((1,), (1,)), ((), ())), preferred_element_type=F32)


def dot_tn(left, right):
    return lax.dot_general(left, right, (((0,), (0,)), ((), ())), preferred_element_type=F32)


def lanes_of(values):
    return lax.broadcasted_iota(jnp.int32, values.shape, 1)


def swap_halves(values):
    ahead = pltpu.roll(values, PAIR - HS // 2, 1)
    behind = pltpu.roll(values, HS // 2, 1)
    return jnp.where(lanes_of(values) % HS < HS // 2, ahead, behind)


def rope_tables(segments, first_row, rows):
    row_segment = lax.dynamic_slice_in_dim(segments, first_row, rows, 0)
    doc_start = jnp.sum((segments[None, :] < row_segment[:, None]).astype(jnp.int32), axis=1)
    place = (first_row + jnp.arange(rows, dtype=jnp.int32) - doc_start).astype(F32)
    lane = jnp.arange(PAIR, dtype=jnp.int32)
    frequency = jnp.exp((lane % (HS // 2)).astype(F32) * (-2.0 * math.log(rope_base) / HS))
    angles = place[:, None] * frequency[None, :]
    sign = jnp.where(lane % HS < HS // 2, -1.0, 1.0)
    return jnp.cos(angles), jnp.sin(angles) * sign[None, :]


def project_kernel(x_ref, gain_ref, wq_ref, wk_ref, wv_ref, cos_ref, sin_ref, n_ref, q_ref, kv_ref):
    wide = x_ref[...].astype(F32)
    scale = lax.rsqrt(jnp.mean(wide * wide, axis=-1, keepdims=True) + epsilon)
    normed = (wide * scale * gain_ref[...]).astype(BF16)
    n_ref[...] = normed
    cos, sin = cos_ref[...], sin_ref[...]
    queries = dot_nn(normed, wq_ref[...])
    for start in range(0, queries.shape[1], PAIR):
        part = queries[:, start : start + PAIR]
        q_ref[:, start : start + PAIR] = (part * cos + swap_halves(part) * sin).astype(BF16)
    keys = dot_nn(normed, wk_ref[...])
    keys = keys * cos + swap_halves(keys) * sin
    values = dot_nn(normed, wv_ref[...])
    low_half = lanes_of(keys) < HS
    kv_ref[:, :PAIR] = jnp.where(low_half, keys, pltpu.roll(values, HS, 1)).astype(BF16)
    kv_ref[:, PAIR:] = jnp.where(low_half, pltpu.roll(keys, HS, 1), values).astype(BF16)


def project(tokens, gain, w_query, w_key, w_value, cos, sin):
    rows, width = tokens.shape
    block = rows // 2
    full = lambda array: pl.BlockSpec(array.shape, lambda i: (0, 0))
    tile = lambda columns: pl.BlockSpec((block, columns), lambda i: (i, 0))
    return pl.pallas_call(
        project_kernel,
        grid=(rows // block,),
        in_specs=[
            tile(width),
            full(gain),
            full(w_query),
            full(w_key),
            full(w_value),
            tile(PAIR),
            tile(PAIR),
        ],
        out_specs=[tile(width), tile(w_query.shape[1]), tile(2 * PAIR)],
        out_shape=[
            jax.ShapeDtypeStruct((rows, width), BF16),
            jax.ShapeDtypeStruct((rows, w_query.shape[1]), BF16),
            jax.ShapeDtypeStruct((rows, 2 * PAIR), BF16),
        ],
        cost_estimate=pl.CostEstimate(
            flops=2 * rows * width * (w_query.shape[1] + 2 * PAIR),
            bytes_accessed=8 << 20,
            transcendentals=0,
        ),
        name="project",
    )(tokens, gain, w_query, w_key, w_value, cos, sin)


def write_bias(bias_ref, key_ref, row_ref):
    keys, rows = bias_ref.shape
    key_place = lax.broadcasted_iota(jnp.int32, (keys, rows), 0) - (keys - rows)
    row_place = lax.broadcasted_iota(jnp.int32, (keys, rows), 1)
    allowed = (key_ref[...] == row_ref[...]) & (key_place <= row_place)
    bias_ref[...] = jnp.where(allowed, 0.0, masked_score)


def attend_kernel(q_ref, far_ref, near_ref, own_ref, key_ref, row_ref, out_ref, log_ref, bias_ref, kv_ref):
    @pl.when(pl.program_id(0) == 0)
    def _():
        write_bias(bias_ref, key_ref, row_ref)

    rows = q_ref.shape[0]
    for at, ref in enumerate((far_ref, near_ref, own_ref)):
        kv_ref[at * rows : (at + 1) * rows, :] = ref[...]
    key_value = kv_ref[...]
    flipped = key_value.T
    q_flipped = (q_ref[...].astype(F32) * HS ** (-0.5)).astype(BF16).T
    outs = []
    for head in range(2):
        scores = dot_nn(key_value[:, :HS], q_flipped[head * HS : (head + 1) * HS, :]) + bias_ref[...]
        top = jnp.max(scores, axis=0, keepdims=True)
        powers = jnp.exp(scores - top)
        total = jnp.sum(powers, axis=0, keepdims=True)
        mixed = dot_nn(flipped[HS:, :], powers.astype(BF16))
        outs.append(mixed / total)
        log_ref[0, head : head + 1, :] = top + jnp.log(total)
    out_ref[...] = jnp.concatenate(outs, axis=0).T.astype(BF16)


def attend(queries, far, near, own, key_segment, row_segment):
    rows, width = queries.shape
    pairs = width // PAIR
    per_group = pairs // 2
    pair_tile = pl.BlockSpec((rows, PAIR), lambda p: (0, p))
    kv_tile = pl.BlockSpec((rows, PAIR), lambda p: (0, p // per_group))
    return pl.pallas_call(
        attend_kernel,
        grid=(pairs,),
        in_specs=[
            pair_tile,
            kv_tile,
            kv_tile,
            kv_tile,
            pl.BlockSpec(key_segment.shape, lambda p: (0, 0)),
            pl.BlockSpec(row_segment.shape, lambda p: (0, 0)),
        ],
        out_specs=[pair_tile, pl.BlockSpec((1, 2, rows), lambda p: (p, 0, 0))],
        out_shape=[
            jax.ShapeDtypeStruct((rows, width), BF16),
            jax.ShapeDtypeStruct((pairs, 2, rows), F32),
        ],
        scratch_shapes=[pltpu.VMEM((3 * rows, rows), F32), pltpu.VMEM((3 * rows, PAIR), BF16)],
        cost_estimate=pl.CostEstimate(
            flops=16 << 30, bytes_accessed=4 << 20, transcendentals=3 * rows * rows * 2 * pairs
        ),
        name="attend",
    )(queries, far, near, own, key_segment, row_segment)


def attend_back_kernel(
    q_ref, far_ref, near_ref, own_ref, key_ref, row_ref, out_ref, grad_ref, log_ref, cos_ref, sin_ref,
    dq_ref, dfar_ref, dnear_ref, down_ref, bias_ref, kv_ref, dkv_ref, per_group,
):
    step = pl.program_id(0)

    @pl.when(step == 0)
    def _():
        write_bias(bias_ref, key_ref, row_ref)

    rows = q_ref.shape[0]
    for at, ref in enumerate((far_ref, near_ref, own_ref)):
        kv_ref[at * rows : (at + 1) * rows, :] = ref[...]
    key_value = kv_ref[...]
    flipped = key_value[:, :].T
    scaled = (q_ref[...].astype(F32) * HS ** (-0.5)).astype(BF16)
    q_flipped = scaled.T
    grad = grad_ref[...]
    grad_flipped = grad.T
    product = (out_ref[...].astype(F32) * grad.astype(F32)).T
    dqs, dkey, dvalue = [], None, None
    for head in range(2):
        here = slice(head * HS, (head + 1) * HS)
        scores = dot_nn(key_value[:, :HS], q_flipped[here, :]) + bias_ref[...]
        shares = jnp.exp(scores - log_ref[0, head : head + 1, :])
        grad_shares = dot_nn(key_value[:, HS:], grad_flipped[here, :])
        delta = jnp.sum(product[here, :], axis=0, keepdims=True)
        grad_scores = (shares * (grad_shares - delta)).astype(BF16)
        value_part = dot_nn(shares.astype(BF16), grad[:, here])
        key_part = dot_nn(grad_scores, scaled[:, here])
        dvalue = value_part if dvalue is None else dvalue + value_part
        dkey = key_part if dkey is None else dkey + key_part
        dqs.append(dot_nn(flipped[:HS, :], grad_scores))
    dq = jnp.concatenate(dqs, axis=0).T * HS ** (-0.5)
    dq_ref[...] = (dq * cos_ref[...] - swap_halves(dq) * sin_ref[...]).astype(BF16)
    both = jnp.concatenate([dkey, dvalue], axis=1)

    @pl.when(step % per_group == 0)
    def _():
        dkv_ref[...] = both

    @pl.when(step % per_group != 0)
    def _():
        dkv_ref[...] += both

    @pl.when(step % per_group == per_group - 1)
    def _():
        dfar_ref[...] = dkv_ref[:rows, :].astype(BF16)
        dnear_ref[...] = dkv_ref[rows : 2 * rows, :].astype(BF16)
        down_ref[...] = dkv_ref[2 * rows :, :]


def attend_back(queries, far, near, own, key_segment, row_segment, mixed, grad, logs, cos, sin):
    rows, width = queries.shape
    pairs = width // PAIR
    per_group = pairs // 2
    pair_tile = pl.BlockSpec((rows, PAIR), lambda p: (0, p))
    kv_tile = pl.BlockSpec((rows, PAIR), lambda p: (0, p // per_group))
    full = lambda array: pl.BlockSpec(array.shape, lambda p: (0, 0))
    return pl.pallas_call(
        functools.partial(attend_back_kernel, per_group=per_group),
        grid=(pairs,),
        in_specs=[
            pair_tile,
            kv_tile,
            kv_tile,
            kv_tile,
            full(key_segment),
            full(row_segment),
            pair_tile,
            pair_tile,
            pl.BlockSpec((1, 2, rows), lambda p: (p, 0, 0)),
            full(cos),
            full(sin),
        ],
        out_specs=[pair_tile, kv_tile, kv_tile, kv_tile],
        out_shape=[
            jax.ShapeDtypeStruct((rows, width), BF16),
            jax.ShapeDtypeStruct((rows, 2 * PAIR), BF16),
            jax.ShapeDtypeStruct((rows, 2 * PAIR), BF16),
            jax.ShapeDtypeStruct((rows, 2 * PAIR), F32),
        ],
        scratch_shapes=[
            pltpu.VMEM((3 * rows, rows), F32),
            pltpu.VMEM((3 * rows, PAIR), BF16),
            pltpu.VMEM((3 * rows, PAIR), F32),
        ],
        cost_estimate=pl.CostEstimate(
            flops=40 << 30, bytes_accessed=6 << 20, transcendentals=3 * rows * rows * 2 * pairs
        ),
        name="attend_back",
    )(queries, far, near, own, key_segment, row_segment, mixed, grad, logs, cos, sin)


def line_sum_kernel(modes, chunks, *refs):
    count = len(modes)
    a_refs, w_refs, out_ref = refs[:count], refs[count : 2 * count], refs[2 * count]
    rest = refs[2 * count + 1 :]
    w_bufs = rest[:count]
    part, first, second, total, w_sem, send_sem, recv_sem = rest[count:]
    width = part.shape[2]
    place = lax.axis_index("mp")
    pair = place + 1 - 2 * lax.rem(place, 2)
    across = 3 - place
    is_mid = (place == 1) | (place == 2)
    is_end = (place == 0) | (place == 3)

    def weight(at, c):
        if modes[at] == "nt":
            source = w_refs[at].at[pl.ds(pl.multiple_of(c * width, width), width), :]
        else:
            source = w_refs[at].at[:, pl.ds(pl.multiple_of(c * width, width), width)]
        return pltpu.make_async_copy(source, w_bufs[at].at[c], w_sem.at[at, c])

    def remote(kind, source, target, c, device):
        return pltpu.make_async_remote_copy(
            src_ref=source.at[c],
            dst_ref=target.at[c],
            send_sem=send_sem.at[kind, c],
            recv_sem=recv_sem.at[kind, c],
            device_id={"mp": device},
            device_id_type=MESH,
        )

    def up(c):
        return remote(0, part, first, c, pair)

    def over(c):
        return remote(1, part, second, c, across)

    def down(c):
        return remote(2, total, total, c, pair)

    def start_weights(c, carry):
        for at in range(count):
            weight(at, c).start()
        return carry

    lax.fori_loop(0, chunks, start_weights, 0)
    barrier = pltpu.get_barrier_semaphore()
    pl.semaphore_signal(barrier, inc=1, device_id={"mp": pair}, device_id_type=MESH)

    @pl.when(is_mid)
    def _():
        pl.semaphore_signal(barrier, inc=1, device_id={"mp": across}, device_id_type=MESH)
        pl.semaphore_wait(barrier, 2)

    @pl.when(is_end)
    def _():
        pl.semaphore_wait(barrier, 1)

    def step(t, carry):
        @pl.when(t < chunks)
        def _():
            value = None
            for at in range(count):
                weight(at, t).wait()
                dot = dot_nt if modes[at] == "nt" else dot_nn
                term = dot(a_refs[at][...], w_bufs[at][t])
                value = term if value is None else value + term
            part[t] = value.astype(BF16)

            @pl.when(is_end)
            def _():
                up(t).start()

        @pl.when(is_mid & (t >= 1) & (t < chunks + 1))
        def _():
            c = t - 1
            up(c).wait_recv()
            part[c] = (part[c].astype(F32) + first[c].astype(F32)).astype(BF16)
            over(c).start()

        @pl.when(is_mid & (t >= OVER_LAG))
        def _():
            c = t - OVER_LAG
            over(c).wait_recv()
            total[c] = (part[c].astype(F32) + second[c].astype(F32)).astype(BF16)
            down(c).start()

        return carry

    lax.fori_loop(0, chunks + OVER_LAG, step, 0)

    def finish(c, carry):
        @pl.when(is_end)
        def _():
            up(c).wait_send()
            down(c).wait_recv()

        @pl.when(is_mid)
        def _():
            over(c).wait_send()
            down(c).wait_send()

        out_ref[:, pl.ds(pl.multiple_of(c * width, width), width)] = total[c]
        return carry

    lax.fori_loop(0, chunks, finish, 0)


def line_sum(pairs, call_id, chunks=16):
    lefts = [left for left, _, _ in pairs]
    rights = [right for _, right, _ in pairs]
    modes = tuple(mode for _, _, mode in pairs)
    rows = lefts[0].shape[0]
    columns = rights[0].shape[0] if modes[0] == "nt" else rights[0].shape[1]
    width = columns // chunks
    count = len(pairs)
    bufs = [
        pltpu.VMEM((chunks, width, left.shape[1]) if mode == "nt" else (chunks, left.shape[1], width), BF16)
        for left, _, mode in pairs
    ]
    flops = sum(2 * rows * columns * left.shape[1] for left in lefts)
    moved = sum(right.size * 2 for right in rights)
    block = pltpu.VMEM((chunks, rows, width), BF16)
    return pl.pallas_call(
        functools.partial(line_sum_kernel, modes, chunks),
        out_shape=jax.ShapeDtypeStruct((rows, columns), BF16),
        in_specs=[pl.BlockSpec(memory_space=pltpu.VMEM)] * count
        + [pl.BlockSpec(memory_space=pl.ANY)] * count,
        out_specs=pl.BlockSpec(memory_space=pltpu.VMEM),
        scratch_shapes=bufs
        + [
            block,
            block,
            block,
            block,
            pltpu.SemaphoreType.DMA((count, chunks)),
            pltpu.SemaphoreType.DMA((3, chunks)),
            pltpu.SemaphoreType.DMA((3, chunks)),
        ],
        compiler_params=pltpu.CompilerParams(collective_id=call_id, has_side_effects=True),
        cost_estimate=pl.CostEstimate(
            flops=flops + (40 << 30), bytes_accessed=moved, transcendentals=0
        ),
        name=f"line_sum_{call_id}",
    )(*lefts, *rights)

LAG = 2
UP_LAG = 1
OVER_LAG = 3


def exchange_kernel(plan, *refs):
    left_count, rights, sums, flips_before, spans, out_count, units, chunks, period, active = plan
    refs = list(refs)

    def take(n):
        got = refs[:n]
        del refs[:n]
        return got

    weights = [item for group in sums for item in group]
    left_refs, right_refs, w_refs = take(left_count), take(len(rights)), take(len(weights))
    (out_ref,) = take(1)
    grad_refs = take(out_count)
    stage, flip, right_all = take(3)
    w_bufs = take(len(weights))
    part, first, second, away, come_one, come_two, come_three, result = take(8)
    in_sem, right_sem, w_sem, ar_send, ar_recv, core_send, core_recv, two_send, two_recv, three_send, three_recv, out_sem = refs
    width = part.shape[2]
    block = come_three.shape[1]
    all_chunks = chunks * len(sums)
    place = lax.axis_index("mp")
    seq, batch = lax.axis_index("seq"), lax.axis_index("batch")
    core, chip = lax.rem(seq, 2), lax.div(seq, 2)
    sibling = seq + 1 - 2 * core
    beside = seq + 2 - 4 * chip
    pair = place + 1 - 2 * lax.rem(place, 2)
    across = 3 - place
    is_mid = (place == 1) | (place == 2)
    is_end = (place == 0) | (place == 3)

    def columns_of(c):
        return pl.ds(pl.multiple_of(c * width, width), width)

    def weight(at, group, c):
        here = columns_of(c - group * chunks)
        source = w_refs[at].at[here, :] if weights[at][2] == "nt" else w_refs[at].at[:, here]
        slot = lax.rem(c, 3)
        return pltpu.make_async_copy(source, w_bufs[at].at[slot], w_sem.at[at, slot])

    members = []
    for group, items in enumerate(sums):
        for _ in items:
            members.append(group)

    def load_weights(c):
        for group in range(len(sums)):

            @pl.when((c >= group * chunks) & (c < (group + 1) * chunks))
            def _():
                for at in range(len(weights)):
                    if members[at] == group:
                        weight(at, group, c).start()

    def remote(source, target, send, recv, device):
        return pltpu.make_async_remote_copy(
            src_ref=source, dst_ref=target, send_sem=send, recv_sem=recv, device_id=device, device_id_type=MESH
        )

    def up(c):
        return remote(part.at[c], first.at[c], ar_send.at[0, c], ar_recv.at[0, c], {"mp": pair})

    def over(c):
        return remote(part.at[c], second.at[c], ar_send.at[1, c], ar_recv.at[1, c], {"mp": across})

    def down(c):
        here = out_ref.at[:, columns_of(c)]
        return remote(here, here, ar_send.at[2, c], ar_recv.at[2, c], {"mp": pair})

    def to_core(u):
        return remote(away.at[lax.rem(u, 2)], come_one.at[u], core_send.at[u], core_recv.at[u], {"seq": sibling})

    def chip_first(u):
        return 1 - lax.rem(u, 2)

    def sent_at(u, k):
        x_first = chip_first(u)
        return x_first * (2 * k + 1 - chip) + (1 - x_first) * (2 * (1 - batch) + k)

    def kept_at(u, k):
        x_first = chip_first(u)
        return x_first * (2 * k + chip) + (1 - x_first) * (2 * batch + k)

    def own_at(u):
        x_first = chip_first(u)
        return x_first * batch + (1 - x_first) * chip

    def device_of(x_way):
        return {
            "seq": x_way * beside + (1 - x_way) * seq,
            "batch": x_way * batch + (1 - x_way) * (1 - batch),
        }

    def second_hop(u, k):
        return remote(
            come_one.at[u, sent_at(u, k)], come_two.at[u, k], two_send.at[k, u], two_recv.at[k, u], device_of(chip_first(u))
        )

    def third_hop(u):
        return remote(
            come_two.at[u, 1 - own_at(u)], come_three.at[u], three_send.at[u], three_recv.at[u], device_of(1 - chip_first(u))
        )

    def left_copy(at):
        return pltpu.make_async_copy(left_refs[at], stage, in_sem.at[at])

    def right_copy(at):
        offset, source, size = rights[at]
        return pltpu.make_async_copy(
            right_refs[at].at[:, source : source + size], right_all.at[:, offset : offset + size], right_sem.at[at]
        )

    def out_copy(at, u):
        kind, index, offset, start, size = spans[at]
        slot = lax.rem(u, 2)
        if size < block:
            source = result.at[slot, :, start % block : start % block + size]
            target = grad_refs[index].at[:, offset : offset + size]
        else:
            source = result.at[slot]
            here = pl.ds(pl.multiple_of((u - start // block) * block + offset, block), block)
            target = grad_refs[index].at[here, :] if kind == "turned" else grad_refs[index].at[:, here]
        return pltpu.make_async_copy(source, target, out_sem.at[at, slot])

    def units_of(at):
        _, _, _, start, size = spans[at]
        return start // block, max((start + size) // block, start // block + 1)

    load_weights(0)
    load_weights(1)
    for at in range(len(rights)):
        right_copy(at).start()
    left_copy(0).start()

    barrier = pltpu.get_barrier_semaphore()
    for device in ({"mp": pair}, {"seq": sibling}, {"seq": beside}, {"batch": 1 - batch}):
        pl.semaphore_signal(barrier, inc=1, device_id=device, device_id_type=MESH)

    @pl.when(is_mid)
    def _():
        pl.semaphore_signal(barrier, inc=1, device_id={"mp": across}, device_id_type=MESH)
        pl.semaphore_wait(barrier, 5)

    @pl.when(is_end)
    def _():
        pl.semaphore_wait(barrier, 4)

    for at in range(len(rights)):
        right_copy(at).wait()

    def left_of(u):
        index = 0
        for at in range(1, left_count):
            index = index + (u >= flips_before[at]).astype(jnp.int32)
        return index

    def product(u, at, side):
        row = pl.multiple_of((2 * at + side) * block, block)
        column = pl.multiple_of(u * block, block)
        return dot_nn(flip[left_of(u), pl.ds(row, block), :], right_all[:, pl.ds(column, block)])

    def step_of(u):
        return (u // active) * period + u % active

    def on_unit(t, body):
        u = lax.div(t, period) * active + lax.rem(t, period)

        @pl.when((t >= 0) & (lax.rem(t, period) < active) & (u < units))
        def _():
            body(u)

    def first_stage(u):
        @pl.when(u >= 2)
        def _():
            to_core(u - 2).wait_send()

        for at in range(4):
            away[lax.rem(u, 2), at] = product(u, at, 1 - core).astype(BF16)
        to_core(u).start()

    def second_stage(u):
        to_core(u).wait_recv()
        for at in range(4):
            come_one[u, at] = (product(u, at, core) + come_one[u, at].astype(F32)).astype(BF16)
        for k in range(2):
            second_hop(u, k).start()

    def third_stage(u):
        for k in range(2):
            second_hop(u, k).wait_recv()
        sent = 1 - own_at(u)
        come_two[u, sent] = (come_two[u, sent].astype(F32) + come_one[u, kept_at(u, sent)].astype(F32)).astype(BF16)
        third_hop(u).start()

    def last_stage(u):
        third_hop(u).wait_recv()
        own = own_at(u)
        value = come_three[u].astype(F32) + come_two[u, own].astype(F32) + come_one[u, kept_at(u, own)].astype(F32)
        for at in range(len(spans)):
            low, high = units_of(at)

            @pl.when((u - 2 >= low) & (u - 2 < high))
            def _():
                out_copy(at, u - 2).wait()

        for kind in ("turned", "plain"):
            mine = [units_of(at) for at in range(len(spans)) if spans[at][0] == kind]
            if mine:
                low, high = min(m[0] for m in mine), max(m[1] for m in mine)

                @pl.when((u >= low) & (u < high))
                def _():
                    result[lax.rem(u, 2)] = value.T if kind == "turned" else value

        for at in range(len(spans)):
            low, high = units_of(at)

            @pl.when((u >= low) & (u < high))
            def _():
                out_copy(at, u).start()

    def step(t, carry):
        for group, items in enumerate(sums):

            @pl.when((t >= group * chunks) & (t < (group + 1) * chunks))
            def _():
                value = None
                for at, (start, size, mode) in enumerate(weights):
                    if members[at] == group:
                        weight(at, group, t).wait()
                        dot = dot_nt if mode == "nt" else dot_nn
                        term = dot(right_all[:, start : start + size], w_bufs[at][lax.rem(t, 3)])
                        value = term if value is None else value + term
                part[t] = value.astype(BF16)

        @pl.when(t < all_chunks)
        def _():
            @pl.when(is_end)
            def _():
                up(t).start()

            load_weights(t + 2)

        @pl.when(is_mid & (t >= UP_LAG) & (t < all_chunks + UP_LAG))
        def _():
            c = t - UP_LAG
            up(c).wait_recv()
            part[c] = (part[c].astype(F32) + first[c].astype(F32)).astype(BF16)
            over(c).start()

        @pl.when(is_mid & (t >= OVER_LAG) & (t < all_chunks + OVER_LAG))
        def _():
            c = t - OVER_LAG
            over(c).wait_recv()
            out_ref[:, columns_of(c)] = (part[c].astype(F32) + second[c].astype(F32)).astype(BF16)
            down(c).start()

        for at in range(left_count):

            @pl.when(t == max(step_of(flips_before[at]) - 2, at))
            def _():
                left_copy(at).wait()

                def turn(k, carry):
                    here = pl.ds(pl.multiple_of(k * block, block), block)
                    flip[at, here, :] = stage[:, here].T
                    return carry

                lax.fori_loop(0, flip.shape[1] // block, turn, 0)
                if at + 1 < left_count:
                    left_copy(at + 1).start()

        on_unit(t, first_stage)
        on_unit(t - 1, second_stage)
        on_unit(t - 1 - LAG, third_stage)
        on_unit(t - 1 - 2 * LAG, last_stage)
        return carry

    lax.fori_loop(0, max(step_of(units - 1) + 2 + 2 * LAG, all_chunks + OVER_LAG), step, 0)

    def finish(c, carry):
        @pl.when(is_end)
        def _():
            up(c).wait_send()
            down(c).wait_recv()

        @pl.when(is_mid)
        def _():
            over(c).wait_send()
            down(c).wait_send()

        return carry

    lax.fori_loop(0, all_chunks, finish, 0)

    def settle(u, carry):
        for k in range(2):
            second_hop(u, k).wait_send()
        third_hop(u).wait_send()
        return carry

    lax.fori_loop(0, units, settle, 0)
    for u in (units - 2, units - 1):
        to_core(u).wait_send()
        for at in range(len(spans)):
            low, high = units_of(at)
            if low <= u < high:
                out_copy(at, u).wait()


def exchange(lefts, rights, sums, flips_before, outs, spans, units, call_id, pace, chunks=16):
    rows, depth = lefts[0].shape
    block = depth // 8
    placed, at = [], 0
    for _, source, size in rights:
        placed.append((at, source, size))
        at += size
    weights = [item[0] for group in sums for item in group]
    columns = weights[0].shape[0] if sums[0][0][3] == "nt" else weights[0].shape[1]
    width = columns // chunks
    sum_plan = [[item[1:] for item in group] for group in sums]
    plan = (len(lefts), placed, sum_plan, flips_before, spans, len(outs), units, chunks, *pace)
    any_space = pl.BlockSpec(memory_space=pl.ANY)
    line_block = pltpu.VMEM((chunks * len(sums), rows, width), BF16)
    dma = pltpu.SemaphoreType.DMA
    all_chunks = chunks * len(sums)
    flops = sum(2 * rows * columns * size for group in sum_plan for _, size, _ in group) + 2 * rows * depth * at
    return pl.pallas_call(
        functools.partial(exchange_kernel, plan),
        out_shape=[jax.ShapeDtypeStruct((rows, columns * len(sums)), BF16)]
        + [jax.ShapeDtypeStruct(shape, F32) for shape in outs],
        in_specs=[any_space] * (len(lefts) + len(rights) + len(weights)),
        out_specs=[pl.BlockSpec(memory_space=pltpu.VMEM)] + [any_space] * len(outs),
        scratch_shapes=[
            pltpu.VMEM((rows, depth), BF16),
            pltpu.VMEM((len(lefts), depth, rows), BF16),
            pltpu.VMEM((rows, at), BF16),
        ]
        + [
            pltpu.VMEM((3, width, size) if mode == "nt" else (3, size, width), BF16)
            for group in sum_plan
            for _, size, mode in group
        ]
        + [
            line_block,
            line_block,
            line_block,
            pltpu.VMEM((2, 4, block, block), BF16),
            pltpu.VMEM((units, 4, block, block), BF16),
            pltpu.VMEM((units, 2, block, block), BF16),
            pltpu.VMEM((units, block, block), BF16),
            pltpu.VMEM((2, block, block), F32),
            dma((len(lefts),)),
            dma((len(rights),)),
            dma((len(weights), 3)),
            dma((3, all_chunks)),
            dma((3, all_chunks)),
            dma((units,)),
            dma((units,)),
            dma((2, units)),
            dma((2, units)),
            dma((units,)),
            dma((units,)),
            dma((len(spans), 2)),
        ],
        compiler_params=pltpu.CompilerParams(
            collective_id=call_id, has_side_effects=True, vmem_limit_bytes=62 << 20
        ),
        cost_estimate=pl.CostEstimate(flops=flops + (50 << 30), bytes_accessed=20 << 20, transcendentals=0),
        name=f"exchange_{call_id}",
    )(*lefts, *[right[0] for right in rights], *weights)


def final_kernel(gn_ref, x_ref, gm_ref, gain_ref, mlp_ref, out_ref, gains_ref, acc, parts, come, send_sem, recv_sem):
    seq, batch = lax.axis_index("seq"), lax.axis_index("batch")
    seq_count = lax.axis_size("seq")
    peers = parts.shape[0]
    block = parts.shape[2]
    me = batch * seq_count + seq

    def peer(k):
        there = lax.rem(me + k, peers)
        return there, {"batch": lax.div(there, seq_count), "seq": lax.rem(there, seq_count)}

    def copy(k):
        there, device = peer(k)
        return pltpu.make_async_remote_copy(
            src_ref=parts.at[there],
            dst_ref=come.at[k],
            send_sem=send_sem.at[k],
            recv_sem=recv_sem.at[k],
            device_id=device,
            device_id_type=MESH,
        )

    barrier = pltpu.get_barrier_semaphore()
    for k in range(1, peers):
        pl.semaphore_signal(barrier, inc=1, device_id=peer(k)[1], device_id_type=MESH)
    rows = x_ref.shape[0]
    tile = rows // 8
    gain = gain_ref[...]
    acc[...] = jnp.zeros_like(acc)

    def rows_step(i, carry):
        here = pl.ds(pl.multiple_of(i * tile, tile), tile)
        wide = x_ref[here, :].astype(F32)
        grad = gn_ref[here, :].astype(F32)
        scale = lax.rsqrt(jnp.mean(wide * wide, axis=-1, keepdims=True) + epsilon)
        scaled = grad * gain
        mean = jnp.mean(wide * scaled, axis=-1, keepdims=True)
        result = gm_ref[here, :] + scale * scaled - wide * (scale * scale * scale) * mean
        out_ref[here, :] = result.astype(BF16)
        acc[...] += jnp.sum(grad * wide * scale, axis=0, keepdims=True)
        return carry

    lax.fori_loop(0, 8, rows_step, 0)
    for k in range(peers):
        here = slice(k * block, (k + 1) * block)
        parts[k, 0:1, :] = acc[:, here]
        parts[k, 1:2, :] = mlp_ref[:, here]
    pl.semaphore_wait(barrier, peers - 1)
    for k in range(1, peers):
        copy(k).start()
    total = parts[me]
    for k in range(1, peers):
        copy(k).wait_recv()
        total = total + come[k]
    gains_ref[...] = total
    for k in range(1, peers):
        copy(k).wait_send()


def final(grad_normed, tokens, grad_middle, gain, mlp_part, call_id):
    rows, width = tokens.shape
    peers = lax.axis_size("batch") * lax.axis_size("seq")
    block = width // peers
    vmem = pl.BlockSpec(memory_space=pltpu.VMEM)
    return pl.pallas_call(
        final_kernel,
        out_shape=[jax.ShapeDtypeStruct((rows, width), BF16), jax.ShapeDtypeStruct((2, block), F32)],
        in_specs=[vmem] * 5,
        out_specs=[vmem, vmem],
        scratch_shapes=[
            pltpu.VMEM((1, width), F32),
            pltpu.VMEM((peers, 2, block), F32),
            pltpu.VMEM((peers, 2, block), F32),
            pltpu.SemaphoreType.DMA((peers,)),
            pltpu.SemaphoreType.DMA((peers,)),
        ],
        compiler_params=pltpu.CompilerParams(collective_id=call_id, has_side_effects=True),
        name="final",
    )(grad_normed, tokens, grad_middle, gain, mlp_part)


def scatter_sum(left, right):
    rows, depth = left.shape
    columns = right.shape[1]
    batch_count = lax.axis_size("batch")
    seq_index = lax.axis_index("seq")
    core, chip = seq_index % 2, seq_index // 2
    block = depth // (4 * batch_count)
    split = left.reshape(rows, batch_count, 2, 2, block)
    size = lax.axis_size("seq")

    def product(at):
        taken = lax.dynamic_index_in_dim(split, at, 3, keepdims=False).reshape(rows, depth // 2)
        return dot_tn(taken, right)

    away = product(1 - core).astype(BF16)
    arrived = lax.ppermute(away, "seq", [(s, s ^ 1) for s in range(size)])
    kept = (product(core) + arrived.astype(F32)).astype(BF16)
    kept = kept.reshape(batch_count, 2, block, columns)
    half = columns // 2

    def over_chip(values, axis):
        sent = lax.dynamic_index_in_dim(values, 1 - chip, axis, keepdims=False)
        stay = lax.dynamic_index_in_dim(values, chip, axis, keepdims=False)
        came = lax.ppermute(sent, "seq", [(s, s ^ 2) for s in range(size)])
        return stay.astype(F32) + came.astype(F32)

    def over_batch(values):
        if batch_count == 2:
            here = lax.axis_index("batch")
            sent = lax.dynamic_index_in_dim(values, 1 - here, 0, keepdims=False)
            stay = lax.dynamic_index_in_dim(values, here, 0, keepdims=False)
            came = lax.ppermute(sent, "batch", [(0, 1), (1, 0)])
            return stay.astype(F32) + came.astype(F32)
        return lax.psum_scatter(values, "batch", scatter_dimension=0, tiled=False).astype(F32)

    one = over_batch(over_chip(kept[..., :half], 1).astype(BF16))
    two = over_chip(over_batch(kept[..., half:]).astype(BF16), 0)
    return jnp.concatenate([one, two], axis=1)


def local(
    tokens, segment_ids, attn_gain, w_query, w_key, w_value, w_output, mlp_gain, w_gate, w_up, w_down, cotangent
):
    rows, width = tokens.shape
    seq_count = lax.axis_size("seq")
    seq_index = lax.axis_index("seq")
    segments = segment_ids[0]
    first_row = seq_index * rows
    reach = LONGEST // rows
    cos, sin = rope_tables(segments, first_row, rows)
    row_segment = lax.dynamic_slice_in_dim(segments, first_row, rows, 0)[None, :]
    padded = jnp.concatenate([jnp.full((LONGEST,), -1, jnp.int32), segments])
    key_segment = lax.dynamic_slice_in_dim(padded, first_row, rows + LONGEST, 0)[:, None]

    normed, queries, own = project(tokens, attn_gain[None, :], w_query, w_key, w_value, cos, sin)
    near = lax.ppermute(own, "seq", [(s, s + 1) for s in range(seq_count - 1)])
    far = lax.ppermute(own, "seq", [(s, s + 2) for s in range(seq_count - 2)])
    mixed, logs = attend(queries, far, near, own, key_segment, row_segment)

    branch = line_sum([(mixed, w_output, "nn")], 1).astype(F32)
    wide = tokens.astype(F32)
    middle = wide + branch
    scale_two = lax.rsqrt(jnp.mean(middle * middle, axis=-1, keepdims=True) + epsilon)
    normed_two = (middle * scale_two * mlp_gain).astype(BF16)
    gate_pre = dot_nn(normed_two, w_gate)
    up_pre = dot_nn(normed_two, w_up)
    sigmoid_gate = jax.nn.sigmoid(gate_pre)
    swish = gate_pre * sigmoid_gate
    active = (swish * up_pre).astype(BF16)
    grad_active = dot_nt(cotangent, w_down)
    grad_gate_low = (grad_active * up_pre * sigmoid_gate * (1.0 + gate_pre * (1.0 - sigmoid_gate))).astype(BF16)
    grad_up_low = (grad_active * swish).astype(BF16)
    fused = lax.axis_size("batch") == 2
    hidden = w_gate.shape[1]
    unit = width // 8
    early = hidden * 5 // 8 // unit * unit
    if fused:
        sums, grad_gate, grad_up, grad_down_one = exchange(
            [normed_two, cotangent],
            [(grad_gate_low, 0, hidden), (grad_up_low, 0, hidden), (active, 0, hidden)],
            [
                [(w_gate, 0, hidden, "nt"), (w_up, hidden, hidden, "nt")],
                [(w_down, 2 * hidden, hidden, "nn")],
            ],
            (0, 2 * hidden // unit),
            [(unit, hidden), (unit, hidden), (early, unit)],
            [
                ("plain", 0, 0, 0, hidden),
                ("plain", 1, 0, hidden, hidden),
                ("turned", 2, 0, 2 * hidden, early),
            ],
            (2 * hidden + early) // unit,
            2,
            (3, 2),
        )
        grad_normed_two, mlp_out = sums[:, :width], sums[:, width:]
    else:
        grad_normed_two = line_sum([(grad_gate_low, w_gate, "nt"), (grad_up_low, w_up, "nt")], 2)
        grad_gate = scatter_sum(normed_two, grad_gate_low)
        grad_up = scatter_sum(normed_two, grad_up_low)
        mlp_out = lax.psum(dot_nn(active, w_down).astype(BF16), "mp")
    output = (middle + mlp_out.astype(F32)).astype(BF16)
    grad_normed_two = grad_normed_two.astype(F32)
    scaled_two = grad_normed_two * mlp_gain
    grad_middle = (
        cotangent.astype(F32)
        + scale_two * scaled_two
        - middle
        * (scale_two * scale_two * scale_two)
        * jnp.mean(middle * scaled_two, axis=-1, keepdims=True)
    )
    grad_mlp_gain = jnp.sum(grad_normed_two * middle * scale_two, axis=0)
    grad_branch = grad_middle.astype(BF16)
    grad_mixed = dot_nt(grad_branch, w_output).astype(BF16)
    grad_query_pre, dfar, dnear, down = attend_back(
        queries, far, near, own, key_segment, row_segment, mixed, grad_mixed, logs, cos, sin
    )
    from_near = lax.ppermute(dnear, "seq", [(s + 1, s) for s in range(seq_count - 1)])
    from_far = lax.ppermute(dfar, "seq", [(s + 2, s) for s in range(seq_count - 2)])
    grad_pair = down + from_near.astype(F32) + from_far.astype(F32)
    grad_keys = jnp.concatenate([grad_pair[:, :HS], grad_pair[:, PAIR : PAIR + HS]], axis=1)
    grad_values = jnp.concatenate([grad_pair[:, HS:PAIR], grad_pair[:, PAIR + HS :]], axis=1)
    quarter = HS // 2
    swapped = jnp.concatenate(
        [grad_keys[:, (at ^ 1) * quarter : ((at ^ 1) + 1) * quarter] for at in range(4)], axis=1
    )
    grad_key_pre = (grad_keys * cos - swapped * sin).astype(BF16)
    grad_value_pre = grad_values.astype(BF16)

    query_width = grad_query_pre.shape[1]
    if fused:
        late, mixed_width = hidden - early, mixed.shape[1]
        query_at = late + mixed_width
        key_at = query_at + query_width
        grad_normed, grad_down_two, grad_output, grad_query, grad_key, grad_value = exchange(
            [cotangent, grad_branch, normed],
            [
                (active, early, late),
                (mixed, 0, mixed_width),
                (grad_query_pre, 0, query_width),
                (grad_key_pre, 0, PAIR),
                (grad_value_pre, 0, PAIR),
            ],
            [
                [
                    (w_query, query_at, query_width, "nt"),
                    (w_key, key_at, PAIR, "nt"),
                    (w_value, key_at + PAIR, PAIR, "nt"),
                ]
            ],
            (0, late // unit, query_at // unit),
            [(late, unit), (mixed_width, unit), (unit, query_width), (unit, PAIR), (unit, PAIR)],
            [
                ("turned", 0, 0, 0, late),
                ("turned", 1, 0, late, mixed_width),
                ("plain", 2, 0, query_at, query_width),
                ("plain", 3, 0, key_at, PAIR),
                ("plain", 4, 0, key_at + PAIR, PAIR),
            ],
            (key_at + 2 * PAIR) // unit,
            3,
            (2, 1),
        )
        grad_down = jnp.concatenate([grad_down_one, grad_down_two], axis=0)
    else:
        grad_down = scatter_sum(cotangent, active).T
        grad_output = scatter_sum(grad_branch, mixed).T
        grad_qkv = scatter_sum(normed, jnp.concatenate([grad_query_pre, grad_key_pre, grad_value_pre], axis=1))
        grad_query = grad_qkv[:, :query_width]
        grad_key = grad_qkv[:, query_width : query_width + PAIR]
        grad_value = grad_qkv[:, query_width + PAIR :]
        grad_normed = line_sum(
            [(grad_query_pre, w_query, "nt"), (grad_key_pre, w_key, "nt"), (grad_value_pre, w_value, "nt")], 3
        )
    grad_tokens, gains = final(
        grad_normed, tokens, grad_middle, attn_gain[None, :], grad_mlp_gain[None, :], 4
    )
    return (
        output,
        grad_tokens,
        gains[0],
        grad_query,
        grad_key,
        grad_value,
        grad_output,
        gains[1],
        grad_gate,
        grad_up,
        grad_down,
    )


def solution(mesh):
    tokens_spec = P(("batch", "seq"), None)
    in_specs = (
        tokens_spec,
        P("batch", None),
        P(),
        P(None, "mp"),
        P(None, "mp"),
        P(None, "mp"),
        P("mp", None),
        P(),
        P(None, "mp"),
        P(None, "mp"),
        P("mp", None),
        tokens_spec,
    )
    row_split = P(("batch", "seq"), "mp")
    column_split = P("mp", ("batch", "seq"))
    out_specs = (
        tokens_spec,
        tokens_spec,
        P(("batch", "seq")),
        row_split,
        row_split,
        row_split,
        column_split,
        P(("batch", "seq")),
        row_split,
        row_split,
        column_split,
    )
    return jax.shard_map(local, mesh=mesh, in_specs=in_specs, out_specs=out_specs, check_vma=False)
```

```python
import functools
import math

import jax
import jax.numpy as jnp
from jax import lax
from jax.experimental import pallas as pl
from jax.experimental.pallas import tpu as pltpu
from jax.sharding import PartitionSpec as P

HS = 64
PAIR = 2 * HS
LONGEST = 1024
rope_base = 500000.0
epsilon = 1e-05
masked_score = -1e30
MESH = pl.DeviceIdType.MESH
F32 = jnp.float32
BF16 = jnp.bfloat16


def dot_nn(left, right):
    return lax.dot_general(left, right, (((1,), (0,)), ((), ())), preferred_element_type=F32)


def dot_nt(left, right):
    return lax.dot_general(left, right, (((1,), (1,)), ((), ())), preferred_element_type=F32)


def dot_tn(left, right):
    return lax.dot_general(left, right, (((0,), (0,)), ((), ())), preferred_element_type=F32)


def lanes_of(values):
    return lax.broadcasted_iota(jnp.int32, values.shape, 1)


def swap_halves(values):
    ahead = pltpu.roll(values, PAIR - HS // 2, 1)
    behind = pltpu.roll(values, HS // 2, 1)
    return jnp.where(lanes_of(values) % HS < HS // 2, ahead, behind)


def rope_tables(segments, first_row, rows):
    row_segment = lax.dynamic_slice_in_dim(segments, first_row, rows, 0)
    doc_start = jnp.sum((segments[None, :] < row_segment[:, None]).astype(jnp.int32), axis=1)
    place = (first_row + jnp.arange(rows, dtype=jnp.int32) - doc_start).astype(F32)
    lane = jnp.arange(PAIR, dtype=jnp.int32)
    frequency = jnp.exp((lane % (HS // 2)).astype(F32) * (-2.0 * math.log(rope_base) / HS))
    angles = place[:, None] * frequency[None, :]
    sign = jnp.where(lane % HS < HS // 2, -1.0, 1.0)
    return jnp.cos(angles), jnp.sin(angles) * sign[None, :]


def project_kernel(x_ref, gain_ref, wq_ref, wk_ref, wv_ref, cos_ref, sin_ref, n_ref, q_ref, kv_ref):
    wide = x_ref[...].astype(F32)
    scale = lax.rsqrt(jnp.mean(wide * wide, axis=-1, keepdims=True) + epsilon)
    normed = (wide * scale * gain_ref[...]).astype(BF16)
    n_ref[...] = normed
    cos, sin = cos_ref[...], sin_ref[...]
    queries = dot_nn(normed, wq_ref[...])
    for start in range(0, queries.shape[1], PAIR):
        part = queries[:, start : start + PAIR]
        q_ref[:, start : start + PAIR] = (part * cos + swap_halves(part) * sin).astype(BF16)
    keys = dot_nn(normed, wk_ref[...])
    keys = keys * cos + swap_halves(keys) * sin
    values = dot_nn(normed, wv_ref[...])
    low_half = lanes_of(keys) < HS
    kv_ref[:, :PAIR] = jnp.where(low_half, keys, pltpu.roll(values, HS, 1)).astype(BF16)
    kv_ref[:, PAIR:] = jnp.where(low_half, pltpu.roll(keys, HS, 1), values).astype(BF16)


def project(tokens, gain, w_query, w_key, w_value, cos, sin):
    rows, width = tokens.shape
    block = rows // 2
    full = lambda array: pl.BlockSpec(array.shape, lambda i: (0, 0))
    tile = lambda columns: pl.BlockSpec((block, columns), lambda i: (i, 0))
    return pl.pallas_call(
        project_kernel,
        grid=(rows // block,),
        in_specs=[
            tile(width),
            full(gain),
            full(w_query),
            full(w_key),
            full(w_value),
            tile(PAIR),
            tile(PAIR),
        ],
        out_specs=[tile(width), tile(w_query.shape[1]), tile(2 * PAIR)],
        out_shape=[
            jax.ShapeDtypeStruct((rows, width), BF16),
            jax.ShapeDtypeStruct((rows, w_query.shape[1]), BF16),
            jax.ShapeDtypeStruct((rows, 2 * PAIR), BF16),
        ],
        cost_estimate=pl.CostEstimate(
            flops=2 * rows * width * (w_query.shape[1] + 2 * PAIR),
            bytes_accessed=8 << 20,
            transcendentals=0,
        ),
        name="project",
    )(tokens, gain, w_query, w_key, w_value, cos, sin)


def write_bias(bias_ref, key_ref, row_ref):
    keys, rows = bias_ref.shape
    key_place = lax.broadcasted_iota(jnp.int32, (keys, rows), 0) - (keys - rows)
    row_place = lax.broadcasted_iota(jnp.int32, (keys, rows), 1)
    allowed = (key_ref[...] == row_ref[...]) & (key_place <= row_place)
    bias_ref[...] = jnp.where(allowed, 0.0, masked_score)


def attend_kernel(q_ref, far_ref, near_ref, own_ref, key_ref, row_ref, out_ref, log_ref, bias_ref, kv_ref):
    @pl.when(pl.program_id(0) == 0)
    def _():
        write_bias(bias_ref, key_ref, row_ref)

    rows = q_ref.shape[0]
    for at, ref in enumerate((far_ref, near_ref, own_ref)):
        kv_ref[at * rows : (at + 1) * rows, :] = ref[...]
    key_value = kv_ref[...]
    flipped = key_value.T
    q_flipped = (q_ref[...].astype(F32) * HS ** (-0.5)).astype(BF16).T
    outs = []
    for head in range(2):
        scores = dot_nn(key_value[:, :HS], q_flipped[head * HS : (head + 1) * HS, :]) + bias_ref[...]
        top = jnp.max(scores, axis=0, keepdims=True)
        powers = jnp.exp(scores - top)
        total = jnp.sum(powers, axis=0, keepdims=True)
        mixed = dot_nn(flipped[HS:, :], powers.astype(BF16))
        outs.append(mixed / total)
        log_ref[0, head : head + 1, :] = top + jnp.log(total)
    out_ref[...] = jnp.concatenate(outs, axis=0).T.astype(BF16)


def attend(queries, far, near, own, key_segment, row_segment):
    rows, width = queries.shape
    pairs = width // PAIR
    per_group = pairs // 2
    pair_tile = pl.BlockSpec((rows, PAIR), lambda p: (0, p))
    kv_tile = pl.BlockSpec((rows, PAIR), lambda p: (0, p // per_group))
    return pl.pallas_call(
        attend_kernel,
        grid=(pairs,),
        in_specs=[
            pair_tile,
            kv_tile,
            kv_tile,
            kv_tile,
            pl.BlockSpec(key_segment.shape, lambda p: (0, 0)),
            pl.BlockSpec(row_segment.shape, lambda p: (0, 0)),
        ],
        out_specs=[pair_tile, pl.BlockSpec((1, 2, rows), lambda p: (p, 0, 0))],
        out_shape=[
            jax.ShapeDtypeStruct((rows, width), BF16),
            jax.ShapeDtypeStruct((pairs, 2, rows), F32),
        ],
        scratch_shapes=[pltpu.VMEM((3 * rows, rows), F32), pltpu.VMEM((3 * rows, PAIR), BF16)],
        cost_estimate=pl.CostEstimate(
            flops=16 << 30, bytes_accessed=4 << 20, transcendentals=3 * rows * rows * 2 * pairs
        ),
        name="attend",
    )(queries, far, near, own, key_segment, row_segment)


def attend_back_kernel(
    q_ref, far_ref, near_ref, own_ref, key_ref, row_ref, out_ref, grad_ref, log_ref, cos_ref, sin_ref,
    dq_ref, dfar_ref, dnear_ref, down_ref, bias_ref, kv_ref, dkv_ref, per_group,
):
    step = pl.program_id(0)

    @pl.when(step == 0)
    def _():
        write_bias(bias_ref, key_ref, row_ref)

    rows = q_ref.shape[0]
    for at, ref in enumerate((far_ref, near_ref, own_ref)):
        kv_ref[at * rows : (at + 1) * rows, :] = ref[...]
    key_value = kv_ref[...]
    flipped = key_value[:, :].T
    scaled = (q_ref[...].astype(F32) * HS ** (-0.5)).astype(BF16)
    q_flipped = scaled.T
    grad = grad_ref[...]
    grad_flipped = grad.T
    product = (out_ref[...].astype(F32) * grad.astype(F32)).T
    dqs, dkey, dvalue = [], None, None
    for head in range(2):
        here = slice(head * HS, (head + 1) * HS)
        scores = dot_nn(key_value[:, :HS], q_flipped[here, :]) + bias_ref[...]
        shares = jnp.exp(scores - log_ref[0, head : head + 1, :])
        grad_shares = dot_nn(key_value[:, HS:], grad_flipped[here, :])
        delta = jnp.sum(product[here, :], axis=0, keepdims=True)
        grad_scores = (shares * (grad_shares - delta)).astype(BF16)
        value_part = dot_nn(shares.astype(BF16), grad[:, here])
        key_part = dot_nn(grad_scores, scaled[:, here])
        dvalue = value_part if dvalue is None else dvalue + value_part
        dkey = key_part if dkey is None else dkey + key_part
        dqs.append(dot_nn(flipped[:HS, :], grad_scores))
    dq = jnp.concatenate(dqs, axis=0).T * HS ** (-0.5)
    dq_ref[...] = (dq * cos_ref[...] - swap_halves(dq) * sin_ref[...]).astype(BF16)
    both = jnp.concatenate([dkey, dvalue], axis=1)

    @pl.when(step % per_group == 0)
    def _():
        dkv_ref[...] = both

    @pl.when(step % per_group != 0)
    def _():
        dkv_ref[...] += both

    @pl.when(step % per_group == per_group - 1)
    def _():
        dfar_ref[...] = dkv_ref[:rows, :].astype(BF16)
        dnear_ref[...] = dkv_ref[rows : 2 * rows, :].astype(BF16)
        down_ref[...] = dkv_ref[2 * rows :, :]


def attend_back(queries, far, near, own, key_segment, row_segment, mixed, grad, logs, cos, sin):
    rows, width = queries.shape
    pairs = width // PAIR
    per_group = pairs // 2
    pair_tile = pl.BlockSpec((rows, PAIR), lambda p: (0, p))
    kv_tile = pl.BlockSpec((rows, PAIR), lambda p: (0, p // per_group))
    full = lambda array: pl.BlockSpec(array.shape, lambda p: (0, 0))
    return pl.pallas_call(
        functools.partial(attend_back_kernel, per_group=per_group),
        grid=(pairs,),
        in_specs=[
            pair_tile,
            kv_tile,
            kv_tile,
            kv_tile,
            full(key_segment),
            full(row_segment),
            pair_tile,
            pair_tile,
            pl.BlockSpec((1, 2, rows), lambda p: (p, 0, 0)),
            full(cos),
            full(sin),
        ],
        out_specs=[pair_tile, kv_tile, kv_tile, kv_tile],
        out_shape=[
            jax.ShapeDtypeStruct((rows, width), BF16),
            jax.ShapeDtypeStruct((rows, 2 * PAIR), BF16),
            jax.ShapeDtypeStruct((rows, 2 * PAIR), BF16),
            jax.ShapeDtypeStruct((rows, 2 * PAIR), F32),
        ],
        scratch_shapes=[
            pltpu.VMEM((3 * rows, rows), F32),
            pltpu.VMEM((3 * rows, PAIR), BF16),
            pltpu.VMEM((3 * rows, PAIR), F32),
        ],
        cost_estimate=pl.CostEstimate(
            flops=40 << 30, bytes_accessed=6 << 20, transcendentals=3 * rows * rows * 2 * pairs
        ),
        name="attend_back",
    )(queries, far, near, own, key_segment, row_segment, mixed, grad, logs, cos, sin)


def line_sum_kernel(modes, chunks, *refs):
    count = len(modes)
    a_refs, w_refs, out_ref = refs[:count], refs[count : 2 * count], refs[2 * count]
    rest = refs[2 * count + 1 :]
    w_bufs = rest[:count]
    part, first, second, total, w_sem, send_sem, recv_sem = rest[count:]
    width = part.shape[2]
    place = lax.axis_index("mp")
    pair = place + 1 - 2 * lax.rem(place, 2)
    across = 3 - place
    is_mid = (place == 1) | (place == 2)
    is_end = (place == 0) | (place == 3)

    def weight(at, c):
        if modes[at] == "nt":
            source = w_refs[at].at[pl.ds(pl.multiple_of(c * width, width), width), :]
        else:
            source = w_refs[at].at[:, pl.ds(pl.multiple_of(c * width, width), width)]
        return pltpu.make_async_copy(source, w_bufs[at].at[c], w_sem.at[at, c])

    def remote(kind, source, target, c, device):
        return pltpu.make_async_remote_copy(
            src_ref=source.at[c],
            dst_ref=target.at[c],
            send_sem=send_sem.at[kind, c],
            recv_sem=recv_sem.at[kind, c],
            device_id={"mp": device},
            device_id_type=MESH,
        )

    def up(c):
        return remote(0, part, first, c, pair)

    def over(c):
        return remote(1, part, second, c, across)

    def down(c):
        return remote(2, total, total, c, pair)

    def start_weights(c, carry):
        for at in range(count):
            weight(at, c).start()
        return carry

    lax.fori_loop(0, chunks, start_weights, 0)
    barrier = pltpu.get_barrier_semaphore()
    pl.semaphore_signal(barrier, inc=1, device_id={"mp": pair}, device_id_type=MESH)

    @pl.when(is_mid)
    def _():
        pl.semaphore_signal(barrier, inc=1, device_id={"mp": across}, device_id_type=MESH)
        pl.semaphore_wait(barrier, 2)

    @pl.when(is_end)
    def _():
        pl.semaphore_wait(barrier, 1)

    def step(t, carry):
        @pl.when(t < chunks)
        def _():
            value = None
            for at in range(count):
                weight(at, t).wait()
                dot = dot_nt if modes[at] == "nt" else dot_nn
                term = dot(a_refs[at][...], w_bufs[at][t])
                value = term if value is None else value + term
            part[t] = value.astype(BF16)

            @pl.when(is_end)
            def _():
                up(t).start()

        @pl.when(is_mid & (t >= 1) & (t < chunks + 1))
        def _():
            c = t - 1
            up(c).wait_recv()
            part[c] = (part[c].astype(F32) + first[c].astype(F32)).astype(BF16)
            over(c).start()

        @pl.when(is_mid & (t >= OVER_LAG))
        def _():
            c = t - OVER_LAG
            over(c).wait_recv()
            total[c] = (part[c].astype(F32) + second[c].astype(F32)).astype(BF16)
            down(c).start()

        return carry

    lax.fori_loop(0, chunks + OVER_LAG, step, 0)

    def finish(c, carry):
        @pl.when(is_end)
        def _():
            up(c).wait_send()
            down(c).wait_recv()

        @pl.when(is_mid)
        def _():
            over(c).wait_send()
            down(c).wait_send()

        out_ref[:, pl.ds(pl.multiple_of(c * width, width), width)] = total[c]
        return carry

    lax.fori_loop(0, chunks, finish, 0)


def line_sum(pairs, call_id, chunks=16):
    lefts = [left for left, _, _ in pairs]
    rights = [right for _, right, _ in pairs]
    modes = tuple(mode for _, _, mode in pairs)
    rows = lefts[0].shape[0]
    columns = rights[0].shape[0] if modes[0] == "nt" else rights[0].shape[1]
    width = columns // chunks
    count = len(pairs)
    bufs = [
        pltpu.VMEM((chunks, width, left.shape[1]) if mode == "nt" else (chunks, left.shape[1], width), BF16)
        for left, _, mode in pairs
    ]
    flops = sum(2 * rows * columns * left.shape[1] for left in lefts)
    moved = sum(right.size * 2 for right in rights)
    block = pltpu.VMEM((chunks, rows, width), BF16)
    return pl.pallas_call(
        functools.partial(line_sum_kernel, modes, chunks),
        out_shape=jax.ShapeDtypeStruct((rows, columns), BF16),
        in_specs=[pl.BlockSpec(memory_space=pltpu.VMEM)] * count
        + [pl.BlockSpec(memory_space=pl.ANY)] * count,
        out_specs=pl.BlockSpec(memory_space=pltpu.VMEM),
        scratch_shapes=bufs
        + [
            block,
            block,
            block,
            block,
            pltpu.SemaphoreType.DMA((count, chunks)),
            pltpu.SemaphoreType.DMA((3, chunks)),
            pltpu.SemaphoreType.DMA((3, chunks)),
        ],
        compiler_params=pltpu.CompilerParams(collective_id=call_id, has_side_effects=True),
        cost_estimate=pl.CostEstimate(
            flops=flops + (40 << 30), bytes_accessed=moved, transcendentals=0
        ),
        name=f"line_sum_{call_id}",
    )(*lefts, *rights)

LAG = 3
UP_LAG = 1
OVER_LAG = 3
DOWN_LAG = 6
TILES = 8


def exchange_kernel(plan, *refs):
    left_count, rights, sums, flips_before, spans, out_count, units, chunks, period, active, ending, given, made = plan
    refs = list(refs)

    def take(n):
        got = refs[:n]
        del refs[:n]
        return got

    weights = [item for group in sums for item in group]
    left_refs, right_refs, w_refs = take(left_count), take(len(rights)), take(len(weights))
    given_refs = take(given)
    grad_refs, made_refs = take(out_count), take(made)
    stage, flip, right_all, out_ref = take(4)
    w_bufs = take(len(weights))
    part, first, second, away, come_one, come_two, come_three, result = take(8)
    given_bufs, made_bufs = take(given), take(made - (ending == "branch"))
    acc, gain_parts, gain_come, given_sem, made_sem, gain_send, gain_recv = take(7)
    in_sem, right_sem, w_sem, ar_send, ar_recv, core_send, core_recv, two_send, two_recv, three_send, three_recv, out_sem = refs
    width = part.shape[2]
    block = come_three.shape[1]
    all_chunks = chunks * len(sums)
    place = lax.axis_index("mp")
    seq, batch = lax.axis_index("seq"), lax.axis_index("batch")
    core, chip = lax.rem(seq, 2), lax.div(seq, 2)
    sibling = seq + 1 - 2 * core
    beside = seq + 2 - 4 * chip
    pair = place + 1 - 2 * lax.rem(place, 2)
    across = 3 - place
    is_mid = (place == 1) | (place == 2)
    is_end = (place == 0) | (place == 3)

    def columns_of(c):
        return pl.ds(pl.multiple_of(c * width, width), width)

    def weight(at, group, c):
        here = columns_of(c - group * chunks)
        source = w_refs[at].at[here, :] if weights[at][2] == "nt" else w_refs[at].at[:, here]
        slot = lax.rem(c, 3)
        return pltpu.make_async_copy(source, w_bufs[at].at[slot], w_sem.at[at, slot])

    members = []
    for group, items in enumerate(sums):
        for _ in items:
            members.append(group)

    def load_weights(c):
        for group in range(len(sums)):

            @pl.when((c >= group * chunks) & (c < (group + 1) * chunks))
            def _():
                for at in range(len(weights)):
                    if members[at] == group:
                        weight(at, group, c).start()

    def remote(source, target, send, recv, device):
        return pltpu.make_async_remote_copy(
            src_ref=source, dst_ref=target, send_sem=send, recv_sem=recv, device_id=device, device_id_type=MESH
        )

    def slot_of(c):
        return lax.rem(c, chunks)

    def up(c):
        slot = slot_of(c)
        return remote(part.at[slot], first.at[slot], ar_send.at[0, c], ar_recv.at[0, c], {"mp": pair})

    def over(c):
        slot = slot_of(c)
        return remote(part.at[slot], second.at[slot], ar_send.at[1, c], ar_recv.at[1, c], {"mp": across})

    def down(c):
        here = out_ref.at[:, columns_of(c)]
        return remote(here, here, ar_send.at[2, c], ar_recv.at[2, c], {"mp": pair})

    def to_core(u):
        return remote(away.at[lax.rem(u, 2)], come_one.at[u], core_send.at[u], core_recv.at[u], {"seq": sibling})

    def chip_first(u):
        return 1 - lax.rem(u, 2)

    def sent_at(u, k):
        x_first = chip_first(u)
        return x_first * (2 * k + 1 - chip) + (1 - x_first) * (2 * (1 - batch) + k)

    def kept_at(u, k):
        x_first = chip_first(u)
        return x_first * (2 * k + chip) + (1 - x_first) * (2 * batch + k)

    def own_at(u):
        x_first = chip_first(u)
        return x_first * batch + (1 - x_first) * chip

    def device_of(x_way):
        return {
            "seq": x_way * beside + (1 - x_way) * seq,
            "batch": x_way * batch + (1 - x_way) * (1 - batch),
        }

    def second_hop(u, k):
        return remote(
            come_one.at[u, sent_at(u, k)], come_two.at[u, k], two_send.at[k, u], two_recv.at[k, u], device_of(chip_first(u))
        )

    def third_hop(u):
        return remote(
            come_two.at[u, 1 - own_at(u)], come_three.at[u], three_send.at[u], three_recv.at[u], device_of(1 - chip_first(u))
        )

    def left_copy(at):
        return pltpu.make_async_copy(left_refs[at], stage, in_sem.at[at])

    def right_copy(at):
        offset, source, size = rights[at]
        return pltpu.make_async_copy(
            right_refs[at].at[:, source : source + size], right_all.at[:, offset : offset + size], right_sem.at[at]
        )

    def out_copy(at, u):
        kind, index, offset, start, size = spans[at]
        slot = lax.rem(u, 2)
        if size < block:
            source = result.at[slot, :, start % block : start % block + size]
            target = grad_refs[index].at[:, offset : offset + size]
        else:
            source = result.at[slot]
            here = pl.ds(pl.multiple_of((u - start // block) * block + offset, block), block)
            target = grad_refs[index].at[here, :] if kind == "turned" else grad_refs[index].at[:, here]
        return pltpu.make_async_copy(source, target, out_sem.at[at, slot])

    def units_of(at):
        _, _, _, start, size = spans[at]
        return start // block, max((start + size) // block, start // block + 1)

    seq_count = lax.axis_size("seq")
    peers = lax.axis_size("batch") * seq_count
    me = batch * seq_count + seq

    def peer(k):
        there = lax.rem(me + k, peers)
        return there, {"batch": lax.div(there, seq_count), "seq": lax.rem(there, seq_count)}

    def gain_copy(k):
        there, device = peer(k)
        return remote(gain_parts.at[there], gain_come.at[k], gain_send.at[k], gain_recv.at[k], device)

    def given_copy(at):
        return pltpu.make_async_copy(given_refs[at], given_bufs[at], given_sem.at[at])

    def made_copy(at):
        source = out_ref.at[:, columns // 2 :] if ending == "branch" and at == made - 1 else made_bufs[at]
        return pltpu.make_async_copy(source, made_refs[at], made_sem.at[at])

    columns = out_ref.shape[1]
    rows = out_ref.shape[0]
    tile = rows // TILES

    def tile_of(i):
        return pl.ds(pl.multiple_of(i * tile, tile), tile)

    def branch_rows(i):
        here = tile_of(i)
        gm_buf, gb_buf, _ = made_bufs[:3]
        x_buf, b_buf, gain_buf, _ = given_bufs
        grad = out_ref[here, : columns // 2].astype(F32)
        middle = x_buf[here, :].astype(F32) + b_buf[here, :].astype(F32)
        scale = lax.rsqrt(jnp.mean(middle * middle, axis=-1, keepdims=True) + epsilon)
        scaled = grad * gain_buf[...]
        mean = jnp.mean(middle * scaled, axis=-1, keepdims=True)
        value = stage[here, :].astype(F32) + scale * scaled - middle * (scale * scale * scale) * mean
        gm_buf[here, :] = value
        gb_buf[here, :] = value.astype(BF16)
        acc[...] += jnp.sum(grad * middle * scale, axis=0, keepdims=True)

    def branch_end():
        made_bufs[2][...] = dot_nt(made_bufs[1][...], given_bufs[3][...]).astype(BF16)
        made_bufs[3][...] = acc[...]
        for at in range(4):
            made_copy(at).start()

    def token_rows(i, carry):
        here = tile_of(i)
        x_buf, gm_buf, gain_buf, _ = given_bufs
        wide = x_buf[here, :].astype(F32)
        grad = out_ref[here, :].astype(F32)
        scale = lax.rsqrt(jnp.mean(wide * wide, axis=-1, keepdims=True) + epsilon)
        scaled = grad * gain_buf[...]
        mean = jnp.mean(wide * scaled, axis=-1, keepdims=True)
        value = gm_buf[here, :] + scale * scaled - wide * (scale * scale * scale) * mean
        made_bufs[0][here, :] = value.astype(BF16)
        acc[...] += jnp.sum(grad * wide * scale, axis=0, keepdims=True)
        return carry

    acc[...] = jnp.zeros_like(acc)
    load_weights(0)
    load_weights(1)
    for at in range(len(rights)):
        right_copy(at).start()
    left_copy(0).start()
    for at in range(given):
        given_copy(at).start()

    barrier = pltpu.get_barrier_semaphore()
    if ending == "tokens":
        greeted = [{"mp": pair}] + [peer(k)[1] for k in range(1, peers)]
    else:
        greeted = [{"mp": pair}, {"seq": sibling}, {"seq": beside}, {"batch": 1 - batch}]
    for device in greeted:
        pl.semaphore_signal(barrier, inc=1, device_id=device, device_id_type=MESH)

    @pl.when(is_mid)
    def _():
        pl.semaphore_signal(barrier, inc=1, device_id={"mp": across}, device_id_type=MESH)
        pl.semaphore_wait(barrier, len(greeted) + 1)

    @pl.when(is_end)
    def _():
        pl.semaphore_wait(barrier, len(greeted))

    for at in range(len(rights)):
        right_copy(at).wait()

    def left_of(u):
        index = 0
        for at in range(1, left_count):
            index = index + (u >= flips_before[at]).astype(jnp.int32)
        return index

    def product(u, at, side):
        row = pl.multiple_of((2 * at + side) * block, block)
        column = pl.multiple_of(u * block, block)
        return dot_nn(flip[left_of(u), pl.ds(row, block), :], right_all[:, pl.ds(column, block)])

    def step_of(u):
        return (u // active) * period + u % active

    def on_unit(t, body):
        u = lax.div(t, period) * active + lax.rem(t, period)

        @pl.when((t >= 0) & (lax.rem(t, period) < active) & (u < units))
        def _():
            body(u)

    def first_stage(u):
        @pl.when(u >= 2)
        def _():
            to_core(u - 2).wait_send()

        for at in range(4):
            away[lax.rem(u, 2), at] = product(u, at, 1 - core).astype(BF16)
        to_core(u).start()

    def second_stage(u):
        to_core(u).wait_recv()
        for at in range(4):
            come_one[u, at] = (product(u, at, core) + come_one[u, at].astype(F32)).astype(BF16)
        for k in range(2):
            second_hop(u, k).start()

    def third_stage(u):
        for k in range(2):
            second_hop(u, k).wait_recv()
        sent = 1 - own_at(u)
        come_two[u, sent] = (come_two[u, sent].astype(F32) + come_one[u, kept_at(u, sent)].astype(F32)).astype(BF16)
        third_hop(u).start()

    def last_stage(u):
        third_hop(u).wait_recv()
        own = own_at(u)
        value = come_three[u].astype(F32) + come_two[u, own].astype(F32) + come_one[u, kept_at(u, own)].astype(F32)
        for at in range(len(spans)):
            low, high = units_of(at)

            @pl.when((u - 2 >= low) & (u - 2 < high))
            def _():
                out_copy(at, u - 2).wait()

        for kind in ("turned", "plain"):
            mine = [units_of(at) for at in range(len(spans)) if spans[at][0] == kind]
            if mine:
                low, high = min(m[0] for m in mine), max(m[1] for m in mine)

                @pl.when((u >= low) & (u < high))
                def _():
                    result[lax.rem(u, 2)] = value.T if kind == "turned" else value

        for at in range(len(spans)):
            low, high = units_of(at)

            @pl.when((u >= low) & (u < high))
            def _():
                out_copy(at, u).start()

    def step(t, carry):
        @pl.when((t >= chunks) & (t < all_chunks))
        def _():
            @pl.when(is_end)
            def _():
                up(t - chunks).wait_send()

            @pl.when(is_mid)
            def _():
                over(t - chunks).wait_send()

        for group, items in enumerate(sums):

            @pl.when((t >= group * chunks) & (t < (group + 1) * chunks))
            def _():
                value = None
                for at, (start, size, mode) in enumerate(weights):
                    if members[at] == group:
                        weight(at, group, t).wait()
                        dot = dot_nt if mode == "nt" else dot_nn
                        term = dot(right_all[:, start : start + size], w_bufs[at][lax.rem(t, 3)])
                        value = term if value is None else value + term
                part[slot_of(t)] = value.astype(BF16)

        @pl.when(t < all_chunks)
        def _():
            @pl.when(is_end)
            def _():
                up(t).start()

            load_weights(t + 2)

        @pl.when(is_mid & (t >= UP_LAG) & (t < all_chunks + UP_LAG))
        def _():
            c = t - UP_LAG
            up(c).wait_recv()
            slot = slot_of(c)
            part[slot] = (part[slot].astype(F32) + first[slot].astype(F32)).astype(BF16)
            over(c).start()

        @pl.when(is_mid & (t >= OVER_LAG) & (t < all_chunks + OVER_LAG))
        def _():
            c = t - OVER_LAG
            over(c).wait_recv()
            slot = slot_of(c)
            out_ref[:, columns_of(c)] = (part[slot].astype(F32) + second[slot].astype(F32)).astype(BF16)
            down(c).start()

        @pl.when(is_end & (t >= DOWN_LAG) & (t < all_chunks + DOWN_LAG))
        def _():
            down(t - DOWN_LAG).wait_recv()

        for at in range(left_count):

            @pl.when(t == max(step_of(flips_before[at]) - 2, at))
            def _():
                left_copy(at).wait()

                def turn(k, carry):
                    here = pl.ds(pl.multiple_of(k * block, block), block)
                    flip[at, here, :] = stage[:, here].T
                    return carry

                lax.fori_loop(0, flip.shape[1] // block, turn, 0)
                if at + 1 < left_count:
                    left_copy(at + 1).start()

        on_unit(t, first_stage)
        on_unit(t - 1, second_stage)
        on_unit(t - 1 - LAG, third_stage)
        on_unit(t - 1 - 2 * LAG, last_stage)
        if ending == "branch":

            @pl.when(t == chunks + DOWN_LAG)
            def _():
                for at in range(given):
                    given_copy(at).wait()

            @pl.when((t >= chunks + DOWN_LAG) & (t < chunks + DOWN_LAG + TILES))
            def _():
                branch_rows(t - chunks - DOWN_LAG)

            @pl.when(t == chunks + DOWN_LAG + TILES)
            def _():
                branch_end()

        return carry

    lax.fori_loop(0, max(step_of(units - 1) + 2 + 2 * LAG, all_chunks + DOWN_LAG), step, 0)
    if ending == "branch":
        made_copy(made - 1).start()
    else:
        for at in range(given):
            given_copy(at).wait()
        lax.fori_loop(0, TILES, token_rows, 0)
        made_copy(0).start()
        part_width = columns // peers
        for k in range(peers):
            here = slice(k * part_width, (k + 1) * part_width)
            gain_parts[k, 0:1, :] = acc[:, here]
            gain_parts[k, 1:2, :] = given_bufs[3][:, here]
        for k in range(1, peers):
            gain_copy(k).start()

    def finish(c, carry):
        @pl.when(is_mid)
        def _():
            down(c).wait_send()

        return carry

    lax.fori_loop(0, all_chunks, finish, 0)

    def finish_last(c, carry):
        @pl.when(is_end)
        def _():
            up(c).wait_send()

        @pl.when(is_mid)
        def _():
            over(c).wait_send()

        return carry

    lax.fori_loop(all_chunks - chunks, all_chunks, finish_last, 0)

    def settle(u, carry):
        for k in range(2):
            second_hop(u, k).wait_send()
        third_hop(u).wait_send()
        return carry

    lax.fori_loop(0, units, settle, 0)
    for u in (units - 2, units - 1):
        to_core(u).wait_send()
        for at in range(len(spans)):
            low, high = units_of(at)
            if low <= u < high:
                out_copy(at, u).wait()
    if ending == "tokens":
        gains = gain_parts[me]
        for k in range(1, peers):
            gain_copy(k).wait_recv()
            gains = gains + gain_come[k]
        made_bufs[1][...] = gains
        made_copy(1).start()
        for k in range(1, peers):
            gain_copy(k).wait_send()
    for at in range(made):
        made_copy(at).wait()


def exchange(lefts, rights, sums, flips_before, outs, spans, units, call_id, pace, ending, given, made, chunks=16):
    rows, depth = lefts[0].shape
    block = depth // 8
    placed, at = [], 0
    for _, source, size in rights:
        placed.append((at, source, size))
        at += size
    weights = [item[0] for group in sums for item in group]
    columns = weights[0].shape[0] if sums[0][0][3] == "nt" else weights[0].shape[1]
    width = columns // chunks
    sum_plan = [[item[1:] for item in group] for group in sums]
    plan = (len(lefts), placed, sum_plan, flips_before, spans, len(outs), units, chunks, *pace, ending, len(given), len(made))
    any_space = pl.BlockSpec(memory_space=pl.ANY)
    line_block = pltpu.VMEM((chunks, rows, width), BF16)
    peers = lax.axis_size("batch") * lax.axis_size("seq")
    kept = made[:-1] if ending == "branch" else made
    dma = pltpu.SemaphoreType.DMA
    all_chunks = chunks * len(sums)
    flops = sum(2 * rows * columns * size for group in sum_plan for _, size, _ in group) + 2 * rows * depth * at
    return pl.pallas_call(
        functools.partial(exchange_kernel, plan),
        out_shape=[jax.ShapeDtypeStruct(shape, F32) for shape in outs]
        + [jax.ShapeDtypeStruct(shape, kind) for shape, kind in made],
        in_specs=[any_space] * (len(lefts) + len(rights) + len(weights) + len(given)),
        out_specs=[any_space] * (len(outs) + len(made)),
        scratch_shapes=[
            pltpu.VMEM((rows, depth), BF16),
            pltpu.VMEM((len(lefts), depth, rows), BF16),
            pltpu.VMEM((rows, at), BF16),
            pltpu.VMEM((rows, columns * len(sums)), BF16),
        ]
        + [
            pltpu.VMEM((3, width, size) if mode == "nt" else (3, size, width), BF16)
            for group in sum_plan
            for _, size, mode in group
        ]
        + [
            line_block,
            line_block,
            line_block,
            pltpu.VMEM((2, 4, block, block), BF16),
            pltpu.VMEM((units, 4, block, block), BF16),
            pltpu.VMEM((units, 2, block, block), BF16),
            pltpu.VMEM((units, block, block), BF16),
            pltpu.VMEM((2, block, block), F32),
        ]
        + [pltpu.VMEM(value.shape, value.dtype) for value in given]
        + [pltpu.VMEM(shape, kind) for shape, kind in kept]
        + [
            pltpu.VMEM((1, depth), F32),
            pltpu.VMEM((peers, 2, depth // peers), F32),
            pltpu.VMEM((peers, 2, depth // peers), F32),
            dma((len(given),)),
            dma((len(made),)),
            dma((peers,)),
            dma((peers,)),
            dma((len(lefts),)),
            dma((len(rights),)),
            dma((len(weights), 3)),
            dma((3, all_chunks)),
            dma((3, all_chunks)),
            dma((units,)),
            dma((units,)),
            dma((2, units)),
            dma((2, units)),
            dma((units,)),
            dma((units,)),
            dma((len(spans), 2)),
        ],
        compiler_params=pltpu.CompilerParams(
            collective_id=call_id, has_side_effects=True, vmem_limit_bytes=62 << 20
        ),
        cost_estimate=pl.CostEstimate(flops=flops + (50 << 30), bytes_accessed=20 << 20, transcendentals=0),
        name=f"exchange_{call_id}",
    )(*lefts, *[right[0] for right in rights], *weights, *given)


def final_kernel(gn_ref, x_ref, gm_ref, gain_ref, mlp_ref, out_ref, gains_ref, acc, parts, come, send_sem, recv_sem):
    seq, batch = lax.axis_index("seq"), lax.axis_index("batch")
    seq_count = lax.axis_size("seq")
    peers = parts.shape[0]
    block = parts.shape[2]
    me = batch * seq_count + seq

    def peer(k):
        there = lax.rem(me + k, peers)
        return there, {"batch": lax.div(there, seq_count), "seq": lax.rem(there, seq_count)}

    def copy(k):
        there, device = peer(k)
        return pltpu.make_async_remote_copy(
            src_ref=parts.at[there],
            dst_ref=come.at[k],
            send_sem=send_sem.at[k],
            recv_sem=recv_sem.at[k],
            device_id=device,
            device_id_type=MESH,
        )

    barrier = pltpu.get_barrier_semaphore()
    for k in range(1, peers):
        pl.semaphore_signal(barrier, inc=1, device_id=peer(k)[1], device_id_type=MESH)
    rows = x_ref.shape[0]
    tile = rows // 8
    gain = gain_ref[...]
    acc[...] = jnp.zeros_like(acc)

    def rows_step(i, carry):
        here = pl.ds(pl.multiple_of(i * tile, tile), tile)
        wide = x_ref[here, :].astype(F32)
        grad = gn_ref[here, :].astype(F32)
        scale = lax.rsqrt(jnp.mean(wide * wide, axis=-1, keepdims=True) + epsilon)
        scaled = grad * gain
        mean = jnp.mean(wide * scaled, axis=-1, keepdims=True)
        result = gm_ref[here, :] + scale * scaled - wide * (scale * scale * scale) * mean
        out_ref[here, :] = result.astype(BF16)
        acc[...] += jnp.sum(grad * wide * scale, axis=0, keepdims=True)
        return carry

    lax.fori_loop(0, 8, rows_step, 0)
    for k in range(peers):
        here = slice(k * block, (k + 1) * block)
        parts[k, 0:1, :] = acc[:, here]
        parts[k, 1:2, :] = mlp_ref[:, here]
    pl.semaphore_wait(barrier, peers - 1)
    for k in range(1, peers):
        copy(k).start()
    total = parts[me]
    for k in range(1, peers):
        copy(k).wait_recv()
        total = total + come[k]
    gains_ref[...] = total
    for k in range(1, peers):
        copy(k).wait_send()


def final(grad_normed, tokens, grad_middle, gain, mlp_part, call_id):
    rows, width = tokens.shape
    peers = lax.axis_size("batch") * lax.axis_size("seq")
    block = width // peers
    vmem = pl.BlockSpec(memory_space=pltpu.VMEM)
    return pl.pallas_call(
        final_kernel,
        out_shape=[jax.ShapeDtypeStruct((rows, width), BF16), jax.ShapeDtypeStruct((2, block), F32)],
        in_specs=[vmem] * 5,
        out_specs=[vmem, vmem],
        scratch_shapes=[
            pltpu.VMEM((1, width), F32),
            pltpu.VMEM((peers, 2, block), F32),
            pltpu.VMEM((peers, 2, block), F32),
            pltpu.SemaphoreType.DMA((peers,)),
            pltpu.SemaphoreType.DMA((peers,)),
        ],
        compiler_params=pltpu.CompilerParams(collective_id=call_id, has_side_effects=True),
        name="final",
    )(grad_normed, tokens, grad_middle, gain, mlp_part)


def scatter_sum(left, right):
    rows, depth = left.shape
    columns = right.shape[1]
    batch_count = lax.axis_size("batch")
    seq_index = lax.axis_index("seq")
    core, chip = seq_index % 2, seq_index // 2
    block = depth // (4 * batch_count)
    split = left.reshape(rows, batch_count, 2, 2, block)
    size = lax.axis_size("seq")

    def product(at):
        taken = lax.dynamic_index_in_dim(split, at, 3, keepdims=False).reshape(rows, depth // 2)
        return dot_tn(taken, right)

    away = product(1 - core).astype(BF16)
    arrived = lax.ppermute(away, "seq", [(s, s ^ 1) for s in range(size)])
    kept = (product(core) + arrived.astype(F32)).astype(BF16)
    kept = kept.reshape(batch_count, 2, block, columns)
    half = columns // 2

    def over_chip(values, axis):
        sent = lax.dynamic_index_in_dim(values, 1 - chip, axis, keepdims=False)
        stay = lax.dynamic_index_in_dim(values, chip, axis, keepdims=False)
        came = lax.ppermute(sent, "seq", [(s, s ^ 2) for s in range(size)])
        return stay.astype(F32) + came.astype(F32)

    def over_batch(values):
        if batch_count == 2:
            here = lax.axis_index("batch")
            sent = lax.dynamic_index_in_dim(values, 1 - here, 0, keepdims=False)
            stay = lax.dynamic_index_in_dim(values, here, 0, keepdims=False)
            came = lax.ppermute(sent, "batch", [(0, 1), (1, 0)])
            return stay.astype(F32) + came.astype(F32)
        return lax.psum_scatter(values, "batch", scatter_dimension=0, tiled=False).astype(F32)

    one = over_batch(over_chip(kept[..., :half], 1).astype(BF16))
    two = over_chip(over_batch(kept[..., half:]).astype(BF16), 0)
    return jnp.concatenate([one, two], axis=1)


def local(
    tokens, segment_ids, attn_gain, w_query, w_key, w_value, w_output, mlp_gain, w_gate, w_up, w_down, cotangent
):
    rows, width = tokens.shape
    seq_count = lax.axis_size("seq")
    seq_index = lax.axis_index("seq")
    segments = segment_ids[0]
    first_row = seq_index * rows
    reach = LONGEST // rows
    cos, sin = rope_tables(segments, first_row, rows)
    row_segment = lax.dynamic_slice_in_dim(segments, first_row, rows, 0)[None, :]
    padded = jnp.concatenate([jnp.full((LONGEST,), -1, jnp.int32), segments])
    key_segment = lax.dynamic_slice_in_dim(padded, first_row, rows + LONGEST, 0)[:, None]

    normed, queries, own = project(tokens, attn_gain[None, :], w_query, w_key, w_value, cos, sin)
    near = lax.ppermute(own, "seq", [(s, s + 1) for s in range(seq_count - 1)])
    far = lax.ppermute(own, "seq", [(s, s + 2) for s in range(seq_count - 2)])
    mixed, logs = attend(queries, far, near, own, key_segment, row_segment)

    branch_low = line_sum([(mixed, w_output, "nn")], 1)
    branch = branch_low.astype(F32)
    wide = tokens.astype(F32)
    middle = wide + branch
    scale_two = lax.rsqrt(jnp.mean(middle * middle, axis=-1, keepdims=True) + epsilon)
    normed_two = (middle * scale_two * mlp_gain).astype(BF16)
    gate_pre = dot_nn(normed_two, w_gate)
    up_pre = dot_nn(normed_two, w_up)
    sigmoid_gate = jax.nn.sigmoid(gate_pre)
    swish = gate_pre * sigmoid_gate
    active = (swish * up_pre).astype(BF16)
    grad_active = dot_nt(cotangent, w_down)
    grad_gate_low = (grad_active * up_pre * sigmoid_gate * (1.0 + gate_pre * (1.0 - sigmoid_gate))).astype(BF16)
    grad_up_low = (grad_active * swish).astype(BF16)
    fused = lax.axis_size("batch") == 2
    hidden = w_gate.shape[1]
    unit = width // 8
    early = hidden * 5 // 8 // unit * unit
    if fused:
        grad_gate, grad_up, grad_down_one, grad_middle, grad_branch, grad_mixed, grad_mlp_gain, mlp_out = exchange(
            [normed_two, cotangent],
            [(grad_gate_low, 0, hidden), (grad_up_low, 0, hidden), (active, 0, hidden)],
            [
                [(w_gate, 0, hidden, "nt"), (w_up, hidden, hidden, "nt")],
                [(w_down, 2 * hidden, hidden, "nn")],
            ],
            (0, 2 * hidden // unit),
            [(unit, hidden), (unit, hidden), (early, unit)],
            [
                ("plain", 0, 0, 0, hidden),
                ("plain", 1, 0, hidden, hidden),
                ("turned", 2, 0, 2 * hidden, early),
            ],
            (2 * hidden + early) // unit,
            2,
            (3, 2),
            "branch",
            [tokens, branch_low, mlp_gain[None, :], w_output],
            [
                ((rows, width), F32),
                ((rows, width), BF16),
                ((rows, mixed.shape[1]), BF16),
                ((1, width), F32),
                ((rows, width), BF16),
            ],
        )
    else:
        grad_normed_two = line_sum([(grad_gate_low, w_gate, "nt"), (grad_up_low, w_up, "nt")], 2)
        grad_gate = scatter_sum(normed_two, grad_gate_low)
        grad_up = scatter_sum(normed_two, grad_up_low)
        mlp_out = lax.psum(dot_nn(active, w_down).astype(BF16), "mp")
        grad_normed_two = grad_normed_two.astype(F32)
        scaled_two = grad_normed_two * mlp_gain
        grad_middle = (
            cotangent.astype(F32)
            + scale_two * scaled_two
            - middle
            * (scale_two * scale_two * scale_two)
            * jnp.mean(middle * scaled_two, axis=-1, keepdims=True)
        )
        grad_mlp_gain = jnp.sum(grad_normed_two * middle * scale_two, axis=0)[None, :]
        grad_branch = grad_middle.astype(BF16)
        grad_mixed = dot_nt(grad_branch, w_output).astype(BF16)
    output = (middle + mlp_out.astype(F32)).astype(BF16)

    grad_query_pre, dfar, dnear, down = attend_back(
        queries, far, near, own, key_segment, row_segment, mixed, grad_mixed, logs, cos, sin
    )
    from_near = lax.ppermute(dnear, "seq", [(s + 1, s) for s in range(seq_count - 1)])
    from_far = lax.ppermute(dfar, "seq", [(s + 2, s) for s in range(seq_count - 2)])
    grad_pair = down + from_near.astype(F32) + from_far.astype(F32)
    grad_keys = jnp.concatenate([grad_pair[:, :HS], grad_pair[:, PAIR : PAIR + HS]], axis=1)
    grad_values = jnp.concatenate([grad_pair[:, HS:PAIR], grad_pair[:, PAIR + HS :]], axis=1)
    quarter = HS // 2
    swapped = jnp.concatenate(
        [grad_keys[:, (at ^ 1) * quarter : ((at ^ 1) + 1) * quarter] for at in range(4)], axis=1
    )
    grad_key_pre = (grad_keys * cos - swapped * sin).astype(BF16)
    grad_value_pre = grad_values.astype(BF16)

    query_width = grad_query_pre.shape[1]
    if fused:
        late, mixed_width = hidden - early, mixed.shape[1]
        query_at = late + mixed_width
        key_at = query_at + query_width
        grad_down_two, grad_output, grad_query, grad_key, grad_value, grad_tokens, gains = exchange(
            [cotangent, grad_branch, normed],
            [
                (active, early, late),
                (mixed, 0, mixed_width),
                (grad_query_pre, 0, query_width),
                (grad_key_pre, 0, PAIR),
                (grad_value_pre, 0, PAIR),
            ],
            [
                [
                    (w_query, query_at, query_width, "nt"),
                    (w_key, key_at, PAIR, "nt"),
                    (w_value, key_at + PAIR, PAIR, "nt"),
                ]
            ],
            (0, late // unit, query_at // unit),
            [(late, unit), (mixed_width, unit), (unit, query_width), (unit, PAIR), (unit, PAIR)],
            [
                ("turned", 0, 0, 0, late),
                ("turned", 1, 0, late, mixed_width),
                ("plain", 2, 0, query_at, query_width),
                ("plain", 3, 0, key_at, PAIR),
                ("plain", 4, 0, key_at + PAIR, PAIR),
            ],
            (key_at + 2 * PAIR) // unit,
            3,
            (2, 1),
            "tokens",
            [tokens, grad_middle, attn_gain[None, :], grad_mlp_gain],
            [((rows, width), BF16), ((2, unit), F32)],
        )
        grad_down = jnp.concatenate([grad_down_one, grad_down_two], axis=0)
    else:
        grad_down = scatter_sum(cotangent, active).T
        grad_output = scatter_sum(grad_branch, mixed).T
        grad_qkv = scatter_sum(normed, jnp.concatenate([grad_query_pre, grad_key_pre, grad_value_pre], axis=1))
        grad_query = grad_qkv[:, :query_width]
        grad_key = grad_qkv[:, query_width : query_width + PAIR]
        grad_value = grad_qkv[:, query_width + PAIR :]
        grad_normed = line_sum(
            [(grad_query_pre, w_query, "nt"), (grad_key_pre, w_key, "nt"), (grad_value_pre, w_value, "nt")], 3
        )
        grad_tokens, gains = final(grad_normed, tokens, grad_middle, attn_gain[None, :], grad_mlp_gain, 4)
    return (
        output,
        grad_tokens,
        gains[0],
        grad_query,
        grad_key,
        grad_value,
        grad_output,
        gains[1],
        grad_gate,
        grad_up,
        grad_down,
    )


def solution(mesh):
    tokens_spec = P(("batch", "seq"), None)
    in_specs = (
        tokens_spec,
        P("batch", None),
        P(),
        P(None, "mp"),
        P(None, "mp"),
        P(None, "mp"),
        P("mp", None),
        P(),
        P(None, "mp"),
        P(None, "mp"),
        P("mp", None),
        tokens_spec,
    )
    row_split = P(("batch", "seq"), "mp")
    column_split = P("mp", ("batch", "seq"))
    out_specs = (
        tokens_spec,
        tokens_spec,
        P(("batch", "seq")),
        row_split,
        row_split,
        row_split,
        column_split,
        P(("batch", "seq")),
        row_split,
        row_split,
        column_split,
    )
    return jax.shard_map(local, mesh=mesh, in_specs=in_specs, out_specs=out_specs, check_vma=False)
```

```python
import functools
import math

import jax
import jax.numpy as jnp
from jax import lax
from jax.experimental import pallas as pl
from jax.experimental.pallas import tpu as pltpu
from jax.sharding import PartitionSpec as P

HS = 64
PAIR = 2 * HS
LONGEST = 1024
rope_base = 500000.0
epsilon = 1e-05
masked_score = -1e30
MESH = pl.DeviceIdType.MESH
F32 = jnp.float32
BF16 = jnp.bfloat16


def dot_nn(left, right):
    return lax.dot_general(left, right, (((1,), (0,)), ((), ())), preferred_element_type=F32)


def dot_nt(left, right):
    return lax.dot_general(left, right, (((1,), (1,)), ((), ())), preferred_element_type=F32)


def dot_tn(left, right):
    return lax.dot_general(left, right, (((0,), (0,)), ((), ())), preferred_element_type=F32)


def lanes_of(values):
    return lax.broadcasted_iota(jnp.int32, values.shape, 1)


def swap_halves(values):
    ahead = pltpu.roll(values, PAIR - HS // 2, 1)
    behind = pltpu.roll(values, HS // 2, 1)
    return jnp.where(lanes_of(values) % HS < HS // 2, ahead, behind)


def rope_tables(segments, first_row, rows):
    row_segment = lax.dynamic_slice_in_dim(segments, first_row, rows, 0)
    doc_start = jnp.sum((segments[None, :] < row_segment[:, None]).astype(jnp.int32), axis=1)
    place = (first_row + jnp.arange(rows, dtype=jnp.int32) - doc_start).astype(F32)
    lane = jnp.arange(PAIR, dtype=jnp.int32)
    frequency = jnp.exp((lane % (HS // 2)).astype(F32) * (-2.0 * math.log(rope_base) / HS))
    angles = place[:, None] * frequency[None, :]
    sign = jnp.where(lane % HS < HS // 2, -1.0, 1.0)
    return jnp.cos(angles), jnp.sin(angles) * sign[None, :]


def project_kernel(
    x_ref, gain_ref, wk_ref, wv_ref, cos_ref, sin_ref, cot_hbm, wq_hbm, wd_hbm,
    n_hbm, q_hbm, kv_hbm, ga_hbm,
    n_ref, q_ref, kv_ref, ga_ref, cot_ref, wq_ref, wd_ref, load_sem, wd_sem, send_sem, recv_sem, out_sem,
):
    rows = x_ref.shape[0]
    seq, seq_count = lax.axis_index("seq"), lax.axis_size("seq")
    hidden = wd_hbm.shape[0]
    width = wd_ref.shape[1]
    chunks = hidden // width
    block = rows // 2
    loads = [
        pltpu.make_async_copy(wq_hbm, wq_ref, load_sem.at[0]),
        pltpu.make_async_copy(cot_hbm, cot_ref, load_sem.at[1]),
    ]

    def weight(c):
        slot = lax.rem(c, 3)
        here = pl.ds(pl.multiple_of(c * width, width), width)
        return pltpu.make_async_copy(wd_hbm.at[here, :], wd_ref.at[slot], wd_sem.at[slot])

    def out_copy(at):
        source = (n_ref, q_ref, kv_ref, ga_ref)[at]
        return pltpu.make_async_copy(source, (n_hbm, q_hbm, kv_hbm, ga_hbm)[at], out_sem.at[at])

    def send(away):
        return pltpu.make_async_remote_copy(
            src_ref=kv_ref.at[2],
            dst_ref=kv_ref.at[2 - away],
            send_sem=send_sem.at[away],
            recv_sem=recv_sem.at[away],
            device_id={"seq": lax.rem(seq + away, seq_count)},
            device_id_type=MESH,
        )

    for load in loads:
        load.start()
    weight(0).start()
    weight(1).start()
    for away in (1, 2):

        @pl.when(seq < away)
        def _():
            kv_ref[2 - away] = jnp.zeros(kv_ref.shape[1:], BF16)

    barrier = pltpu.get_barrier_semaphore()
    for away in range(1, seq_count):
        there = lax.rem(seq + away, seq_count)
        pl.semaphore_signal(barrier, inc=1, device_id={"seq": there}, device_id_type=MESH)

    for half in range(2):
        here = slice(half * block, (half + 1) * block)
        cos, sin = cos_ref[here, :], sin_ref[here, :]
        wide = x_ref[here, :].astype(F32)
        scale = lax.rsqrt(jnp.mean(wide * wide, axis=-1, keepdims=True) + epsilon)
        normed = (wide * scale * gain_ref[...]).astype(BF16)
        n_ref[here, :] = normed
        keys = dot_nn(normed, wk_ref[...])
        keys = keys * cos + swap_halves(keys) * sin
        values = dot_nn(normed, wv_ref[...])
        low_half = lanes_of(keys) < HS
        kv_ref[2, here, :PAIR] = jnp.where(low_half, keys, pltpu.roll(values, HS, 1)).astype(BF16)
        kv_ref[2, here, PAIR:] = jnp.where(low_half, pltpu.roll(keys, HS, 1), values).astype(BF16)
    pl.semaphore_wait(barrier, seq_count - 1)
    for away in (1, 2):

        @pl.when(seq + away < seq_count)
        def _():
            send(away).start()

    out_copy(0).start()
    for load in loads:
        load.wait()
    for half in range(2):
        here = slice(half * block, (half + 1) * block)
        cos, sin = cos_ref[here, :], sin_ref[here, :]
        queries = dot_nn(n_ref[here, :], wq_ref[...])
        for start in range(0, queries.shape[1], PAIR):
            part = queries[:, start : start + PAIR]
            q_ref[here, start : start + PAIR] = (part * cos + swap_halves(part) * sin).astype(BF16)
    out_copy(1).start()

    def step(c, carry):
        weight(c).wait()

        @pl.when(c + 2 < chunks)
        def _():
            weight(c + 2).start()

        here = pl.ds(pl.multiple_of(c * width, width), width)
        ga_ref[:, here] = dot_nt(cot_ref[...], wd_ref[lax.rem(c, 3)]).astype(BF16)
        return carry

    lax.fori_loop(0, chunks, step, 0)
    out_copy(3).start()
    for away in (1, 2):

        @pl.when(seq >= away)
        def _():
            send(away).wait_recv()

    out_copy(2).start()
    for away in (1, 2):

        @pl.when(seq + away < seq_count)
        def _():
            send(away).wait_send()

    for at in range(4):
        out_copy(at).wait()


def project(tokens, gain, w_query, w_key, w_value, cos, sin, cotangent, w_down, call_id):
    rows, width = tokens.shape
    columns, hidden = w_query.shape[1], w_down.shape[0]
    chunk = 256
    vmem, any_space = pl.BlockSpec(memory_space=pltpu.VMEM), pl.BlockSpec(memory_space=pl.ANY)
    shapes = [(rows, width), (rows, columns), (3, rows, 2 * PAIR), (rows, hidden)]
    dma = pltpu.SemaphoreType.DMA
    return pl.pallas_call(
        project_kernel,
        in_specs=[vmem] * 6 + [any_space] * 3,
        out_specs=[any_space] * 4,
        out_shape=[jax.ShapeDtypeStruct(shape, BF16) for shape in shapes],
        scratch_shapes=[pltpu.VMEM(shape, BF16) for shape in shapes]
        + [
            pltpu.VMEM((rows, width), BF16),
            pltpu.VMEM(w_query.shape, BF16),
            pltpu.VMEM((3, chunk, width), BF16),
            dma((2,)),
            dma((3,)),
            dma((3,)),
            dma((3,)),
            dma((4,)),
        ],
        compiler_params=pltpu.CompilerParams(
            collective_id=call_id, has_side_effects=True, vmem_limit_bytes=62 << 20
        ),
        name="project",
    )(tokens, gain, w_key, w_value, cos, sin, cotangent, w_query, w_down)


def write_bias(bias_ref, key_ref, row_ref):
    keys, rows = bias_ref.shape
    key_place = lax.broadcasted_iota(jnp.int32, (keys, rows), 0) - (keys - rows)
    row_place = lax.broadcasted_iota(jnp.int32, (keys, rows), 1)
    allowed = (key_ref[...] == row_ref[...]) & (key_place <= row_place)
    bias_ref[...] = jnp.where(allowed, 0.0, masked_score)


def attend_kernel(q_ref, kv_ref, key_ref, row_ref, out_ref, log_ref, bias_ref):
    @pl.when(pl.program_id(0) == 0)
    def _():
        write_bias(bias_ref, key_ref, row_ref)

    key_value = kv_ref[...]
    flipped = key_value.T
    q_flipped = (q_ref[...].astype(F32) * HS ** (-0.5)).astype(BF16).T
    outs = []
    for head in range(2):
        scores = dot_nn(key_value[:, :HS], q_flipped[head * HS : (head + 1) * HS, :]) + bias_ref[...]
        top = jnp.max(scores, axis=0, keepdims=True)
        powers = jnp.exp(scores - top)
        total = jnp.sum(powers, axis=0, keepdims=True)
        mixed = dot_nn(flipped[HS:, :], powers.astype(BF16))
        outs.append(mixed / total)
        log_ref[0, head : head + 1, :] = top + jnp.log(total)
    out_ref[...] = jnp.concatenate(outs, axis=0).T.astype(BF16)


def attend(queries, key_value, key_segment, row_segment):
    rows, width = queries.shape
    pairs = width // PAIR
    per_group = pairs // 2
    pair_tile = pl.BlockSpec((rows, PAIR), lambda p: (0, p))
    kv_tile = pl.BlockSpec((3 * rows, PAIR), lambda p: (0, p // per_group))
    return pl.pallas_call(
        attend_kernel,
        grid=(pairs,),
        in_specs=[
            pair_tile,
            kv_tile,
            pl.BlockSpec(key_segment.shape, lambda p: (0, 0)),
            pl.BlockSpec(row_segment.shape, lambda p: (0, 0)),
        ],
        out_specs=[pair_tile, pl.BlockSpec((1, 2, rows), lambda p: (p, 0, 0))],
        out_shape=[
            jax.ShapeDtypeStruct((rows, width), BF16),
            jax.ShapeDtypeStruct((pairs, 2, rows), F32),
        ],
        scratch_shapes=[pltpu.VMEM((3 * rows, rows), F32)],
        cost_estimate=pl.CostEstimate(
            flops=16 << 30, bytes_accessed=4 << 20, transcendentals=3 * rows * rows * 2 * pairs
        ),
        name="attend",
    )(queries, key_value, key_segment, row_segment)


def attend_back_kernel(
    q_ref, kv_ref, key_ref, row_ref, out_ref, grad_ref, log_ref, cos_ref, sin_ref,
    dq_ref, dfar_ref, dnear_ref, down_ref, bias_ref, dkv_ref, per_group,
):
    step = pl.program_id(0)

    @pl.when(step == 0)
    def _():
        write_bias(bias_ref, key_ref, row_ref)

    rows = q_ref.shape[0]
    key_value = kv_ref[...]
    flipped = key_value[:, :].T
    scaled = (q_ref[...].astype(F32) * HS ** (-0.5)).astype(BF16)
    q_flipped = scaled.T
    grad = grad_ref[...]
    grad_flipped = grad.T
    product = (out_ref[...].astype(F32) * grad.astype(F32)).T
    dqs, dkey, dvalue = [], None, None
    for head in range(2):
        here = slice(head * HS, (head + 1) * HS)
        scores = dot_nn(key_value[:, :HS], q_flipped[here, :]) + bias_ref[...]
        shares = jnp.exp(scores - log_ref[0, head : head + 1, :])
        grad_shares = dot_nn(key_value[:, HS:], grad_flipped[here, :])
        delta = jnp.sum(product[here, :], axis=0, keepdims=True)
        grad_scores = (shares * (grad_shares - delta)).astype(BF16)
        value_part = dot_nn(shares.astype(BF16), grad[:, here])
        key_part = dot_nn(grad_scores, scaled[:, here])
        dvalue = value_part if dvalue is None else dvalue + value_part
        dkey = key_part if dkey is None else dkey + key_part
        dqs.append(dot_nn(flipped[:HS, :], grad_scores))
    dq = jnp.concatenate(dqs, axis=0).T * HS ** (-0.5)
    dq_ref[...] = (dq * cos_ref[...] - swap_halves(dq) * sin_ref[...]).astype(BF16)
    both = jnp.concatenate([dkey, dvalue], axis=1)

    @pl.when(step % per_group == 0)
    def _():
        dkv_ref[...] = both

    @pl.when(step % per_group != 0)
    def _():
        dkv_ref[...] += both

    @pl.when(step % per_group == per_group - 1)
    def _():
        dfar_ref[...] = dkv_ref[:rows, :].astype(BF16)
        dnear_ref[...] = dkv_ref[rows : 2 * rows, :].astype(BF16)
        down_ref[...] = dkv_ref[2 * rows :, :]


def attend_back(queries, key_value, key_segment, row_segment, mixed, grad, logs, cos, sin):
    rows, width = queries.shape
    pairs = width // PAIR
    per_group = pairs // 2
    pair_tile = pl.BlockSpec((rows, PAIR), lambda p: (0, p))
    kv_tile = pl.BlockSpec((rows, PAIR), lambda p: (0, p // per_group))
    wide_tile = pl.BlockSpec((3 * rows, PAIR), lambda p: (0, p // per_group))
    full = lambda array: pl.BlockSpec(array.shape, lambda p: (0, 0))
    return pl.pallas_call(
        functools.partial(attend_back_kernel, per_group=per_group),
        grid=(pairs,),
        in_specs=[
            pair_tile,
            wide_tile,
            full(key_segment),
            full(row_segment),
            pair_tile,
            pair_tile,
            pl.BlockSpec((1, 2, rows), lambda p: (p, 0, 0)),
            full(cos),
            full(sin),
        ],
        out_specs=[pair_tile, kv_tile, kv_tile, kv_tile],
        out_shape=[
            jax.ShapeDtypeStruct((rows, width), BF16),
            jax.ShapeDtypeStruct((rows, 2 * PAIR), BF16),
            jax.ShapeDtypeStruct((rows, 2 * PAIR), BF16),
            jax.ShapeDtypeStruct((rows, 2 * PAIR), F32),
        ],
        scratch_shapes=[
            pltpu.VMEM((3 * rows, rows), F32),
            pltpu.VMEM((3 * rows, PAIR), F32),
        ],
        cost_estimate=pl.CostEstimate(
            flops=40 << 30, bytes_accessed=6 << 20, transcendentals=3 * rows * rows * 2 * pairs
        ),
        name="attend_back",
    )(queries, key_value, key_segment, row_segment, mixed, grad, logs, cos, sin)


def line_sum_kernel(modes, chunks, *refs):
    count = len(modes)
    a_refs, w_refs, out_ref = refs[:count], refs[count : 2 * count], refs[2 * count]
    rest = refs[2 * count + 1 :]
    w_bufs = rest[:count]
    part, first, second, total, w_sem, send_sem, recv_sem = rest[count:]
    width = part.shape[2]
    place = lax.axis_index("mp")
    pair = place + 1 - 2 * lax.rem(place, 2)
    across = 3 - place
    is_mid = (place == 1) | (place == 2)
    is_end = (place == 0) | (place == 3)

    def weight(at, c):
        if modes[at] == "nt":
            source = w_refs[at].at[pl.ds(pl.multiple_of(c * width, width), width), :]
        else:
            source = w_refs[at].at[:, pl.ds(pl.multiple_of(c * width, width), width)]
        return pltpu.make_async_copy(source, w_bufs[at].at[c], w_sem.at[at, c])

    def remote(kind, source, target, c, device):
        return pltpu.make_async_remote_copy(
            src_ref=source.at[c],
            dst_ref=target.at[c],
            send_sem=send_sem.at[kind, c],
            recv_sem=recv_sem.at[kind, c],
            device_id={"mp": device},
            device_id_type=MESH,
        )

    def up(c):
        return remote(0, part, first, c, pair)

    def over(c):
        return remote(1, part, second, c, across)

    def down(c):
        return remote(2, total, total, c, pair)

    def start_weights(c, carry):
        for at in range(count):
            weight(at, c).start()
        return carry

    lax.fori_loop(0, chunks, start_weights, 0)
    barrier = pltpu.get_barrier_semaphore()
    pl.semaphore_signal(barrier, inc=1, device_id={"mp": pair}, device_id_type=MESH)

    @pl.when(is_mid)
    def _():
        pl.semaphore_signal(barrier, inc=1, device_id={"mp": across}, device_id_type=MESH)
        pl.semaphore_wait(barrier, 2)

    @pl.when(is_end)
    def _():
        pl.semaphore_wait(barrier, 1)

    def step(t, carry):
        @pl.when(t < chunks)
        def _():
            value = None
            for at in range(count):
                weight(at, t).wait()
                dot = dot_nt if modes[at] == "nt" else dot_nn
                term = dot(a_refs[at][...], w_bufs[at][t])
                value = term if value is None else value + term
            part[t] = value.astype(BF16)

            @pl.when(is_end)
            def _():
                up(t).start()

        @pl.when(is_mid & (t >= 1) & (t < chunks + 1))
        def _():
            c = t - 1
            up(c).wait_recv()
            part[c] = (part[c].astype(F32) + first[c].astype(F32)).astype(BF16)
            over(c).start()

        @pl.when(is_mid & (t >= OVER_LAG))
        def _():
            c = t - OVER_LAG
            over(c).wait_recv()
            total[c] = (part[c].astype(F32) + second[c].astype(F32)).astype(BF16)
            down(c).start()

        return carry

    lax.fori_loop(0, chunks + OVER_LAG, step, 0)

    def finish(c, carry):
        @pl.when(is_end)
        def _():
            up(c).wait_send()
            down(c).wait_recv()

        @pl.when(is_mid)
        def _():
            over(c).wait_send()
            down(c).wait_send()

        out_ref[:, pl.ds(pl.multiple_of(c * width, width), width)] = total[c]
        return carry

    lax.fori_loop(0, chunks, finish, 0)


def line_sum(pairs, call_id, chunks=16):
    lefts = [left for left, _, _ in pairs]
    rights = [right for _, right, _ in pairs]
    modes = tuple(mode for _, _, mode in pairs)
    rows = lefts[0].shape[0]
    columns = rights[0].shape[0] if modes[0] == "nt" else rights[0].shape[1]
    width = columns // chunks
    count = len(pairs)
    bufs = [
        pltpu.VMEM((chunks, width, left.shape[1]) if mode == "nt" else (chunks, left.shape[1], width), BF16)
        for left, _, mode in pairs
    ]
    flops = sum(2 * rows * columns * left.shape[1] for left in lefts)
    moved = sum(right.size * 2 for right in rights)
    block = pltpu.VMEM((chunks, rows, width), BF16)
    return pl.pallas_call(
        functools.partial(line_sum_kernel, modes, chunks),
        out_shape=jax.ShapeDtypeStruct((rows, columns), BF16),
        in_specs=[pl.BlockSpec(memory_space=pltpu.VMEM)] * count
        + [pl.BlockSpec(memory_space=pl.ANY)] * count,
        out_specs=pl.BlockSpec(memory_space=pltpu.VMEM),
        scratch_shapes=bufs
        + [
            block,
            block,
            block,
            block,
            pltpu.SemaphoreType.DMA((count, chunks)),
            pltpu.SemaphoreType.DMA((3, chunks)),
            pltpu.SemaphoreType.DMA((3, chunks)),
        ],
        compiler_params=pltpu.CompilerParams(collective_id=call_id, has_side_effects=True),
        cost_estimate=pl.CostEstimate(
            flops=flops + (40 << 30), bytes_accessed=moved, transcendentals=0
        ),
        name=f"line_sum_{call_id}",
    )(*lefts, *rights)

LAG = 3
UP_LAG = 1
OVER_LAG = 3
DOWN_LAG = 8
HALVES = 1
TILES = 8


def exchange_kernel(plan, *refs):
    left_count, rights, sums, flips_before, spans, out_count, units, chunks, period, active, ending, given, made = plan
    refs = list(refs)

    def take(n):
        got = refs[:n]
        del refs[:n]
        return got

    weights = [item for group in sums for item in group]
    left_refs, right_refs, w_refs = take(left_count), take(len(rights)), take(len(weights))
    given_refs = take(given)
    grad_refs, made_refs = take(out_count), take(made)
    stage, flip, right_all, out_ref = take(4)
    w_bufs = take(len(weights))
    part, first, second, away, come_one, come_two, come_three, result = take(8)
    given_bufs, made_bufs = take(given), take(made - (ending == "branch"))
    acc, gain_parts, gain_come, given_sem, made_sem, gain_send, gain_recv = take(7)
    in_sem, right_sem, w_sem, ar_send, ar_recv, core_send, core_recv, two_send, two_recv, three_send, three_recv, out_sem = refs
    width = part.shape[2]
    block = come_three.shape[1]
    all_chunks = chunks * len(sums)
    place = lax.axis_index("mp")
    seq, batch = lax.axis_index("seq"), lax.axis_index("batch")
    core, chip = lax.rem(seq, 2), lax.div(seq, 2)
    sibling = seq + 1 - 2 * core
    beside = seq + 2 - 4 * chip
    pair = place + 1 - 2 * lax.rem(place, 2)
    across = 3 - place
    is_mid = (place == 1) | (place == 2)
    is_end = (place == 0) | (place == 3)

    def columns_of(c):
        return pl.ds(pl.multiple_of(c * width, width), width)

    def weight(at, group, c):
        here = columns_of(c - group * chunks)
        source = w_refs[at].at[here, :] if weights[at][2] == "nt" else w_refs[at].at[:, here]
        slot = lax.rem(c, 3)
        return pltpu.make_async_copy(source, w_bufs[at].at[slot], w_sem.at[at, slot])

    members = []
    for group, items in enumerate(sums):
        for _ in items:
            members.append(group)

    def load_weights(c):
        for group in range(len(sums)):

            @pl.when((c >= group * chunks) & (c < (group + 1) * chunks))
            def _():
                for at in range(len(weights)):
                    if members[at] == group:
                        weight(at, group, c).start()

    def remote(source, target, send, recv, device):
        return pltpu.make_async_remote_copy(
            src_ref=source, dst_ref=target, send_sem=send, recv_sem=recv, device_id=device, device_id_type=MESH
        )

    def slot_of(c):
        return lax.rem(c, chunks)

    high = part.shape[1] // HALVES

    def rows_of(h):
        return slice(h * high, (h + 1) * high)

    def up(c, h):
        slot = slot_of(c)
        source, target = part.at[slot, rows_of(h)], first.at[slot, rows_of(h)]
        return remote(source, target, ar_send.at[0, h, c], ar_recv.at[0, h, c], {"mp": pair})

    def over(c, h):
        slot = slot_of(c)
        source, target = part.at[slot, rows_of(h)], second.at[slot, rows_of(h)]
        return remote(source, target, ar_send.at[1, h, c], ar_recv.at[1, h, c], {"mp": across})

    def down(c, h):
        here = out_ref.at[rows_of(h), columns_of(c)]
        return remote(here, here, ar_send.at[2, h, c], ar_recv.at[2, h, c], {"mp": pair})

    def to_core(u):
        return remote(away.at[lax.rem(u, 2)], come_one.at[u], core_send.at[u], core_recv.at[u], {"seq": sibling})

    def chip_first(u):
        return 1 - lax.rem(u, 2)

    def sent_at(u, k):
        x_first = chip_first(u)
        return x_first * (2 * k + 1 - chip) + (1 - x_first) * (2 * (1 - batch) + k)

    def kept_at(u, k):
        x_first = chip_first(u)
        return x_first * (2 * k + chip) + (1 - x_first) * (2 * batch + k)

    def own_at(u):
        x_first = chip_first(u)
        return x_first * batch + (1 - x_first) * chip

    def device_of(x_way):
        return {
            "seq": x_way * beside + (1 - x_way) * seq,
            "batch": x_way * batch + (1 - x_way) * (1 - batch),
        }

    def second_hop(u, k):
        return remote(
            come_one.at[u, sent_at(u, k)], come_two.at[u, k], two_send.at[k, u], two_recv.at[k, u], device_of(chip_first(u))
        )

    def third_hop(u):
        return remote(
            come_two.at[u, 1 - own_at(u)], come_three.at[u], three_send.at[u], three_recv.at[u], device_of(1 - chip_first(u))
        )

    def left_copy(at):
        return pltpu.make_async_copy(left_refs[at], stage, in_sem.at[at])

    def right_copy(at):
        offset, source, size = rights[at]
        return pltpu.make_async_copy(
            right_refs[at].at[:, source : source + size], right_all.at[:, offset : offset + size], right_sem.at[at]
        )

    def out_copy(at, u):
        kind, index, offset, start, size = spans[at]
        slot = lax.rem(u, 2)
        if size < block:
            source = result.at[slot, :, start % block : start % block + size]
            target = grad_refs[index].at[:, offset : offset + size]
        else:
            source = result.at[slot]
            here = pl.ds(pl.multiple_of((u - start // block) * block + offset, block), block)
            target = grad_refs[index].at[here, :] if kind == "turned" else grad_refs[index].at[:, here]
        return pltpu.make_async_copy(source, target, out_sem.at[at, slot])

    def units_of(at):
        _, _, _, start, size = spans[at]
        return start // block, max((start + size) // block, start // block + 1)

    seq_count = lax.axis_size("seq")
    peers = lax.axis_size("batch") * seq_count
    me = batch * seq_count + seq

    def peer(k):
        there = lax.rem(me + k, peers)
        return there, {"batch": lax.div(there, seq_count), "seq": lax.rem(there, seq_count)}

    def gain_copy(k):
        there, device = peer(k)
        return remote(gain_parts.at[there], gain_come.at[k], gain_send.at[k], gain_recv.at[k], device)

    def given_copy(at):
        return pltpu.make_async_copy(given_refs[at], given_bufs[at], given_sem.at[at])

    def made_copy(at):
        source = out_ref.at[:, columns // 2 :] if ending == "branch" and at == made - 1 else made_bufs[at]
        return pltpu.make_async_copy(source, made_refs[at], made_sem.at[at])

    columns = out_ref.shape[1]
    rows = out_ref.shape[0]
    tile = rows // TILES

    def tile_of(i):
        return pl.ds(pl.multiple_of(i * tile, tile), tile)

    def branch_rows(i):
        here = tile_of(i)
        gm_buf, gb_buf, _ = made_bufs[:3]
        x_buf, b_buf, gain_buf, _ = given_bufs
        grad = out_ref[here, : columns // 2].astype(F32)
        middle = x_buf[here, :].astype(F32) + b_buf[here, :].astype(F32)
        scale = lax.rsqrt(jnp.mean(middle * middle, axis=-1, keepdims=True) + epsilon)
        scaled = grad * gain_buf[...]
        mean = jnp.mean(middle * scaled, axis=-1, keepdims=True)
        value = stage[here, :].astype(F32) + scale * scaled - middle * (scale * scale * scale) * mean
        gm_buf[here, :] = value
        gb_buf[here, :] = value.astype(BF16)
        acc[...] += jnp.sum(grad * middle * scale, axis=0, keepdims=True)

    def branch_end():
        made_bufs[2][...] = dot_nt(made_bufs[1][...], given_bufs[3][...]).astype(BF16)
        made_bufs[3][...] = acc[...]
        for at in range(4):
            made_copy(at).start()

    def token_rows(i, carry):
        here = tile_of(i)
        x_buf, gm_buf, gain_buf, _ = given_bufs
        wide = x_buf[here, :].astype(F32)
        grad = out_ref[here, :].astype(F32)
        scale = lax.rsqrt(jnp.mean(wide * wide, axis=-1, keepdims=True) + epsilon)
        scaled = grad * gain_buf[...]
        mean = jnp.mean(wide * scaled, axis=-1, keepdims=True)
        value = gm_buf[here, :] + scale * scaled - wide * (scale * scale * scale) * mean
        made_bufs[0][here, :] = value.astype(BF16)
        acc[...] += jnp.sum(grad * wide * scale, axis=0, keepdims=True)
        return carry

    acc[...] = jnp.zeros_like(acc)
    load_weights(0)
    load_weights(1)
    for at in range(len(rights)):
        right_copy(at).start()
    left_copy(0).start()
    for at in range(given):
        given_copy(at).start()

    barrier = pltpu.get_barrier_semaphore()
    if ending == "tokens":
        greeted = [{"mp": pair}] + [peer(k)[1] for k in range(1, peers)]
    else:
        greeted = [{"mp": pair}, {"seq": sibling}, {"seq": beside}, {"batch": 1 - batch}]
    for device in greeted:
        pl.semaphore_signal(barrier, inc=1, device_id=device, device_id_type=MESH)

    @pl.when(is_mid)
    def _():
        pl.semaphore_signal(barrier, inc=1, device_id={"mp": across}, device_id_type=MESH)
        pl.semaphore_wait(barrier, len(greeted) + 1)

    @pl.when(is_end)
    def _():
        pl.semaphore_wait(barrier, len(greeted))

    for at in range(len(rights)):
        right_copy(at).wait()

    def left_of(u):
        index = 0
        for at in range(1, left_count):
            index = index + (u >= flips_before[at]).astype(jnp.int32)
        return index

    def product(u, at, side):
        row = pl.multiple_of((2 * at + side) * block, block)
        column = pl.multiple_of(u * block, block)
        return dot_nn(flip[left_of(u), pl.ds(row, block), :], right_all[:, pl.ds(column, block)])

    def step_of(u):
        return (u // active) * period + u % active

    def on_unit(t, body):
        u = lax.div(t, period) * active + lax.rem(t, period)

        @pl.when((t >= 0) & (lax.rem(t, period) < active) & (u < units))
        def _():
            body(u)

    def first_stage(u):
        @pl.when(u >= 2)
        def _():
            to_core(u - 2).wait_send()

        for at in range(4):
            away[lax.rem(u, 2), at] = product(u, at, 1 - core).astype(BF16)
        to_core(u).start()

    def second_stage(u):
        to_core(u).wait_recv()
        for at in range(4):
            come_one[u, at] = (product(u, at, core) + come_one[u, at].astype(F32)).astype(BF16)
        for k in range(2):
            second_hop(u, k).start()

    def third_stage(u):
        for k in range(2):
            second_hop(u, k).wait_recv()
        sent = 1 - own_at(u)
        come_two[u, sent] = (come_two[u, sent].astype(F32) + come_one[u, kept_at(u, sent)].astype(F32)).astype(BF16)
        third_hop(u).start()

    def last_stage(u):
        third_hop(u).wait_recv()
        own = own_at(u)
        value = come_three[u].astype(F32) + come_two[u, own].astype(F32) + come_one[u, kept_at(u, own)].astype(F32)
        for at in range(len(spans)):
            low, high = units_of(at)

            @pl.when((u - 2 >= low) & (u - 2 < high))
            def _():
                out_copy(at, u - 2).wait()

        for kind in ("turned", "plain"):
            mine = [units_of(at) for at in range(len(spans)) if spans[at][0] == kind]
            if mine:
                low, high = min(m[0] for m in mine), max(m[1] for m in mine)

                @pl.when((u >= low) & (u < high))
                def _():
                    result[lax.rem(u, 2)] = value.T if kind == "turned" else value

        for at in range(len(spans)):
            low, high = units_of(at)

            @pl.when((u >= low) & (u < high))
            def _():
                out_copy(at, u).start()

    def step(t, carry):
        @pl.when((t >= chunks) & (t < all_chunks))
        def _():
            @pl.when(is_end)
            def _():
                for h in range(HALVES):
                    up(t - chunks, h).wait_send()

            @pl.when(is_mid)
            def _():
                for h in range(HALVES):
                    over(t - chunks, h).wait_send()

        for group, items in enumerate(sums):

            @pl.when((t >= group * chunks) & (t < (group + 1) * chunks))
            def _():
                value = None
                for at, (start, size, mode) in enumerate(weights):
                    if members[at] == group:
                        weight(at, group, t).wait()
                        dot = dot_nt if mode == "nt" else dot_nn
                        term = dot(right_all[:, start : start + size], w_bufs[at][lax.rem(t, 3)])
                        value = term if value is None else value + term
                part[slot_of(t)] = value.astype(BF16)

        @pl.when(t < all_chunks)
        def _():
            @pl.when(is_end)
            def _():
                for h in range(HALVES):
                    up(t, h).start()

            load_weights(t + 2)

        @pl.when(is_mid & (t >= UP_LAG) & (t < all_chunks + UP_LAG))
        def _():
            c = t - UP_LAG
            slot = slot_of(c)
            for h in range(HALVES):
                here = rows_of(h)
                up(c, h).wait_recv()
                part[slot, here] = (part[slot, here].astype(F32) + first[slot, here].astype(F32)).astype(BF16)
                over(c, h).start()

        @pl.when(is_mid & (t >= OVER_LAG) & (t < all_chunks + OVER_LAG))
        def _():
            c = t - OVER_LAG
            slot = slot_of(c)
            for h in range(HALVES):
                here = rows_of(h)
                over(c, h).wait_recv()
                value = part[slot, here].astype(F32) + second[slot, here].astype(F32)
                out_ref[here, columns_of(c)] = value.astype(BF16)
                down(c, h).start()

        @pl.when(is_end & (t >= DOWN_LAG) & (t < all_chunks + DOWN_LAG))
        def _():
            for h in range(HALVES):
                down(t - DOWN_LAG, h).wait_recv()

        for at in range(left_count):

            @pl.when(t == max(step_of(flips_before[at]) - 2, at))
            def _():
                left_copy(at).wait()

                def turn(k, carry):
                    here = pl.ds(pl.multiple_of(k * block, block), block)
                    flip[at, here, :] = stage[:, here].T
                    return carry

                lax.fori_loop(0, flip.shape[1] // block, turn, 0)
                if at + 1 < left_count:
                    left_copy(at + 1).start()

        on_unit(t, first_stage)
        on_unit(t - 1, second_stage)
        on_unit(t - 1 - LAG, third_stage)
        on_unit(t - 1 - 2 * LAG, last_stage)
        if ending == "branch":

            @pl.when(t == chunks + DOWN_LAG)
            def _():
                for at in range(given):
                    given_copy(at).wait()

            @pl.when((t >= chunks + DOWN_LAG) & (t < chunks + DOWN_LAG + TILES))
            def _():
                branch_rows(t - chunks - DOWN_LAG)

            @pl.when(t == chunks + DOWN_LAG + TILES)
            def _():
                branch_end()

        return carry

    lax.fori_loop(0, max(step_of(units - 1) + 2 + 2 * LAG, all_chunks + DOWN_LAG), step, 0)
    if ending == "branch":
        made_copy(made - 1).start()
    else:
        for at in range(given):
            given_copy(at).wait()
        lax.fori_loop(0, TILES, token_rows, 0)
        made_copy(0).start()
        part_width = columns // peers
        for k in range(peers):
            here = slice(k * part_width, (k + 1) * part_width)
            gain_parts[k, 0:1, :] = acc[:, here]
            gain_parts[k, 1:2, :] = given_bufs[3][:, here]
        for k in range(1, peers):
            gain_copy(k).start()

    def finish(c, carry):
        @pl.when(is_mid)
        def _():
            for h in range(HALVES):
                down(c, h).wait_send()

        return carry

    lax.fori_loop(0, all_chunks, finish, 0)

    def finish_last(c, carry):
        @pl.when(is_end)
        def _():
            for h in range(HALVES):
                up(c, h).wait_send()

        @pl.when(is_mid)
        def _():
            for h in range(HALVES):
                over(c, h).wait_send()

        return carry

    lax.fori_loop(all_chunks - chunks, all_chunks, finish_last, 0)

    def settle(u, carry):
        for k in range(2):
            second_hop(u, k).wait_send()
        third_hop(u).wait_send()
        return carry

    lax.fori_loop(0, units, settle, 0)
    for u in (units - 2, units - 1):
        to_core(u).wait_send()
        for at in range(len(spans)):
            low, high = units_of(at)
            if low <= u < high:
                out_copy(at, u).wait()
    if ending == "tokens":
        gains = gain_parts[me]
        for k in range(1, peers):
            gain_copy(k).wait_recv()
            gains = gains + gain_come[k]
        made_bufs[1][...] = gains
        made_copy(1).start()
        for k in range(1, peers):
            gain_copy(k).wait_send()
    for at in range(made):
        made_copy(at).wait()


def exchange(lefts, rights, sums, flips_before, outs, spans, units, call_id, pace, ending, given, made, chunks=16):
    rows, depth = lefts[0].shape
    block = depth // 8
    placed, at = [], 0
    for _, source, size in rights:
        placed.append((at, source, size))
        at += size
    weights = [item[0] for group in sums for item in group]
    columns = weights[0].shape[0] if sums[0][0][3] == "nt" else weights[0].shape[1]
    width = columns // chunks
    sum_plan = [[item[1:] for item in group] for group in sums]
    plan = (len(lefts), placed, sum_plan, flips_before, spans, len(outs), units, chunks, *pace, ending, len(given), len(made))
    any_space = pl.BlockSpec(memory_space=pl.ANY)
    line_block = pltpu.VMEM((chunks, rows, width), BF16)
    peers = lax.axis_size("batch") * lax.axis_size("seq")
    kept = made[:-1] if ending == "branch" else made
    dma = pltpu.SemaphoreType.DMA
    all_chunks = chunks * len(sums)
    flops = sum(2 * rows * columns * size for group in sum_plan for _, size, _ in group) + 2 * rows * depth * at
    return pl.pallas_call(
        functools.partial(exchange_kernel, plan),
        out_shape=[jax.ShapeDtypeStruct(shape, F32) for shape in outs]
        + [jax.ShapeDtypeStruct(shape, kind) for shape, kind in made],
        in_specs=[any_space] * (len(lefts) + len(rights) + len(weights) + len(given)),
        out_specs=[any_space] * (len(outs) + len(made)),
        scratch_shapes=[
            pltpu.VMEM((rows, depth), BF16),
            pltpu.VMEM((len(lefts), depth, rows), BF16),
            pltpu.VMEM((rows, at), BF16),
            pltpu.VMEM((rows, columns * len(sums)), BF16),
        ]
        + [
            pltpu.VMEM((3, width, size) if mode == "nt" else (3, size, width), BF16)
            for group in sum_plan
            for _, size, mode in group
        ]
        + [
            line_block,
            line_block,
            line_block,
            pltpu.VMEM((2, 4, block, block), BF16),
            pltpu.VMEM((units, 4, block, block), BF16),
            pltpu.VMEM((units, 2, block, block), BF16),
            pltpu.VMEM((units, block, block), BF16),
            pltpu.VMEM((2, block, block), F32),
        ]
        + [pltpu.VMEM(value.shape, value.dtype) for value in given]
        + [pltpu.VMEM(shape, kind) for shape, kind in kept]
        + [
            pltpu.VMEM((1, depth), F32),
            pltpu.VMEM((peers, 2, depth // peers), F32),
            pltpu.VMEM((peers, 2, depth // peers), F32),
            dma((len(given),)),
            dma((len(made),)),
            dma((peers,)),
            dma((peers,)),
            dma((len(lefts),)),
            dma((len(rights),)),
            dma((len(weights), 3)),
            dma((3, HALVES, all_chunks)),
            dma((3, HALVES, all_chunks)),
            dma((units,)),
            dma((units,)),
            dma((2, units)),
            dma((2, units)),
            dma((units,)),
            dma((units,)),
            dma((len(spans), 2)),
        ],
        compiler_params=pltpu.CompilerParams(
            collective_id=call_id, has_side_effects=True, vmem_limit_bytes=62 << 20
        ),
        cost_estimate=pl.CostEstimate(flops=flops + (50 << 30), bytes_accessed=20 << 20, transcendentals=0),
        name=f"exchange_{call_id}",
    )(*lefts, *[right[0] for right in rights], *weights, *given)


def forward_kernel(
    mixed_ref, x_ref, gain_ref, wo_hbm, wg_hbm, wu_hbm, ga_hbm,
    branch_hbm, n_hbm, act_hbm, gg_hbm, gu_hbm,
    branch, n_ref, act_ref, gg_ref, gu_ref, ga_ref, gate_acc, up_acc, squares, wo_buf, w_buf, part, first, second,
    ga_sem, wo_sem, w_sem, ar_send, ar_recv, out_sem,
):
    chunks, rows, width = part.shape
    total_columns = branch.shape[1]
    place = lax.axis_index("mp")
    pair = place + 1 - 2 * lax.rem(place, 2)
    across = 3 - place
    is_mid = (place == 1) | (place == 2)
    is_end = (place == 0) | (place == 3)
    high = rows // HALVES
    deep = w_buf.shape[2]

    def columns_of(c):
        return pl.ds(pl.multiple_of(c * width, width), width)

    def rows_of(h):
        return slice(h * high, (h + 1) * high)

    def remote(source, target, kind, h, c, device):
        return pltpu.make_async_remote_copy(
            src_ref=source,
            dst_ref=target,
            send_sem=ar_send.at[kind, h, c],
            recv_sem=ar_recv.at[kind, h, c],
            device_id={"mp": device},
            device_id_type=MESH,
        )

    def up(c, h):
        return remote(part.at[c, rows_of(h)], first.at[c, rows_of(h)], 0, h, c, pair)

    def over(c, h):
        return remote(part.at[c, rows_of(h)], second.at[c, rows_of(h)], 1, h, c, across)

    def down(c, h):
        here = branch.at[rows_of(h), columns_of(c)]
        return remote(here, here, 2, h, c, pair)

    def out_weight(c):
        slot = lax.rem(c, 3)
        return pltpu.make_async_copy(wo_hbm.at[:, columns_of(c)], wo_buf.at[slot], wo_sem.at[slot])

    def deep_of(p):
        return pl.ds(pl.multiple_of(p * deep, deep), deep)

    def weight(at, p):
        slot = lax.rem(p, 3)
        source = (wg_hbm, wu_hbm)[at].at[deep_of(p), :]
        return pltpu.make_async_copy(source, w_buf.at[at, slot], w_sem.at[at, slot])

    ga_copy = pltpu.make_async_copy(ga_hbm, ga_ref, ga_sem.at[0])
    out_weight(0).start()
    out_weight(1).start()
    for p in range(2):
        for at in range(2):
            weight(at, p).start()
    ga_copy.start()
    barrier = pltpu.get_barrier_semaphore()
    pl.semaphore_signal(barrier, inc=1, device_id={"mp": pair}, device_id_type=MESH)

    @pl.when(is_mid)
    def _():
        pl.semaphore_signal(barrier, inc=1, device_id={"mp": across}, device_id_type=MESH)
        pl.semaphore_wait(barrier, 2)

    @pl.when(is_end)
    def _():
        pl.semaphore_wait(barrier, 1)

    squares[...] = jnp.zeros_like(squares)
    per_deep = deep // width

    def step(t, carry):
        @pl.when(t < chunks)
        def _():
            out_weight(t).wait()
            part[t] = dot_nn(mixed_ref[...], wo_buf[lax.rem(t, 3)]).astype(BF16)

            @pl.when(is_end)
            def _():
                for h in range(HALVES):
                    up(t, h).start()

            @pl.when(t + 2 < chunks)
            def _():
                out_weight(t + 2).start()

        @pl.when(is_mid & (t >= UP_LAG) & (t < chunks + UP_LAG))
        def _():
            c = t - UP_LAG
            for h in range(HALVES):
                here = rows_of(h)
                up(c, h).wait_recv()
                part[c, here] = (part[c, here].astype(F32) + first[c, here].astype(F32)).astype(BF16)
                over(c, h).start()

        @pl.when(is_mid & (t >= OVER_LAG) & (t < chunks + OVER_LAG))
        def _():
            c = t - OVER_LAG
            for h in range(HALVES):
                here = rows_of(h)
                over(c, h).wait_recv()
                value = part[c, here].astype(F32) + second[c, here].astype(F32)
                branch[here, columns_of(c)] = value.astype(BF16)
                down(c, h).start()

        @pl.when(is_end & (t >= DOWN_LAG))
        def _():
            for h in range(HALVES):
                down(t - DOWN_LAG, h).wait_recv()

        @pl.when((t >= DOWN_LAG) & (lax.rem(t - DOWN_LAG, per_deep) == per_deep - 1))
        def _():
            p = lax.div(t - DOWN_LAG, per_deep)
            here = deep_of(p)
            middle = x_ref[:, here].astype(F32) + branch[:, here].astype(F32)
            squares[...] += jnp.sum(middle * middle, axis=-1, keepdims=True)
            scaled = (middle * gain_ref[:, here]).astype(BF16)
            for at, acc in enumerate((gate_acc, up_acc)):
                weight(at, p).wait()
                value = dot_nn(scaled, w_buf[at, lax.rem(p, 3)])

                @pl.when(p == 0)
                def _():
                    acc[...] = value

                @pl.when(p > 0)
                def _():
                    acc[...] += value

            @pl.when((p + 2) * deep < total_columns)
            def _():
                for at in range(2):
                    weight(at, p + 2).start()

        return carry

    lax.fori_loop(0, chunks + DOWN_LAG, step, 0)
    ga_copy.wait()
    tile = rows // TILES
    outs = [(n_ref, n_hbm), (act_ref, act_hbm), (gg_ref, gg_hbm), (gu_ref, gu_hbm)]

    def out_copy(at, i):
        here = pl.ds(pl.multiple_of(i * tile, tile), tile)
        return pltpu.make_async_copy(outs[at][0].at[here, :], outs[at][1].at[here, :], out_sem.at[at, i])

    branch_copy = pltpu.make_async_copy(branch, branch_hbm, ga_sem.at[1])
    branch_copy.start()

    def rows_step(i, carry):
        here = pl.ds(pl.multiple_of(i * tile, tile), tile)
        scale = lax.rsqrt(squares[here, :1] * (1.0 / total_columns) + epsilon)
        middle = x_ref[here, :].astype(F32) + branch[here, :].astype(F32)
        n_ref[here, :] = (middle * scale * gain_ref[...]).astype(BF16)
        gate = gate_acc[here, :] * scale
        up_pre = up_acc[here, :] * scale
        grad = ga_ref[here, :].astype(F32)
        sigmoid = jax.nn.sigmoid(gate)
        swish = gate * sigmoid
        act_ref[here, :] = (swish * up_pre).astype(BF16)
        gu_ref[here, :] = (grad * swish).astype(BF16)
        gg_ref[here, :] = (grad * up_pre * sigmoid * (1.0 + gate * (1.0 - sigmoid))).astype(BF16)
        for at in range(4):
            out_copy(at, i).start()
        return carry

    lax.fori_loop(0, TILES, rows_step, 0)

    def finish(c, carry):
        @pl.when(is_end)
        def _():
            for h in range(HALVES):
                up(c, h).wait_send()

        @pl.when(is_mid)
        def _():
            for h in range(HALVES):
                over(c, h).wait_send()
                down(c, h).wait_send()

        return carry

    lax.fori_loop(0, chunks, finish, 0)

    def drain(i, carry):
        for at in range(4):
            out_copy(at, i).wait()
        return carry

    lax.fori_loop(0, TILES, drain, 0)
    branch_copy.wait()


def forward(mixed, tokens, gain, w_output, w_gate, w_up, grad_active, call_id, chunks=16, deep=256):
    rows, columns = tokens.shape
    hidden = w_gate.shape[1]
    width = columns // chunks
    vmem, any_space = pl.BlockSpec(memory_space=pltpu.VMEM), pl.BlockSpec(memory_space=pl.ANY)
    dma = pltpu.SemaphoreType.DMA
    shapes = [(rows, columns), (rows, columns), (rows, hidden), (rows, hidden), (rows, hidden)]
    line_block = pltpu.VMEM((chunks, rows, width), BF16)
    return pl.pallas_call(
        forward_kernel,
        in_specs=[vmem] * 3 + [any_space] * 4,
        out_specs=[any_space] * 5,
        out_shape=[jax.ShapeDtypeStruct(shape, BF16) for shape in shapes],
        scratch_shapes=[pltpu.VMEM(shape, BF16) for shape in shapes]
        + [
            pltpu.VMEM((rows, hidden), BF16),
            pltpu.VMEM((rows, hidden), F32),
            pltpu.VMEM((rows, hidden), F32),
            pltpu.VMEM((rows, PAIR), F32),
            pltpu.VMEM((3, mixed.shape[1], width), BF16),
            pltpu.VMEM((2, 3, deep, hidden), BF16),
            line_block,
            line_block,
            line_block,
            dma((2,)),
            dma((3,)),
            dma((2, 3)),
            dma((3, HALVES, chunks)),
            dma((3, HALVES, chunks)),
            dma((4, TILES)),
        ],
        compiler_params=pltpu.CompilerParams(
            collective_id=call_id, has_side_effects=True, vmem_limit_bytes=62 << 20
        ),
        name="forward",
    )(mixed, tokens, gain, w_output, w_gate, w_up, grad_active)


def final_kernel(gn_ref, x_ref, gm_ref, gain_ref, mlp_ref, out_ref, gains_ref, acc, parts, come, send_sem, recv_sem):
    seq, batch = lax.axis_index("seq"), lax.axis_index("batch")
    seq_count = lax.axis_size("seq")
    peers = parts.shape[0]
    block = parts.shape[2]
    me = batch * seq_count + seq

    def peer(k):
        there = lax.rem(me + k, peers)
        return there, {"batch": lax.div(there, seq_count), "seq": lax.rem(there, seq_count)}

    def copy(k):
        there, device = peer(k)
        return pltpu.make_async_remote_copy(
            src_ref=parts.at[there],
            dst_ref=come.at[k],
            send_sem=send_sem.at[k],
            recv_sem=recv_sem.at[k],
            device_id=device,
            device_id_type=MESH,
        )

    barrier = pltpu.get_barrier_semaphore()
    for k in range(1, peers):
        pl.semaphore_signal(barrier, inc=1, device_id=peer(k)[1], device_id_type=MESH)
    rows = x_ref.shape[0]
    tile = rows // 8
    gain = gain_ref[...]
    acc[...] = jnp.zeros_like(acc)

    def rows_step(i, carry):
        here = pl.ds(pl.multiple_of(i * tile, tile), tile)
        wide = x_ref[here, :].astype(F32)
        grad = gn_ref[here, :].astype(F32)
        scale = lax.rsqrt(jnp.mean(wide * wide, axis=-1, keepdims=True) + epsilon)
        scaled = grad * gain
        mean = jnp.mean(wide * scaled, axis=-1, keepdims=True)
        result = gm_ref[here, :] + scale * scaled - wide * (scale * scale * scale) * mean
        out_ref[here, :] = result.astype(BF16)
        acc[...] += jnp.sum(grad * wide * scale, axis=0, keepdims=True)
        return carry

    lax.fori_loop(0, 8, rows_step, 0)
    for k in range(peers):
        here = slice(k * block, (k + 1) * block)
        parts[k, 0:1, :] = acc[:, here]
        parts[k, 1:2, :] = mlp_ref[:, here]
    pl.semaphore_wait(barrier, peers - 1)
    for k in range(1, peers):
        copy(k).start()
    total = parts[me]
    for k in range(1, peers):
        copy(k).wait_recv()
        total = total + come[k]
    gains_ref[...] = total
    for k in range(1, peers):
        copy(k).wait_send()


def final(grad_normed, tokens, grad_middle, gain, mlp_part, call_id):
    rows, width = tokens.shape
    peers = lax.axis_size("batch") * lax.axis_size("seq")
    block = width // peers
    vmem = pl.BlockSpec(memory_space=pltpu.VMEM)
    return pl.pallas_call(
        final_kernel,
        out_shape=[jax.ShapeDtypeStruct((rows, width), BF16), jax.ShapeDtypeStruct((2, block), F32)],
        in_specs=[vmem] * 5,
        out_specs=[vmem, vmem],
        scratch_shapes=[
            pltpu.VMEM((1, width), F32),
            pltpu.VMEM((peers, 2, block), F32),
            pltpu.VMEM((peers, 2, block), F32),
            pltpu.SemaphoreType.DMA((peers,)),
            pltpu.SemaphoreType.DMA((peers,)),
        ],
        compiler_params=pltpu.CompilerParams(collective_id=call_id, has_side_effects=True),
        name="final",
    )(grad_normed, tokens, grad_middle, gain, mlp_part)


def settle_kernel(places, *refs):
    count = len(places)
    sources, targets = refs[:count], refs[count : -count - 2]
    bufs, load_sem, store_sem = refs[-count - 2 : -2], refs[-2], refs[-1]

    def load(at):
        return pltpu.make_async_copy(sources[at], bufs[at], load_sem.at[at])

    def store(at):
        index, row = places[at]
        target = targets[index].at[row : row + bufs[at].shape[0], :]
        return pltpu.make_async_copy(bufs[at], target, store_sem.at[at])

    for at in range(count):
        load(at).start()
    for at in range(count):
        load(at).wait()
        store(at).start()
    for at in range(count):
        store(at).wait()


def settle(groups):
    places, shapes, arrays = [], [], []
    for index, group in enumerate(groups):
        row = 0
        for array in group:
            places.append((index, row))
            arrays.append(array)
            row += array.shape[0]
        shapes.append(jax.ShapeDtypeStruct((row, group[0].shape[1]), group[0].dtype))
    any_space = pl.BlockSpec(memory_space=pl.ANY)
    dma = pltpu.SemaphoreType.DMA
    return pl.pallas_call(
        functools.partial(settle_kernel, places),
        in_specs=[any_space] * len(arrays),
        out_specs=[any_space] * len(groups),
        out_shape=shapes,
        scratch_shapes=[pltpu.VMEM(array.shape, array.dtype) for array in arrays]
        + [dma((len(arrays),)), dma((len(arrays),))],
        compiler_params=pltpu.CompilerParams(vmem_limit_bytes=62 << 20),
        name="settle",
    )(*arrays)


def scatter_sum(left, right):
    rows, depth = left.shape
    columns = right.shape[1]
    batch_count = lax.axis_size("batch")
    seq_index = lax.axis_index("seq")
    core, chip = seq_index % 2, seq_index // 2
    block = depth // (4 * batch_count)
    split = left.reshape(rows, batch_count, 2, 2, block)
    size = lax.axis_size("seq")

    def product(at):
        taken = lax.dynamic_index_in_dim(split, at, 3, keepdims=False).reshape(rows, depth // 2)
        return dot_tn(taken, right)

    away = product(1 - core).astype(BF16)
    arrived = lax.ppermute(away, "seq", [(s, s ^ 1) for s in range(size)])
    kept = (product(core) + arrived.astype(F32)).astype(BF16)
    kept = kept.reshape(batch_count, 2, block, columns)
    half = columns // 2

    def over_chip(values, axis):
        sent = lax.dynamic_index_in_dim(values, 1 - chip, axis, keepdims=False)
        stay = lax.dynamic_index_in_dim(values, chip, axis, keepdims=False)
        came = lax.ppermute(sent, "seq", [(s, s ^ 2) for s in range(size)])
        return stay.astype(F32) + came.astype(F32)

    def over_batch(values):
        if batch_count == 2:
            here = lax.axis_index("batch")
            sent = lax.dynamic_index_in_dim(values, 1 - here, 0, keepdims=False)
            stay = lax.dynamic_index_in_dim(values, here, 0, keepdims=False)
            came = lax.ppermute(sent, "batch", [(0, 1), (1, 0)])
            return stay.astype(F32) + came.astype(F32)
        return lax.psum_scatter(values, "batch", scatter_dimension=0, tiled=False).astype(F32)

    one = over_batch(over_chip(kept[..., :half], 1).astype(BF16))
    two = over_chip(over_batch(kept[..., half:]).astype(BF16), 0)
    return jnp.concatenate([one, two], axis=1)


def local(
    tokens, segment_ids, attn_gain, w_query, w_key, w_value, w_output, mlp_gain, w_gate, w_up, w_down, cotangent
):
    rows, width = tokens.shape
    seq_count = lax.axis_size("seq")
    seq_index = lax.axis_index("seq")
    segments = segment_ids[0]
    first_row = seq_index * rows
    reach = LONGEST // rows
    cos, sin = rope_tables(segments, first_row, rows)
    row_segment = lax.dynamic_slice_in_dim(segments, first_row, rows, 0)[None, :]
    padded = jnp.concatenate([jnp.full((LONGEST,), -1, jnp.int32), segments])
    key_segment = lax.dynamic_slice_in_dim(padded, first_row, rows + LONGEST, 0)[:, None]

    normed, queries, key_value, grad_active = project(
        tokens, attn_gain[None, :], w_query, w_key, w_value, cos, sin, cotangent, w_down, 5
    )
    key_value = key_value.reshape(3 * rows, 2 * PAIR)
    mixed, logs = attend(queries, key_value, key_segment, row_segment)
    branch_low, normed_two, active, grad_gate_low, grad_up_low = forward(
        mixed, tokens, mlp_gain[None, :], w_output, w_gate, w_up, grad_active, 1
    )
    wide = tokens.astype(F32)
    middle = wide + branch_low.astype(F32)
    fused = lax.axis_size("batch") == 2
    hidden = w_gate.shape[1]
    unit = width // 8
    early = hidden * 5 // 8 // unit * unit
    if fused:
        grad_gate, grad_up, grad_down_one, grad_middle, grad_branch, grad_mixed, grad_mlp_gain, mlp_out = exchange(
            [normed_two, cotangent],
            [(grad_gate_low, 0, hidden), (grad_up_low, 0, hidden), (active, 0, hidden)],
            [
                [(w_gate, 0, hidden, "nt"), (w_up, hidden, hidden, "nt")],
                [(w_down, 2 * hidden, hidden, "nn")],
            ],
            (0, 2 * hidden // unit),
            [(unit, hidden), (unit, hidden), (early, unit)],
            [
                ("plain", 0, 0, 0, hidden),
                ("plain", 1, 0, hidden, hidden),
                ("turned", 2, 0, 2 * hidden, early),
            ],
            (2 * hidden + early) // unit,
            2,
            (3, 2),
            "branch",
            [tokens, branch_low, mlp_gain[None, :], w_output],
            [
                ((rows, width), F32),
                ((rows, width), BF16),
                ((rows, mixed.shape[1]), BF16),
                ((1, width), F32),
                ((rows, width), BF16),
            ],
        )
    else:
        grad_normed_two = line_sum([(grad_gate_low, w_gate, "nt"), (grad_up_low, w_up, "nt")], 2)
        grad_gate = scatter_sum(normed_two, grad_gate_low)
        grad_up = scatter_sum(normed_two, grad_up_low)
        mlp_out = lax.psum(dot_nn(active, w_down).astype(BF16), "mp")
        grad_normed_two = grad_normed_two.astype(F32)
        scaled_two = grad_normed_two * mlp_gain
        scale_two = lax.rsqrt(jnp.mean(middle * middle, axis=-1, keepdims=True) + epsilon)
        grad_middle = (
            cotangent.astype(F32)
            + scale_two * scaled_two
            - middle
            * (scale_two * scale_two * scale_two)
            * jnp.mean(middle * scaled_two, axis=-1, keepdims=True)
        )
        grad_mlp_gain = jnp.sum(grad_normed_two * middle * scale_two, axis=0)[None, :]
        grad_branch = grad_middle.astype(BF16)
        grad_mixed = dot_nt(grad_branch, w_output).astype(BF16)
    output = (middle + mlp_out.astype(F32)).astype(BF16)

    grad_query_pre, dfar, dnear, down = attend_back(
        queries, key_value, key_segment, row_segment, mixed, grad_mixed, logs, cos, sin
    )
    from_near = lax.ppermute(dnear, "seq", [(s + 1, s) for s in range(seq_count - 1)])
    from_far = lax.ppermute(dfar, "seq", [(s + 2, s) for s in range(seq_count - 2)])
    grad_pair = down + from_near.astype(F32) + from_far.astype(F32)
    grad_keys = jnp.concatenate([grad_pair[:, :HS], grad_pair[:, PAIR : PAIR + HS]], axis=1)
    grad_values = jnp.concatenate([grad_pair[:, HS:PAIR], grad_pair[:, PAIR + HS :]], axis=1)
    quarter = HS // 2
    swapped = jnp.concatenate(
        [grad_keys[:, (at ^ 1) * quarter : ((at ^ 1) + 1) * quarter] for at in range(4)], axis=1
    )
    grad_key_pre = (grad_keys * cos - swapped * sin).astype(BF16)
    grad_value_pre = grad_values.astype(BF16)

    query_width = grad_query_pre.shape[1]
    if fused:
        late, mixed_width = hidden - early, mixed.shape[1]
        query_at = late + mixed_width
        key_at = query_at + query_width
        grad_down_two, grad_output, grad_query, grad_key, grad_value, grad_tokens, gains = exchange(
            [cotangent, grad_branch, normed],
            [
                (active, early, late),
                (mixed, 0, mixed_width),
                (grad_query_pre, 0, query_width),
                (grad_key_pre, 0, PAIR),
                (grad_value_pre, 0, PAIR),
            ],
            [
                [
                    (w_query, query_at, query_width, "nt"),
                    (w_key, key_at, PAIR, "nt"),
                    (w_value, key_at + PAIR, PAIR, "nt"),
                ]
            ],
            (0, late // unit, query_at // unit),
            [(late, unit), (mixed_width, unit), (unit, query_width), (unit, PAIR), (unit, PAIR)],
            [
                ("turned", 0, 0, 0, late),
                ("turned", 1, 0, late, mixed_width),
                ("plain", 2, 0, query_at, query_width),
                ("plain", 3, 0, key_at, PAIR),
                ("plain", 4, 0, key_at + PAIR, PAIR),
            ],
            (key_at + 2 * PAIR) // unit,
            3,
            (2, 1),
            "tokens",
            [tokens, grad_middle, attn_gain[None, :], grad_mlp_gain],
            [((rows, width), BF16), ((2, unit), F32)],
        )
        grad_gate, grad_up, grad_down, grad_output, grad_query, grad_key, grad_value, grad_tokens = settle(
            [
                [grad_gate],
                [grad_up],
                [grad_down_one, grad_down_two],
                [grad_output],
                [grad_query],
                [grad_key],
                [grad_value],
                [grad_tokens],
            ]
        )
    else:
        grad_down = scatter_sum(cotangent, active).T
        grad_output = scatter_sum(grad_branch, mixed).T
        grad_qkv = scatter_sum(normed, jnp.concatenate([grad_query_pre, grad_key_pre, grad_value_pre], axis=1))
        grad_query = grad_qkv[:, :query_width]
        grad_key = grad_qkv[:, query_width : query_width + PAIR]
        grad_value = grad_qkv[:, query_width + PAIR :]
        grad_normed = line_sum(
            [(grad_query_pre, w_query, "nt"), (grad_key_pre, w_key, "nt"), (grad_value_pre, w_value, "nt")], 3
        )
        grad_tokens, gains = final(grad_normed, tokens, grad_middle, attn_gain[None, :], grad_mlp_gain, 4)
    return (
        output,
        grad_tokens,
        gains[0],
        grad_query,
        grad_key,
        grad_value,
        grad_output,
        gains[1],
        grad_gate,
        grad_up,
        grad_down,
    )


def solution(mesh):
    tokens_spec = P(("batch", "seq"), None)
    in_specs = (
        tokens_spec,
        P("batch", None),
        P(),
        P(None, "mp"),
        P(None, "mp"),
        P(None, "mp"),
        P("mp", None),
        P(),
        P(None, "mp"),
        P(None, "mp"),
        P("mp", None),
        tokens_spec,
    )
    row_split = P(("batch", "seq"), "mp")
    column_split = P("mp", ("batch", "seq"))
    out_specs = (
        tokens_spec,
        tokens_spec,
        P(("batch", "seq")),
        row_split,
        row_split,
        row_split,
        column_split,
        P(("batch", "seq")),
        row_split,
        row_split,
        column_split,
    )
    return jax.shard_map(local, mesh=mesh, in_specs=in_specs, out_specs=out_specs, check_vma=False)
```

```python
import functools
import math

import jax
import jax.numpy as jnp
from jax import lax
from jax.experimental import pallas as pl
from jax.experimental.pallas import tpu as pltpu
from jax.sharding import PartitionSpec as P

HS = 64
PAIR = 2 * HS
LONGEST = 1024
rope_base = 500000.0
epsilon = 1e-05
masked_score = -1e30
MESH = pl.DeviceIdType.MESH
F32 = jnp.float32
BF16 = jnp.bfloat16


def dot_nn(left, right):
    return lax.dot_general(left, right, (((1,), (0,)), ((), ())), preferred_element_type=F32)


def dot_nt(left, right):
    return lax.dot_general(left, right, (((1,), (1,)), ((), ())), preferred_element_type=F32)


def dot_tn(left, right):
    return lax.dot_general(left, right, (((0,), (0,)), ((), ())), preferred_element_type=F32)


def lanes_of(values):
    return lax.broadcasted_iota(jnp.int32, values.shape, 1)


def swap_halves(values):
    ahead = pltpu.roll(values, PAIR - HS // 2, 1)
    behind = pltpu.roll(values, HS // 2, 1)
    return jnp.where(lanes_of(values) % HS < HS // 2, ahead, behind)


def rope_tables(segments, first_row, rows):
    row_segment = lax.dynamic_slice_in_dim(segments, first_row, rows, 0)
    doc_start = jnp.sum((segments[None, :] < row_segment[:, None]).astype(jnp.int32), axis=1)
    place = (first_row + jnp.arange(rows, dtype=jnp.int32) - doc_start).astype(F32)
    lane = jnp.arange(PAIR, dtype=jnp.int32)
    frequency = jnp.exp((lane % (HS // 2)).astype(F32) * (-2.0 * math.log(rope_base) / HS))
    angles = place[:, None] * frequency[None, :]
    sign = jnp.where(lane % HS < HS // 2, -1.0, 1.0)
    return jnp.cos(angles), jnp.sin(angles) * sign[None, :]


def project_kernel(
    x_ref, gain_ref, wk_ref, wv_ref, cos_ref, sin_ref, cot_hbm, wq_hbm, wd_hbm,
    n_hbm, q_hbm, kv_hbm, ga_hbm,
    n_ref, q_ref, kv_ref, ga_ref, cot_ref, wq_ref, wd_ref, load_sem, wd_sem, send_sem, recv_sem, out_sem,
):
    rows = x_ref.shape[0]
    seq, seq_count = lax.axis_index("seq"), lax.axis_size("seq")
    hidden = wd_hbm.shape[0]
    width = wd_ref.shape[1]
    chunks = hidden // width
    block = rows // 2
    loads = [
        pltpu.make_async_copy(wq_hbm, wq_ref, load_sem.at[0]),
        pltpu.make_async_copy(cot_hbm, cot_ref, load_sem.at[1]),
    ]

    def weight(c):
        slot = lax.rem(c, 3)
        here = pl.ds(pl.multiple_of(c * width, width), width)
        return pltpu.make_async_copy(wd_hbm.at[here, :], wd_ref.at[slot], wd_sem.at[slot])

    def out_copy(at):
        source = (n_ref, q_ref, kv_ref, ga_ref)[at]
        return pltpu.make_async_copy(source, (n_hbm, q_hbm, kv_hbm, ga_hbm)[at], out_sem.at[at])

    def send(away):
        return pltpu.make_async_remote_copy(
            src_ref=kv_ref.at[2],
            dst_ref=kv_ref.at[2 - away],
            send_sem=send_sem.at[away],
            recv_sem=recv_sem.at[away],
            device_id={"seq": lax.rem(seq + away, seq_count)},
            device_id_type=MESH,
        )

    for load in loads:
        load.start()
    weight(0).start()
    weight(1).start()
    for away in (1, 2):

        @pl.when(seq < away)
        def _():
            kv_ref[2 - away] = jnp.zeros(kv_ref.shape[1:], BF16)

    barrier = pltpu.get_barrier_semaphore()
    for away in range(1, seq_count):
        there = lax.rem(seq + away, seq_count)
        pl.semaphore_signal(barrier, inc=1, device_id={"seq": there}, device_id_type=MESH)

    for half in range(2):
        here = slice(half * block, (half + 1) * block)
        cos, sin = cos_ref[here, :], sin_ref[here, :]
        wide = x_ref[here, :].astype(F32)
        scale = lax.rsqrt(jnp.mean(wide * wide, axis=-1, keepdims=True) + epsilon)
        normed = (wide * scale * gain_ref[...]).astype(BF16)
        n_ref[here, :] = normed
        keys = dot_nn(normed, wk_ref[...])
        keys = keys * cos + swap_halves(keys) * sin
        values = dot_nn(normed, wv_ref[...])
        low_half = lanes_of(keys) < HS
        kv_ref[2, here, :PAIR] = jnp.where(low_half, keys, pltpu.roll(values, HS, 1)).astype(BF16)
        kv_ref[2, here, PAIR:] = jnp.where(low_half, pltpu.roll(keys, HS, 1), values).astype(BF16)
    pl.semaphore_wait(barrier, seq_count - 1)
    for away in (1, 2):

        @pl.when(seq + away < seq_count)
        def _():
            send(away).start()

    out_copy(0).start()
    for load in loads:
        load.wait()
    for half in range(2):
        here = slice(half * block, (half + 1) * block)
        cos, sin = cos_ref[here, :], sin_ref[here, :]
        queries = dot_nn(n_ref[here, :], wq_ref[...])
        for start in range(0, queries.shape[1], PAIR):
            part = queries[:, start : start + PAIR]
            q_ref[here, start : start + PAIR] = (part * cos + swap_halves(part) * sin).astype(BF16)
    out_copy(1).start()

    def step(c, carry):
        weight(c).wait()

        @pl.when(c + 2 < chunks)
        def _():
            weight(c + 2).start()

        here = pl.ds(pl.multiple_of(c * width, width), width)
        ga_ref[:, here] = dot_nt(cot_ref[...], wd_ref[lax.rem(c, 3)]).astype(BF16)
        return carry

    lax.fori_loop(0, chunks, step, 0)
    out_copy(3).start()
    for away in (1, 2):

        @pl.when(seq >= away)
        def _():
            send(away).wait_recv()

    out_copy(2).start()
    for away in (1, 2):

        @pl.when(seq + away < seq_count)
        def _():
            send(away).wait_send()

    for at in range(4):
        out_copy(at).wait()


def project(tokens, gain, w_query, w_key, w_value, cos, sin, cotangent, w_down, call_id):
    rows, width = tokens.shape
    columns, hidden = w_query.shape[1], w_down.shape[0]
    chunk = 256
    vmem, any_space = pl.BlockSpec(memory_space=pltpu.VMEM), pl.BlockSpec(memory_space=pl.ANY)
    shapes = [(rows, width), (rows, columns), (3, rows, 2 * PAIR), (rows, hidden)]
    dma = pltpu.SemaphoreType.DMA
    return pl.pallas_call(
        project_kernel,
        in_specs=[vmem] * 6 + [any_space] * 3,
        out_specs=[any_space] * 4,
        out_shape=[jax.ShapeDtypeStruct(shape, BF16) for shape in shapes],
        scratch_shapes=[pltpu.VMEM(shape, BF16) for shape in shapes]
        + [
            pltpu.VMEM((rows, width), BF16),
            pltpu.VMEM(w_query.shape, BF16),
            pltpu.VMEM((3, chunk, width), BF16),
            dma((2,)),
            dma((3,)),
            dma((3,)),
            dma((3,)),
            dma((4,)),
        ],
        compiler_params=pltpu.CompilerParams(
            collective_id=call_id, has_side_effects=True, vmem_limit_bytes=62 << 20
        ),
        name="project",
    )(tokens, gain, w_key, w_value, cos, sin, cotangent, w_query, w_down)


def write_bias(bias_ref, key_ref, row_ref):
    keys, rows = bias_ref.shape
    key_place = lax.broadcasted_iota(jnp.int32, (keys, rows), 0) - (keys - rows)
    row_place = lax.broadcasted_iota(jnp.int32, (keys, rows), 1)
    allowed = (key_ref[...] == row_ref[...]) & (key_place <= row_place)
    bias_ref[...] = jnp.where(allowed, 0.0, masked_score)


def attend_kernel(q_ref, kv_ref, key_ref, row_ref, out_ref, log_ref, bias_ref):
    @pl.when(pl.program_id(0) == 0)
    def _():
        write_bias(bias_ref, key_ref, row_ref)

    key_value = kv_ref[...]
    flipped = key_value.T
    q_flipped = (q_ref[...].astype(F32) * HS ** (-0.5)).astype(BF16).T
    outs = []
    for head in range(2):
        scores = dot_nn(key_value[:, :HS], q_flipped[head * HS : (head + 1) * HS, :]) + bias_ref[...]
        top = jnp.max(scores, axis=0, keepdims=True)
        powers = jnp.exp(scores - top)
        total = jnp.sum(powers, axis=0, keepdims=True)
        mixed = dot_nn(flipped[HS:, :], powers.astype(BF16))
        outs.append(mixed / total)
        log_ref[0, head : head + 1, :] = top + jnp.log(total)
    out_ref[...] = jnp.concatenate(outs, axis=0).T.astype(BF16)


def attend(queries, key_value, key_segment, row_segment):
    rows, width = queries.shape
    pairs = width // PAIR
    per_group = pairs // 2
    pair_tile = pl.BlockSpec((rows, PAIR), lambda p: (0, p))
    kv_tile = pl.BlockSpec((3 * rows, PAIR), lambda p: (0, p // per_group))
    return pl.pallas_call(
        attend_kernel,
        grid=(pairs,),
        in_specs=[
            pair_tile,
            kv_tile,
            pl.BlockSpec(key_segment.shape, lambda p: (0, 0)),
            pl.BlockSpec(row_segment.shape, lambda p: (0, 0)),
        ],
        out_specs=[pair_tile, pl.BlockSpec((1, 2, rows), lambda p: (p, 0, 0))],
        out_shape=[
            jax.ShapeDtypeStruct((rows, width), BF16),
            jax.ShapeDtypeStruct((pairs, 2, rows), F32),
        ],
        scratch_shapes=[pltpu.VMEM((3 * rows, rows), F32)],
        cost_estimate=pl.CostEstimate(
            flops=16 << 30, bytes_accessed=4 << 20, transcendentals=3 * rows * rows * 2 * pairs
        ),
        name="attend",
    )(queries, key_value, key_segment, row_segment)


def attend_back_kernel(
    q_ref, kv_ref, key_ref, row_ref, out_ref, grad_ref, log_ref, cos_ref, sin_ref,
    dq_ref, dk_ref, dv_ref, bias_ref, dkv_ref, own_ref, sent_ref, come_ref, send_sem, recv_sem, per_group,
):
    step = pl.program_id(0)
    seq, seq_count = lax.axis_index("seq"), lax.axis_size("seq")
    barrier = pltpu.get_barrier_semaphore()

    def back(group, away):
        return pltpu.make_async_remote_copy(
            src_ref=sent_ref.at[group, 2 - away],
            dst_ref=come_ref.at[group, 2 - away],
            send_sem=send_sem.at[group, 2 - away],
            recv_sem=recv_sem.at[group, 2 - away],
            device_id={"seq": lax.rem(seq + seq_count - away, seq_count)},
            device_id_type=MESH,
        )

    @pl.when(step == 0)
    def _():
        for away in range(1, seq_count):
            there = lax.rem(seq + away, seq_count)
            pl.semaphore_signal(barrier, inc=1, device_id={"seq": there}, device_id_type=MESH)
        write_bias(bias_ref, key_ref, row_ref)

    rows = q_ref.shape[0]
    key_value = kv_ref[...]
    flipped = key_value[:, :].T
    scaled = (q_ref[...].astype(F32) * HS ** (-0.5)).astype(BF16)
    q_flipped = scaled.T
    grad = grad_ref[...]
    grad_flipped = grad.T
    product = (out_ref[...].astype(F32) * grad.astype(F32)).T
    dqs, dkey, dvalue = [], None, None
    for head in range(2):
        here = slice(head * HS, (head + 1) * HS)
        scores = dot_nn(key_value[:, :HS], q_flipped[here, :]) + bias_ref[...]
        shares = jnp.exp(scores - log_ref[0, head : head + 1, :])
        grad_shares = dot_nn(key_value[:, HS:], grad_flipped[here, :])
        delta = jnp.sum(product[here, :], axis=0, keepdims=True)
        grad_scores = (shares * (grad_shares - delta)).astype(BF16)
        value_part = dot_nn(shares.astype(BF16), grad[:, here])
        key_part = dot_nn(grad_scores, scaled[:, here])
        dvalue = value_part if dvalue is None else dvalue + value_part
        dkey = key_part if dkey is None else dkey + key_part
        dqs.append(dot_nn(flipped[:HS, :], grad_scores))
    dq = jnp.concatenate(dqs, axis=0).T * HS ** (-0.5)
    dq_ref[...] = (dq * cos_ref[...] - swap_halves(dq) * sin_ref[...]).astype(BF16)
    both = jnp.concatenate([dkey, dvalue], axis=1)

    @pl.when(step % per_group == 0)
    def _():
        dkv_ref[...] = both

    @pl.when(step % per_group != 0)
    def _():
        dkv_ref[...] += both

    for group in range(2):

        @pl.when(step == (group + 1) * per_group - 1)
        def _():
            sent_ref[group, 0] = dkv_ref[:rows, :].astype(BF16)
            sent_ref[group, 1] = dkv_ref[rows : 2 * rows, :].astype(BF16)
            own_ref[group] = dkv_ref[2 * rows :, :]
            if group == 0:
                pl.semaphore_wait(barrier, seq_count - 1)
            for away in (1, 2):

                @pl.when(seq >= away)
                def _():
                    back(group, away).start()

    @pl.when(step == 2 * per_group - 1)
    def _():
        for group in range(2):
            for away in (1, 2):

                @pl.when(seq + away < seq_count)
                def _():
                    back(group, away).wait_recv()
                    own_ref[group] += come_ref[group, 2 - away].astype(F32)

        one, two = own_ref[0], own_ref[1]
        low_half = lanes_of(one) < HS
        keys = jnp.where(low_half, one, pltpu.roll(two, HS, 1))
        dk_ref[...] = (keys * cos_ref[...] - swap_halves(keys) * sin_ref[...]).astype(BF16)
        dv_ref[...] = jnp.where(low_half, pltpu.roll(one, HS, 1), two).astype(BF16)
        for group in range(2):
            for away in (1, 2):

                @pl.when(seq >= away)
                def _():
                    back(group, away).wait_send()


def attend_back(queries, key_value, key_segment, row_segment, mixed, grad, logs, cos, sin, call_id):
    rows, width = queries.shape
    pairs = width // PAIR
    per_group = pairs // 2
    pair_tile = pl.BlockSpec((rows, PAIR), lambda p: (0, p))
    whole = pl.BlockSpec((rows, PAIR), lambda p: (0, 0))
    wide_tile = pl.BlockSpec((3 * rows, PAIR), lambda p: (0, p // per_group))
    full = lambda array: pl.BlockSpec(array.shape, lambda p: (0, 0))
    return pl.pallas_call(
        functools.partial(attend_back_kernel, per_group=per_group),
        grid=(pairs,),
        in_specs=[
            pair_tile,
            wide_tile,
            full(key_segment),
            full(row_segment),
            pair_tile,
            pair_tile,
            pl.BlockSpec((1, 2, rows), lambda p: (p, 0, 0)),
            full(cos),
            full(sin),
        ],
        out_specs=[pair_tile, whole, whole],
        out_shape=[
            jax.ShapeDtypeStruct((rows, width), BF16),
            jax.ShapeDtypeStruct((rows, PAIR), BF16),
            jax.ShapeDtypeStruct((rows, PAIR), BF16),
        ],
        scratch_shapes=[
            pltpu.VMEM((3 * rows, rows), F32),
            pltpu.VMEM((3 * rows, PAIR), F32),
            pltpu.VMEM((2, rows, PAIR), F32),
            pltpu.VMEM((2, 2, rows, PAIR), BF16),
            pltpu.VMEM((2, 2, rows, PAIR), BF16),
            pltpu.SemaphoreType.DMA((2, 2)),
            pltpu.SemaphoreType.DMA((2, 2)),
        ],
        compiler_params=pltpu.CompilerParams(collective_id=call_id, has_side_effects=True),
        cost_estimate=pl.CostEstimate(
            flops=40 << 30, bytes_accessed=6 << 20, transcendentals=3 * rows * rows * 2 * pairs
        ),
        name="attend_back",
    )(queries, key_value, key_segment, row_segment, mixed, grad, logs, cos, sin)


def line_sum_kernel(modes, chunks, *refs):
    count = len(modes)
    a_refs, w_refs, out_ref = refs[:count], refs[count : 2 * count], refs[2 * count]
    rest = refs[2 * count + 1 :]
    w_bufs = rest[:count]
    part, first, second, total, w_sem, send_sem, recv_sem = rest[count:]
    width = part.shape[2]
    place = lax.axis_index("mp")
    pair = place + 1 - 2 * lax.rem(place, 2)
    across = 3 - place
    is_mid = (place == 1) | (place == 2)
    is_end = (place == 0) | (place == 3)

    def weight(at, c):
        if modes[at] == "nt":
            source = w_refs[at].at[pl.ds(pl.multiple_of(c * width, width), width), :]
        else:
            source = w_refs[at].at[:, pl.ds(pl.multiple_of(c * width, width), width)]
        return pltpu.make_async_copy(source, w_bufs[at].at[c], w_sem.at[at, c])

    def remote(kind, source, target, c, device):
        return pltpu.make_async_remote_copy(
            src_ref=source.at[c],
            dst_ref=target.at[c],
            send_sem=send_sem.at[kind, c],
            recv_sem=recv_sem.at[kind, c],
            device_id={"mp": device},
            device_id_type=MESH,
        )

    def up(c):
        return remote(0, part, first, c, pair)

    def over(c):
        return remote(1, part, second, c, across)

    def down(c):
        return remote(2, total, total, c, pair)

    def start_weights(c, carry):
        for at in range(count):
            weight(at, c).start()
        return carry

    lax.fori_loop(0, chunks, start_weights, 0)
    barrier = pltpu.get_barrier_semaphore()
    pl.semaphore_signal(barrier, inc=1, device_id={"mp": pair}, device_id_type=MESH)

    @pl.when(is_mid)
    def _():
        pl.semaphore_signal(barrier, inc=1, device_id={"mp": across}, device_id_type=MESH)
        pl.semaphore_wait(barrier, 2)

    @pl.when(is_end)
    def _():
        pl.semaphore_wait(barrier, 1)

    def step(t, carry):
        @pl.when(t < chunks)
        def _():
            value = None
            for at in range(count):
                weight(at, t).wait()
                dot = dot_nt if modes[at] == "nt" else dot_nn
                term = dot(a_refs[at][...], w_bufs[at][t])
                value = term if value is None else value + term
            part[t] = value.astype(BF16)

            @pl.when(is_end)
            def _():
                up(t).start()

        @pl.when(is_mid & (t >= 1) & (t < chunks + 1))
        def _():
            c = t - 1
            up(c).wait_recv()
            part[c] = (part[c].astype(F32) + first[c].astype(F32)).astype(BF16)
            over(c).start()

        @pl.when(is_mid & (t >= OVER_LAG))
        def _():
            c = t - OVER_LAG
            over(c).wait_recv()
            total[c] = (part[c].astype(F32) + second[c].astype(F32)).astype(BF16)
            down(c).start()

        return carry

    lax.fori_loop(0, chunks + OVER_LAG, step, 0)

    def finish(c, carry):
        @pl.when(is_end)
        def _():
            up(c).wait_send()
            down(c).wait_recv()

        @pl.when(is_mid)
        def _():
            over(c).wait_send()
            down(c).wait_send()

        out_ref[:, pl.ds(pl.multiple_of(c * width, width), width)] = total[c]
        return carry

    lax.fori_loop(0, chunks, finish, 0)


def line_sum(pairs, call_id, chunks=16):
    lefts = [left for left, _, _ in pairs]
    rights = [right for _, right, _ in pairs]
    modes = tuple(mode for _, _, mode in pairs)
    rows = lefts[0].shape[0]
    columns = rights[0].shape[0] if modes[0] == "nt" else rights[0].shape[1]
    width = columns // chunks
    count = len(pairs)
    bufs = [
        pltpu.VMEM((chunks, width, left.shape[1]) if mode == "nt" else (chunks, left.shape[1], width), BF16)
        for left, _, mode in pairs
    ]
    flops = sum(2 * rows * columns * left.shape[1] for left in lefts)
    moved = sum(right.size * 2 for right in rights)
    block = pltpu.VMEM((chunks, rows, width), BF16)
    return pl.pallas_call(
        functools.partial(line_sum_kernel, modes, chunks),
        out_shape=jax.ShapeDtypeStruct((rows, columns), BF16),
        in_specs=[pl.BlockSpec(memory_space=pltpu.VMEM)] * count
        + [pl.BlockSpec(memory_space=pl.ANY)] * count,
        out_specs=pl.BlockSpec(memory_space=pltpu.VMEM),
        scratch_shapes=bufs
        + [
            block,
            block,
            block,
            block,
            pltpu.SemaphoreType.DMA((count, chunks)),
            pltpu.SemaphoreType.DMA((3, chunks)),
            pltpu.SemaphoreType.DMA((3, chunks)),
        ],
        compiler_params=pltpu.CompilerParams(collective_id=call_id, has_side_effects=True),
        cost_estimate=pl.CostEstimate(
            flops=flops + (40 << 30), bytes_accessed=moved, transcendentals=0
        ),
        name=f"line_sum_{call_id}",
    )(*lefts, *rights)

LAG = 3
UP_LAG = 1
OVER_LAG = 3
DOWN_LAG = 8
HALVES = 1
TILES = 8


def exchange_kernel(plan, *refs):
    left_count, rights, sums, flips_before, spans, out_count, units, chunks, period, active, ending, given, made = plan
    refs = list(refs)

    def take(n):
        got = refs[:n]
        del refs[:n]
        return got

    weights = [item for group in sums for item in group]
    left_refs, right_refs, w_refs = take(left_count), take(len(rights)), take(len(weights))
    given_refs = take(given)
    grad_refs, made_refs = take(out_count), take(made)
    stage, flip, right_all, out_ref = take(4)
    w_bufs = take(len(weights))
    part, first, second, away, come_one, come_two, come_three, result = take(8)
    given_bufs, made_bufs = take(given), take(made - (ending == "branch"))
    acc, gain_parts, gain_come, given_sem, made_sem, gain_send, gain_recv = take(7)
    in_sem, right_sem, w_sem, ar_send, ar_recv, core_send, core_recv, two_send, two_recv, three_send, three_recv, out_sem = refs
    width = part.shape[2]
    block = come_three.shape[1]
    all_chunks = chunks * len(sums)
    place = lax.axis_index("mp")
    seq, batch = lax.axis_index("seq"), lax.axis_index("batch")
    core, chip = lax.rem(seq, 2), lax.div(seq, 2)
    sibling = seq + 1 - 2 * core
    beside = seq + 2 - 4 * chip
    pair = place + 1 - 2 * lax.rem(place, 2)
    across = 3 - place
    is_mid = (place == 1) | (place == 2)
    is_end = (place == 0) | (place == 3)

    def columns_of(c):
        return pl.ds(pl.multiple_of(c * width, width), width)

    def weight(at, group, c):
        here = columns_of(c - group * chunks)
        source = w_refs[at].at[here, :] if weights[at][2] == "nt" else w_refs[at].at[:, here]
        slot = lax.rem(c, 3)
        return pltpu.make_async_copy(source, w_bufs[at].at[slot], w_sem.at[at, slot])

    members = []
    for group, items in enumerate(sums):
        for _ in items:
            members.append(group)

    def load_weights(c):
        for group in range(len(sums)):

            @pl.when((c >= group * chunks) & (c < (group + 1) * chunks))
            def _():
                for at in range(len(weights)):
                    if members[at] == group:
                        weight(at, group, c).start()

    def remote(source, target, send, recv, device):
        return pltpu.make_async_remote_copy(
            src_ref=source, dst_ref=target, send_sem=send, recv_sem=recv, device_id=device, device_id_type=MESH
        )

    def slot_of(c):
        return lax.rem(c, chunks)

    high = part.shape[1] // HALVES

    def rows_of(h):
        return slice(h * high, (h + 1) * high)

    def up(c, h):
        slot = slot_of(c)
        source, target = part.at[slot, rows_of(h)], first.at[slot, rows_of(h)]
        return remote(source, target, ar_send.at[0, h, c], ar_recv.at[0, h, c], {"mp": pair})

    def over(c, h):
        slot = slot_of(c)
        source, target = part.at[slot, rows_of(h)], second.at[slot, rows_of(h)]
        return remote(source, target, ar_send.at[1, h, c], ar_recv.at[1, h, c], {"mp": across})

    def down(c, h):
        here = out_ref.at[rows_of(h), columns_of(c)]
        return remote(here, here, ar_send.at[2, h, c], ar_recv.at[2, h, c], {"mp": pair})

    def to_core(u):
        return remote(away.at[lax.rem(u, 2)], come_one.at[u], core_send.at[u], core_recv.at[u], {"seq": sibling})

    def chip_first(u):
        return 1 - lax.rem(u, 2)

    def sent_at(u, k):
        x_first = chip_first(u)
        return x_first * (2 * k + 1 - chip) + (1 - x_first) * (2 * (1 - batch) + k)

    def kept_at(u, k):
        x_first = chip_first(u)
        return x_first * (2 * k + chip) + (1 - x_first) * (2 * batch + k)

    def own_at(u):
        x_first = chip_first(u)
        return x_first * batch + (1 - x_first) * chip

    def device_of(x_way):
        return {
            "seq": x_way * beside + (1 - x_way) * seq,
            "batch": x_way * batch + (1 - x_way) * (1 - batch),
        }

    def second_hop(u, k):
        return remote(
            come_one.at[u, sent_at(u, k)], come_two.at[u, k], two_send.at[k, u], two_recv.at[k, u], device_of(chip_first(u))
        )

    def third_hop(u):
        return remote(
            come_two.at[u, 1 - own_at(u)], come_three.at[u], three_send.at[u], three_recv.at[u], device_of(1 - chip_first(u))
        )

    def left_copy(at):
        return pltpu.make_async_copy(left_refs[at], stage, in_sem.at[at])

    def right_copy(at):
        offset, source, size = rights[at]
        return pltpu.make_async_copy(
            right_refs[at].at[:, source : source + size], right_all.at[:, offset : offset + size], right_sem.at[at]
        )

    def out_copy(at, u):
        kind, index, offset, start, size = spans[at]
        slot = lax.rem(u, 2)
        if size < block:
            source = result.at[slot, :, start % block : start % block + size]
            target = grad_refs[index].at[:, offset : offset + size]
        else:
            source = result.at[slot]
            here = pl.ds(pl.multiple_of((u - start // block) * block + offset, block), block)
            target = grad_refs[index].at[here, :] if kind == "turned" else grad_refs[index].at[:, here]
        return pltpu.make_async_copy(source, target, out_sem.at[at, slot])

    def units_of(at):
        _, _, _, start, size = spans[at]
        return start // block, max((start + size) // block, start // block + 1)

    seq_count = lax.axis_size("seq")
    peers = lax.axis_size("batch") * seq_count
    me = batch * seq_count + seq

    def peer(k):
        there = lax.rem(me + k, peers)
        return there, {"batch": lax.div(there, seq_count), "seq": lax.rem(there, seq_count)}

    def gain_copy(k):
        there, device = peer(k)
        return remote(gain_parts.at[there], gain_come.at[k], gain_send.at[k], gain_recv.at[k], device)

    def given_copy(at):
        return pltpu.make_async_copy(given_refs[at], given_bufs[at], given_sem.at[at])

    def made_copy(at):
        source = out_ref.at[:, columns // 2 :] if ending == "branch" and at == made - 1 else made_bufs[at]
        return pltpu.make_async_copy(source, made_refs[at], made_sem.at[at])

    columns = out_ref.shape[1]
    rows = out_ref.shape[0]
    tile = rows // TILES

    def tile_of(i):
        return pl.ds(pl.multiple_of(i * tile, tile), tile)

    def branch_rows(i):
        here = tile_of(i)
        gm_buf, gb_buf, _ = made_bufs[:3]
        x_buf, b_buf, gain_buf, _ = given_bufs
        grad = out_ref[here, : columns // 2].astype(F32)
        middle = x_buf[here, :].astype(F32) + b_buf[here, :].astype(F32)
        scale = lax.rsqrt(jnp.mean(middle * middle, axis=-1, keepdims=True) + epsilon)
        scaled = grad * gain_buf[...]
        mean = jnp.mean(middle * scaled, axis=-1, keepdims=True)
        value = stage[here, :].astype(F32) + scale * scaled - middle * (scale * scale * scale) * mean
        gm_buf[here, :] = value
        gb_buf[here, :] = value.astype(BF16)
        acc[...] += jnp.sum(grad * middle * scale, axis=0, keepdims=True)

    def branch_end():
        made_bufs[2][...] = dot_nt(made_bufs[1][...], given_bufs[3][...]).astype(BF16)
        made_bufs[3][...] = acc[...]
        for at in range(4):
            made_copy(at).start()

    def token_rows(i, carry):
        here = tile_of(i)
        x_buf, gm_buf, gain_buf = given_bufs[:3]
        wide = x_buf[here, :].astype(F32)
        grad = out_ref[here, :].astype(F32)
        scale = lax.rsqrt(jnp.mean(wide * wide, axis=-1, keepdims=True) + epsilon)
        scaled = grad * gain_buf[...]
        mean = jnp.mean(wide * scaled, axis=-1, keepdims=True)
        value = gm_buf[here, :] + scale * scaled - wide * (scale * scale * scale) * mean
        made_bufs[0][here, :] = value.astype(BF16)
        acc[...] += jnp.sum(grad * wide * scale, axis=0, keepdims=True)
        return carry

    def output_rows(i):
        here = tile_of(i)
        x_buf, b_buf, m_buf = given_bufs[0], given_bufs[4], given_bufs[5]
        value = x_buf[here, :].astype(F32) + b_buf[here, :].astype(F32) + m_buf[here, :].astype(F32)
        made_bufs[2][here, :] = value.astype(BF16)

    acc[...] = jnp.zeros_like(acc)
    load_weights(0)
    load_weights(1)
    for at in range(len(rights)):
        right_copy(at).start()
    left_copy(0).start()
    for at in range(given):
        given_copy(at).start()

    barrier = pltpu.get_barrier_semaphore()
    if ending == "tokens":
        greeted = [{"mp": pair}] + [peer(k)[1] for k in range(1, peers)]
    else:
        greeted = [{"mp": pair}, {"seq": sibling}, {"seq": beside}, {"batch": 1 - batch}]
    for device in greeted:
        pl.semaphore_signal(barrier, inc=1, device_id=device, device_id_type=MESH)

    @pl.when(is_mid)
    def _():
        pl.semaphore_signal(barrier, inc=1, device_id={"mp": across}, device_id_type=MESH)
        pl.semaphore_wait(barrier, len(greeted) + 1)

    @pl.when(is_end)
    def _():
        pl.semaphore_wait(barrier, len(greeted))

    for at in range(len(rights)):
        right_copy(at).wait()

    def left_of(u):
        index = 0
        for at in range(1, left_count):
            index = index + (u >= flips_before[at]).astype(jnp.int32)
        return index

    def product(u, at, side):
        row = pl.multiple_of((2 * at + side) * block, block)
        column = pl.multiple_of(u * block, block)
        return dot_nn(flip[left_of(u), pl.ds(row, block), :], right_all[:, pl.ds(column, block)])

    def step_of(u):
        return (u // active) * period + u % active

    def on_unit(t, body):
        u = lax.div(t, period) * active + lax.rem(t, period)

        @pl.when((t >= 0) & (lax.rem(t, period) < active) & (u < units))
        def _():
            body(u)

    def first_stage(u):
        @pl.when(u >= 2)
        def _():
            to_core(u - 2).wait_send()

        for at in range(4):
            away[lax.rem(u, 2), at] = product(u, at, 1 - core).astype(BF16)
        to_core(u).start()

    def second_stage(u):
        to_core(u).wait_recv()
        for at in range(4):
            come_one[u, at] = (product(u, at, core) + come_one[u, at].astype(F32)).astype(BF16)
        for k in range(2):
            second_hop(u, k).start()

    def third_stage(u):
        for k in range(2):
            second_hop(u, k).wait_recv()
        sent = 1 - own_at(u)
        come_two[u, sent] = (come_two[u, sent].astype(F32) + come_one[u, kept_at(u, sent)].astype(F32)).astype(BF16)
        third_hop(u).start()

    def last_stage(u):
        third_hop(u).wait_recv()
        own = own_at(u)
        value = come_three[u].astype(F32) + come_two[u, own].astype(F32) + come_one[u, kept_at(u, own)].astype(F32)
        for at in range(len(spans)):
            low, high = units_of(at)

            @pl.when((u - 2 >= low) & (u - 2 < high))
            def _():
                out_copy(at, u - 2).wait()

        for kind in ("turned", "plain"):
            mine = [units_of(at) for at in range(len(spans)) if spans[at][0] == kind]
            if mine:
                low, high = min(m[0] for m in mine), max(m[1] for m in mine)

                @pl.when((u >= low) & (u < high))
                def _():
                    result[lax.rem(u, 2)] = value.T if kind == "turned" else value

        for at in range(len(spans)):
            low, high = units_of(at)

            @pl.when((u >= low) & (u < high))
            def _():
                out_copy(at, u).start()

    def step(t, carry):
        @pl.when((t >= chunks) & (t < all_chunks))
        def _():
            @pl.when(is_end)
            def _():
                for h in range(HALVES):
                    up(t - chunks, h).wait_send()

            @pl.when(is_mid)
            def _():
                for h in range(HALVES):
                    over(t - chunks, h).wait_send()

        for group, items in enumerate(sums):

            @pl.when((t >= group * chunks) & (t < (group + 1) * chunks))
            def _():
                value = None
                for at, (start, size, mode) in enumerate(weights):
                    if members[at] == group:
                        weight(at, group, t).wait()
                        dot = dot_nt if mode == "nt" else dot_nn
                        term = dot(right_all[:, start : start + size], w_bufs[at][lax.rem(t, 3)])
                        value = term if value is None else value + term
                part[slot_of(t)] = value.astype(BF16)

        @pl.when(t < all_chunks)
        def _():
            @pl.when(is_end)
            def _():
                for h in range(HALVES):
                    up(t, h).start()

            load_weights(t + 2)

        @pl.when(is_mid & (t >= UP_LAG) & (t < all_chunks + UP_LAG))
        def _():
            c = t - UP_LAG
            slot = slot_of(c)
            for h in range(HALVES):
                here = rows_of(h)
                up(c, h).wait_recv()
                part[slot, here] = (part[slot, here].astype(F32) + first[slot, here].astype(F32)).astype(BF16)
                over(c, h).start()

        @pl.when(is_mid & (t >= OVER_LAG) & (t < all_chunks + OVER_LAG))
        def _():
            c = t - OVER_LAG
            slot = slot_of(c)
            for h in range(HALVES):
                here = rows_of(h)
                over(c, h).wait_recv()
                value = part[slot, here].astype(F32) + second[slot, here].astype(F32)
                out_ref[here, columns_of(c)] = value.astype(BF16)
                down(c, h).start()

        @pl.when(is_end & (t >= DOWN_LAG) & (t < all_chunks + DOWN_LAG))
        def _():
            for h in range(HALVES):
                down(t - DOWN_LAG, h).wait_recv()

        for at in range(left_count):

            @pl.when(t == max(step_of(flips_before[at]) - 2, at))
            def _():
                left_copy(at).wait()

                def turn(k, carry):
                    here = pl.ds(pl.multiple_of(k * block, block), block)
                    flip[at, here, :] = stage[:, here].T
                    return carry

                lax.fori_loop(0, flip.shape[1] // block, turn, 0)
                if at + 1 < left_count:
                    left_copy(at + 1).start()

        on_unit(t, first_stage)
        on_unit(t - 1, second_stage)
        on_unit(t - 1 - LAG, third_stage)
        on_unit(t - 1 - 2 * LAG, last_stage)
        if ending == "branch":

            @pl.when(t == chunks + DOWN_LAG)
            def _():
                for at in range(given):
                    given_copy(at).wait()

            @pl.when((t >= chunks + DOWN_LAG) & (t < chunks + DOWN_LAG + TILES))
            def _():
                branch_rows(t - chunks - DOWN_LAG)

            @pl.when(t == chunks + DOWN_LAG + TILES)
            def _():
                branch_end()

        else:

            @pl.when(t == TILES // 2)
            def _():
                for at in range(given):
                    given_copy(at).wait()

            @pl.when((t >= TILES // 2) & (t < TILES // 2 + TILES))
            def _():
                output_rows(t - TILES // 2)

            @pl.when(t == TILES // 2 + TILES)
            def _():
                made_copy(2).start()

        return carry

    lax.fori_loop(0, max(step_of(units - 1) + 2 + 2 * LAG, all_chunks + DOWN_LAG), step, 0)
    if ending == "branch":
        made_copy(made - 1).start()
    else:
        lax.fori_loop(0, TILES, token_rows, 0)
        made_copy(0).start()
        part_width = columns // peers
        for k in range(peers):
            here = slice(k * part_width, (k + 1) * part_width)
            gain_parts[k, 0:1, :] = acc[:, here]
            gain_parts[k, 1:2, :] = given_bufs[3][:, here]
        for k in range(1, peers):
            gain_copy(k).start()

    def finish(c, carry):
        @pl.when(is_mid)
        def _():
            for h in range(HALVES):
                down(c, h).wait_send()

        return carry

    lax.fori_loop(0, all_chunks, finish, 0)

    def finish_last(c, carry):
        @pl.when(is_end)
        def _():
            for h in range(HALVES):
                up(c, h).wait_send()

        @pl.when(is_mid)
        def _():
            for h in range(HALVES):
                over(c, h).wait_send()

        return carry

    lax.fori_loop(all_chunks - chunks, all_chunks, finish_last, 0)

    def settle(u, carry):
        for k in range(2):
            second_hop(u, k).wait_send()
        third_hop(u).wait_send()
        return carry

    lax.fori_loop(0, units, settle, 0)
    for u in (units - 2, units - 1):
        to_core(u).wait_send()
        for at in range(len(spans)):
            low, high = units_of(at)
            if low <= u < high:
                out_copy(at, u).wait()
    if ending == "tokens":
        gains = gain_parts[me]
        for k in range(1, peers):
            gain_copy(k).wait_recv()
            gains = gains + gain_come[k]
        made_bufs[1][...] = gains
        made_copy(1).start()
        for k in range(1, peers):
            gain_copy(k).wait_send()
    for at in range(made):
        made_copy(at).wait()


def exchange(lefts, rights, sums, flips_before, outs, spans, units, call_id, pace, ending, given, made, chunks=16):
    rows, depth = lefts[0].shape
    block = depth // 8
    placed, at = [], 0
    for _, source, size in rights:
        placed.append((at, source, size))
        at += size
    weights = [item[0] for group in sums for item in group]
    columns = weights[0].shape[0] if sums[0][0][3] == "nt" else weights[0].shape[1]
    width = columns // chunks
    sum_plan = [[item[1:] for item in group] for group in sums]
    plan = (len(lefts), placed, sum_plan, flips_before, spans, len(outs), units, chunks, *pace, ending, len(given), len(made))
    any_space = pl.BlockSpec(memory_space=pl.ANY)
    line_block = pltpu.VMEM((chunks, rows, width), BF16)
    peers = lax.axis_size("batch") * lax.axis_size("seq")
    kept = made[:-1] if ending == "branch" else made
    dma = pltpu.SemaphoreType.DMA
    all_chunks = chunks * len(sums)
    flops = sum(2 * rows * columns * size for group in sum_plan for _, size, _ in group) + 2 * rows * depth * at
    return pl.pallas_call(
        functools.partial(exchange_kernel, plan),
        out_shape=[jax.ShapeDtypeStruct(shape, F32) for shape in outs]
        + [jax.ShapeDtypeStruct(shape, kind) for shape, kind in made],
        in_specs=[any_space] * (len(lefts) + len(rights) + len(weights) + len(given)),
        out_specs=[any_space] * (len(outs) + len(made)),
        scratch_shapes=[
            pltpu.VMEM((rows, depth), BF16),
            pltpu.VMEM((len(lefts), depth, rows), BF16),
            pltpu.VMEM((rows, at), BF16),
            pltpu.VMEM((rows, columns * len(sums)), BF16),
        ]
        + [
            pltpu.VMEM((3, width, size) if mode == "nt" else (3, size, width), BF16)
            for group in sum_plan
            for _, size, mode in group
        ]
        + [
            line_block,
            line_block,
            line_block,
            pltpu.VMEM((2, 4, block, block), BF16),
            pltpu.VMEM((units, 4, block, block), BF16),
            pltpu.VMEM((units, 2, block, block), BF16),
            pltpu.VMEM((units, block, block), BF16),
            pltpu.VMEM((2, block, block), F32),
        ]
        + [pltpu.VMEM(value.shape, value.dtype) for value in given]
        + [pltpu.VMEM(shape, kind) for shape, kind in kept]
        + [
            pltpu.VMEM((1, depth), F32),
            pltpu.VMEM((peers, 2, depth // peers), F32),
            pltpu.VMEM((peers, 2, depth // peers), F32),
            dma((len(given),)),
            dma((len(made),)),
            dma((peers,)),
            dma((peers,)),
            dma((len(lefts),)),
            dma((len(rights),)),
            dma((len(weights), 3)),
            dma((3, HALVES, all_chunks)),
            dma((3, HALVES, all_chunks)),
            dma((units,)),
            dma((units,)),
            dma((2, units)),
            dma((2, units)),
            dma((units,)),
            dma((units,)),
            dma((len(spans), 2)),
        ],
        compiler_params=pltpu.CompilerParams(
            collective_id=call_id, has_side_effects=True, vmem_limit_bytes=62 << 20
        ),
        cost_estimate=pl.CostEstimate(flops=flops + (50 << 30), bytes_accessed=20 << 20, transcendentals=0),
        name=f"exchange_{call_id}",
    )(*lefts, *[right[0] for right in rights], *weights, *given)


def forward_kernel(
    mixed_ref, x_ref, gain_ref, wo_hbm, wg_hbm, wu_hbm, ga_hbm,
    branch_hbm, n_hbm, act_hbm, gg_hbm, gu_hbm,
    branch, n_ref, act_ref, gg_ref, gu_ref, ga_ref, gate_acc, up_acc, squares, wo_buf, w_buf, part, first, second,
    ga_sem, wo_sem, w_sem, ar_send, ar_recv, out_sem,
):
    chunks, rows, width = part.shape
    total_columns = branch.shape[1]
    place = lax.axis_index("mp")
    pair = place + 1 - 2 * lax.rem(place, 2)
    across = 3 - place
    is_mid = (place == 1) | (place == 2)
    is_end = (place == 0) | (place == 3)
    high = rows // HALVES
    deep = w_buf.shape[2]

    def columns_of(c):
        return pl.ds(pl.multiple_of(c * width, width), width)

    def rows_of(h):
        return slice(h * high, (h + 1) * high)

    def remote(source, target, kind, h, c, device):
        return pltpu.make_async_remote_copy(
            src_ref=source,
            dst_ref=target,
            send_sem=ar_send.at[kind, h, c],
            recv_sem=ar_recv.at[kind, h, c],
            device_id={"mp": device},
            device_id_type=MESH,
        )

    def up(c, h):
        return remote(part.at[c, rows_of(h)], first.at[c, rows_of(h)], 0, h, c, pair)

    def over(c, h):
        return remote(part.at[c, rows_of(h)], second.at[c, rows_of(h)], 1, h, c, across)

    def down(c, h):
        here = branch.at[rows_of(h), columns_of(c)]
        return remote(here, here, 2, h, c, pair)

    def out_weight(c):
        slot = lax.rem(c, 3)
        return pltpu.make_async_copy(wo_hbm.at[:, columns_of(c)], wo_buf.at[slot], wo_sem.at[slot])

    def deep_of(p):
        return pl.ds(pl.multiple_of(p * deep, deep), deep)

    def weight(at, p):
        slot = lax.rem(p, 3)
        source = (wg_hbm, wu_hbm)[at].at[deep_of(p), :]
        return pltpu.make_async_copy(source, w_buf.at[at, slot], w_sem.at[at, slot])

    ga_copy = pltpu.make_async_copy(ga_hbm, ga_ref, ga_sem.at[0])
    out_weight(0).start()
    out_weight(1).start()
    for p in range(2):
        for at in range(2):
            weight(at, p).start()
    ga_copy.start()
    barrier = pltpu.get_barrier_semaphore()
    pl.semaphore_signal(barrier, inc=1, device_id={"mp": pair}, device_id_type=MESH)

    @pl.when(is_mid)
    def _():
        pl.semaphore_signal(barrier, inc=1, device_id={"mp": across}, device_id_type=MESH)
        pl.semaphore_wait(barrier, 2)

    @pl.when(is_end)
    def _():
        pl.semaphore_wait(barrier, 1)

    squares[...] = jnp.zeros_like(squares)
    per_deep = deep // width

    def step(t, carry):
        @pl.when(t < chunks)
        def _():
            out_weight(t).wait()
            part[t] = dot_nn(mixed_ref[...], wo_buf[lax.rem(t, 3)]).astype(BF16)

            @pl.when(is_end)
            def _():
                for h in range(HALVES):
                    up(t, h).start()

            @pl.when(t + 2 < chunks)
            def _():
                out_weight(t + 2).start()

        @pl.when(is_mid & (t >= UP_LAG) & (t < chunks + UP_LAG))
        def _():
            c = t - UP_LAG
            for h in range(HALVES):
                here = rows_of(h)
                up(c, h).wait_recv()
                part[c, here] = (part[c, here].astype(F32) + first[c, here].astype(F32)).astype(BF16)
                over(c, h).start()

        @pl.when(is_mid & (t >= OVER_LAG) & (t < chunks + OVER_LAG))
        def _():
            c = t - OVER_LAG
            for h in range(HALVES):
                here = rows_of(h)
                over(c, h).wait_recv()
                value = part[c, here].astype(F32) + second[c, here].astype(F32)
                branch[here, columns_of(c)] = value.astype(BF16)
                down(c, h).start()

        @pl.when(is_end & (t >= DOWN_LAG))
        def _():
            for h in range(HALVES):
                down(t - DOWN_LAG, h).wait_recv()

        @pl.when((t >= DOWN_LAG) & (lax.rem(t - DOWN_LAG, per_deep) == per_deep - 1))
        def _():
            p = lax.div(t - DOWN_LAG, per_deep)
            here = deep_of(p)
            middle = x_ref[:, here].astype(F32) + branch[:, here].astype(F32)
            squares[...] += jnp.sum(middle * middle, axis=-1, keepdims=True)
            scaled = (middle * gain_ref[:, here]).astype(BF16)
            for at, acc in enumerate((gate_acc, up_acc)):
                weight(at, p).wait()
                value = dot_nn(scaled, w_buf[at, lax.rem(p, 3)])

                @pl.when(p == 0)
                def _():
                    acc[...] = value

                @pl.when(p > 0)
                def _():
                    acc[...] += value

            @pl.when((p + 2) * deep < total_columns)
            def _():
                for at in range(2):
                    weight(at, p + 2).start()

        return carry

    lax.fori_loop(0, chunks + DOWN_LAG, step, 0)
    ga_copy.wait()
    tile = rows // TILES
    outs = [(n_ref, n_hbm), (act_ref, act_hbm), (gg_ref, gg_hbm), (gu_ref, gu_hbm)]

    def out_copy(at, i):
        here = pl.ds(pl.multiple_of(i * tile, tile), tile)
        return pltpu.make_async_copy(outs[at][0].at[here, :], outs[at][1].at[here, :], out_sem.at[at, i])

    branch_copy = pltpu.make_async_copy(branch, branch_hbm, ga_sem.at[1])
    branch_copy.start()

    def rows_step(i, carry):
        here = pl.ds(pl.multiple_of(i * tile, tile), tile)
        scale = lax.rsqrt(squares[here, :1] * (1.0 / total_columns) + epsilon)
        middle = x_ref[here, :].astype(F32) + branch[here, :].astype(F32)
        n_ref[here, :] = (middle * scale * gain_ref[...]).astype(BF16)
        gate = gate_acc[here, :] * scale
        up_pre = up_acc[here, :] * scale
        grad = ga_ref[here, :].astype(F32)
        sigmoid = jax.nn.sigmoid(gate)
        swish = gate * sigmoid
        act_ref[here, :] = (swish * up_pre).astype(BF16)
        gu_ref[here, :] = (grad * swish).astype(BF16)
        gg_ref[here, :] = (grad * up_pre * sigmoid * (1.0 + gate * (1.0 - sigmoid))).astype(BF16)
        for at in range(4):
            out_copy(at, i).start()
        return carry

    lax.fori_loop(0, TILES, rows_step, 0)

    def finish(c, carry):
        @pl.when(is_end)
        def _():
            for h in range(HALVES):
                up(c, h).wait_send()

        @pl.when(is_mid)
        def _():
            for h in range(HALVES):
                over(c, h).wait_send()
                down(c, h).wait_send()

        return carry

    lax.fori_loop(0, chunks, finish, 0)

    def drain(i, carry):
        for at in range(4):
            out_copy(at, i).wait()
        return carry

    lax.fori_loop(0, TILES, drain, 0)
    branch_copy.wait()


def forward(mixed, tokens, gain, w_output, w_gate, w_up, grad_active, call_id, chunks=16, deep=256):
    rows, columns = tokens.shape
    hidden = w_gate.shape[1]
    width = columns // chunks
    vmem, any_space = pl.BlockSpec(memory_space=pltpu.VMEM), pl.BlockSpec(memory_space=pl.ANY)
    dma = pltpu.SemaphoreType.DMA
    shapes = [(rows, columns), (rows, columns), (rows, hidden), (rows, hidden), (rows, hidden)]
    line_block = pltpu.VMEM((chunks, rows, width), BF16)
    return pl.pallas_call(
        forward_kernel,
        in_specs=[vmem] * 3 + [any_space] * 4,
        out_specs=[any_space] * 5,
        out_shape=[jax.ShapeDtypeStruct(shape, BF16) for shape in shapes],
        scratch_shapes=[pltpu.VMEM(shape, BF16) for shape in shapes]
        + [
            pltpu.VMEM((rows, hidden), BF16),
            pltpu.VMEM((rows, hidden), F32),
            pltpu.VMEM((rows, hidden), F32),
            pltpu.VMEM((rows, PAIR), F32),
            pltpu.VMEM((3, mixed.shape[1], width), BF16),
            pltpu.VMEM((2, 3, deep, hidden), BF16),
            line_block,
            line_block,
            line_block,
            dma((2,)),
            dma((3,)),
            dma((2, 3)),
            dma((3, HALVES, chunks)),
            dma((3, HALVES, chunks)),
            dma((4, TILES)),
        ],
        compiler_params=pltpu.CompilerParams(
            collective_id=call_id, has_side_effects=True, vmem_limit_bytes=62 << 20
        ),
        name="forward",
    )(mixed, tokens, gain, w_output, w_gate, w_up, grad_active)


def final_kernel(gn_ref, x_ref, gm_ref, gain_ref, mlp_ref, out_ref, gains_ref, acc, parts, come, send_sem, recv_sem):
    seq, batch = lax.axis_index("seq"), lax.axis_index("batch")
    seq_count = lax.axis_size("seq")
    peers = parts.shape[0]
    block = parts.shape[2]
    me = batch * seq_count + seq

    def peer(k):
        there = lax.rem(me + k, peers)
        return there, {"batch": lax.div(there, seq_count), "seq": lax.rem(there, seq_count)}

    def copy(k):
        there, device = peer(k)
        return pltpu.make_async_remote_copy(
            src_ref=parts.at[there],
            dst_ref=come.at[k],
            send_sem=send_sem.at[k],
            recv_sem=recv_sem.at[k],
            device_id=device,
            device_id_type=MESH,
        )

    barrier = pltpu.get_barrier_semaphore()
    for k in range(1, peers):
        pl.semaphore_signal(barrier, inc=1, device_id=peer(k)[1], device_id_type=MESH)
    rows = x_ref.shape[0]
    tile = rows // 8
    gain = gain_ref[...]
    acc[...] = jnp.zeros_like(acc)

    def rows_step(i, carry):
        here = pl.ds(pl.multiple_of(i * tile, tile), tile)
        wide = x_ref[here, :].astype(F32)
        grad = gn_ref[here, :].astype(F32)
        scale = lax.rsqrt(jnp.mean(wide * wide, axis=-1, keepdims=True) + epsilon)
        scaled = grad * gain
        mean = jnp.mean(wide * scaled, axis=-1, keepdims=True)
        result = gm_ref[here, :] + scale * scaled - wide * (scale * scale * scale) * mean
        out_ref[here, :] = result.astype(BF16)
        acc[...] += jnp.sum(grad * wide * scale, axis=0, keepdims=True)
        return carry

    lax.fori_loop(0, 8, rows_step, 0)
    for k in range(peers):
        here = slice(k * block, (k + 1) * block)
        parts[k, 0:1, :] = acc[:, here]
        parts[k, 1:2, :] = mlp_ref[:, here]
    pl.semaphore_wait(barrier, peers - 1)
    for k in range(1, peers):
        copy(k).start()
    total = parts[me]
    for k in range(1, peers):
        copy(k).wait_recv()
        total = total + come[k]
    gains_ref[...] = total
    for k in range(1, peers):
        copy(k).wait_send()


def final(grad_normed, tokens, grad_middle, gain, mlp_part, call_id):
    rows, width = tokens.shape
    peers = lax.axis_size("batch") * lax.axis_size("seq")
    block = width // peers
    vmem = pl.BlockSpec(memory_space=pltpu.VMEM)
    return pl.pallas_call(
        final_kernel,
        out_shape=[jax.ShapeDtypeStruct((rows, width), BF16), jax.ShapeDtypeStruct((2, block), F32)],
        in_specs=[vmem] * 5,
        out_specs=[vmem, vmem],
        scratch_shapes=[
            pltpu.VMEM((1, width), F32),
            pltpu.VMEM((peers, 2, block), F32),
            pltpu.VMEM((peers, 2, block), F32),
            pltpu.SemaphoreType.DMA((peers,)),
            pltpu.SemaphoreType.DMA((peers,)),
        ],
        compiler_params=pltpu.CompilerParams(collective_id=call_id, has_side_effects=True),
        name="final",
    )(grad_normed, tokens, grad_middle, gain, mlp_part)


def settle_kernel(places, *refs):
    count = len(places)
    sources, targets = refs[:count], refs[count : -count - 2]
    bufs, load_sem, store_sem = refs[-count - 2 : -2], refs[-2], refs[-1]

    def load(at):
        return pltpu.make_async_copy(sources[at], bufs[at], load_sem.at[at])

    def store(at):
        index, row = places[at]
        target = targets[index].at[row : row + bufs[at].shape[0], :]
        return pltpu.make_async_copy(bufs[at], target, store_sem.at[at])

    for at in range(count):
        load(at).start()
    for at in range(count):
        load(at).wait()
        store(at).start()
    for at in range(count):
        store(at).wait()


def settle(groups):
    places, shapes, arrays = [], [], []
    for index, group in enumerate(groups):
        row = 0
        for array in group:
            places.append((index, row))
            arrays.append(array)
            row += array.shape[0]
        shapes.append(jax.ShapeDtypeStruct((row, group[0].shape[1]), group[0].dtype))
    any_space = pl.BlockSpec(memory_space=pl.ANY)
    dma = pltpu.SemaphoreType.DMA
    return pl.pallas_call(
        functools.partial(settle_kernel, places),
        in_specs=[any_space] * len(arrays),
        out_specs=[any_space] * len(groups),
        out_shape=shapes,
        scratch_shapes=[pltpu.VMEM(array.shape, array.dtype) for array in arrays]
        + [dma((len(arrays),)), dma((len(arrays),))],
        compiler_params=pltpu.CompilerParams(vmem_limit_bytes=62 << 20),
        name="settle",
    )(*arrays)


def scatter_sum(left, right):
    rows, depth = left.shape
    columns = right.shape[1]
    batch_count = lax.axis_size("batch")
    seq_index = lax.axis_index("seq")
    core, chip = seq_index % 2, seq_index // 2
    block = depth // (4 * batch_count)
    split = left.reshape(rows, batch_count, 2, 2, block)
    size = lax.axis_size("seq")

    def product(at):
        taken = lax.dynamic_index_in_dim(split, at, 3, keepdims=False).reshape(rows, depth // 2)
        return dot_tn(taken, right)

    away = product(1 - core).astype(BF16)
    arrived = lax.ppermute(away, "seq", [(s, s ^ 1) for s in range(size)])
    kept = (product(core) + arrived.astype(F32)).astype(BF16)
    kept = kept.reshape(batch_count, 2, block, columns)
    half = columns // 2

    def over_chip(values, axis):
        sent = lax.dynamic_index_in_dim(values, 1 - chip, axis, keepdims=False)
        stay = lax.dynamic_index_in_dim(values, chip, axis, keepdims=False)
        came = lax.ppermute(sent, "seq", [(s, s ^ 2) for s in range(size)])
        return stay.astype(F32) + came.astype(F32)

    def over_batch(values):
        if batch_count == 2:
            here = lax.axis_index("batch")
            sent = lax.dynamic_index_in_dim(values, 1 - here, 0, keepdims=False)
            stay = lax.dynamic_index_in_dim(values, here, 0, keepdims=False)
            came = lax.ppermute(sent, "batch", [(0, 1), (1, 0)])
            return stay.astype(F32) + came.astype(F32)
        return lax.psum_scatter(values, "batch", scatter_dimension=0, tiled=False).astype(F32)

    one = over_batch(over_chip(kept[..., :half], 1).astype(BF16))
    two = over_chip(over_batch(kept[..., half:]).astype(BF16), 0)
    return jnp.concatenate([one, two], axis=1)


def local(
    tokens, segment_ids, attn_gain, w_query, w_key, w_value, w_output, mlp_gain, w_gate, w_up, w_down, cotangent
):
    rows, width = tokens.shape
    seq_count = lax.axis_size("seq")
    seq_index = lax.axis_index("seq")
    segments = segment_ids[0]
    first_row = seq_index * rows
    reach = LONGEST // rows
    cos, sin = rope_tables(segments, first_row, rows)
    row_segment = lax.dynamic_slice_in_dim(segments, first_row, rows, 0)[None, :]
    padded = jnp.concatenate([jnp.full((LONGEST,), -1, jnp.int32), segments])
    key_segment = lax.dynamic_slice_in_dim(padded, first_row, rows + LONGEST, 0)[:, None]

    normed, queries, key_value, grad_active = project(
        tokens, attn_gain[None, :], w_query, w_key, w_value, cos, sin, cotangent, w_down, 5
    )
    key_value = key_value.reshape(3 * rows, 2 * PAIR)
    mixed, logs = attend(queries, key_value, key_segment, row_segment)
    branch_low, normed_two, active, grad_gate_low, grad_up_low = forward(
        mixed, tokens, mlp_gain[None, :], w_output, w_gate, w_up, grad_active, 1
    )
    wide = tokens.astype(F32)
    middle = wide + branch_low.astype(F32)
    fused = lax.axis_size("batch") == 2
    hidden = w_gate.shape[1]
    unit = width // 8
    early = hidden * 5 // 8 // unit * unit
    if fused:
        grad_gate, grad_up, grad_down_one, grad_middle, grad_branch, grad_mixed, grad_mlp_gain, mlp_out = exchange(
            [normed_two, cotangent],
            [(grad_gate_low, 0, hidden), (grad_up_low, 0, hidden), (active, 0, hidden)],
            [
                [(w_gate, 0, hidden, "nt"), (w_up, hidden, hidden, "nt")],
                [(w_down, 2 * hidden, hidden, "nn")],
            ],
            (0, 2 * hidden // unit),
            [(unit, hidden), (unit, hidden), (early, unit)],
            [
                ("plain", 0, 0, 0, hidden),
                ("plain", 1, 0, hidden, hidden),
                ("turned", 2, 0, 2 * hidden, early),
            ],
            (2 * hidden + early) // unit,
            2,
            (3, 2),
            "branch",
            [tokens, branch_low, mlp_gain[None, :], w_output],
            [
                ((rows, width), F32),
                ((rows, width), BF16),
                ((rows, mixed.shape[1]), BF16),
                ((1, width), F32),
                ((rows, width), BF16),
            ],
        )
    else:
        grad_normed_two = line_sum([(grad_gate_low, w_gate, "nt"), (grad_up_low, w_up, "nt")], 2)
        grad_gate = scatter_sum(normed_two, grad_gate_low)
        grad_up = scatter_sum(normed_two, grad_up_low)
        mlp_out = lax.psum(dot_nn(active, w_down).astype(BF16), "mp")
        grad_normed_two = grad_normed_two.astype(F32)
        scaled_two = grad_normed_two * mlp_gain
        scale_two = lax.rsqrt(jnp.mean(middle * middle, axis=-1, keepdims=True) + epsilon)
        grad_middle = (
            cotangent.astype(F32)
            + scale_two * scaled_two
            - middle
            * (scale_two * scale_two * scale_two)
            * jnp.mean(middle * scaled_two, axis=-1, keepdims=True)
        )
        grad_mlp_gain = jnp.sum(grad_normed_two * middle * scale_two, axis=0)[None, :]
        grad_branch = grad_middle.astype(BF16)
        grad_mixed = dot_nt(grad_branch, w_output).astype(BF16)

    grad_query_pre, grad_key_pre, grad_value_pre = attend_back(
        queries, key_value, key_segment, row_segment, mixed, grad_mixed, logs, cos, sin, 6
    )
    query_width = grad_query_pre.shape[1]
    if fused:
        late, mixed_width = hidden - early, mixed.shape[1]
        query_at = late + mixed_width
        key_at = query_at + query_width
        grad_down_two, grad_output, grad_query, grad_key, grad_value, grad_tokens, gains, output = exchange(
            [cotangent, grad_branch, normed],
            [
                (active, early, late),
                (mixed, 0, mixed_width),
                (grad_query_pre, 0, query_width),
                (grad_key_pre, 0, PAIR),
                (grad_value_pre, 0, PAIR),
            ],
            [
                [
                    (w_query, query_at, query_width, "nt"),
                    (w_key, key_at, PAIR, "nt"),
                    (w_value, key_at + PAIR, PAIR, "nt"),
                ]
            ],
            (0, late // unit, query_at // unit),
            [(late, unit), (mixed_width, unit), (unit, query_width), (unit, PAIR), (unit, PAIR)],
            [
                ("turned", 0, 0, 0, late),
                ("turned", 1, 0, late, mixed_width),
                ("plain", 2, 0, query_at, query_width),
                ("plain", 3, 0, key_at, PAIR),
                ("plain", 4, 0, key_at + PAIR, PAIR),
            ],
            (key_at + 2 * PAIR) // unit,
            3,
            (2, 1),
            "tokens",
            [tokens, grad_middle, attn_gain[None, :], grad_mlp_gain, branch_low, mlp_out],
            [((rows, width), BF16), ((2, unit), F32), ((rows, width), BF16)],
        )
        grad_gate, grad_up, grad_down, grad_output, grad_query, grad_key, grad_value, grad_tokens, output = settle(
            [
                [grad_gate],
                [grad_up],
                [grad_down_one, grad_down_two],
                [grad_output],
                [grad_query],
                [grad_key],
                [grad_value],
                [grad_tokens],
                [output],
            ]
        )
    else:
        output = (middle + mlp_out.astype(F32)).astype(BF16)
        grad_down = scatter_sum(cotangent, active).T
        grad_output = scatter_sum(grad_branch, mixed).T
        grad_qkv = scatter_sum(normed, jnp.concatenate([grad_query_pre, grad_key_pre, grad_value_pre], axis=1))
        grad_query = grad_qkv[:, :query_width]
        grad_key = grad_qkv[:, query_width : query_width + PAIR]
        grad_value = grad_qkv[:, query_width + PAIR :]
        grad_normed = line_sum(
            [(grad_query_pre, w_query, "nt"), (grad_key_pre, w_key, "nt"), (grad_value_pre, w_value, "nt")], 3
        )
        grad_tokens, gains = final(grad_normed, tokens, grad_middle, attn_gain[None, :], grad_mlp_gain, 4)
    return (
        output,
        grad_tokens,
        gains[0],
        grad_query,
        grad_key,
        grad_value,
        grad_output,
        gains[1],
        grad_gate,
        grad_up,
        grad_down,
    )


def solution(mesh):
    tokens_spec = P(("batch", "seq"), None)
    in_specs = (
        tokens_spec,
        P("batch", None),
        P(),
        P(None, "mp"),
        P(None, "mp"),
        P(None, "mp"),
        P("mp", None),
        P(),
        P(None, "mp"),
        P(None, "mp"),
        P("mp", None),
        tokens_spec,
    )
    row_split = P(("batch", "seq"), "mp")
    column_split = P("mp", ("batch", "seq"))
    out_specs = (
        tokens_spec,
        tokens_spec,
        P(("batch", "seq")),
        row_split,
        row_split,
        row_split,
        column_split,
        P(("batch", "seq")),
        row_split,
        row_split,
        column_split,
    )
    return jax.shard_map(local, mesh=mesh, in_specs=in_specs, out_specs=out_specs, check_vma=False)
```

```python
import functools
import math

import jax
import jax.numpy as jnp
from jax import lax
from jax.experimental import pallas as pl
from jax.experimental.pallas import tpu as pltpu
from jax.sharding import PartitionSpec as P

HS = 64
PAIR = 2 * HS
LONGEST = 1024
FORWARD_ROWS = 256
BACKWARD_ROWS = 128
rope_base = 500000.0
epsilon = 1e-05
masked_score = -1e30
MESH = pl.DeviceIdType.MESH
F32 = jnp.float32
BF16 = jnp.bfloat16


def dot_nn(left, right):
    return lax.dot_general(left, right, (((1,), (0,)), ((), ())), preferred_element_type=F32)


def dot_nt(left, right):
    return lax.dot_general(left, right, (((1,), (1,)), ((), ())), preferred_element_type=F32)


def dot_tn(left, right):
    return lax.dot_general(left, right, (((0,), (0,)), ((), ())), preferred_element_type=F32)


def lanes_of(values):
    return lax.broadcasted_iota(jnp.int32, values.shape, 1)


def swap_halves(values):
    ahead = pltpu.roll(values, PAIR - HS // 2, 1)
    behind = pltpu.roll(values, HS // 2, 1)
    return jnp.where(lanes_of(values) % HS < HS // 2, ahead, behind)


def rope_tables(segments, first_row, rows):
    row_segment = lax.dynamic_slice_in_dim(segments, first_row, rows, 0)
    doc_start = jnp.sum((segments[None, :] < row_segment[:, None]).astype(jnp.int32), axis=1)
    place = (first_row + jnp.arange(rows, dtype=jnp.int32) - doc_start).astype(F32)
    lane = jnp.arange(PAIR, dtype=jnp.int32)
    frequency = jnp.exp((lane % (HS // 2)).astype(F32) * (-2.0 * math.log(rope_base) / HS))
    angles = place[:, None] * frequency[None, :]
    sign = jnp.where(lane % HS < HS // 2, -1.0, 1.0)
    return jnp.cos(angles), jnp.sin(angles) * sign[None, :]


def project_kernel(
    x_ref, gain_ref, wk_ref, wv_ref, cos_ref, sin_ref, cot_hbm, wq_hbm, wd_hbm,
    n_hbm, q_hbm, kv_hbm, ga_hbm,
    n_ref, q_ref, kv_ref, ga_ref, cot_ref, wq_ref, wd_ref, load_sem, wd_sem, send_sem, recv_sem, out_sem,
):
    rows = x_ref.shape[0]
    seq, seq_count = lax.axis_index("seq"), lax.axis_size("seq")
    hidden = wd_hbm.shape[0]
    width = wd_ref.shape[1]
    chunks = hidden // width
    block = rows // 2
    loads = [
        pltpu.make_async_copy(wq_hbm, wq_ref, load_sem.at[0]),
        pltpu.make_async_copy(cot_hbm, cot_ref, load_sem.at[1]),
    ]

    def weight(c):
        slot = lax.rem(c, 3)
        here = pl.ds(pl.multiple_of(c * width, width), width)
        return pltpu.make_async_copy(wd_hbm.at[here, :], wd_ref.at[slot], wd_sem.at[slot])

    def out_copy(at):
        source = (n_ref, q_ref, kv_ref, ga_ref)[at]
        return pltpu.make_async_copy(source, (n_hbm, q_hbm, kv_hbm, ga_hbm)[at], out_sem.at[at])

    def send(away):
        return pltpu.make_async_remote_copy(
            src_ref=kv_ref.at[2],
            dst_ref=kv_ref.at[2 - away],
            send_sem=send_sem.at[away],
            recv_sem=recv_sem.at[away],
            device_id={"seq": lax.rem(seq + away, seq_count)},
            device_id_type=MESH,
        )

    for load in loads:
        load.start()
    weight(0).start()
    weight(1).start()
    for away in (1, 2):

        @pl.when(seq < away)
        def _():
            kv_ref[2 - away] = jnp.zeros(kv_ref.shape[1:], BF16)

    barrier = pltpu.get_barrier_semaphore()
    for away in range(1, seq_count):
        there = lax.rem(seq + away, seq_count)
        pl.semaphore_signal(barrier, inc=1, device_id={"seq": there}, device_id_type=MESH)

    for half in range(2):
        here = slice(half * block, (half + 1) * block)
        cos, sin = cos_ref[here, :], sin_ref[here, :]
        wide = x_ref[here, :].astype(F32)
        scale = lax.rsqrt(jnp.mean(wide * wide, axis=-1, keepdims=True) + epsilon)
        normed = (wide * scale * gain_ref[...]).astype(BF16)
        n_ref[here, :] = normed
        keys = dot_nn(normed, wk_ref[...])
        keys = keys * cos + swap_halves(keys) * sin
        values = dot_nn(normed, wv_ref[...])
        low_half = lanes_of(keys) < HS
        kv_ref[2, here, :PAIR] = jnp.where(low_half, keys, pltpu.roll(values, HS, 1)).astype(BF16)
        kv_ref[2, here, PAIR:] = jnp.where(low_half, pltpu.roll(keys, HS, 1), values).astype(BF16)
    pl.semaphore_wait(barrier, seq_count - 1)
    for away in (1, 2):

        @pl.when(seq + away < seq_count)
        def _():
            send(away).start()

    out_copy(0).start()
    for load in loads:
        load.wait()
    for half in range(2):
        here = slice(half * block, (half + 1) * block)
        cos, sin = cos_ref[here, :], sin_ref[here, :]
        queries = dot_nn(n_ref[here, :], wq_ref[...])
        for start in range(0, queries.shape[1], PAIR):
            part = queries[:, start : start + PAIR]
            q_ref[here, start : start + PAIR] = (part * cos + swap_halves(part) * sin).astype(BF16)
    out_copy(1).start()

    def step(c, carry):
        weight(c).wait()

        @pl.when(c + 2 < chunks)
        def _():
            weight(c + 2).start()

        here = pl.ds(pl.multiple_of(c * width, width), width)
        ga_ref[:, here] = dot_nt(cot_ref[...], wd_ref[lax.rem(c, 3)]).astype(BF16)
        return carry

    lax.fori_loop(0, chunks, step, 0)
    out_copy(3).start()
    for away in (1, 2):

        @pl.when(seq >= away)
        def _():
            send(away).wait_recv()

    out_copy(2).start()
    for away in (1, 2):

        @pl.when(seq + away < seq_count)
        def _():
            send(away).wait_send()

    for at in range(4):
        out_copy(at).wait()


def project(tokens, gain, w_query, w_key, w_value, cos, sin, cotangent, w_down, call_id):
    rows, width = tokens.shape
    columns, hidden = w_query.shape[1], w_down.shape[0]
    chunk = 256
    vmem, any_space = pl.BlockSpec(memory_space=pltpu.VMEM), pl.BlockSpec(memory_space=pl.ANY)
    shapes = [(rows, width), (rows, columns), (3, rows, 2 * PAIR), (rows, hidden)]
    dma = pltpu.SemaphoreType.DMA
    return pl.pallas_call(
        project_kernel,
        in_specs=[vmem] * 6 + [any_space] * 3,
        out_specs=[any_space] * 4,
        out_shape=[jax.ShapeDtypeStruct(shape, BF16) for shape in shapes],
        scratch_shapes=[pltpu.VMEM(shape, BF16) for shape in shapes]
        + [
            pltpu.VMEM((rows, width), BF16),
            pltpu.VMEM(w_query.shape, BF16),
            pltpu.VMEM((3, chunk, width), BF16),
            dma((2,)),
            dma((3,)),
            dma((3,)),
            dma((3,)),
            dma((4,)),
        ],
        compiler_params=pltpu.CompilerParams(
            collective_id=call_id, has_side_effects=True, vmem_limit_bytes=62 << 20
        ),
        name="project",
    )(tokens, gain, w_key, w_value, cos, sin, cotangent, w_query, w_down)


def write_bias(bias_ref, key_ref, row_ref):
    tiles, span, both = bias_ref.shape
    size = both // 2
    key_place = lax.broadcasted_iota(jnp.int32, (span, size), 0) - LONGEST
    row_place = lax.broadcasted_iota(jnp.int32, (span, size), 1)
    for tile in range(tiles):
        start = tile * size
        same = key_ref[start : start + span, :] == row_ref[:, start : start + size]
        bias = jnp.where(same & (key_place <= row_place), 0.0, masked_score)
        bias_ref[tile] = jnp.concatenate([bias, bias], axis=1)


def bias_scratch(rows, size):
    assert LONGEST + rows == 3 * rows
    return pltpu.VMEM((rows // size, LONGEST + size, 2 * size), F32)


def heads_beside(values, here):
    return jnp.concatenate([values[:HS, here], values[HS:, here]], axis=1)


def heads_below(values, here):
    return jnp.concatenate([values[here, :HS], values[here, HS:]], axis=0)


def heads_stacked(values):
    size = values.shape[1] // 2
    return jnp.concatenate([values[:, :size], values[:, size:]], axis=0)


def attend_kernel(q_ref, kv_ref, key_ref, row_ref, out_ref, log_ref, bias_ref):
    @pl.when(pl.program_id(0) == 0)
    def _():
        write_bias(bias_ref, key_ref, row_ref)

    key_value = kv_ref[...]
    flipped = key_value.T
    q_flipped = (q_ref[...].astype(F32) * HS ** (-0.5)).astype(BF16).T
    tiles, span, both = bias_ref.shape
    size = both // 2
    for tile in range(tiles):
        here = slice(tile * size, (tile + 1) * size)
        keys = slice(tile * size, tile * size + span)
        scores = dot_nn(key_value[keys, :HS], heads_beside(q_flipped, here)) + bias_ref[tile]
        top = jnp.max(scores, axis=0, keepdims=True)
        powers = jnp.exp(scores - top)
        total = jnp.sum(powers, axis=0, keepdims=True)
        mixed = dot_nn(flipped[HS:, keys], powers.astype(BF16)) / total
        logs = top + jnp.log(total)
        log_ref[0, 0:1, here] = logs[:, :size]
        log_ref[0, 1:2, here] = logs[:, size:]
        out_ref[here, :] = heads_stacked(mixed).T.astype(BF16)


def attend(queries, key_value, key_segment, row_segment):
    rows, width = queries.shape
    pairs = width // PAIR
    per_group = pairs // 2
    pair_tile = pl.BlockSpec((rows, PAIR), lambda p: (0, p))
    kv_tile = pl.BlockSpec((3 * rows, PAIR), lambda p: (0, p // per_group))
    return pl.pallas_call(
        attend_kernel,
        grid=(pairs,),
        in_specs=[
            pair_tile,
            kv_tile,
            pl.BlockSpec(key_segment.shape, lambda p: (0, 0)),
            pl.BlockSpec(row_segment.shape, lambda p: (0, 0)),
        ],
        out_specs=[pair_tile, pl.BlockSpec((1, 2, rows), lambda p: (p, 0, 0))],
        out_shape=[
            jax.ShapeDtypeStruct((rows, width), BF16),
            jax.ShapeDtypeStruct((pairs, 2, rows), F32),
        ],
        scratch_shapes=[bias_scratch(rows, FORWARD_ROWS)],
        cost_estimate=pl.CostEstimate(
            flops=16 << 30, bytes_accessed=4 << 20, transcendentals=3 * rows * rows * 2 * pairs
        ),
        name="attend",
    )(queries, key_value, key_segment, row_segment)


def attend_back_kernel(
    q_ref, kv_ref, key_ref, row_ref, out_ref, grad_ref, log_ref, cos_ref, sin_ref,
    dq_ref, dk_ref, dv_ref, bias_ref, dkv_ref, own_ref, sent_ref, come_ref, send_sem, recv_sem, per_group,
):
    step = pl.program_id(0)
    seq, seq_count = lax.axis_index("seq"), lax.axis_size("seq")
    barrier = pltpu.get_barrier_semaphore()

    def back(group, away):
        return pltpu.make_async_remote_copy(
            src_ref=sent_ref.at[group, 2 - away],
            dst_ref=come_ref.at[group, 2 - away],
            send_sem=send_sem.at[group, 2 - away],
            recv_sem=recv_sem.at[group, 2 - away],
            device_id={"seq": lax.rem(seq + seq_count - away, seq_count)},
            device_id_type=MESH,
        )

    @pl.when(step == 0)
    def _():
        for away in range(1, seq_count):
            there = lax.rem(seq + away, seq_count)
            pl.semaphore_signal(barrier, inc=1, device_id={"seq": there}, device_id_type=MESH)
        write_bias(bias_ref, key_ref, row_ref)

    rows = q_ref.shape[0]
    key_value = kv_ref[...]
    flipped = key_value[:, :].T
    scaled = (q_ref[...].astype(F32) * HS ** (-0.5)).astype(BF16)
    q_flipped = scaled.T
    grad = grad_ref[...]
    grad_flipped = grad.T
    product = (out_ref[...].astype(F32) * grad.astype(F32)).T
    tiles, span, both = bias_ref.shape
    size = both // 2

    @pl.when(step % per_group == 0)
    def _():
        dkv_ref[...] = jnp.zeros_like(dkv_ref)

    for tile in range(tiles):
        here = slice(tile * size, (tile + 1) * size)
        keys = slice(tile * size, tile * size + span)
        logs = jnp.concatenate([log_ref[0, 0:1, here], log_ref[0, 1:2, here]], axis=1)
        delta = jnp.sum(heads_beside(product, here), axis=0, keepdims=True)
        scores = dot_nn(key_value[keys, :HS], heads_beside(q_flipped, here)) + bias_ref[tile]
        shares = jnp.exp(scores - logs)
        grad_shares = dot_nn(key_value[keys, HS:], heads_beside(grad_flipped, here))
        grad_scores = (shares * (grad_shares - delta)).astype(BF16)
        dvalue = dot_nn(shares.astype(BF16), heads_below(grad, here))
        dkey = dot_nn(grad_scores, heads_below(scaled, here))
        dkv_ref[keys, :] += jnp.concatenate([dkey, dvalue], axis=1)
        dq = heads_stacked(dot_nn(flipped[:HS, keys], grad_scores)).T * HS ** (-0.5)
        dq_ref[here, :] = (dq * cos_ref[here, :] - swap_halves(dq) * sin_ref[here, :]).astype(BF16)

    for group in range(2):

        @pl.when(step == (group + 1) * per_group - 1)
        def _():
            sent_ref[group, 0] = dkv_ref[:rows, :].astype(BF16)
            sent_ref[group, 1] = dkv_ref[rows : 2 * rows, :].astype(BF16)
            own_ref[group] = dkv_ref[2 * rows :, :]
            if group == 0:
                pl.semaphore_wait(barrier, seq_count - 1)
            for away in (1, 2):

                @pl.when(seq >= away)
                def _():
                    back(group, away).start()

    @pl.when(step == 2 * per_group - 1)
    def _():
        for group in range(2):
            for away in (1, 2):

                @pl.when(seq + away < seq_count)
                def _():
                    back(group, away).wait_recv()
                    own_ref[group] += come_ref[group, 2 - away].astype(F32)

        one, two = own_ref[0], own_ref[1]
        low_half = lanes_of(one) < HS
        keys = jnp.where(low_half, one, pltpu.roll(two, HS, 1))
        dk_ref[...] = (keys * cos_ref[...] - swap_halves(keys) * sin_ref[...]).astype(BF16)
        dv_ref[...] = jnp.where(low_half, pltpu.roll(one, HS, 1), two).astype(BF16)
        for group in range(2):
            for away in (1, 2):

                @pl.when(seq >= away)
                def _():
                    back(group, away).wait_send()


def attend_back(queries, key_value, key_segment, row_segment, mixed, grad, logs, cos, sin, call_id):
    rows, width = queries.shape
    pairs = width // PAIR
    per_group = pairs // 2
    pair_tile = pl.BlockSpec((rows, PAIR), lambda p: (0, p))
    whole = pl.BlockSpec((rows, PAIR), lambda p: (0, 0))
    wide_tile = pl.BlockSpec((3 * rows, PAIR), lambda p: (0, p // per_group))
    full = lambda array: pl.BlockSpec(array.shape, lambda p: (0, 0))
    return pl.pallas_call(
        functools.partial(attend_back_kernel, per_group=per_group),
        grid=(pairs,),
        in_specs=[
            pair_tile,
            wide_tile,
            full(key_segment),
            full(row_segment),
            pair_tile,
            pair_tile,
            pl.BlockSpec((1, 2, rows), lambda p: (p, 0, 0)),
            full(cos),
            full(sin),
        ],
        out_specs=[pair_tile, whole, whole],
        out_shape=[
            jax.ShapeDtypeStruct((rows, width), BF16),
            jax.ShapeDtypeStruct((rows, PAIR), BF16),
            jax.ShapeDtypeStruct((rows, PAIR), BF16),
        ],
        scratch_shapes=[
            bias_scratch(rows, BACKWARD_ROWS),
            pltpu.VMEM((3 * rows, PAIR), F32),
            pltpu.VMEM((2, rows, PAIR), F32),
            pltpu.VMEM((2, 2, rows, PAIR), BF16),
            pltpu.VMEM((2, 2, rows, PAIR), BF16),
            pltpu.SemaphoreType.DMA((2, 2)),
            pltpu.SemaphoreType.DMA((2, 2)),
        ],
        compiler_params=pltpu.CompilerParams(collective_id=call_id, has_side_effects=True),
        cost_estimate=pl.CostEstimate(
            flops=40 << 30, bytes_accessed=6 << 20, transcendentals=3 * rows * rows * 2 * pairs
        ),
        name="attend_back",
    )(queries, key_value, key_segment, row_segment, mixed, grad, logs, cos, sin)


def line_sum_kernel(modes, chunks, *refs):
    count = len(modes)
    a_refs, w_refs, out_ref = refs[:count], refs[count : 2 * count], refs[2 * count]
    rest = refs[2 * count + 1 :]
    w_bufs = rest[:count]
    part, first, second, total, w_sem, send_sem, recv_sem = rest[count:]
    width = part.shape[2]
    place = lax.axis_index("mp")
    pair = place + 1 - 2 * lax.rem(place, 2)
    across = 3 - place
    is_mid = (place == 1) | (place == 2)
    is_end = (place == 0) | (place == 3)

    def weight(at, c):
        if modes[at] == "nt":
            source = w_refs[at].at[pl.ds(pl.multiple_of(c * width, width), width), :]
        else:
            source = w_refs[at].at[:, pl.ds(pl.multiple_of(c * width, width), width)]
        return pltpu.make_async_copy(source, w_bufs[at].at[c], w_sem.at[at, c])

    def remote(kind, source, target, c, device):
        return pltpu.make_async_remote_copy(
            src_ref=source.at[c],
            dst_ref=target.at[c],
            send_sem=send_sem.at[kind, c],
            recv_sem=recv_sem.at[kind, c],
            device_id={"mp": device},
            device_id_type=MESH,
        )

    def up(c):
        return remote(0, part, first, c, pair)

    def over(c):
        return remote(1, part, second, c, across)

    def down(c):
        return remote(2, total, total, c, pair)

    def start_weights(c, carry):
        for at in range(count):
            weight(at, c).start()
        return carry

    lax.fori_loop(0, chunks, start_weights, 0)
    barrier = pltpu.get_barrier_semaphore()
    pl.semaphore_signal(barrier, inc=1, device_id={"mp": pair}, device_id_type=MESH)

    @pl.when(is_mid)
    def _():
        pl.semaphore_signal(barrier, inc=1, device_id={"mp": across}, device_id_type=MESH)
        pl.semaphore_wait(barrier, 2)

    @pl.when(is_end)
    def _():
        pl.semaphore_wait(barrier, 1)

    def step(t, carry):
        @pl.when(t < chunks)
        def _():
            value = None
            for at in range(count):
                weight(at, t).wait()
                dot = dot_nt if modes[at] == "nt" else dot_nn
                term = dot(a_refs[at][...], w_bufs[at][t])
                value = term if value is None else value + term
            part[t] = value.astype(BF16)

            @pl.when(is_end)
            def _():
                up(t).start()

        @pl.when(is_mid & (t >= 1) & (t < chunks + 1))
        def _():
            c = t - 1
            up(c).wait_recv()
            part[c] = (part[c].astype(F32) + first[c].astype(F32)).astype(BF16)
            over(c).start()

        @pl.when(is_mid & (t >= OVER_LAG))
        def _():
            c = t - OVER_LAG
            over(c).wait_recv()
            total[c] = (part[c].astype(F32) + second[c].astype(F32)).astype(BF16)
            down(c).start()

        return carry

    lax.fori_loop(0, chunks + OVER_LAG, step, 0)

    def finish(c, carry):
        @pl.when(is_end)
        def _():
            up(c).wait_send()
            down(c).wait_recv()

        @pl.when(is_mid)
        def _():
            over(c).wait_send()
            down(c).wait_send()

        out_ref[:, pl.ds(pl.multiple_of(c * width, width), width)] = total[c]
        return carry

    lax.fori_loop(0, chunks, finish, 0)


def line_sum(pairs, call_id, chunks=16):
    lefts = [left for left, _, _ in pairs]
    rights = [right for _, right, _ in pairs]
    modes = tuple(mode for _, _, mode in pairs)
    rows = lefts[0].shape[0]
    columns = rights[0].shape[0] if modes[0] == "nt" else rights[0].shape[1]
    width = columns // chunks
    count = len(pairs)
    bufs = [
        pltpu.VMEM((chunks, width, left.shape[1]) if mode == "nt" else (chunks, left.shape[1], width), BF16)
        for left, _, mode in pairs
    ]
    flops = sum(2 * rows * columns * left.shape[1] for left in lefts)
    moved = sum(right.size * 2 for right in rights)
    block = pltpu.VMEM((chunks, rows, width), BF16)
    return pl.pallas_call(
        functools.partial(line_sum_kernel, modes, chunks),
        out_shape=jax.ShapeDtypeStruct((rows, columns), BF16),
        in_specs=[pl.BlockSpec(memory_space=pltpu.VMEM)] * count
        + [pl.BlockSpec(memory_space=pl.ANY)] * count,
        out_specs=pl.BlockSpec(memory_space=pltpu.VMEM),
        scratch_shapes=bufs
        + [
            block,
            block,
            block,
            block,
            pltpu.SemaphoreType.DMA((count, chunks)),
            pltpu.SemaphoreType.DMA((3, chunks)),
            pltpu.SemaphoreType.DMA((3, chunks)),
        ],
        compiler_params=pltpu.CompilerParams(collective_id=call_id, has_side_effects=True),
        cost_estimate=pl.CostEstimate(
            flops=flops + (40 << 30), bytes_accessed=moved, transcendentals=0
        ),
        name=f"line_sum_{call_id}",
    )(*lefts, *rights)

LAG = 3
UP_LAG = 1
OVER_LAG = 3
DOWN_LAG = 8
HALVES = 1
TILES = 8


def exchange_kernel(plan, *refs):
    left_count, rights, sums, flips_before, spans, out_count, units, chunks, period, active, ending, given, made = plan
    refs = list(refs)

    def take(n):
        got = refs[:n]
        del refs[:n]
        return got

    weights = [item for group in sums for item in group]
    left_refs, right_refs, w_refs = take(left_count), take(len(rights)), take(len(weights))
    given_refs = take(given)
    grad_refs, made_refs = take(out_count), take(made)
    stage, flip, right_all, out_ref = take(4)
    w_bufs = take(len(weights))
    part, first, second, away, come_one, come_two, come_three, result = take(8)
    given_bufs, made_bufs = take(given), take(made - (ending == "branch"))
    acc, gain_parts, gain_come, given_sem, made_sem, gain_send, gain_recv = take(7)
    in_sem, right_sem, w_sem, ar_send, ar_recv, core_send, core_recv, two_send, two_recv, three_send, three_recv, out_sem = refs
    width = part.shape[2]
    block = come_three.shape[1]
    all_chunks = chunks * len(sums)
    place = lax.axis_index("mp")
    seq, batch = lax.axis_index("seq"), lax.axis_index("batch")
    core, chip = lax.rem(seq, 2), lax.div(seq, 2)
    sibling = seq + 1 - 2 * core
    beside = seq + 2 - 4 * chip
    pair = place + 1 - 2 * lax.rem(place, 2)
    across = 3 - place
    is_mid = (place == 1) | (place == 2)
    is_end = (place == 0) | (place == 3)

    def columns_of(c):
        return pl.ds(pl.multiple_of(c * width, width), width)

    def weight(at, group, c):
        here = columns_of(c - group * chunks)
        source = w_refs[at].at[here, :] if weights[at][2] == "nt" else w_refs[at].at[:, here]
        slot = lax.rem(c, 3)
        return pltpu.make_async_copy(source, w_bufs[at].at[slot], w_sem.at[at, slot])

    members = []
    for group, items in enumerate(sums):
        for _ in items:
            members.append(group)

    def load_weights(c):
        for group in range(len(sums)):

            @pl.when((c >= group * chunks) & (c < (group + 1) * chunks))
            def _():
                for at in range(len(weights)):
                    if members[at] == group:
                        weight(at, group, c).start()

    def remote(source, target, send, recv, device):
        return pltpu.make_async_remote_copy(
            src_ref=source, dst_ref=target, send_sem=send, recv_sem=recv, device_id=device, device_id_type=MESH
        )

    def slot_of(c):
        return lax.rem(c, chunks)

    high = part.shape[1] // HALVES

    def rows_of(h):
        return slice(h * high, (h + 1) * high)

    def up(c, h):
        slot = slot_of(c)
        source, target = part.at[slot, rows_of(h)], first.at[slot, rows_of(h)]
        return remote(source, target, ar_send.at[0, h, c], ar_recv.at[0, h, c], {"mp": pair})

    def over(c, h):
        slot = slot_of(c)
        source, target = part.at[slot, rows_of(h)], second.at[slot, rows_of(h)]
        return remote(source, target, ar_send.at[1, h, c], ar_recv.at[1, h, c], {"mp": across})

    def down(c, h):
        here = out_ref.at[rows_of(h), columns_of(c)]
        return remote(here, here, ar_send.at[2, h, c], ar_recv.at[2, h, c], {"mp": pair})

    def to_core(u):
        return remote(away.at[lax.rem(u, 2)], come_one.at[u], core_send.at[u], core_recv.at[u], {"seq": sibling})

    def chip_first(u):
        return 1 - lax.rem(u, 2)

    def sent_at(u, k):
        x_first = chip_first(u)
        return x_first * (2 * k + 1 - chip) + (1 - x_first) * (2 * (1 - batch) + k)

    def kept_at(u, k):
        x_first = chip_first(u)
        return x_first * (2 * k + chip) + (1 - x_first) * (2 * batch + k)

    def own_at(u):
        x_first = chip_first(u)
        return x_first * batch + (1 - x_first) * chip

    def device_of(x_way):
        return {
            "seq": x_way * beside + (1 - x_way) * seq,
            "batch": x_way * batch + (1 - x_way) * (1 - batch),
        }

    def second_hop(u, k):
        return remote(
            come_one.at[u, sent_at(u, k)], come_two.at[u, k], two_send.at[k, u], two_recv.at[k, u], device_of(chip_first(u))
        )

    def third_hop(u):
        return remote(
            come_two.at[u, 1 - own_at(u)], come_three.at[u], three_send.at[u], three_recv.at[u], device_of(1 - chip_first(u))
        )

    def left_copy(at):
        return pltpu.make_async_copy(left_refs[at], stage, in_sem.at[at])

    def right_copy(at):
        offset, source, size = rights[at]
        return pltpu.make_async_copy(
            right_refs[at].at[:, source : source + size], right_all.at[:, offset : offset + size], right_sem.at[at]
        )

    def out_copy(at, u):
        kind, index, offset, start, size = spans[at]
        slot = lax.rem(u, 2)
        if size < block:
            source = result.at[slot, :, start % block : start % block + size]
            target = grad_refs[index].at[:, offset : offset + size]
        else:
            source = result.at[slot]
            here = pl.ds(pl.multiple_of((u - start // block) * block + offset, block), block)
            target = grad_refs[index].at[here, :] if kind == "turned" else grad_refs[index].at[:, here]
        return pltpu.make_async_copy(source, target, out_sem.at[at, slot])

    def units_of(at):
        _, _, _, start, size = spans[at]
        return start // block, max((start + size) // block, start // block + 1)

    seq_count = lax.axis_size("seq")
    peers = lax.axis_size("batch") * seq_count
    me = batch * seq_count + seq

    def peer(k):
        there = lax.rem(me + k, peers)
        return there, {"batch": lax.div(there, seq_count), "seq": lax.rem(there, seq_count)}

    def gain_copy(k):
        there, device = peer(k)
        return remote(gain_parts.at[there], gain_come.at[k], gain_send.at[k], gain_recv.at[k], device)

    def given_copy(at):
        return pltpu.make_async_copy(given_refs[at], given_bufs[at], given_sem.at[at])

    def made_copy(at):
        source = out_ref.at[:, columns // 2 :] if ending == "branch" and at == made - 1 else made_bufs[at]
        return pltpu.make_async_copy(source, made_refs[at], made_sem.at[at])

    columns = out_ref.shape[1]
    rows = out_ref.shape[0]
    tile = rows // TILES

    def tile_of(i):
        return pl.ds(pl.multiple_of(i * tile, tile), tile)

    def branch_rows(i):
        here = tile_of(i)
        gm_buf, gb_buf, _ = made_bufs[:3]
        x_buf, b_buf, gain_buf, _ = given_bufs
        grad = out_ref[here, : columns // 2].astype(F32)
        middle = x_buf[here, :].astype(F32) + b_buf[here, :].astype(F32)
        scale = lax.rsqrt(jnp.mean(middle * middle, axis=-1, keepdims=True) + epsilon)
        scaled = grad * gain_buf[...]
        mean = jnp.mean(middle * scaled, axis=-1, keepdims=True)
        value = stage[here, :].astype(F32) + scale * scaled - middle * (scale * scale * scale) * mean
        gm_buf[here, :] = value
        gb_buf[here, :] = value.astype(BF16)
        acc[...] += jnp.sum(grad * middle * scale, axis=0, keepdims=True)

    def branch_end():
        made_bufs[2][...] = dot_nt(made_bufs[1][...], given_bufs[3][...]).astype(BF16)
        made_bufs[3][...] = acc[...]
        for at in range(4):
            made_copy(at).start()

    def token_rows(i, carry):
        here = tile_of(i)
        x_buf, gm_buf, gain_buf = given_bufs[:3]
        wide = x_buf[here, :].astype(F32)
        grad = out_ref[here, :].astype(F32)
        scale = lax.rsqrt(jnp.mean(wide * wide, axis=-1, keepdims=True) + epsilon)
        scaled = grad * gain_buf[...]
        mean = jnp.mean(wide * scaled, axis=-1, keepdims=True)
        value = gm_buf[here, :] + scale * scaled - wide * (scale * scale * scale) * mean
        made_bufs[0][here, :] = value.astype(BF16)
        acc[...] += jnp.sum(grad * wide * scale, axis=0, keepdims=True)
        return carry

    def output_rows(i):
        here = tile_of(i)
        x_buf, b_buf, m_buf = given_bufs[0], given_bufs[4], given_bufs[5]
        value = x_buf[here, :].astype(F32) + b_buf[here, :].astype(F32) + m_buf[here, :].astype(F32)
        made_bufs[2][here, :] = value.astype(BF16)

    acc[...] = jnp.zeros_like(acc)
    load_weights(0)
    load_weights(1)
    for at in range(len(rights)):
        right_copy(at).start()
    left_copy(0).start()
    for at in range(given):
        given_copy(at).start()

    barrier = pltpu.get_barrier_semaphore()
    if ending == "tokens":
        greeted = [{"mp": pair}] + [peer(k)[1] for k in range(1, peers)]
    else:
        greeted = [{"mp": pair}, {"seq": sibling}, {"seq": beside}, {"batch": 1 - batch}]
    for device in greeted:
        pl.semaphore_signal(barrier, inc=1, device_id=device, device_id_type=MESH)

    @pl.when(is_mid)
    def _():
        pl.semaphore_signal(barrier, inc=1, device_id={"mp": across}, device_id_type=MESH)
        pl.semaphore_wait(barrier, len(greeted) + 1)

    @pl.when(is_end)
    def _():
        pl.semaphore_wait(barrier, len(greeted))

    for at in range(len(rights)):
        right_copy(at).wait()

    def left_of(u):
        index = 0
        for at in range(1, left_count):
            index = index + (u >= flips_before[at]).astype(jnp.int32)
        return index

    def product(u, at, side):
        row = pl.multiple_of((2 * at + side) * block, block)
        column = pl.multiple_of(u * block, block)
        return dot_nn(flip[left_of(u), pl.ds(row, block), :], right_all[:, pl.ds(column, block)])

    def step_of(u):
        return (u // active) * period + u % active

    def on_unit(t, body):
        u = lax.div(t, period) * active + lax.rem(t, period)

        @pl.when((t >= 0) & (lax.rem(t, period) < active) & (u < units))
        def _():
            body(u)

    def first_stage(u):
        @pl.when(u >= 2)
        def _():
            to_core(u - 2).wait_send()

        for at in range(4):
            away[lax.rem(u, 2), at] = product(u, at, 1 - core).astype(BF16)
        to_core(u).start()

    def second_stage(u):
        to_core(u).wait_recv()
        for at in range(4):
            come_one[u, at] = (product(u, at, core) + come_one[u, at].astype(F32)).astype(BF16)
        for k in range(2):
            second_hop(u, k).start()

    def third_stage(u):
        for k in range(2):
            second_hop(u, k).wait_recv()
        sent = 1 - own_at(u)
        come_two[u, sent] = (come_two[u, sent].astype(F32) + come_one[u, kept_at(u, sent)].astype(F32)).astype(BF16)
        third_hop(u).start()

    def last_stage(u):
        third_hop(u).wait_recv()
        own = own_at(u)
        value = come_three[u].astype(F32) + come_two[u, own].astype(F32) + come_one[u, kept_at(u, own)].astype(F32)
        for at in range(len(spans)):
            low, high = units_of(at)

            @pl.when((u - 2 >= low) & (u - 2 < high))
            def _():
                out_copy(at, u - 2).wait()

        for kind in ("turned", "plain"):
            mine = [units_of(at) for at in range(len(spans)) if spans[at][0] == kind]
            if mine:
                low, high = min(m[0] for m in mine), max(m[1] for m in mine)

                @pl.when((u >= low) & (u < high))
                def _():
                    result[lax.rem(u, 2)] = value.T if kind == "turned" else value

        for at in range(len(spans)):
            low, high = units_of(at)

            @pl.when((u >= low) & (u < high))
            def _():
                out_copy(at, u).start()

    def step(t, carry):
        @pl.when((t >= chunks) & (t < all_chunks))
        def _():
            @pl.when(is_end)
            def _():
                for h in range(HALVES):
                    up(t - chunks, h).wait_send()

            @pl.when(is_mid)
            def _():
                for h in range(HALVES):
                    over(t - chunks, h).wait_send()

        for group, items in enumerate(sums):

            @pl.when((t >= group * chunks) & (t < (group + 1) * chunks))
            def _():
                value = None
                for at, (start, size, mode) in enumerate(weights):
                    if members[at] == group:
                        weight(at, group, t).wait()
                        dot = dot_nt if mode == "nt" else dot_nn
                        term = dot(right_all[:, start : start + size], w_bufs[at][lax.rem(t, 3)])
                        value = term if value is None else value + term
                part[slot_of(t)] = value.astype(BF16)

        @pl.when(t < all_chunks)
        def _():
            @pl.when(is_end)
            def _():
                for h in range(HALVES):
                    up(t, h).start()

            load_weights(t + 2)

        @pl.when(is_mid & (t >= UP_LAG) & (t < all_chunks + UP_LAG))
        def _():
            c = t - UP_LAG
            slot = slot_of(c)
            for h in range(HALVES):
                here = rows_of(h)
                up(c, h).wait_recv()
                part[slot, here] = (part[slot, here].astype(F32) + first[slot, here].astype(F32)).astype(BF16)
                over(c, h).start()

        @pl.when(is_mid & (t >= OVER_LAG) & (t < all_chunks + OVER_LAG))
        def _():
            c = t - OVER_LAG
            slot = slot_of(c)
            for h in range(HALVES):
                here = rows_of(h)
                over(c, h).wait_recv()
                value = part[slot, here].astype(F32) + second[slot, here].astype(F32)
                out_ref[here, columns_of(c)] = value.astype(BF16)
                down(c, h).start()

        @pl.when(is_end & (t >= DOWN_LAG) & (t < all_chunks + DOWN_LAG))
        def _():
            for h in range(HALVES):
                down(t - DOWN_LAG, h).wait_recv()

        for at in range(left_count):

            @pl.when(t == max(step_of(flips_before[at]) - 2, at))
            def _():
                left_copy(at).wait()

                def turn(k, carry):
                    here = pl.ds(pl.multiple_of(k * block, block), block)
                    flip[at, here, :] = stage[:, here].T
                    return carry

                lax.fori_loop(0, flip.shape[1] // block, turn, 0)
                if at + 1 < left_count:
                    left_copy(at + 1).start()

        on_unit(t, first_stage)
        on_unit(t - 1, second_stage)
        on_unit(t - 1 - LAG, third_stage)
        on_unit(t - 1 - 2 * LAG, last_stage)
        if ending == "branch":

            @pl.when(t == chunks + DOWN_LAG)
            def _():
                for at in range(given):
                    given_copy(at).wait()

            @pl.when((t >= chunks + DOWN_LAG) & (t < chunks + DOWN_LAG + TILES))
            def _():
                branch_rows(t - chunks - DOWN_LAG)

            @pl.when(t == chunks + DOWN_LAG + TILES)
            def _():
                branch_end()

        else:

            @pl.when(t == TILES // 2)
            def _():
                for at in range(given):
                    given_copy(at).wait()

            @pl.when((t >= TILES // 2) & (t < TILES // 2 + TILES))
            def _():
                output_rows(t - TILES // 2)

            @pl.when(t == TILES // 2 + TILES)
            def _():
                made_copy(2).start()

        return carry

    lax.fori_loop(0, max(step_of(units - 1) + 2 + 2 * LAG, all_chunks + DOWN_LAG), step, 0)
    if ending == "branch":
        made_copy(made - 1).start()
    else:
        lax.fori_loop(0, TILES, token_rows, 0)
        made_copy(0).start()
        part_width = columns // peers
        for k in range(peers):
            here = slice(k * part_width, (k + 1) * part_width)
            gain_parts[k, 0:1, :] = acc[:, here]
            gain_parts[k, 1:2, :] = given_bufs[3][:, here]
        for k in range(1, peers):
            gain_copy(k).start()

    def finish(c, carry):
        @pl.when(is_mid)
        def _():
            for h in range(HALVES):
                down(c, h).wait_send()

        return carry

    lax.fori_loop(0, all_chunks, finish, 0)

    def finish_last(c, carry):
        @pl.when(is_end)
        def _():
            for h in range(HALVES):
                up(c, h).wait_send()

        @pl.when(is_mid)
        def _():
            for h in range(HALVES):
                over(c, h).wait_send()

        return carry

    lax.fori_loop(all_chunks - chunks, all_chunks, finish_last, 0)

    def settle(u, carry):
        for k in range(2):
            second_hop(u, k).wait_send()
        third_hop(u).wait_send()
        return carry

    lax.fori_loop(0, units, settle, 0)
    for u in (units - 2, units - 1):
        to_core(u).wait_send()
        for at in range(len(spans)):
            low, high = units_of(at)
            if low <= u < high:
                out_copy(at, u).wait()
    if ending == "tokens":
        gains = gain_parts[me]
        for k in range(1, peers):
            gain_copy(k).wait_recv()
            gains = gains + gain_come[k]
        made_bufs[1][...] = gains
        made_copy(1).start()
        for k in range(1, peers):
            gain_copy(k).wait_send()
    for at in range(made):
        made_copy(at).wait()


def exchange(lefts, rights, sums, flips_before, outs, spans, units, call_id, pace, ending, given, made, chunks=16):
    rows, depth = lefts[0].shape
    block = depth // 8
    placed, at = [], 0
    for _, source, size in rights:
        placed.append((at, source, size))
        at += size
    weights = [item[0] for group in sums for item in group]
    columns = weights[0].shape[0] if sums[0][0][3] == "nt" else weights[0].shape[1]
    width = columns // chunks
    sum_plan = [[item[1:] for item in group] for group in sums]
    plan = (len(lefts), placed, sum_plan, flips_before, spans, len(outs), units, chunks, *pace, ending, len(given), len(made))
    any_space = pl.BlockSpec(memory_space=pl.ANY)
    line_block = pltpu.VMEM((chunks, rows, width), BF16)
    peers = lax.axis_size("batch") * lax.axis_size("seq")
    kept = made[:-1] if ending == "branch" else made
    dma = pltpu.SemaphoreType.DMA
    all_chunks = chunks * len(sums)
    flops = sum(2 * rows * columns * size for group in sum_plan for _, size, _ in group) + 2 * rows * depth * at
    return pl.pallas_call(
        functools.partial(exchange_kernel, plan),
        out_shape=[jax.ShapeDtypeStruct(shape, F32) for shape in outs]
        + [jax.ShapeDtypeStruct(shape, kind) for shape, kind in made],
        in_specs=[any_space] * (len(lefts) + len(rights) + len(weights) + len(given)),
        out_specs=[any_space] * (len(outs) + len(made)),
        scratch_shapes=[
            pltpu.VMEM((rows, depth), BF16),
            pltpu.VMEM((len(lefts), depth, rows), BF16),
            pltpu.VMEM((rows, at), BF16),
            pltpu.VMEM((rows, columns * len(sums)), BF16),
        ]
        + [
            pltpu.VMEM((3, width, size) if mode == "nt" else (3, size, width), BF16)
            for group in sum_plan
            for _, size, mode in group
        ]
        + [
            line_block,
            line_block,
            line_block,
            pltpu.VMEM((2, 4, block, block), BF16),
            pltpu.VMEM((units, 4, block, block), BF16),
            pltpu.VMEM((units, 2, block, block), BF16),
            pltpu.VMEM((units, block, block), BF16),
            pltpu.VMEM((2, block, block), F32),
        ]
        + [pltpu.VMEM(value.shape, value.dtype) for value in given]
        + [pltpu.VMEM(shape, kind) for shape, kind in kept]
        + [
            pltpu.VMEM((1, depth), F32),
            pltpu.VMEM((peers, 2, depth // peers), F32),
            pltpu.VMEM((peers, 2, depth // peers), F32),
            dma((len(given),)),
            dma((len(made),)),
            dma((peers,)),
            dma((peers,)),
            dma((len(lefts),)),
            dma((len(rights),)),
            dma((len(weights), 3)),
            dma((3, HALVES, all_chunks)),
            dma((3, HALVES, all_chunks)),
            dma((units,)),
            dma((units,)),
            dma((2, units)),
            dma((2, units)),
            dma((units,)),
            dma((units,)),
            dma((len(spans), 2)),
        ],
        compiler_params=pltpu.CompilerParams(
            collective_id=call_id, has_side_effects=True, vmem_limit_bytes=62 << 20
        ),
        cost_estimate=pl.CostEstimate(flops=flops + (50 << 30), bytes_accessed=20 << 20, transcendentals=0),
        name=f"exchange_{call_id}",
    )(*lefts, *[right[0] for right in rights], *weights, *given)


def forward_kernel(
    mixed_ref, x_ref, gain_ref, wo_hbm, wg_hbm, wu_hbm, ga_hbm,
    branch_hbm, n_hbm, act_hbm, gg_hbm, gu_hbm,
    branch, n_ref, act_ref, gg_ref, gu_ref, ga_ref, gate_acc, up_acc, squares, wo_buf, w_buf, part, first, second,
    ga_sem, wo_sem, w_sem, ar_send, ar_recv, out_sem,
):
    chunks, rows, width = part.shape
    total_columns = branch.shape[1]
    place = lax.axis_index("mp")
    pair = place + 1 - 2 * lax.rem(place, 2)
    across = 3 - place
    is_mid = (place == 1) | (place == 2)
    is_end = (place == 0) | (place == 3)
    high = rows // HALVES
    deep = w_buf.shape[2]

    def columns_of(c):
        return pl.ds(pl.multiple_of(c * width, width), width)

    def rows_of(h):
        return slice(h * high, (h + 1) * high)

    def remote(source, target, kind, h, c, device):
        return pltpu.make_async_remote_copy(
            src_ref=source,
            dst_ref=target,
            send_sem=ar_send.at[kind, h, c],
            recv_sem=ar_recv.at[kind, h, c],
            device_id={"mp": device},
            device_id_type=MESH,
        )

    def up(c, h):
        return remote(part.at[c, rows_of(h)], first.at[c, rows_of(h)], 0, h, c, pair)

    def over(c, h):
        return remote(part.at[c, rows_of(h)], second.at[c, rows_of(h)], 1, h, c, across)

    def down(c, h):
        here = branch.at[rows_of(h), columns_of(c)]
        return remote(here, here, 2, h, c, pair)

    def out_weight(c):
        slot = lax.rem(c, 3)
        return pltpu.make_async_copy(wo_hbm.at[:, columns_of(c)], wo_buf.at[slot], wo_sem.at[slot])

    def deep_of(p):
        return pl.ds(pl.multiple_of(p * deep, deep), deep)

    def weight(at, p):
        slot = lax.rem(p, 3)
        source = (wg_hbm, wu_hbm)[at].at[deep_of(p), :]
        return pltpu.make_async_copy(source, w_buf.at[at, slot], w_sem.at[at, slot])

    ga_copy = pltpu.make_async_copy(ga_hbm, ga_ref, ga_sem.at[0])
    out_weight(0).start()
    out_weight(1).start()
    for p in range(2):
        for at in range(2):
            weight(at, p).start()
    ga_copy.start()
    barrier = pltpu.get_barrier_semaphore()
    pl.semaphore_signal(barrier, inc=1, device_id={"mp": pair}, device_id_type=MESH)

    @pl.when(is_mid)
    def _():
        pl.semaphore_signal(barrier, inc=1, device_id={"mp": across}, device_id_type=MESH)
        pl.semaphore_wait(barrier, 2)

    @pl.when(is_end)
    def _():
        pl.semaphore_wait(barrier, 1)

    squares[...] = jnp.zeros_like(squares)
    per_deep = deep // width

    def step(t, carry):
        @pl.when(t < chunks)
        def _():
            out_weight(t).wait()
            part[t] = dot_nn(mixed_ref[...], wo_buf[lax.rem(t, 3)]).astype(BF16)

            @pl.when(is_end)
            def _():
                for h in range(HALVES):
                    up(t, h).start()

            @pl.when(t + 2 < chunks)
            def _():
                out_weight(t + 2).start()

        @pl.when(is_mid & (t >= UP_LAG) & (t < chunks + UP_LAG))
        def _():
            c = t - UP_LAG
            for h in range(HALVES):
                here = rows_of(h)
                up(c, h).wait_recv()
                part[c, here] = (part[c, here].astype(F32) + first[c, here].astype(F32)).astype(BF16)
                over(c, h).start()

        @pl.when(is_mid & (t >= OVER_LAG) & (t < chunks + OVER_LAG))
        def _():
            c = t - OVER_LAG
            for h in range(HALVES):
                here = rows_of(h)
                over(c, h).wait_recv()
                value = part[c, here].astype(F32) + second[c, here].astype(F32)
                branch[here, columns_of(c)] = value.astype(BF16)
                down(c, h).start()

        @pl.when(is_end & (t >= DOWN_LAG))
        def _():
            for h in range(HALVES):
                down(t - DOWN_LAG, h).wait_recv()

        @pl.when((t >= DOWN_LAG) & (lax.rem(t - DOWN_LAG, per_deep) == per_deep - 1))
        def _():
            p = lax.div(t - DOWN_LAG, per_deep)
            here = deep_of(p)
            middle = x_ref[:, here].astype(F32) + branch[:, here].astype(F32)
            squares[...] += jnp.sum(middle * middle, axis=-1, keepdims=True)
            scaled = (middle * gain_ref[:, here]).astype(BF16)
            for at, acc in enumerate((gate_acc, up_acc)):
                weight(at, p).wait()
                value = dot_nn(scaled, w_buf[at, lax.rem(p, 3)])

                @pl.when(p == 0)
                def _():
                    acc[...] = value

                @pl.when(p > 0)
                def _():
                    acc[...] += value

            @pl.when((p + 2) * deep < total_columns)
            def _():
                for at in range(2):
                    weight(at, p + 2).start()

        return carry

    lax.fori_loop(0, chunks + DOWN_LAG, step, 0)
    ga_copy.wait()
    tile = rows // TILES
    outs = [(n_ref, n_hbm), (act_ref, act_hbm), (gg_ref, gg_hbm), (gu_ref, gu_hbm)]

    def out_copy(at, i):
        here = pl.ds(pl.multiple_of(i * tile, tile), tile)
        return pltpu.make_async_copy(outs[at][0].at[here, :], outs[at][1].at[here, :], out_sem.at[at, i])

    branch_copy = pltpu.make_async_copy(branch, branch_hbm, ga_sem.at[1])
    branch_copy.start()

    def rows_step(i, carry):
        here = pl.ds(pl.multiple_of(i * tile, tile), tile)
        scale = lax.rsqrt(squares[here, :1] * (1.0 / total_columns) + epsilon)
        middle = x_ref[here, :].astype(F32) + branch[here, :].astype(F32)
        n_ref[here, :] = (middle * scale * gain_ref[...]).astype(BF16)
        gate = gate_acc[here, :] * scale
        up_pre = up_acc[here, :] * scale
        grad = ga_ref[here, :].astype(F32)
        sigmoid = jax.nn.sigmoid(gate)
        swish = gate * sigmoid
        act_ref[here, :] = (swish * up_pre).astype(BF16)
        gu_ref[here, :] = (grad * swish).astype(BF16)
        gg_ref[here, :] = (grad * up_pre * sigmoid * (1.0 + gate * (1.0 - sigmoid))).astype(BF16)
        for at in range(4):
            out_copy(at, i).start()
        return carry

    lax.fori_loop(0, TILES, rows_step, 0)

    def finish(c, carry):
        @pl.when(is_end)
        def _():
            for h in range(HALVES):
                up(c, h).wait_send()

        @pl.when(is_mid)
        def _():
            for h in range(HALVES):
                over(c, h).wait_send()
                down(c, h).wait_send()

        return carry

    lax.fori_loop(0, chunks, finish, 0)

    def drain(i, carry):
        for at in range(4):
            out_copy(at, i).wait()
        return carry

    lax.fori_loop(0, TILES, drain, 0)
    branch_copy.wait()


def forward(mixed, tokens, gain, w_output, w_gate, w_up, grad_active, call_id, chunks=16, deep=256):
    rows, columns = tokens.shape
    hidden = w_gate.shape[1]
    width = columns // chunks
    vmem, any_space = pl.BlockSpec(memory_space=pltpu.VMEM), pl.BlockSpec(memory_space=pl.ANY)
    dma = pltpu.SemaphoreType.DMA
    shapes = [(rows, columns), (rows, columns), (rows, hidden), (rows, hidden), (rows, hidden)]
    line_block = pltpu.VMEM((chunks, rows, width), BF16)
    return pl.pallas_call(
        forward_kernel,
        in_specs=[vmem] * 3 + [any_space] * 4,
        out_specs=[any_space] * 5,
        out_shape=[jax.ShapeDtypeStruct(shape, BF16) for shape in shapes],
        scratch_shapes=[pltpu.VMEM(shape, BF16) for shape in shapes]
        + [
            pltpu.VMEM((rows, hidden), BF16),
            pltpu.VMEM((rows, hidden), F32),
            pltpu.VMEM((rows, hidden), F32),
            pltpu.VMEM((rows, PAIR), F32),
            pltpu.VMEM((3, mixed.shape[1], width), BF16),
            pltpu.VMEM((2, 3, deep, hidden), BF16),
            line_block,
            line_block,
            line_block,
            dma((2,)),
            dma((3,)),
            dma((2, 3)),
            dma((3, HALVES, chunks)),
            dma((3, HALVES, chunks)),
            dma((4, TILES)),
        ],
        compiler_params=pltpu.CompilerParams(
            collective_id=call_id, has_side_effects=True, vmem_limit_bytes=62 << 20
        ),
        name="forward",
    )(mixed, tokens, gain, w_output, w_gate, w_up, grad_active)


def final_kernel(gn_ref, x_ref, gm_ref, gain_ref, mlp_ref, out_ref, gains_ref, acc, parts, come, send_sem, recv_sem):
    seq, batch = lax.axis_index("seq"), lax.axis_index("batch")
    seq_count = lax.axis_size("seq")
    peers = parts.shape[0]
    block = parts.shape[2]
    me = batch * seq_count + seq

    def peer(k):
        there = lax.rem(me + k, peers)
        return there, {"batch": lax.div(there, seq_count), "seq": lax.rem(there, seq_count)}

    def copy(k):
        there, device = peer(k)
        return pltpu.make_async_remote_copy(
            src_ref=parts.at[there],
            dst_ref=come.at[k],
            send_sem=send_sem.at[k],
            recv_sem=recv_sem.at[k],
            device_id=device,
            device_id_type=MESH,
        )

    barrier = pltpu.get_barrier_semaphore()
    for k in range(1, peers):
        pl.semaphore_signal(barrier, inc=1, device_id=peer(k)[1], device_id_type=MESH)
    rows = x_ref.shape[0]
    tile = rows // 8
    gain = gain_ref[...]
    acc[...] = jnp.zeros_like(acc)

    def rows_step(i, carry):
        here = pl.ds(pl.multiple_of(i * tile, tile), tile)
        wide = x_ref[here, :].astype(F32)
        grad = gn_ref[here, :].astype(F32)
        scale = lax.rsqrt(jnp.mean(wide * wide, axis=-1, keepdims=True) + epsilon)
        scaled = grad * gain
        mean = jnp.mean(wide * scaled, axis=-1, keepdims=True)
        result = gm_ref[here, :] + scale * scaled - wide * (scale * scale * scale) * mean
        out_ref[here, :] = result.astype(BF16)
        acc[...] += jnp.sum(grad * wide * scale, axis=0, keepdims=True)
        return carry

    lax.fori_loop(0, 8, rows_step, 0)
    for k in range(peers):
        here = slice(k * block, (k + 1) * block)
        parts[k, 0:1, :] = acc[:, here]
        parts[k, 1:2, :] = mlp_ref[:, here]
    pl.semaphore_wait(barrier, peers - 1)
    for k in range(1, peers):
        copy(k).start()
    total = parts[me]
    for k in range(1, peers):
        copy(k).wait_recv()
        total = total + come[k]
    gains_ref[...] = total
    for k in range(1, peers):
        copy(k).wait_send()


def final(grad_normed, tokens, grad_middle, gain, mlp_part, call_id):
    rows, width = tokens.shape
    peers = lax.axis_size("batch") * lax.axis_size("seq")
    block = width // peers
    vmem = pl.BlockSpec(memory_space=pltpu.VMEM)
    return pl.pallas_call(
        final_kernel,
        out_shape=[jax.ShapeDtypeStruct((rows, width), BF16), jax.ShapeDtypeStruct((2, block), F32)],
        in_specs=[vmem] * 5,
        out_specs=[vmem, vmem],
        scratch_shapes=[
            pltpu.VMEM((1, width), F32),
            pltpu.VMEM((peers, 2, block), F32),
            pltpu.VMEM((peers, 2, block), F32),
            pltpu.SemaphoreType.DMA((peers,)),
            pltpu.SemaphoreType.DMA((peers,)),
        ],
        compiler_params=pltpu.CompilerParams(collective_id=call_id, has_side_effects=True),
        name="final",
    )(grad_normed, tokens, grad_middle, gain, mlp_part)


def settle_kernel(places, *refs):
    count = len(places)
    sources, targets = refs[:count], refs[count : -count - 2]
    bufs, load_sem, store_sem = refs[-count - 2 : -2], refs[-2], refs[-1]

    def load(at):
        return pltpu.make_async_copy(sources[at], bufs[at], load_sem.at[at])

    def store(at):
        index, row = places[at]
        target = targets[index].at[row : row + bufs[at].shape[0], :]
        return pltpu.make_async_copy(bufs[at], target, store_sem.at[at])

    for at in range(count):
        load(at).start()
    for at in range(count):
        load(at).wait()
        store(at).start()
    for at in range(count):
        store(at).wait()


def settle(groups):
    places, shapes, arrays = [], [], []
    for index, group in enumerate(groups):
        row = 0
        for array in group:
            places.append((index, row))
            arrays.append(array)
            row += array.shape[0]
        shapes.append(jax.ShapeDtypeStruct((row, group[0].shape[1]), group[0].dtype))
    any_space = pl.BlockSpec(memory_space=pl.ANY)
    dma = pltpu.SemaphoreType.DMA
    return pl.pallas_call(
        functools.partial(settle_kernel, places),
        in_specs=[any_space] * len(arrays),
        out_specs=[any_space] * len(groups),
        out_shape=shapes,
        scratch_shapes=[pltpu.VMEM(array.shape, array.dtype) for array in arrays]
        + [dma((len(arrays),)), dma((len(arrays),))],
        compiler_params=pltpu.CompilerParams(vmem_limit_bytes=62 << 20),
        name="settle",
    )(*arrays)


def scatter_sum(left, right):
    rows, depth = left.shape
    columns = right.shape[1]
    batch_count = lax.axis_size("batch")
    seq_index = lax.axis_index("seq")
    core, chip = seq_index % 2, seq_index // 2
    block = depth // (4 * batch_count)
    split = left.reshape(rows, batch_count, 2, 2, block)
    size = lax.axis_size("seq")

    def product(at):
        taken = lax.dynamic_index_in_dim(split, at, 3, keepdims=False).reshape(rows, depth // 2)
        return dot_tn(taken, right)

    away = product(1 - core).astype(BF16)
    arrived = lax.ppermute(away, "seq", [(s, s ^ 1) for s in range(size)])
    kept = (product(core) + arrived.astype(F32)).astype(BF16)
    kept = kept.reshape(batch_count, 2, block, columns)
    half = columns // 2

    def over_chip(values, axis):
        sent = lax.dynamic_index_in_dim(values, 1 - chip, axis, keepdims=False)
        stay = lax.dynamic_index_in_dim(values, chip, axis, keepdims=False)
        came = lax.ppermute(sent, "seq", [(s, s ^ 2) for s in range(size)])
        return stay.astype(F32) + came.astype(F32)

    def over_batch(values):
        if batch_count == 2:
            here = lax.axis_index("batch")
            sent = lax.dynamic_index_in_dim(values, 1 - here, 0, keepdims=False)
            stay = lax.dynamic_index_in_dim(values, here, 0, keepdims=False)
            came = lax.ppermute(sent, "batch", [(0, 1), (1, 0)])
            return stay.astype(F32) + came.astype(F32)
        return lax.psum_scatter(values, "batch", scatter_dimension=0, tiled=False).astype(F32)

    one = over_batch(over_chip(kept[..., :half], 1).astype(BF16))
    two = over_chip(over_batch(kept[..., half:]).astype(BF16), 0)
    return jnp.concatenate([one, two], axis=1)


def local(
    tokens, segment_ids, attn_gain, w_query, w_key, w_value, w_output, mlp_gain, w_gate, w_up, w_down, cotangent
):
    rows, width = tokens.shape
    seq_count = lax.axis_size("seq")
    seq_index = lax.axis_index("seq")
    segments = segment_ids[0]
    first_row = seq_index * rows
    reach = LONGEST // rows
    cos, sin = rope_tables(segments, first_row, rows)
    row_segment = lax.dynamic_slice_in_dim(segments, first_row, rows, 0)[None, :]
    padded = jnp.concatenate([jnp.full((LONGEST,), -1, jnp.int32), segments])
    key_segment = lax.dynamic_slice_in_dim(padded, first_row, rows + LONGEST, 0)[:, None]

    normed, queries, key_value, grad_active = project(
        tokens, attn_gain[None, :], w_query, w_key, w_value, cos, sin, cotangent, w_down, 5
    )
    key_value = key_value.reshape(3 * rows, 2 * PAIR)
    mixed, logs = attend(queries, key_value, key_segment, row_segment)
    branch_low, normed_two, active, grad_gate_low, grad_up_low = forward(
        mixed, tokens, mlp_gain[None, :], w_output, w_gate, w_up, grad_active, 1
    )
    wide = tokens.astype(F32)
    middle = wide + branch_low.astype(F32)
    fused = lax.axis_size("batch") == 2
    hidden = w_gate.shape[1]
    unit = width // 8
    early = hidden * 5 // 8 // unit * unit
    if fused:
        grad_gate, grad_up, grad_down_one, grad_middle, grad_branch, grad_mixed, grad_mlp_gain, mlp_out = exchange(
            [normed_two, cotangent],
            [(grad_gate_low, 0, hidden), (grad_up_low, 0, hidden), (active, 0, hidden)],
            [
                [(w_gate, 0, hidden, "nt"), (w_up, hidden, hidden, "nt")],
                [(w_down, 2 * hidden, hidden, "nn")],
            ],
            (0, 2 * hidden // unit),
            [(unit, hidden), (unit, hidden), (early, unit)],
            [
                ("plain", 0, 0, 0, hidden),
                ("plain", 1, 0, hidden, hidden),
                ("turned", 2, 0, 2 * hidden, early),
            ],
            (2 * hidden + early) // unit,
            2,
            (3, 2),
            "branch",
            [tokens, branch_low, mlp_gain[None, :], w_output],
            [
                ((rows, width), F32),
                ((rows, width), BF16),
                ((rows, mixed.shape[1]), BF16),
                ((1, width), F32),
                ((rows, width), BF16),
            ],
        )
    else:
        grad_normed_two = line_sum([(grad_gate_low, w_gate, "nt"), (grad_up_low, w_up, "nt")], 2)
        grad_gate = scatter_sum(normed_two, grad_gate_low)
        grad_up = scatter_sum(normed_two, grad_up_low)
        mlp_out = lax.psum(dot_nn(active, w_down).astype(BF16), "mp")
        grad_normed_two = grad_normed_two.astype(F32)
        scaled_two = grad_normed_two * mlp_gain
        scale_two = lax.rsqrt(jnp.mean(middle * middle, axis=-1, keepdims=True) + epsilon)
        grad_middle = (
            cotangent.astype(F32)
            + scale_two * scaled_two
            - middle
            * (scale_two * scale_two * scale_two)
            * jnp.mean(middle * scaled_two, axis=-1, keepdims=True)
        )
        grad_mlp_gain = jnp.sum(grad_normed_two * middle * scale_two, axis=0)[None, :]
        grad_branch = grad_middle.astype(BF16)
        grad_mixed = dot_nt(grad_branch, w_output).astype(BF16)

    grad_query_pre, grad_key_pre, grad_value_pre = attend_back(
        queries, key_value, key_segment, row_segment, mixed, grad_mixed, logs, cos, sin, 6
    )
    query_width = grad_query_pre.shape[1]
    if fused:
        late, mixed_width = hidden - early, mixed.shape[1]
        query_at = late + mixed_width
        key_at = query_at + query_width
        grad_down_two, grad_output, grad_query, grad_key, grad_value, grad_tokens, gains, output = exchange(
            [cotangent, grad_branch, normed],
            [
                (active, early, late),
                (mixed, 0, mixed_width),
                (grad_query_pre, 0, query_width),
                (grad_key_pre, 0, PAIR),
                (grad_value_pre, 0, PAIR),
            ],
            [
                [
                    (w_query, query_at, query_width, "nt"),
                    (w_key, key_at, PAIR, "nt"),
                    (w_value, key_at + PAIR, PAIR, "nt"),
                ]
            ],
            (0, late // unit, query_at // unit),
            [(late, unit), (mixed_width, unit), (unit, query_width), (unit, PAIR), (unit, PAIR)],
            [
                ("turned", 0, 0, 0, late),
                ("turned", 1, 0, late, mixed_width),
                ("plain", 2, 0, query_at, query_width),
                ("plain", 3, 0, key_at, PAIR),
                ("plain", 4, 0, key_at + PAIR, PAIR),
            ],
            (key_at + 2 * PAIR) // unit,
            3,
            (2, 1),
            "tokens",
            [tokens, grad_middle, attn_gain[None, :], grad_mlp_gain, branch_low, mlp_out],
            [((rows, width), BF16), ((2, unit), F32), ((rows, width), BF16)],
        )
        grad_gate, grad_up, grad_down, grad_output, grad_query, grad_key, grad_value, grad_tokens, output = settle(
            [
                [grad_gate],
                [grad_up],
                [grad_down_one, grad_down_two],
                [grad_output],
                [grad_query],
                [grad_key],
                [grad_value],
                [grad_tokens],
                [output],
            ]
        )
    else:
        output = (middle + mlp_out.astype(F32)).astype(BF16)
        grad_down = scatter_sum(cotangent, active).T
        grad_output = scatter_sum(grad_branch, mixed).T
        grad_qkv = scatter_sum(normed, jnp.concatenate([grad_query_pre, grad_key_pre, grad_value_pre], axis=1))
        grad_query = grad_qkv[:, :query_width]
        grad_key = grad_qkv[:, query_width : query_width + PAIR]
        grad_value = grad_qkv[:, query_width + PAIR :]
        grad_normed = line_sum(
            [(grad_query_pre, w_query, "nt"), (grad_key_pre, w_key, "nt"), (grad_value_pre, w_value, "nt")], 3
        )
        grad_tokens, gains = final(grad_normed, tokens, grad_middle, attn_gain[None, :], grad_mlp_gain, 4)
    return (
        output,
        grad_tokens,
        gains[0],
        grad_query,
        grad_key,
        grad_value,
        grad_output,
        gains[1],
        grad_gate,
        grad_up,
        grad_down,
    )


def solution(mesh):
    tokens_spec = P(("batch", "seq"), None)
    in_specs = (
        tokens_spec,
        P("batch", None),
        P(),
        P(None, "mp"),
        P(None, "mp"),
        P(None, "mp"),
        P("mp", None),
        P(),
        P(None, "mp"),
        P(None, "mp"),
        P("mp", None),
        tokens_spec,
    )
    row_split = P(("batch", "seq"), "mp")
    column_split = P("mp", ("batch", "seq"))
    out_specs = (
        tokens_spec,
        tokens_spec,
        P(("batch", "seq")),
        row_split,
        row_split,
        row_split,
        column_split,
        P(("batch", "seq")),
        row_split,
        row_split,
        column_split,
    )
    return jax.shard_map(local, mesh=mesh, in_specs=in_specs, out_specs=out_specs, check_vma=False)
```

```python
import functools
import math

import jax
import jax.numpy as jnp
from jax import lax
from jax.experimental import pallas as pl
from jax.experimental.pallas import tpu as pltpu
from jax.sharding import PartitionSpec as P

HS = 64
PAIR = 2 * HS
LONGEST = 1024
FORWARD_ROWS = 256
BACKWARD_ROWS = 128
rope_base = 500000.0
epsilon = 1e-05
masked_score = -1e30
MESH = pl.DeviceIdType.MESH
F32 = jnp.float32
BF16 = jnp.bfloat16


def dot_nn(left, right):
    return lax.dot_general(left, right, (((1,), (0,)), ((), ())), preferred_element_type=F32)


def dot_nt(left, right):
    return lax.dot_general(left, right, (((1,), (1,)), ((), ())), preferred_element_type=F32)


def dot_tn(left, right):
    return lax.dot_general(left, right, (((0,), (0,)), ((), ())), preferred_element_type=F32)


def lanes_of(values):
    return lax.broadcasted_iota(jnp.int32, values.shape, 1)


def swap_halves(values):
    ahead = pltpu.roll(values, PAIR - HS // 2, 1)
    behind = pltpu.roll(values, HS // 2, 1)
    return jnp.where(lanes_of(values) % HS < HS // 2, ahead, behind)


def rope_tables(segments, first_row, rows):
    row_segment = lax.dynamic_slice_in_dim(segments, first_row, rows, 0)
    doc_start = jnp.sum((segments[None, :] < row_segment[:, None]).astype(jnp.int32), axis=1)
    place = (first_row + jnp.arange(rows, dtype=jnp.int32) - doc_start).astype(F32)
    lane = jnp.arange(PAIR, dtype=jnp.int32)
    frequency = jnp.exp((lane % (HS // 2)).astype(F32) * (-2.0 * math.log(rope_base) / HS))
    angles = place[:, None] * frequency[None, :]
    sign = jnp.where(lane % HS < HS // 2, -1.0, 1.0)
    return jnp.cos(angles), jnp.sin(angles) * sign[None, :]


def project_kernel(
    x_ref, gain_ref, wk_ref, wv_ref, cos_ref, sin_ref, cot_hbm, wq_hbm, wd_hbm,
    n_hbm, q_hbm, kv_hbm, ga_hbm,
    n_ref, q_ref, kv_ref, ga_ref, cot_ref, wq_ref, wd_ref, load_sem, wd_sem, send_sem, recv_sem, out_sem,
):
    rows = x_ref.shape[0]
    seq, seq_count = lax.axis_index("seq"), lax.axis_size("seq")
    hidden = wd_hbm.shape[0]
    width = wd_ref.shape[1]
    chunks = hidden // width
    block = rows // 2
    loads = [
        pltpu.make_async_copy(wq_hbm, wq_ref, load_sem.at[0]),
        pltpu.make_async_copy(cot_hbm, cot_ref, load_sem.at[1]),
    ]

    def weight(c):
        slot = lax.rem(c, 3)
        here = pl.ds(pl.multiple_of(c * width, width), width)
        return pltpu.make_async_copy(wd_hbm.at[here, :], wd_ref.at[slot], wd_sem.at[slot])

    def out_copy(at):
        source = (n_ref, q_ref, kv_ref, ga_ref)[at]
        return pltpu.make_async_copy(source, (n_hbm, q_hbm, kv_hbm, ga_hbm)[at], out_sem.at[at])

    def send(away):
        return pltpu.make_async_remote_copy(
            src_ref=kv_ref.at[2],
            dst_ref=kv_ref.at[2 - away],
            send_sem=send_sem.at[away],
            recv_sem=recv_sem.at[away],
            device_id={"seq": lax.rem(seq + away, seq_count)},
            device_id_type=MESH,
        )

    for load in loads:
        load.start()
    weight(0).start()
    weight(1).start()
    for away in (1, 2):

        @pl.when(seq < away)
        def _():
            kv_ref[2 - away] = jnp.zeros(kv_ref.shape[1:], BF16)

    barrier = pltpu.get_barrier_semaphore()
    for away in range(1, seq_count):
        there = lax.rem(seq + away, seq_count)
        pl.semaphore_signal(barrier, inc=1, device_id={"seq": there}, device_id_type=MESH)

    for half in range(2):
        here = slice(half * block, (half + 1) * block)
        cos, sin = cos_ref[here, :], sin_ref[here, :]
        wide = x_ref[here, :].astype(F32)
        scale = lax.rsqrt(jnp.mean(wide * wide, axis=-1, keepdims=True) + epsilon)
        normed = (wide * scale * gain_ref[...]).astype(BF16)
        n_ref[here, :] = normed
        keys = dot_nn(normed, wk_ref[...])
        keys = keys * cos + swap_halves(keys) * sin
        values = dot_nn(normed, wv_ref[...])
        low_half = lanes_of(keys) < HS
        kv_ref[2, here, :PAIR] = jnp.where(low_half, keys, pltpu.roll(values, HS, 1)).astype(BF16)
        kv_ref[2, here, PAIR:] = jnp.where(low_half, pltpu.roll(keys, HS, 1), values).astype(BF16)
    pl.semaphore_wait(barrier, seq_count - 1)
    for away in (1, 2):

        @pl.when(seq + away < seq_count)
        def _():
            send(away).start()

    out_copy(0).start()
    for load in loads:
        load.wait()
    for half in range(2):
        here = slice(half * block, (half + 1) * block)
        cos, sin = cos_ref[here, :], sin_ref[here, :]
        queries = dot_nn(n_ref[here, :], wq_ref[...])
        for start in range(0, queries.shape[1], PAIR):
            part = queries[:, start : start + PAIR]
            q_ref[here, start : start + PAIR] = (part * cos + swap_halves(part) * sin).astype(BF16)
    out_copy(1).start()

    def step(c, carry):
        weight(c).wait()

        @pl.when(c + 2 < chunks)
        def _():
            weight(c + 2).start()

        here = pl.ds(pl.multiple_of(c * width, width), width)
        ga_ref[:, here] = dot_nt(cot_ref[...], wd_ref[lax.rem(c, 3)]).astype(BF16)
        return carry

    lax.fori_loop(0, chunks, step, 0)
    out_copy(3).start()
    for away in (1, 2):

        @pl.when(seq >= away)
        def _():
            send(away).wait_recv()

    out_copy(2).start()
    for away in (1, 2):

        @pl.when(seq + away < seq_count)
        def _():
            send(away).wait_send()

    for at in range(4):
        out_copy(at).wait()


def project(tokens, gain, w_query, w_key, w_value, cos, sin, cotangent, w_down, call_id):
    rows, width = tokens.shape
    columns, hidden = w_query.shape[1], w_down.shape[0]
    chunk = PROJECT_CHUNK
    vmem, any_space = pl.BlockSpec(memory_space=pltpu.VMEM), pl.BlockSpec(memory_space=pl.ANY)
    shapes = [(rows, width), (rows, columns), (3, rows, 2 * PAIR), (rows, hidden)]
    dma = pltpu.SemaphoreType.DMA
    return pl.pallas_call(
        project_kernel,
        in_specs=[vmem] * 6 + [any_space] * 3,
        out_specs=[any_space] * 4,
        out_shape=[jax.ShapeDtypeStruct(shape, BF16) for shape in shapes],
        scratch_shapes=[pltpu.VMEM(shape, BF16) for shape in shapes]
        + [
            pltpu.VMEM((rows, width), BF16),
            pltpu.VMEM(w_query.shape, BF16),
            pltpu.VMEM((3, chunk, width), BF16),
            dma((2,)),
            dma((3,)),
            dma((3,)),
            dma((3,)),
            dma((4,)),
        ],
        compiler_params=pltpu.CompilerParams(
            collective_id=call_id, has_side_effects=True, vmem_limit_bytes=62 << 20
        ),
        name="project",
    )(tokens, gain, w_key, w_value, cos, sin, cotangent, w_query, w_down)


def write_bias(bias_ref, key_ref, row_ref):
    tiles, span, both = bias_ref.shape
    size = both // 2
    key_place = lax.broadcasted_iota(jnp.int32, (span, size), 0) - LONGEST
    row_place = lax.broadcasted_iota(jnp.int32, (span, size), 1)
    for tile in range(tiles):
        start = tile * size
        same = key_ref[start : start + span, :] == row_ref[:, start : start + size]
        bias = jnp.where(same & (key_place <= row_place), 0.0, masked_score)
        bias_ref[tile] = jnp.concatenate([bias, bias], axis=1)


def bias_scratch(rows, size):
    assert LONGEST + rows == 3 * rows
    return pltpu.VMEM((rows // size, LONGEST + size, 2 * size), F32)


def heads_beside(values, here):
    return jnp.concatenate([values[:HS, here], values[HS:, here]], axis=1)


def heads_below(values, here):
    return jnp.concatenate([values[here, :HS], values[here, HS:]], axis=0)


def heads_stacked(values):
    size = values.shape[1] // 2
    return jnp.concatenate([values[:, :size], values[:, size:]], axis=0)


def attend_kernel(q_ref, kv_ref, key_ref, row_ref, out_ref, log_ref, bias_ref):
    @pl.when(pl.program_id(0) == 0)
    def _():
        write_bias(bias_ref, key_ref, row_ref)

    key_value = kv_ref[...]
    flipped = key_value.T
    q_flipped = (q_ref[...].astype(F32) * HS ** (-0.5)).astype(BF16).T
    tiles, span, both = bias_ref.shape
    size = both // 2
    for tile in range(tiles):
        here = slice(tile * size, (tile + 1) * size)
        keys = slice(tile * size, tile * size + span)
        scores = dot_nn(key_value[keys, :HS], heads_beside(q_flipped, here)) + bias_ref[tile]
        top = jnp.max(scores, axis=0, keepdims=True)
        powers = jnp.exp(scores - top)
        total = jnp.sum(powers, axis=0, keepdims=True)
        mixed = dot_nn(flipped[HS:, keys], powers.astype(BF16)) / total
        logs = top + jnp.log(total)
        log_ref[0, 0:1, here] = logs[:, :size]
        log_ref[0, 1:2, here] = logs[:, size:]
        out_ref[here, :] = heads_stacked(mixed).T.astype(BF16)


def attend(queries, key_value, key_segment, row_segment):
    rows, width = queries.shape
    pairs = width // PAIR
    per_group = pairs // 2
    pair_tile = pl.BlockSpec((rows, PAIR), lambda p: (0, p))
    kv_tile = pl.BlockSpec((3 * rows, PAIR), lambda p: (0, p // per_group))
    return pl.pallas_call(
        attend_kernel,
        grid=(pairs,),
        in_specs=[
            pair_tile,
            kv_tile,
            pl.BlockSpec(key_segment.shape, lambda p: (0, 0)),
            pl.BlockSpec(row_segment.shape, lambda p: (0, 0)),
        ],
        out_specs=[pair_tile, pl.BlockSpec((1, 2, rows), lambda p: (p, 0, 0))],
        out_shape=[
            jax.ShapeDtypeStruct((rows, width), BF16),
            jax.ShapeDtypeStruct((pairs, 2, rows), F32),
        ],
        scratch_shapes=[bias_scratch(rows, FORWARD_ROWS)],
        cost_estimate=pl.CostEstimate(
            flops=16 << 30, bytes_accessed=4 << 20, transcendentals=3 * rows * rows * 2 * pairs
        ),
        name="attend",
    )(queries, key_value, key_segment, row_segment)


def attend_back_kernel(
    q_ref, kv_ref, key_ref, row_ref, out_ref, grad_ref, log_ref, cos_ref, sin_ref,
    dq_ref, dk_ref, dv_ref, bias_ref, dkv_ref, own_ref, sent_ref, come_ref, send_sem, recv_sem, per_group,
):
    step = pl.program_id(0)
    seq, seq_count = lax.axis_index("seq"), lax.axis_size("seq")
    barrier = pltpu.get_barrier_semaphore()

    def back(group, away):
        return pltpu.make_async_remote_copy(
            src_ref=sent_ref.at[group, 2 - away],
            dst_ref=come_ref.at[group, 2 - away],
            send_sem=send_sem.at[group, 2 - away],
            recv_sem=recv_sem.at[group, 2 - away],
            device_id={"seq": lax.rem(seq + seq_count - away, seq_count)},
            device_id_type=MESH,
        )

    @pl.when(step == 0)
    def _():
        for away in range(1, seq_count):
            there = lax.rem(seq + away, seq_count)
            pl.semaphore_signal(barrier, inc=1, device_id={"seq": there}, device_id_type=MESH)
        write_bias(bias_ref, key_ref, row_ref)

    rows = q_ref.shape[0]
    key_value = kv_ref[...]
    flipped = key_value[:, :].T
    scaled = (q_ref[...].astype(F32) * HS ** (-0.5)).astype(BF16)
    q_flipped = scaled.T
    grad = grad_ref[...]
    grad_flipped = grad.T
    product = (out_ref[...].astype(F32) * grad.astype(F32)).T
    tiles, span, both = bias_ref.shape
    size = both // 2

    @pl.when(step % per_group == 0)
    def _():
        dkv_ref[...] = jnp.zeros_like(dkv_ref)

    for tile in range(tiles):
        here = slice(tile * size, (tile + 1) * size)
        keys = slice(tile * size, tile * size + span)
        logs = jnp.concatenate([log_ref[0, 0:1, here], log_ref[0, 1:2, here]], axis=1)
        delta = jnp.sum(heads_beside(product, here), axis=0, keepdims=True)
        scores = dot_nn(key_value[keys, :HS], heads_beside(q_flipped, here)) + bias_ref[tile]
        shares = jnp.exp(scores - logs)
        grad_shares = dot_nn(key_value[keys, HS:], heads_beside(grad_flipped, here))
        grad_scores = (shares * (grad_shares - delta)).astype(BF16)
        dvalue = dot_nn(shares.astype(BF16), heads_below(grad, here))
        dkey = dot_nn(grad_scores, heads_below(scaled, here))
        dkv_ref[keys, :] += jnp.concatenate([dkey, dvalue], axis=1)
        dq = heads_stacked(dot_nn(flipped[:HS, keys], grad_scores)).T * HS ** (-0.5)
        dq_ref[here, :] = (dq * cos_ref[here, :] - swap_halves(dq) * sin_ref[here, :]).astype(BF16)

    for group in range(2):

        @pl.when(step == (group + 1) * per_group - 1)
        def _():
            sent_ref[group, 0] = dkv_ref[:rows, :].astype(BF16)
            sent_ref[group, 1] = dkv_ref[rows : 2 * rows, :].astype(BF16)
            own_ref[group] = dkv_ref[2 * rows :, :]
            if group == 0:
                pl.semaphore_wait(barrier, seq_count - 1)
            for away in (1, 2):

                @pl.when(seq >= away)
                def _():
                    back(group, away).start()

    @pl.when(step == 2 * per_group - 1)
    def _():
        for group in range(2):
            for away in (1, 2):

                @pl.when(seq + away < seq_count)
                def _():
                    back(group, away).wait_recv()
                    own_ref[group] += come_ref[group, 2 - away].astype(F32)

        one, two = own_ref[0], own_ref[1]
        low_half = lanes_of(one) < HS
        keys = jnp.where(low_half, one, pltpu.roll(two, HS, 1))
        dk_ref[...] = (keys * cos_ref[...] - swap_halves(keys) * sin_ref[...]).astype(BF16)
        dv_ref[...] = jnp.where(low_half, pltpu.roll(one, HS, 1), two).astype(BF16)
        for group in range(2):
            for away in (1, 2):

                @pl.when(seq >= away)
                def _():
                    back(group, away).wait_send()


def attend_back(queries, key_value, key_segment, row_segment, mixed, grad, logs, cos, sin, call_id):
    rows, width = queries.shape
    pairs = width // PAIR
    per_group = pairs // 2
    pair_tile = pl.BlockSpec((rows, PAIR), lambda p: (0, p))
    whole = pl.BlockSpec((rows, PAIR), lambda p: (0, 0))
    wide_tile = pl.BlockSpec((3 * rows, PAIR), lambda p: (0, p // per_group))
    full = lambda array: pl.BlockSpec(array.shape, lambda p: (0, 0))
    return pl.pallas_call(
        functools.partial(attend_back_kernel, per_group=per_group),
        grid=(pairs,),
        in_specs=[
            pair_tile,
            wide_tile,
            full(key_segment),
            full(row_segment),
            pair_tile,
            pair_tile,
            pl.BlockSpec((1, 2, rows), lambda p: (p, 0, 0)),
            full(cos),
            full(sin),
        ],
        out_specs=[pair_tile, whole, whole],
        out_shape=[
            jax.ShapeDtypeStruct((rows, width), BF16),
            jax.ShapeDtypeStruct((rows, PAIR), BF16),
            jax.ShapeDtypeStruct((rows, PAIR), BF16),
        ],
        scratch_shapes=[
            bias_scratch(rows, BACKWARD_ROWS),
            pltpu.VMEM((3 * rows, PAIR), F32),
            pltpu.VMEM((2, rows, PAIR), F32),
            pltpu.VMEM((2, 2, rows, PAIR), BF16),
            pltpu.VMEM((2, 2, rows, PAIR), BF16),
            pltpu.SemaphoreType.DMA((2, 2)),
            pltpu.SemaphoreType.DMA((2, 2)),
        ],
        compiler_params=pltpu.CompilerParams(collective_id=call_id, has_side_effects=True),
        cost_estimate=pl.CostEstimate(
            flops=40 << 30, bytes_accessed=6 << 20, transcendentals=3 * rows * rows * 2 * pairs
        ),
        name="attend_back",
    )(queries, key_value, key_segment, row_segment, mixed, grad, logs, cos, sin)


def line_sum_kernel(modes, chunks, *refs):
    count = len(modes)
    a_refs, w_refs, out_ref = refs[:count], refs[count : 2 * count], refs[2 * count]
    rest = refs[2 * count + 1 :]
    w_bufs = rest[:count]
    part, first, second, total, w_sem, send_sem, recv_sem = rest[count:]
    width = part.shape[2]
    place = lax.axis_index("mp")
    pair = place + 1 - 2 * lax.rem(place, 2)
    across = 3 - place
    is_mid = (place == 1) | (place == 2)
    is_end = (place == 0) | (place == 3)

    def weight(at, c):
        if modes[at] == "nt":
            source = w_refs[at].at[pl.ds(pl.multiple_of(c * width, width), width), :]
        else:
            source = w_refs[at].at[:, pl.ds(pl.multiple_of(c * width, width), width)]
        return pltpu.make_async_copy(source, w_bufs[at].at[c], w_sem.at[at, c])

    def remote(kind, source, target, c, device):
        return pltpu.make_async_remote_copy(
            src_ref=source.at[c],
            dst_ref=target.at[c],
            send_sem=send_sem.at[kind, c],
            recv_sem=recv_sem.at[kind, c],
            device_id={"mp": device},
            device_id_type=MESH,
        )

    def up(c):
        return remote(0, part, first, c, pair)

    def over(c):
        return remote(1, part, second, c, across)

    def down(c):
        return remote(2, total, total, c, pair)

    def start_weights(c, carry):
        for at in range(count):
            weight(at, c).start()
        return carry

    lax.fori_loop(0, chunks, start_weights, 0)
    barrier = pltpu.get_barrier_semaphore()
    pl.semaphore_signal(barrier, inc=1, device_id={"mp": pair}, device_id_type=MESH)

    @pl.when(is_mid)
    def _():
        pl.semaphore_signal(barrier, inc=1, device_id={"mp": across}, device_id_type=MESH)
        pl.semaphore_wait(barrier, 2)

    @pl.when(is_end)
    def _():
        pl.semaphore_wait(barrier, 1)

    def step(t, carry):
        @pl.when(t < chunks)
        def _():
            value = None
            for at in range(count):
                weight(at, t).wait()
                dot = dot_nt if modes[at] == "nt" else dot_nn
                term = dot(a_refs[at][...], w_bufs[at][t])
                value = term if value is None else value + term
            part[t] = value.astype(BF16)

            @pl.when(is_end)
            def _():
                up(t).start()

        @pl.when(is_mid & (t >= 1) & (t < chunks + 1))
        def _():
            c = t - 1
            up(c).wait_recv()
            part[c] = (part[c].astype(F32) + first[c].astype(F32)).astype(BF16)
            over(c).start()

        @pl.when(is_mid & (t >= OVER_LAG))
        def _():
            c = t - OVER_LAG
            over(c).wait_recv()
            total[c] = (part[c].astype(F32) + second[c].astype(F32)).astype(BF16)
            down(c).start()

        return carry

    lax.fori_loop(0, chunks + OVER_LAG, step, 0)

    def finish(c, carry):
        @pl.when(is_end)
        def _():
            up(c).wait_send()
            down(c).wait_recv()

        @pl.when(is_mid)
        def _():
            over(c).wait_send()
            down(c).wait_send()

        out_ref[:, pl.ds(pl.multiple_of(c * width, width), width)] = total[c]
        return carry

    lax.fori_loop(0, chunks, finish, 0)


def line_sum(pairs, call_id, chunks=16):
    lefts = [left for left, _, _ in pairs]
    rights = [right for _, right, _ in pairs]
    modes = tuple(mode for _, _, mode in pairs)
    rows = lefts[0].shape[0]
    columns = rights[0].shape[0] if modes[0] == "nt" else rights[0].shape[1]
    width = columns // chunks
    count = len(pairs)
    bufs = [
        pltpu.VMEM((chunks, width, left.shape[1]) if mode == "nt" else (chunks, left.shape[1], width), BF16)
        for left, _, mode in pairs
    ]
    flops = sum(2 * rows * columns * left.shape[1] for left in lefts)
    moved = sum(right.size * 2 for right in rights)
    block = pltpu.VMEM((chunks, rows, width), BF16)
    return pl.pallas_call(
        functools.partial(line_sum_kernel, modes, chunks),
        out_shape=jax.ShapeDtypeStruct((rows, columns), BF16),
        in_specs=[pl.BlockSpec(memory_space=pltpu.VMEM)] * count
        + [pl.BlockSpec(memory_space=pl.ANY)] * count,
        out_specs=pl.BlockSpec(memory_space=pltpu.VMEM),
        scratch_shapes=bufs
        + [
            block,
            block,
            block,
            block,
            pltpu.SemaphoreType.DMA((count, chunks)),
            pltpu.SemaphoreType.DMA((3, chunks)),
            pltpu.SemaphoreType.DMA((3, chunks)),
        ],
        compiler_params=pltpu.CompilerParams(collective_id=call_id, has_side_effects=True),
        cost_estimate=pl.CostEstimate(
            flops=flops + (40 << 30), bytes_accessed=moved, transcendentals=0
        ),
        name=f"line_sum_{call_id}",
    )(*lefts, *rights)

LAG = 3
UP_LAG = 1
OVER_LAG = 3
DOWN_LAG = 8
HALVES = 1
LAST_LAG = 12
TILES = 8
PROJECT_CHUNK = 512


def exchange_kernel(plan, *refs):
    left_count, rights, sums, flips_before, spans, out_count, units, chunks, period, active, ending, given, made = plan
    refs = list(refs)

    def take(n):
        got = refs[:n]
        del refs[:n]
        return got

    weights = [item for group in sums for item in group]
    left_refs, right_refs, w_refs = take(left_count), take(len(rights)), take(len(weights))
    given_refs = take(given)
    grad_refs, made_refs = take(out_count), take(made)
    stage, flip, right_all, out_ref = take(4)
    w_bufs = take(len(weights))
    part, first, second, away, come_one, come_two, come_three, result = take(8)
    given_bufs, made_bufs = take(given), take(made - (ending == "branch"))
    acc, dots, scales, gain_parts, gain_come, given_sem, made_sem, gain_send, gain_recv = take(9)
    in_sem, right_sem, w_sem, ar_send, ar_recv, core_send, core_recv, two_send, two_recv, three_send, three_recv, out_sem = refs
    width = part.shape[2]
    block = come_three.shape[1]
    all_chunks = chunks * len(sums)
    place = lax.axis_index("mp")
    seq, batch = lax.axis_index("seq"), lax.axis_index("batch")
    core, chip = lax.rem(seq, 2), lax.div(seq, 2)
    sibling = seq + 1 - 2 * core
    beside = seq + 2 - 4 * chip
    pair = place + 1 - 2 * lax.rem(place, 2)
    across = 3 - place
    is_mid = (place == 1) | (place == 2)
    is_end = (place == 0) | (place == 3)

    def columns_of(c):
        return pl.ds(pl.multiple_of(c * width, width), width)

    def weight(at, group, c):
        here = columns_of(c - group * chunks)
        source = w_refs[at].at[here, :] if weights[at][2] == "nt" else w_refs[at].at[:, here]
        slot = lax.rem(c, 3)
        return pltpu.make_async_copy(source, w_bufs[at].at[slot], w_sem.at[at, slot])

    members = []
    for group, items in enumerate(sums):
        for _ in items:
            members.append(group)

    def load_weights(c):
        for group in range(len(sums)):

            @pl.when((c >= group * chunks) & (c < (group + 1) * chunks))
            def _():
                for at in range(len(weights)):
                    if members[at] == group:
                        weight(at, group, c).start()

    def remote(source, target, send, recv, device):
        return pltpu.make_async_remote_copy(
            src_ref=source, dst_ref=target, send_sem=send, recv_sem=recv, device_id=device, device_id_type=MESH
        )

    def slot_of(c):
        return lax.rem(c, chunks)

    high = part.shape[1] // HALVES

    def rows_of(h):
        return slice(h * high, (h + 1) * high)

    def up(c, h):
        slot = slot_of(c)
        source, target = part.at[slot, rows_of(h)], first.at[slot, rows_of(h)]
        return remote(source, target, ar_send.at[0, h, c], ar_recv.at[0, h, c], {"mp": pair})

    def over(c, h):
        slot = slot_of(c)
        source, target = part.at[slot, rows_of(h)], second.at[slot, rows_of(h)]
        return remote(source, target, ar_send.at[1, h, c], ar_recv.at[1, h, c], {"mp": across})

    def down(c, h):
        here = out_ref.at[rows_of(h), columns_of(c)]
        return remote(here, here, ar_send.at[2, h, c], ar_recv.at[2, h, c], {"mp": pair})

    def to_core(u):
        return remote(away.at[lax.rem(u, 2)], come_one.at[u], core_send.at[u], core_recv.at[u], {"seq": sibling})

    def chip_first(u):
        return 1 - lax.rem(u, 2)

    def sent_at(u, k):
        x_first = chip_first(u)
        return x_first * (2 * k + 1 - chip) + (1 - x_first) * (2 * (1 - batch) + k)

    def kept_at(u, k):
        x_first = chip_first(u)
        return x_first * (2 * k + chip) + (1 - x_first) * (2 * batch + k)

    def own_at(u):
        x_first = chip_first(u)
        return x_first * batch + (1 - x_first) * chip

    def device_of(x_way):
        return {
            "seq": x_way * beside + (1 - x_way) * seq,
            "batch": x_way * batch + (1 - x_way) * (1 - batch),
        }

    def second_hop(u, k):
        return remote(
            come_one.at[u, sent_at(u, k)], come_two.at[u, k], two_send.at[k, u], two_recv.at[k, u], device_of(chip_first(u))
        )

    def third_hop(u):
        return remote(
            come_two.at[u, 1 - own_at(u)], come_three.at[u], three_send.at[u], three_recv.at[u], device_of(1 - chip_first(u))
        )

    def left_copy(at):
        return pltpu.make_async_copy(left_refs[at], stage, in_sem.at[at])

    def right_copy(at):
        offset, source, size = rights[at]
        return pltpu.make_async_copy(
            right_refs[at].at[:, source : source + size], right_all.at[:, offset : offset + size], right_sem.at[at]
        )

    def out_copy(at, u):
        kind, index, offset, start, size = spans[at]
        slot = lax.rem(u, 2)
        if size < block:
            source = result.at[slot, :, start % block : start % block + size]
            target = grad_refs[index].at[:, offset : offset + size]
        else:
            source = result.at[slot]
            here = pl.ds(pl.multiple_of((u - start // block) * block + offset, block), block)
            target = grad_refs[index].at[here, :] if kind == "turned" else grad_refs[index].at[:, here]
        return pltpu.make_async_copy(source, target, out_sem.at[at, slot])

    def units_of(at):
        _, _, _, start, size = spans[at]
        return start // block, max((start + size) // block, start // block + 1)

    seq_count = lax.axis_size("seq")
    peers = lax.axis_size("batch") * seq_count
    me = batch * seq_count + seq

    def peer(k):
        there = lax.rem(me + k, peers)
        return there, {"batch": lax.div(there, seq_count), "seq": lax.rem(there, seq_count)}

    def gain_copy(k):
        there, device = peer(k)
        return remote(gain_parts.at[there], gain_come.at[k], gain_send.at[k], gain_recv.at[k], device)

    def given_copy(at):
        return pltpu.make_async_copy(given_refs[at], given_bufs[at], given_sem.at[at])

    def made_copy(at):
        source = out_ref.at[:, columns // 2 :] if ending == "branch" and at == made - 1 else made_bufs[at]
        return pltpu.make_async_copy(source, made_refs[at], made_sem.at[at])

    columns = out_ref.shape[1]
    rows = out_ref.shape[0]
    tile = rows // TILES

    def tile_of(i):
        return pl.ds(pl.multiple_of(i * tile, tile), tile)

    def branch_rows(i):
        here = tile_of(i)
        gm_buf, gb_buf, _ = made_bufs[:3]
        x_buf, b_buf, gain_buf, _ = given_bufs
        grad = out_ref[here, : columns // 2].astype(F32)
        middle = x_buf[here, :].astype(F32) + b_buf[here, :].astype(F32)
        scale = lax.rsqrt(jnp.mean(middle * middle, axis=-1, keepdims=True) + epsilon)
        scaled = grad * gain_buf[...]
        mean = jnp.mean(middle * scaled, axis=-1, keepdims=True)
        value = stage[here, :].astype(F32) + scale * scaled - middle * (scale * scale * scale) * mean
        gm_buf[here, :] = value
        gb_buf[here, :] = value.astype(BF16)
        acc[...] += jnp.sum(grad * middle * scale, axis=0, keepdims=True)

    def branch_end():
        made_bufs[2][...] = dot_nt(made_bufs[1][...], given_bufs[3][...]).astype(BF16)
        made_bufs[3][...] = acc[...]
        for at in range(4):
            made_copy(at).start()

    def token_columns(c):
        here = columns_of(c)
        x_buf, _, gain_buf = given_bufs[:3]
        value = out_ref[:, here].astype(F32) * x_buf[:, here].astype(F32)
        dots[...] += value * gain_buf[:, here]
        acc[:, here] = jnp.sum(value * scales[...], axis=0, keepdims=True)

    def token_rows(i, carry):
        here = tile_of(i)
        x_buf, gm_buf, gain_buf = given_bufs[:3]
        scale = scales[here, :1]
        mean = jnp.sum(dots[here, :], axis=-1, keepdims=True) * (1.0 / columns)
        wide = x_buf[here, :].astype(F32)
        scaled = out_ref[here, :].astype(F32) * gain_buf[...]
        value = gm_buf[here, :] + scale * scaled - wide * ((scale * scale * scale) * mean)
        made_bufs[0][here, :] = value.astype(BF16)
        return carry

    def output_rows(i):
        here = tile_of(i)
        x_buf, b_buf, m_buf = given_bufs[0], given_bufs[4], given_bufs[5]
        wide = x_buf[here, :].astype(F32)
        scale = lax.rsqrt(jnp.mean(wide * wide, axis=-1, keepdims=True) + epsilon)
        scales[here, :] = jnp.broadcast_to(scale, (tile, width))
        value = wide + b_buf[here, :].astype(F32) + m_buf[here, :].astype(F32)
        made_bufs[2][here, :] = value.astype(BF16)

    acc[...] = jnp.zeros_like(acc)
    dots[...] = jnp.zeros_like(dots)
    load_weights(0)
    load_weights(1)
    for at in range(len(rights)):
        right_copy(at).start()
    left_copy(0).start()
    for at in range(given):
        given_copy(at).start()

    barrier = pltpu.get_barrier_semaphore()
    if ending == "tokens":
        greeted = [{"mp": pair}] + [peer(k)[1] for k in range(1, peers)]
    else:
        greeted = [{"mp": pair}, {"seq": sibling}, {"seq": beside}, {"batch": 1 - batch}]
    for device in greeted:
        pl.semaphore_signal(barrier, inc=1, device_id=device, device_id_type=MESH)

    @pl.when(is_mid)
    def _():
        pl.semaphore_signal(barrier, inc=1, device_id={"mp": across}, device_id_type=MESH)
        pl.semaphore_wait(barrier, len(greeted) + 1)

    @pl.when(is_end)
    def _():
        pl.semaphore_wait(barrier, len(greeted))

    for at in range(len(rights)):
        right_copy(at).wait()

    def left_of(u):
        index = 0
        for at in range(1, left_count):
            index = index + (u >= flips_before[at]).astype(jnp.int32)
        return index

    def product(u, at, side):
        row = pl.multiple_of((2 * at + side) * block, block)
        column = pl.multiple_of(u * block, block)
        return dot_nn(flip[left_of(u), pl.ds(row, block), :], right_all[:, pl.ds(column, block)])

    def step_of(u):
        return (u // active) * period + u % active

    def on_unit(t, body):
        u = lax.div(t, period) * active + lax.rem(t, period)

        @pl.when((t >= 0) & (lax.rem(t, period) < active) & (u < units))
        def _():
            body(u)

    def first_stage(u):
        @pl.when(u >= 2)
        def _():
            to_core(u - 2).wait_send()

        for at in range(4):
            away[lax.rem(u, 2), at] = product(u, at, 1 - core).astype(BF16)
        to_core(u).start()

    def second_stage(u):
        to_core(u).wait_recv()
        for at in range(4):
            come_one[u, at] = (product(u, at, core) + come_one[u, at].astype(F32)).astype(BF16)
        for k in range(2):
            second_hop(u, k).start()

    def third_stage(u):
        for k in range(2):
            second_hop(u, k).wait_recv()
        sent = 1 - own_at(u)
        come_two[u, sent] = (come_two[u, sent].astype(F32) + come_one[u, kept_at(u, sent)].astype(F32)).astype(BF16)
        third_hop(u).start()

    def last_stage(u):
        third_hop(u).wait_recv()
        own = own_at(u)
        value = come_three[u].astype(F32) + come_two[u, own].astype(F32) + come_one[u, kept_at(u, own)].astype(F32)
        for at in range(len(spans)):
            low, high = units_of(at)

            @pl.when((u - 2 >= low) & (u - 2 < high))
            def _():
                out_copy(at, u - 2).wait()

        for kind in ("turned", "plain"):
            mine = [units_of(at) for at in range(len(spans)) if spans[at][0] == kind]
            if mine:
                low, high = min(m[0] for m in mine), max(m[1] for m in mine)

                @pl.when((u >= low) & (u < high))
                def _():
                    result[lax.rem(u, 2)] = value.T if kind == "turned" else value

        for at in range(len(spans)):
            low, high = units_of(at)

            @pl.when((u >= low) & (u < high))
            def _():
                out_copy(at, u).start()

    def step(t, carry):
        @pl.when((t >= chunks) & (t < all_chunks))
        def _():
            @pl.when(is_end)
            def _():
                for h in range(HALVES):
                    up(t - chunks, h).wait_send()

            @pl.when(is_mid)
            def _():
                for h in range(HALVES):
                    over(t - chunks, h).wait_send()

        for group, items in enumerate(sums):

            @pl.when((t >= group * chunks) & (t < (group + 1) * chunks))
            def _():
                value = None
                for at, (start, size, mode) in enumerate(weights):
                    if members[at] == group:
                        weight(at, group, t).wait()
                        dot = dot_nt if mode == "nt" else dot_nn
                        term = dot(right_all[:, start : start + size], w_bufs[at][lax.rem(t, 3)])
                        value = term if value is None else value + term
                part[slot_of(t)] = value.astype(BF16)

        @pl.when(t < all_chunks)
        def _():
            @pl.when(is_end)
            def _():
                for h in range(HALVES):
                    up(t, h).start()

            load_weights(t + 2)

        @pl.when(is_mid & (t >= UP_LAG) & (t < all_chunks + UP_LAG))
        def _():
            c = t - UP_LAG
            slot = slot_of(c)
            for h in range(HALVES):
                here = rows_of(h)
                up(c, h).wait_recv()
                part[slot, here] = (part[slot, here].astype(F32) + first[slot, here].astype(F32)).astype(BF16)
                over(c, h).start()

        @pl.when(is_mid & (t >= OVER_LAG) & (t < all_chunks + OVER_LAG))
        def _():
            c = t - OVER_LAG
            slot = slot_of(c)
            for h in range(HALVES):
                here = rows_of(h)
                over(c, h).wait_recv()
                value = part[slot, here].astype(F32) + second[slot, here].astype(F32)
                out_ref[here, columns_of(c)] = value.astype(BF16)
                down(c, h).start()

        @pl.when(is_end & (t >= DOWN_LAG) & (t < all_chunks + DOWN_LAG))
        def _():
            for h in range(HALVES):
                down(t - DOWN_LAG, h).wait_recv()

        for at in range(left_count):

            @pl.when(t == max(step_of(flips_before[at]) - 2, at))
            def _():
                left_copy(at).wait()

                def turn(k, carry):
                    here = pl.ds(pl.multiple_of(k * block, block), block)
                    flip[at, here, :] = stage[:, here].T
                    return carry

                lax.fori_loop(0, flip.shape[1] // block, turn, 0)
                if at + 1 < left_count:
                    left_copy(at + 1).start()

        on_unit(t, first_stage)
        on_unit(t - 1, second_stage)
        on_unit(t - 1 - LAG, third_stage)
        on_unit(t - 1 - 2 * LAG, last_stage)
        if ending == "branch":

            @pl.when(t == chunks + DOWN_LAG)
            def _():
                for at in range(given):
                    given_copy(at).wait()

            @pl.when((t >= chunks + DOWN_LAG) & (t < chunks + DOWN_LAG + TILES))
            def _():
                branch_rows(t - chunks - DOWN_LAG)

            @pl.when(t == chunks + DOWN_LAG + TILES)
            def _():
                branch_end()

        else:

            @pl.when(t == TILES // 2)
            def _():
                for at in range(given):
                    given_copy(at).wait()

            @pl.when((t >= TILES // 2) & (t < TILES // 2 + TILES))
            def _():
                output_rows(t - TILES // 2)

            @pl.when(t == TILES // 2 + TILES)
            def _():
                made_copy(2).start()

            @pl.when((t >= LAST_LAG) & (t < all_chunks + LAST_LAG))
            def _():
                token_columns(t - LAST_LAG)

        return carry

    last = all_chunks + (DOWN_LAG if ending == "branch" else LAST_LAG)
    lax.fori_loop(0, max(step_of(units - 1) + 2 + 2 * LAG, last), step, 0)
    if ending == "branch":
        made_copy(made - 1).start()
    else:
        part_width = columns // peers
        for k in range(peers):
            here = slice(k * part_width, (k + 1) * part_width)
            gain_parts[k, 0:1, :] = acc[:, here]
            gain_parts[k, 1:2, :] = given_bufs[3][:, here]
        for k in range(1, peers):
            gain_copy(k).start()
        lax.fori_loop(0, TILES, token_rows, 0)
        made_copy(0).start()

    def finish(c, carry):
        @pl.when(is_mid)
        def _():
            for h in range(HALVES):
                down(c, h).wait_send()

        return carry

    lax.fori_loop(0, all_chunks, finish, 0)

    def finish_last(c, carry):
        @pl.when(is_end)
        def _():
            for h in range(HALVES):
                up(c, h).wait_send()

        @pl.when(is_mid)
        def _():
            for h in range(HALVES):
                over(c, h).wait_send()

        return carry

    lax.fori_loop(all_chunks - chunks, all_chunks, finish_last, 0)

    def settle(u, carry):
        for k in range(2):
            second_hop(u, k).wait_send()
        third_hop(u).wait_send()
        return carry

    lax.fori_loop(0, units, settle, 0)
    for u in (units - 2, units - 1):
        to_core(u).wait_send()
        for at in range(len(spans)):
            low, high = units_of(at)
            if low <= u < high:
                out_copy(at, u).wait()
    if ending == "tokens":
        gains = gain_parts[me]
        for k in range(1, peers):
            gain_copy(k).wait_recv()
            gains = gains + gain_come[k]
        made_bufs[1][...] = gains
        made_copy(1).start()
        for k in range(1, peers):
            gain_copy(k).wait_send()
    for at in range(made):
        made_copy(at).wait()


def exchange(lefts, rights, sums, flips_before, outs, spans, units, call_id, pace, ending, given, made, chunks=16):
    rows, depth = lefts[0].shape
    block = depth // 8
    placed, at = [], 0
    for _, source, size in rights:
        placed.append((at, source, size))
        at += size
    weights = [item[0] for group in sums for item in group]
    columns = weights[0].shape[0] if sums[0][0][3] == "nt" else weights[0].shape[1]
    width = columns // chunks
    sum_plan = [[item[1:] for item in group] for group in sums]
    plan = (len(lefts), placed, sum_plan, flips_before, spans, len(outs), units, chunks, *pace, ending, len(given), len(made))
    any_space = pl.BlockSpec(memory_space=pl.ANY)
    line_block = pltpu.VMEM((chunks, rows, width), BF16)
    peers = lax.axis_size("batch") * lax.axis_size("seq")
    kept = made[:-1] if ending == "branch" else made
    dma = pltpu.SemaphoreType.DMA
    all_chunks = chunks * len(sums)
    flops = sum(2 * rows * columns * size for group in sum_plan for _, size, _ in group) + 2 * rows * depth * at
    return pl.pallas_call(
        functools.partial(exchange_kernel, plan),
        out_shape=[jax.ShapeDtypeStruct(shape, F32) for shape in outs]
        + [jax.ShapeDtypeStruct(shape, kind) for shape, kind in made],
        in_specs=[any_space] * (len(lefts) + len(rights) + len(weights) + len(given)),
        out_specs=[any_space] * (len(outs) + len(made)),
        scratch_shapes=[
            pltpu.VMEM((rows, depth), BF16),
            pltpu.VMEM((len(lefts), depth, rows), BF16),
            pltpu.VMEM((rows, at), BF16),
            pltpu.VMEM((rows, columns * len(sums)), BF16),
        ]
        + [
            pltpu.VMEM((3, width, size) if mode == "nt" else (3, size, width), BF16)
            for group in sum_plan
            for _, size, mode in group
        ]
        + [
            line_block,
            line_block,
            line_block,
            pltpu.VMEM((2, 4, block, block), BF16),
            pltpu.VMEM((units, 4, block, block), BF16),
            pltpu.VMEM((units, 2, block, block), BF16),
            pltpu.VMEM((units, block, block), BF16),
            pltpu.VMEM((2, block, block), F32),
        ]
        + [pltpu.VMEM(value.shape, value.dtype) for value in given]
        + [pltpu.VMEM(shape, kind) for shape, kind in kept]
        + [
            pltpu.VMEM((1, depth), F32),
            pltpu.VMEM((rows, width), F32),
            pltpu.VMEM((rows, width), F32),
            pltpu.VMEM((peers, 2, depth // peers), F32),
            pltpu.VMEM((peers, 2, depth // peers), F32),
            dma((len(given),)),
            dma((len(made),)),
            dma((peers,)),
            dma((peers,)),
            dma((len(lefts),)),
            dma((len(rights),)),
            dma((len(weights), 3)),
            dma((3, HALVES, all_chunks)),
            dma((3, HALVES, all_chunks)),
            dma((units,)),
            dma((units,)),
            dma((2, units)),
            dma((2, units)),
            dma((units,)),
            dma((units,)),
            dma((len(spans), 2)),
        ],
        compiler_params=pltpu.CompilerParams(
            collective_id=call_id, has_side_effects=True, vmem_limit_bytes=62 << 20
        ),
        cost_estimate=pl.CostEstimate(flops=flops + (50 << 30), bytes_accessed=20 << 20, transcendentals=0),
        name=f"exchange_{call_id}",
    )(*lefts, *[right[0] for right in rights], *weights, *given)


def forward_kernel(
    mixed_ref, x_ref, gain_ref, wo_hbm, wg_hbm, wu_hbm, ga_hbm,
    branch_hbm, n_hbm, act_hbm, gg_hbm, gu_hbm,
    branch, n_ref, act_ref, gg_ref, gu_ref, ga_ref, gate_acc, up_acc, squares, wo_buf, w_buf, part, first, second,
    ga_sem, wo_sem, w_sem, ar_send, ar_recv, out_sem,
):
    chunks, rows, width = part.shape
    total_columns = branch.shape[1]
    place = lax.axis_index("mp")
    pair = place + 1 - 2 * lax.rem(place, 2)
    across = 3 - place
    is_mid = (place == 1) | (place == 2)
    is_end = (place == 0) | (place == 3)
    high = rows // HALVES
    deep = w_buf.shape[2]

    def columns_of(c):
        return pl.ds(pl.multiple_of(c * width, width), width)

    def rows_of(h):
        return slice(h * high, (h + 1) * high)

    def remote(source, target, kind, h, c, device):
        return pltpu.make_async_remote_copy(
            src_ref=source,
            dst_ref=target,
            send_sem=ar_send.at[kind, h, c],
            recv_sem=ar_recv.at[kind, h, c],
            device_id={"mp": device},
            device_id_type=MESH,
        )

    def up(c, h):
        return remote(part.at[c, rows_of(h)], first.at[c, rows_of(h)], 0, h, c, pair)

    def over(c, h):
        return remote(part.at[c, rows_of(h)], second.at[c, rows_of(h)], 1, h, c, across)

    def down(c, h):
        here = branch.at[rows_of(h), columns_of(c)]
        return remote(here, here, 2, h, c, pair)

    def out_weight(c):
        slot = lax.rem(c, 3)
        return pltpu.make_async_copy(wo_hbm.at[:, columns_of(c)], wo_buf.at[slot], wo_sem.at[slot])

    def deep_of(p):
        return pl.ds(pl.multiple_of(p * deep, deep), deep)

    def weight(at, p):
        slot = lax.rem(p, 3)
        source = (wg_hbm, wu_hbm)[at].at[deep_of(p), :]
        return pltpu.make_async_copy(source, w_buf.at[at, slot], w_sem.at[at, slot])

    ga_copy = pltpu.make_async_copy(ga_hbm, ga_ref, ga_sem.at[0])
    out_weight(0).start()
    out_weight(1).start()
    for p in range(2):
        for at in range(2):
            weight(at, p).start()
    ga_copy.start()
    barrier = pltpu.get_barrier_semaphore()
    pl.semaphore_signal(barrier, inc=1, device_id={"mp": pair}, device_id_type=MESH)

    @pl.when(is_mid)
    def _():
        pl.semaphore_signal(barrier, inc=1, device_id={"mp": across}, device_id_type=MESH)
        pl.semaphore_wait(barrier, 2)

    @pl.when(is_end)
    def _():
        pl.semaphore_wait(barrier, 1)

    squares[...] = jnp.zeros_like(squares)
    per_deep = deep // width

    def step(t, carry):
        @pl.when(t < chunks)
        def _():
            out_weight(t).wait()
            part[t] = dot_nn(mixed_ref[...], wo_buf[lax.rem(t, 3)]).astype(BF16)

            @pl.when(is_end)
            def _():
                for h in range(HALVES):
                    up(t, h).start()

            @pl.when(t + 2 < chunks)
            def _():
                out_weight(t + 2).start()

        @pl.when(is_mid & (t >= UP_LAG) & (t < chunks + UP_LAG))
        def _():
            c = t - UP_LAG
            for h in range(HALVES):
                here = rows_of(h)
                up(c, h).wait_recv()
                part[c, here] = (part[c, here].astype(F32) + first[c, here].astype(F32)).astype(BF16)
                over(c, h).start()

        @pl.when(is_mid & (t >= OVER_LAG) & (t < chunks + OVER_LAG))
        def _():
            c = t - OVER_LAG
            for h in range(HALVES):
                here = rows_of(h)
                over(c, h).wait_recv()
                value = part[c, here].astype(F32) + second[c, here].astype(F32)
                branch[here, columns_of(c)] = value.astype(BF16)
                down(c, h).start()

        @pl.when(is_end & (t >= DOWN_LAG))
        def _():
            for h in range(HALVES):
                down(t - DOWN_LAG, h).wait_recv()

        @pl.when((t >= DOWN_LAG) & (lax.rem(t - DOWN_LAG, per_deep) == per_deep - 1))
        def _():
            p = lax.div(t - DOWN_LAG, per_deep)
            here = deep_of(p)
            middle = x_ref[:, here].astype(F32) + branch[:, here].astype(F32)
            squares[...] += jnp.sum(middle * middle, axis=-1, keepdims=True)
            scaled = (middle * gain_ref[:, here]).astype(BF16)
            for at, acc in enumerate((gate_acc, up_acc)):
                weight(at, p).wait()
                value = dot_nn(scaled, w_buf[at, lax.rem(p, 3)])

                @pl.when(p == 0)
                def _():
                    acc[...] = value

                @pl.when(p > 0)
                def _():
                    acc[...] += value

            @pl.when((p + 2) * deep < total_columns)
            def _():
                for at in range(2):
                    weight(at, p + 2).start()

        return carry

    lax.fori_loop(0, chunks + DOWN_LAG, step, 0)
    ga_copy.wait()
    tile = rows // TILES
    outs = [(n_ref, n_hbm), (act_ref, act_hbm), (gg_ref, gg_hbm), (gu_ref, gu_hbm)]

    def out_copy(at, i):
        here = pl.ds(pl.multiple_of(i * tile, tile), tile)
        return pltpu.make_async_copy(outs[at][0].at[here, :], outs[at][1].at[here, :], out_sem.at[at, i])

    branch_copy = pltpu.make_async_copy(branch, branch_hbm, ga_sem.at[1])
    branch_copy.start()

    def rows_step(i, carry):
        here = pl.ds(pl.multiple_of(i * tile, tile), tile)
        scale = lax.rsqrt(squares[here, :1] * (1.0 / total_columns) + epsilon)
        middle = x_ref[here, :].astype(F32) + branch[here, :].astype(F32)
        n_ref[here, :] = (middle * scale * gain_ref[...]).astype(BF16)
        gate = gate_acc[here, :] * scale
        up_pre = up_acc[here, :] * scale
        grad = ga_ref[here, :].astype(F32)
        sigmoid = jax.nn.sigmoid(gate)
        swish = gate * sigmoid
        act_ref[here, :] = (swish * up_pre).astype(BF16)
        gu_ref[here, :] = (grad * swish).astype(BF16)
        gg_ref[here, :] = (grad * up_pre * sigmoid * (1.0 + gate * (1.0 - sigmoid))).astype(BF16)
        for at in range(4):
            out_copy(at, i).start()
        return carry

    lax.fori_loop(0, TILES, rows_step, 0)

    def finish(c, carry):
        @pl.when(is_end)
        def _():
            for h in range(HALVES):
                up(c, h).wait_send()

        @pl.when(is_mid)
        def _():
            for h in range(HALVES):
                over(c, h).wait_send()
                down(c, h).wait_send()

        return carry

    lax.fori_loop(0, chunks, finish, 0)

    def drain(i, carry):
        for at in range(4):
            out_copy(at, i).wait()
        return carry

    lax.fori_loop(0, TILES, drain, 0)
    branch_copy.wait()


def forward(mixed, tokens, gain, w_output, w_gate, w_up, grad_active, call_id, chunks=16, deep=256):
    rows, columns = tokens.shape
    hidden = w_gate.shape[1]
    width = columns // chunks
    vmem, any_space = pl.BlockSpec(memory_space=pltpu.VMEM), pl.BlockSpec(memory_space=pl.ANY)
    dma = pltpu.SemaphoreType.DMA
    shapes = [(rows, columns), (rows, columns), (rows, hidden), (rows, hidden), (rows, hidden)]
    line_block = pltpu.VMEM((chunks, rows, width), BF16)
    return pl.pallas_call(
        forward_kernel,
        in_specs=[vmem] * 3 + [any_space] * 4,
        out_specs=[any_space] * 5,
        out_shape=[jax.ShapeDtypeStruct(shape, BF16) for shape in shapes],
        scratch_shapes=[pltpu.VMEM(shape, BF16) for shape in shapes]
        + [
            pltpu.VMEM((rows, hidden), BF16),
            pltpu.VMEM((rows, hidden), F32),
            pltpu.VMEM((rows, hidden), F32),
            pltpu.VMEM((rows, PAIR), F32),
            pltpu.VMEM((3, mixed.shape[1], width), BF16),
            pltpu.VMEM((2, 3, deep, hidden), BF16),
            line_block,
            line_block,
            line_block,
            dma((2,)),
            dma((3,)),
            dma((2, 3)),
            dma((3, HALVES, chunks)),
            dma((3, HALVES, chunks)),
            dma((4, TILES)),
        ],
        compiler_params=pltpu.CompilerParams(
            collective_id=call_id, has_side_effects=True, vmem_limit_bytes=62 << 20
        ),
        name="forward",
    )(mixed, tokens, gain, w_output, w_gate, w_up, grad_active)


def final_kernel(gn_ref, x_ref, gm_ref, gain_ref, mlp_ref, out_ref, gains_ref, acc, parts, come, send_sem, recv_sem):
    seq, batch = lax.axis_index("seq"), lax.axis_index("batch")
    seq_count = lax.axis_size("seq")
    peers = parts.shape[0]
    block = parts.shape[2]
    me = batch * seq_count + seq

    def peer(k):
        there = lax.rem(me + k, peers)
        return there, {"batch": lax.div(there, seq_count), "seq": lax.rem(there, seq_count)}

    def copy(k):
        there, device = peer(k)
        return pltpu.make_async_remote_copy(
            src_ref=parts.at[there],
            dst_ref=come.at[k],
            send_sem=send_sem.at[k],
            recv_sem=recv_sem.at[k],
            device_id=device,
            device_id_type=MESH,
        )

    barrier = pltpu.get_barrier_semaphore()
    for k in range(1, peers):
        pl.semaphore_signal(barrier, inc=1, device_id=peer(k)[1], device_id_type=MESH)
    rows = x_ref.shape[0]
    tile = rows // 8
    gain = gain_ref[...]
    acc[...] = jnp.zeros_like(acc)

    def rows_step(i, carry):
        here = pl.ds(pl.multiple_of(i * tile, tile), tile)
        wide = x_ref[here, :].astype(F32)
        grad = gn_ref[here, :].astype(F32)
        scale = lax.rsqrt(jnp.mean(wide * wide, axis=-1, keepdims=True) + epsilon)
        scaled = grad * gain
        mean = jnp.mean(wide * scaled, axis=-1, keepdims=True)
        result = gm_ref[here, :] + scale * scaled - wide * (scale * scale * scale) * mean
        out_ref[here, :] = result.astype(BF16)
        acc[...] += jnp.sum(grad * wide * scale, axis=0, keepdims=True)
        return carry

    lax.fori_loop(0, 8, rows_step, 0)
    for k in range(peers):
        here = slice(k * block, (k + 1) * block)
        parts[k, 0:1, :] = acc[:, here]
        parts[k, 1:2, :] = mlp_ref[:, here]
    pl.semaphore_wait(barrier, peers - 1)
    for k in range(1, peers):
        copy(k).start()
    total = parts[me]
    for k in range(1, peers):
        copy(k).wait_recv()
        total = total + come[k]
    gains_ref[...] = total
    for k in range(1, peers):
        copy(k).wait_send()


def final(grad_normed, tokens, grad_middle, gain, mlp_part, call_id):
    rows, width = tokens.shape
    peers = lax.axis_size("batch") * lax.axis_size("seq")
    block = width // peers
    vmem = pl.BlockSpec(memory_space=pltpu.VMEM)
    return pl.pallas_call(
        final_kernel,
        out_shape=[jax.ShapeDtypeStruct((rows, width), BF16), jax.ShapeDtypeStruct((2, block), F32)],
        in_specs=[vmem] * 5,
        out_specs=[vmem, vmem],
        scratch_shapes=[
            pltpu.VMEM((1, width), F32),
            pltpu.VMEM((peers, 2, block), F32),
            pltpu.VMEM((peers, 2, block), F32),
            pltpu.SemaphoreType.DMA((peers,)),
            pltpu.SemaphoreType.DMA((peers,)),
        ],
        compiler_params=pltpu.CompilerParams(collective_id=call_id, has_side_effects=True),
        name="final",
    )(grad_normed, tokens, grad_middle, gain, mlp_part)


def settle_kernel(places, *refs):
    count = len(places)
    sources, targets = refs[:count], refs[count : -count - 2]
    bufs, load_sem, store_sem = refs[-count - 2 : -2], refs[-2], refs[-1]

    def load(at):
        return pltpu.make_async_copy(sources[at], bufs[at], load_sem.at[at])

    def store(at):
        index, row = places[at]
        target = targets[index].at[row : row + bufs[at].shape[0], :]
        return pltpu.make_async_copy(bufs[at], target, store_sem.at[at])

    for at in range(count):
        load(at).start()
    for at in range(count):
        load(at).wait()
        store(at).start()
    for at in range(count):
        store(at).wait()


def settle(groups):
    places, shapes, arrays = [], [], []
    for index, group in enumerate(groups):
        row = 0
        for array in group:
            places.append((index, row))
            arrays.append(array)
            row += array.shape[0]
        shapes.append(jax.ShapeDtypeStruct((row, group[0].shape[1]), group[0].dtype))
    any_space = pl.BlockSpec(memory_space=pl.ANY)
    dma = pltpu.SemaphoreType.DMA
    return pl.pallas_call(
        functools.partial(settle_kernel, places),
        in_specs=[any_space] * len(arrays),
        out_specs=[any_space] * len(groups),
        out_shape=shapes,
        scratch_shapes=[pltpu.VMEM(array.shape, array.dtype) for array in arrays]
        + [dma((len(arrays),)), dma((len(arrays),))],
        compiler_params=pltpu.CompilerParams(vmem_limit_bytes=62 << 20),
        name="settle",
    )(*arrays)


def scatter_sum(left, right):
    rows, depth = left.shape
    columns = right.shape[1]
    batch_count = lax.axis_size("batch")
    seq_index = lax.axis_index("seq")
    core, chip = seq_index % 2, seq_index // 2
    block = depth // (4 * batch_count)
    split = left.reshape(rows, batch_count, 2, 2, block)
    size = lax.axis_size("seq")

    def product(at):
        taken = lax.dynamic_index_in_dim(split, at, 3, keepdims=False).reshape(rows, depth // 2)
        return dot_tn(taken, right)

    away = product(1 - core).astype(BF16)
    arrived = lax.ppermute(away, "seq", [(s, s ^ 1) for s in range(size)])
    kept = (product(core) + arrived.astype(F32)).astype(BF16)
    kept = kept.reshape(batch_count, 2, block, columns)
    half = columns // 2

    def over_chip(values, axis):
        sent = lax.dynamic_index_in_dim(values, 1 - chip, axis, keepdims=False)
        stay = lax.dynamic_index_in_dim(values, chip, axis, keepdims=False)
        came = lax.ppermute(sent, "seq", [(s, s ^ 2) for s in range(size)])
        return stay.astype(F32) + came.astype(F32)

    def over_batch(values):
        if batch_count == 2:
            here = lax.axis_index("batch")
            sent = lax.dynamic_index_in_dim(values, 1 - here, 0, keepdims=False)
            stay = lax.dynamic_index_in_dim(values, here, 0, keepdims=False)
            came = lax.ppermute(sent, "batch", [(0, 1), (1, 0)])
            return stay.astype(F32) + came.astype(F32)
        return lax.psum_scatter(values, "batch", scatter_dimension=0, tiled=False).astype(F32)

    one = over_batch(over_chip(kept[..., :half], 1).astype(BF16))
    two = over_chip(over_batch(kept[..., half:]).astype(BF16), 0)
    return jnp.concatenate([one, two], axis=1)


def local(
    tokens, segment_ids, attn_gain, w_query, w_key, w_value, w_output, mlp_gain, w_gate, w_up, w_down, cotangent
):
    rows, width = tokens.shape
    seq_count = lax.axis_size("seq")
    seq_index = lax.axis_index("seq")
    segments = segment_ids[0]
    first_row = seq_index * rows
    reach = LONGEST // rows
    cos, sin = rope_tables(segments, first_row, rows)
    row_segment = lax.dynamic_slice_in_dim(segments, first_row, rows, 0)[None, :]
    padded = jnp.concatenate([jnp.full((LONGEST,), -1, jnp.int32), segments])
    key_segment = lax.dynamic_slice_in_dim(padded, first_row, rows + LONGEST, 0)[:, None]

    normed, queries, key_value, grad_active = project(
        tokens, attn_gain[None, :], w_query, w_key, w_value, cos, sin, cotangent, w_down, 5
    )
    key_value = key_value.reshape(3 * rows, 2 * PAIR)
    mixed, logs = attend(queries, key_value, key_segment, row_segment)
    branch_low, normed_two, active, grad_gate_low, grad_up_low = forward(
        mixed, tokens, mlp_gain[None, :], w_output, w_gate, w_up, grad_active, 1
    )
    wide = tokens.astype(F32)
    middle = wide + branch_low.astype(F32)
    fused = lax.axis_size("batch") == 2
    hidden = w_gate.shape[1]
    unit = width // 8
    early = hidden * 5 // 8 // unit * unit
    if fused:
        grad_gate, grad_up, grad_down_one, grad_middle, grad_branch, grad_mixed, grad_mlp_gain, mlp_out = exchange(
            [normed_two, cotangent],
            [(grad_gate_low, 0, hidden), (grad_up_low, 0, hidden), (active, 0, hidden)],
            [
                [(w_gate, 0, hidden, "nt"), (w_up, hidden, hidden, "nt")],
                [(w_down, 2 * hidden, hidden, "nn")],
            ],
            (0, 2 * hidden // unit),
            [(unit, hidden), (unit, hidden), (early, unit)],
            [
                ("plain", 0, 0, 0, hidden),
                ("plain", 1, 0, hidden, hidden),
                ("turned", 2, 0, 2 * hidden, early),
            ],
            (2 * hidden + early) // unit,
            2,
            (3, 2),
            "branch",
            [tokens, branch_low, mlp_gain[None, :], w_output],
            [
                ((rows, width), F32),
                ((rows, width), BF16),
                ((rows, mixed.shape[1]), BF16),
                ((1, width), F32),
                ((rows, width), BF16),
            ],
        )
    else:
        grad_normed_two = line_sum([(grad_gate_low, w_gate, "nt"), (grad_up_low, w_up, "nt")], 2)
        grad_gate = scatter_sum(normed_two, grad_gate_low)
        grad_up = scatter_sum(normed_two, grad_up_low)
        mlp_out = lax.psum(dot_nn(active, w_down).astype(BF16), "mp")
        grad_normed_two = grad_normed_two.astype(F32)
        scaled_two = grad_normed_two * mlp_gain
        scale_two = lax.rsqrt(jnp.mean(middle * middle, axis=-1, keepdims=True) + epsilon)
        grad_middle = (
            cotangent.astype(F32)
            + scale_two * scaled_two
            - middle
            * (scale_two * scale_two * scale_two)
            * jnp.mean(middle * scaled_two, axis=-1, keepdims=True)
        )
        grad_mlp_gain = jnp.sum(grad_normed_two * middle * scale_two, axis=0)[None, :]
        grad_branch = grad_middle.astype(BF16)
        grad_mixed = dot_nt(grad_branch, w_output).astype(BF16)

    grad_query_pre, grad_key_pre, grad_value_pre = attend_back(
        queries, key_value, key_segment, row_segment, mixed, grad_mixed, logs, cos, sin, 6
    )
    query_width = grad_query_pre.shape[1]
    if fused:
        late, mixed_width = hidden - early, mixed.shape[1]
        query_at = late + mixed_width
        key_at = query_at + query_width
        grad_down_two, grad_output, grad_query, grad_key, grad_value, grad_tokens, gains, output = exchange(
            [cotangent, grad_branch, normed],
            [
                (active, early, late),
                (mixed, 0, mixed_width),
                (grad_query_pre, 0, query_width),
                (grad_key_pre, 0, PAIR),
                (grad_value_pre, 0, PAIR),
            ],
            [
                [
                    (w_query, query_at, query_width, "nt"),
                    (w_key, key_at, PAIR, "nt"),
                    (w_value, key_at + PAIR, PAIR, "nt"),
                ]
            ],
            (0, late // unit, query_at // unit),
            [(late, unit), (mixed_width, unit), (unit, query_width), (unit, PAIR), (unit, PAIR)],
            [
                ("turned", 0, 0, 0, late),
                ("turned", 1, 0, late, mixed_width),
                ("plain", 2, 0, query_at, query_width),
                ("plain", 3, 0, key_at, PAIR),
                ("plain", 4, 0, key_at + PAIR, PAIR),
            ],
            (key_at + 2 * PAIR) // unit,
            3,
            (3, 2),
            "tokens",
            [tokens, grad_middle, attn_gain[None, :], grad_mlp_gain, branch_low, mlp_out],
            [((rows, width), BF16), ((2, unit), F32), ((rows, width), BF16)],
        )
        grad_gate, grad_up, grad_down, grad_output, grad_query, grad_key, grad_value, grad_tokens, output = settle(
            [
                [grad_gate],
                [grad_up],
                [grad_down_one, grad_down_two],
                [grad_output],
                [grad_query],
                [grad_key],
                [grad_value],
                [grad_tokens],
                [output],
            ]
        )
    else:
        output = (middle + mlp_out.astype(F32)).astype(BF16)
        grad_down = scatter_sum(cotangent, active).T
        grad_output = scatter_sum(grad_branch, mixed).T
        grad_qkv = scatter_sum(normed, jnp.concatenate([grad_query_pre, grad_key_pre, grad_value_pre], axis=1))
        grad_query = grad_qkv[:, :query_width]
        grad_key = grad_qkv[:, query_width : query_width + PAIR]
        grad_value = grad_qkv[:, query_width + PAIR :]
        grad_normed = line_sum(
            [(grad_query_pre, w_query, "nt"), (grad_key_pre, w_key, "nt"), (grad_value_pre, w_value, "nt")], 3
        )
        grad_tokens, gains = final(grad_normed, tokens, grad_middle, attn_gain[None, :], grad_mlp_gain, 4)
    return (
        output,
        grad_tokens,
        gains[0],
        grad_query,
        grad_key,
        grad_value,
        grad_output,
        gains[1],
        grad_gate,
        grad_up,
        grad_down,
    )


def solution(mesh):
    tokens_spec = P(("batch", "seq"), None)
    in_specs = (
        tokens_spec,
        P("batch", None),
        P(),
        P(None, "mp"),
        P(None, "mp"),
        P(None, "mp"),
        P("mp", None),
        P(),
        P(None, "mp"),
        P(None, "mp"),
        P("mp", None),
        tokens_spec,
    )
    row_split = P(("batch", "seq"), "mp")
    column_split = P("mp", ("batch", "seq"))
    out_specs = (
        tokens_spec,
        tokens_spec,
        P(("batch", "seq")),
        row_split,
        row_split,
        row_split,
        column_split,
        P(("batch", "seq")),
        row_split,
        row_split,
        column_split,
    )
    return jax.shard_map(local, mesh=mesh, in_specs=in_specs, out_specs=out_specs, check_vma=False)
```

```python
import functools
import math

import jax
import jax.numpy as jnp
from jax import lax
from jax.experimental import pallas as pl
from jax.experimental.pallas import tpu as pltpu
from jax.sharding import PartitionSpec as P

HS = 64
PAIR = 2 * HS
LONGEST = 1024
FORWARD_ROWS = 256
BACKWARD_ROWS = 128
rope_base = 500000.0
epsilon = 1e-05
masked_score = -1e30
MESH = pl.DeviceIdType.MESH
F32 = jnp.float32
BF16 = jnp.bfloat16


def dot_nn(left, right):
    return lax.dot_general(left, right, (((1,), (0,)), ((), ())), preferred_element_type=F32)


def dot_nt(left, right):
    return lax.dot_general(left, right, (((1,), (1,)), ((), ())), preferred_element_type=F32)


def dot_tn(left, right):
    return lax.dot_general(left, right, (((0,), (0,)), ((), ())), preferred_element_type=F32)


def lanes_of(values):
    return lax.broadcasted_iota(jnp.int32, values.shape, 1)


def swap_halves(values):
    ahead = pltpu.roll(values, PAIR - HS // 2, 1)
    behind = pltpu.roll(values, HS // 2, 1)
    return jnp.where(lanes_of(values) % HS < HS // 2, ahead, behind)


def write_tables(seg_ref, cos_ref, sin_ref):
    rows = cos_ref.shape[0]
    first_row = lax.axis_index("seq") * rows
    every = seg_ref[...]
    mine = seg_ref[:, pl.ds(pl.multiple_of(first_row, rows), rows)]
    start = jnp.zeros(mine.shape, F32)
    for number in range(ID_COUNT - 1):
        size = jnp.sum((every == number).astype(F32), axis=1, keepdims=True)
        start = start + jnp.where(mine > number, size, 0.0)
    place = (first_row + lax.broadcasted_iota(jnp.int32, mine.shape, 1)).astype(F32) - start
    lane = lax.broadcasted_iota(jnp.int32, (1, PAIR), 1)
    frequency = jnp.exp((lane % (HS // 2)).astype(F32) * (-2.0 * math.log(rope_base) / HS))
    angles = jnp.broadcast_to(place, (PAIR, rows)).T * frequency
    cos_ref[...] = jnp.cos(angles)
    sin_ref[...] = jnp.sin(angles) * jnp.where(lane % HS < HS // 2, -1.0, 1.0)


def project_kernel(
    x_ref, gain_ref, wk_ref, wv_ref, seg_ref, cot_hbm, wq_hbm, wd_hbm,
    cos_ref, sin_ref, n_hbm, q_hbm, kv_hbm, ga_hbm,
    n_ref, q_ref, kv_ref, ga_ref, cot_ref, wq_ref, wd_ref, load_sem, wd_sem, send_sem, recv_sem, out_sem,
):
    rows = x_ref.shape[0]
    seq, seq_count = lax.axis_index("seq"), lax.axis_size("seq")
    hidden = wd_hbm.shape[0]
    width = wd_ref.shape[1]
    chunks = hidden // width
    block = rows // 2
    loads = [
        pltpu.make_async_copy(wq_hbm, wq_ref, load_sem.at[0]),
        pltpu.make_async_copy(cot_hbm, cot_ref, load_sem.at[1]),
    ]

    def weight(c):
        slot = lax.rem(c, 3)
        here = pl.ds(pl.multiple_of(c * width, width), width)
        return pltpu.make_async_copy(wd_hbm.at[here, :], wd_ref.at[slot], wd_sem.at[slot])

    def out_copy(at):
        source = (n_ref, q_ref, kv_ref, ga_ref)[at]
        return pltpu.make_async_copy(source, (n_hbm, q_hbm, kv_hbm, ga_hbm)[at], out_sem.at[at])

    def send(away):
        return pltpu.make_async_remote_copy(
            src_ref=kv_ref.at[2],
            dst_ref=kv_ref.at[2 - away],
            send_sem=send_sem.at[away],
            recv_sem=recv_sem.at[away],
            device_id={"seq": lax.rem(seq + away, seq_count)},
            device_id_type=MESH,
        )

    for load in loads:
        load.start()
    weight(0).start()
    weight(1).start()
    for away in (1, 2):

        @pl.when(seq < away)
        def _():
            kv_ref[2 - away] = jnp.zeros(kv_ref.shape[1:], BF16)

    barrier = pltpu.get_barrier_semaphore()
    for away in range(1, seq_count):
        there = lax.rem(seq + away, seq_count)
        pl.semaphore_signal(barrier, inc=1, device_id={"seq": there}, device_id_type=MESH)

    write_tables(seg_ref, cos_ref, sin_ref)
    for half in range(2):
        here = slice(half * block, (half + 1) * block)
        cos, sin = cos_ref[here, :], sin_ref[here, :]
        wide = x_ref[here, :].astype(F32)
        scale = lax.rsqrt(jnp.mean(wide * wide, axis=-1, keepdims=True) + epsilon)
        normed = (wide * scale * gain_ref[...]).astype(BF16)
        n_ref[here, :] = normed
        keys = dot_nn(normed, wk_ref[...])
        keys = keys * cos + swap_halves(keys) * sin
        values = dot_nn(normed, wv_ref[...])
        low_half = lanes_of(keys) < HS
        kv_ref[2, here, :PAIR] = jnp.where(low_half, keys, pltpu.roll(values, HS, 1)).astype(BF16)
        kv_ref[2, here, PAIR:] = jnp.where(low_half, pltpu.roll(keys, HS, 1), values).astype(BF16)
    pl.semaphore_wait(barrier, seq_count - 1)
    for away in (1, 2):

        @pl.when(seq + away < seq_count)
        def _():
            send(away).start()

    out_copy(0).start()
    for load in loads:
        load.wait()
    for half in range(2):
        here = slice(half * block, (half + 1) * block)
        cos, sin = cos_ref[here, :], sin_ref[here, :]
        queries = dot_nn(n_ref[here, :], wq_ref[...])
        for start in range(0, queries.shape[1], PAIR):
            part = queries[:, start : start + PAIR]
            q_ref[here, start : start + PAIR] = (part * cos + swap_halves(part) * sin).astype(BF16)
    out_copy(1).start()

    def step(c, carry):
        weight(c).wait()

        @pl.when(c + 2 < chunks)
        def _():
            weight(c + 2).start()

        here = pl.ds(pl.multiple_of(c * width, width), width)
        ga_ref[:, here] = dot_nt(cot_ref[...], wd_ref[lax.rem(c, 3)]).astype(BF16)
        return carry

    lax.fori_loop(0, chunks, step, 0)
    out_copy(3).start()
    for away in (1, 2):

        @pl.when(seq >= away)
        def _():
            send(away).wait_recv()

    out_copy(2).start()
    for away in (1, 2):

        @pl.when(seq + away < seq_count)
        def _():
            send(away).wait_send()

    for at in range(4):
        out_copy(at).wait()


def project(tokens, gain, w_query, w_key, w_value, segment_ids, cotangent, w_down, call_id):
    rows, width = tokens.shape
    columns, hidden = w_query.shape[1], w_down.shape[0]
    chunk = PROJECT_CHUNK
    vmem, any_space = pl.BlockSpec(memory_space=pltpu.VMEM), pl.BlockSpec(memory_space=pl.ANY)
    shapes = [(rows, width), (rows, columns), (3, rows, 2 * PAIR), (rows, hidden)]
    dma = pltpu.SemaphoreType.DMA
    return pl.pallas_call(
        project_kernel,
        in_specs=[vmem] * 5 + [any_space] * 3,
        out_specs=[vmem] * 2 + [any_space] * 4,
        out_shape=[jax.ShapeDtypeStruct((rows, PAIR), F32)] * 2
        + [jax.ShapeDtypeStruct(shape, BF16) for shape in shapes],
        scratch_shapes=[pltpu.VMEM(shape, BF16) for shape in shapes]
        + [
            pltpu.VMEM((rows, width), BF16),
            pltpu.VMEM(w_query.shape, BF16),
            pltpu.VMEM((3, chunk, width), BF16),
            dma((2,)),
            dma((3,)),
            dma((3,)),
            dma((3,)),
            dma((4,)),
        ],
        compiler_params=pltpu.CompilerParams(
            collective_id=call_id, has_side_effects=True, vmem_limit_bytes=62 << 20
        ),
        name="project",
    )(tokens, gain, w_key, w_value, segment_ids, cotangent, w_query, w_down)


def write_bias(bias_ref, seg_ref, padded_ref):
    tiles, span, both = bias_ref.shape
    size = both // 2
    rows = tiles * size
    padded_ref[:, :LONGEST] = jnp.full((1, LONGEST), -1, jnp.int32)
    padded_ref[:, LONGEST:] = seg_ref[...]
    first_row = pl.multiple_of(lax.axis_index("seq") * rows, rows)
    window = padded_ref[:, pl.ds(first_row, LONGEST + rows)].astype(F32)
    beside = jnp.broadcast_to(window, (PAIR, LONGEST + rows)).T
    beside = jnp.concatenate([beside] * (size // PAIR), axis=1)
    key_place = lax.broadcasted_iota(jnp.int32, (span, size), 0) - LONGEST
    row_place = lax.broadcasted_iota(jnp.int32, (span, size), 1)
    for tile in range(tiles):
        start = tile * size
        same = beside[start : start + span, :] == window[:, LONGEST + start : LONGEST + start + size]
        bias = jnp.where(same & (key_place <= row_place), 0.0, masked_score)
        bias_ref[tile] = jnp.concatenate([bias, bias], axis=1)


def bias_scratch(rows, size):
    assert LONGEST + rows == 3 * rows
    return pltpu.VMEM((rows // size, LONGEST + size, 2 * size), F32)


def heads_beside(values, here):
    return jnp.concatenate([values[:HS, here], values[HS:, here]], axis=1)


def heads_below(values, here):
    return jnp.concatenate([values[here, :HS], values[here, HS:]], axis=0)


def heads_stacked(values):
    size = values.shape[1] // 2
    return jnp.concatenate([values[:, :size], values[:, size:]], axis=0)


def attend_kernel(q_ref, kv_ref, seg_ref, out_ref, log_ref, bias_ref, padded_ref):
    @pl.when(pl.program_id(0) == 0)
    def _():
        write_bias(bias_ref, seg_ref, padded_ref)

    key_value = kv_ref[...]
    flipped = key_value.T
    q_flipped = (q_ref[...].astype(F32) * HS ** (-0.5)).astype(BF16).T
    tiles, span, both = bias_ref.shape
    size = both // 2
    for tile in range(tiles):
        here = slice(tile * size, (tile + 1) * size)
        keys = slice(tile * size, tile * size + span)
        scores = dot_nn(key_value[keys, :HS], heads_beside(q_flipped, here)) + bias_ref[tile]
        top = jnp.max(scores, axis=0, keepdims=True)
        powers = jnp.exp(scores - top)
        total = jnp.sum(powers, axis=0, keepdims=True)
        mixed = dot_nn(flipped[HS:, keys], powers.astype(BF16)) / total
        logs = top + jnp.log(total)
        log_ref[0, 0:1, here] = logs[:, :size]
        log_ref[0, 1:2, here] = logs[:, size:]
        out_ref[here, :] = heads_stacked(mixed).T.astype(BF16)


def attend(queries, key_value, segment_ids):
    rows, width = queries.shape
    pairs = width // PAIR
    per_group = pairs // 2
    pair_tile = pl.BlockSpec((rows, PAIR), lambda p: (0, p))
    kv_tile = pl.BlockSpec((3 * rows, PAIR), lambda p: (0, p // per_group))
    return pl.pallas_call(
        attend_kernel,
        grid=(pairs,),
        in_specs=[
            pair_tile,
            kv_tile,
            pl.BlockSpec(segment_ids.shape, lambda p: (0, 0)),
        ],
        out_specs=[pair_tile, pl.BlockSpec((1, 2, rows), lambda p: (p, 0, 0))],
        out_shape=[
            jax.ShapeDtypeStruct((rows, width), BF16),
            jax.ShapeDtypeStruct((pairs, 2, rows), F32),
        ],
        scratch_shapes=[
            bias_scratch(rows, FORWARD_ROWS),
            pltpu.VMEM((1, LONGEST + segment_ids.shape[1]), jnp.int32),
        ],
        cost_estimate=pl.CostEstimate(
            flops=16 << 30, bytes_accessed=4 << 20, transcendentals=3 * rows * rows * 2 * pairs
        ),
        name="attend",
    )(queries, key_value, segment_ids)


def attend_back_kernel(
    q_ref, kv_ref, seg_ref, out_ref, grad_ref, log_ref, cos_ref, sin_ref,
    dq_ref, dk_ref, dv_ref, bias_ref, padded_ref, dkv_ref, own_ref, sent_ref, come_ref, send_sem, recv_sem, per_group,
):
    step = pl.program_id(0)
    seq, seq_count = lax.axis_index("seq"), lax.axis_size("seq")
    barrier = pltpu.get_barrier_semaphore()

    def back(group, away):
        return pltpu.make_async_remote_copy(
            src_ref=sent_ref.at[group, 2 - away],
            dst_ref=come_ref.at[group, 2 - away],
            send_sem=send_sem.at[group, 2 - away],
            recv_sem=recv_sem.at[group, 2 - away],
            device_id={"seq": lax.rem(seq + seq_count - away, seq_count)},
            device_id_type=MESH,
        )

    @pl.when(step == 0)
    def _():
        for away in range(1, seq_count):
            there = lax.rem(seq + away, seq_count)
            pl.semaphore_signal(barrier, inc=1, device_id={"seq": there}, device_id_type=MESH)
        write_bias(bias_ref, seg_ref, padded_ref)

    rows = q_ref.shape[0]
    key_value = kv_ref[...]
    flipped = key_value[:, :].T
    scaled = (q_ref[...].astype(F32) * HS ** (-0.5)).astype(BF16)
    q_flipped = scaled.T
    grad = grad_ref[...]
    grad_flipped = grad.T
    product = (out_ref[...].astype(F32) * grad.astype(F32)).T
    tiles, span, both = bias_ref.shape
    size = both // 2

    @pl.when(step % per_group == 0)
    def _():
        dkv_ref[...] = jnp.zeros_like(dkv_ref)

    for tile in range(tiles):
        here = slice(tile * size, (tile + 1) * size)
        keys = slice(tile * size, tile * size + span)
        logs = jnp.concatenate([log_ref[0, 0:1, here], log_ref[0, 1:2, here]], axis=1)
        delta = jnp.sum(heads_beside(product, here), axis=0, keepdims=True)
        scores = dot_nn(key_value[keys, :HS], heads_beside(q_flipped, here)) + bias_ref[tile]
        shares = jnp.exp(scores - logs)
        grad_shares = dot_nn(key_value[keys, HS:], heads_beside(grad_flipped, here))
        grad_scores = (shares * (grad_shares - delta)).astype(BF16)
        dvalue = dot_nn(shares.astype(BF16), heads_below(grad, here))
        dkey = dot_nn(grad_scores, heads_below(scaled, here))
        dkv_ref[keys, :] += jnp.concatenate([dkey, dvalue], axis=1)
        dq = heads_stacked(dot_nn(flipped[:HS, keys], grad_scores)).T * HS ** (-0.5)
        dq_ref[here, :] = (dq * cos_ref[here, :] - swap_halves(dq) * sin_ref[here, :]).astype(BF16)

    for group in range(2):

        @pl.when(step == (group + 1) * per_group - 1)
        def _():
            sent_ref[group, 0] = dkv_ref[:rows, :].astype(BF16)
            sent_ref[group, 1] = dkv_ref[rows : 2 * rows, :].astype(BF16)
            own_ref[group] = dkv_ref[2 * rows :, :]
            if group == 0:
                pl.semaphore_wait(barrier, seq_count - 1)
            for away in (1, 2):

                @pl.when(seq >= away)
                def _():
                    back(group, away).start()

    @pl.when(step == 2 * per_group - 1)
    def _():
        for group in range(2):
            for away in (1, 2):

                @pl.when(seq + away < seq_count)
                def _():
                    back(group, away).wait_recv()
                    own_ref[group] += come_ref[group, 2 - away].astype(F32)

        one, two = own_ref[0], own_ref[1]
        low_half = lanes_of(one) < HS
        keys = jnp.where(low_half, one, pltpu.roll(two, HS, 1))
        dk_ref[...] = (keys * cos_ref[...] - swap_halves(keys) * sin_ref[...]).astype(BF16)
        dv_ref[...] = jnp.where(low_half, pltpu.roll(one, HS, 1), two).astype(BF16)
        for group in range(2):
            for away in (1, 2):

                @pl.when(seq >= away)
                def _():
                    back(group, away).wait_send()


def attend_back(queries, key_value, segment_ids, mixed, grad, logs, cos, sin, call_id):
    rows, width = queries.shape
    pairs = width // PAIR
    per_group = pairs // 2
    pair_tile = pl.BlockSpec((rows, PAIR), lambda p: (0, p))
    whole = pl.BlockSpec((rows, PAIR), lambda p: (0, 0))
    wide_tile = pl.BlockSpec((3 * rows, PAIR), lambda p: (0, p // per_group))
    full = lambda array: pl.BlockSpec(array.shape, lambda p: (0, 0))
    return pl.pallas_call(
        functools.partial(attend_back_kernel, per_group=per_group),
        grid=(pairs,),
        in_specs=[
            pair_tile,
            wide_tile,
            full(segment_ids),
            pair_tile,
            pair_tile,
            pl.BlockSpec((1, 2, rows), lambda p: (p, 0, 0)),
            full(cos),
            full(sin),
        ],
        out_specs=[pair_tile, whole, whole],
        out_shape=[
            jax.ShapeDtypeStruct((rows, width), BF16),
            jax.ShapeDtypeStruct((rows, PAIR), BF16),
            jax.ShapeDtypeStruct((rows, PAIR), BF16),
        ],
        scratch_shapes=[
            bias_scratch(rows, BACKWARD_ROWS),
            pltpu.VMEM((1, LONGEST + segment_ids.shape[1]), jnp.int32),
            pltpu.VMEM((3 * rows, PAIR), F32),
            pltpu.VMEM((2, rows, PAIR), F32),
            pltpu.VMEM((2, 2, rows, PAIR), BF16),
            pltpu.VMEM((2, 2, rows, PAIR), BF16),
            pltpu.SemaphoreType.DMA((2, 2)),
            pltpu.SemaphoreType.DMA((2, 2)),
        ],
        compiler_params=pltpu.CompilerParams(collective_id=call_id, has_side_effects=True),
        cost_estimate=pl.CostEstimate(
            flops=40 << 30, bytes_accessed=6 << 20, transcendentals=3 * rows * rows * 2 * pairs
        ),
        name="attend_back",
    )(queries, key_value, segment_ids, mixed, grad, logs, cos, sin)


def line_sum_kernel(modes, chunks, *refs):
    count = len(modes)
    a_refs, w_refs, out_ref = refs[:count], refs[count : 2 * count], refs[2 * count]
    rest = refs[2 * count + 1 :]
    w_bufs = rest[:count]
    part, first, second, total, w_sem, send_sem, recv_sem = rest[count:]
    width = part.shape[2]
    place = lax.axis_index("mp")
    pair = place + 1 - 2 * lax.rem(place, 2)
    across = 3 - place
    is_mid = (place == 1) | (place == 2)
    is_end = (place == 0) | (place == 3)

    def weight(at, c):
        if modes[at] == "nt":
            source = w_refs[at].at[pl.ds(pl.multiple_of(c * width, width), width), :]
        else:
            source = w_refs[at].at[:, pl.ds(pl.multiple_of(c * width, width), width)]
        return pltpu.make_async_copy(source, w_bufs[at].at[c], w_sem.at[at, c])

    def remote(kind, source, target, c, device):
        return pltpu.make_async_remote_copy(
            src_ref=source.at[c],
            dst_ref=target.at[c],
            send_sem=send_sem.at[kind, c],
            recv_sem=recv_sem.at[kind, c],
            device_id={"mp": device},
            device_id_type=MESH,
        )

    def up(c):
        return remote(0, part, first, c, pair)

    def over(c):
        return remote(1, part, second, c, across)

    def down(c):
        return remote(2, total, total, c, pair)

    def start_weights(c, carry):
        for at in range(count):
            weight(at, c).start()
        return carry

    lax.fori_loop(0, chunks, start_weights, 0)
    barrier = pltpu.get_barrier_semaphore()
    pl.semaphore_signal(barrier, inc=1, device_id={"mp": pair}, device_id_type=MESH)

    @pl.when(is_mid)
    def _():
        pl.semaphore_signal(barrier, inc=1, device_id={"mp": across}, device_id_type=MESH)
        pl.semaphore_wait(barrier, 2)

    @pl.when(is_end)
    def _():
        pl.semaphore_wait(barrier, 1)

    def step(t, carry):
        @pl.when(t < chunks)
        def _():
            value = None
            for at in range(count):
                weight(at, t).wait()
                dot = dot_nt if modes[at] == "nt" else dot_nn
                term = dot(a_refs[at][...], w_bufs[at][t])
                value = term if value is None else value + term
            part[t] = value.astype(BF16)

            @pl.when(is_end)
            def _():
                up(t).start()

        @pl.when(is_mid & (t >= 1) & (t < chunks + 1))
        def _():
            c = t - 1
            up(c).wait_recv()
            part[c] = (part[c].astype(F32) + first[c].astype(F32)).astype(BF16)
            over(c).start()

        @pl.when(is_mid & (t >= OVER_LAG))
        def _():
            c = t - OVER_LAG
            over(c).wait_recv()
            total[c] = (part[c].astype(F32) + second[c].astype(F32)).astype(BF16)
            down(c).start()

        return carry

    lax.fori_loop(0, chunks + OVER_LAG, step, 0)

    def finish(c, carry):
        @pl.when(is_end)
        def _():
            up(c).wait_send()
            down(c).wait_recv()

        @pl.when(is_mid)
        def _():
            over(c).wait_send()
            down(c).wait_send()

        out_ref[:, pl.ds(pl.multiple_of(c * width, width), width)] = total[c]
        return carry

    lax.fori_loop(0, chunks, finish, 0)


def line_sum(pairs, call_id, chunks=16):
    lefts = [left for left, _, _ in pairs]
    rights = [right for _, right, _ in pairs]
    modes = tuple(mode for _, _, mode in pairs)
    rows = lefts[0].shape[0]
    columns = rights[0].shape[0] if modes[0] == "nt" else rights[0].shape[1]
    width = columns // chunks
    count = len(pairs)
    bufs = [
        pltpu.VMEM((chunks, width, left.shape[1]) if mode == "nt" else (chunks, left.shape[1], width), BF16)
        for left, _, mode in pairs
    ]
    flops = sum(2 * rows * columns * left.shape[1] for left in lefts)
    moved = sum(right.size * 2 for right in rights)
    block = pltpu.VMEM((chunks, rows, width), BF16)
    return pl.pallas_call(
        functools.partial(line_sum_kernel, modes, chunks),
        out_shape=jax.ShapeDtypeStruct((rows, columns), BF16),
        in_specs=[pl.BlockSpec(memory_space=pltpu.VMEM)] * count
        + [pl.BlockSpec(memory_space=pl.ANY)] * count,
        out_specs=pl.BlockSpec(memory_space=pltpu.VMEM),
        scratch_shapes=bufs
        + [
            block,
            block,
            block,
            block,
            pltpu.SemaphoreType.DMA((count, chunks)),
            pltpu.SemaphoreType.DMA((3, chunks)),
            pltpu.SemaphoreType.DMA((3, chunks)),
        ],
        compiler_params=pltpu.CompilerParams(collective_id=call_id, has_side_effects=True),
        cost_estimate=pl.CostEstimate(
            flops=flops + (40 << 30), bytes_accessed=moved, transcendentals=0
        ),
        name=f"line_sum_{call_id}",
    )(*lefts, *rights)

LAG = 3
UP_LAG = 1
OVER_LAG = 3
DOWN_LAG = 8
HALVES = 1
ID_COUNT = 4
LAST_LAG = 12
TILES = 8
PROJECT_CHUNK = 512


def exchange_kernel(plan, *refs):
    left_count, rights, sums, flips_before, spans, out_count, units, chunks, period, active, ending, given, made = plan
    refs = list(refs)

    def take(n):
        got = refs[:n]
        del refs[:n]
        return got

    weights = [item for group in sums for item in group]
    left_refs, right_refs, w_refs = take(left_count), take(len(rights)), take(len(weights))
    given_refs = take(given)
    grad_refs, made_refs = take(out_count), take(made)
    stage, flip, right_all, out_ref = take(4)
    w_bufs = take(len(weights))
    part, first, second, away, come_one, come_two, come_three, result = take(8)
    given_bufs, made_bufs = take(given), take(made - (ending == "branch"))
    acc, dots, scales, gain_parts, gain_come, given_sem, made_sem, gain_send, gain_recv = take(9)
    in_sem, right_sem, w_sem, ar_send, ar_recv, core_send, core_recv, two_send, two_recv, three_send, three_recv, out_sem = refs
    width = part.shape[2]
    block = come_three.shape[1]
    all_chunks = chunks * len(sums)
    place = lax.axis_index("mp")
    seq, batch = lax.axis_index("seq"), lax.axis_index("batch")
    core, chip = lax.rem(seq, 2), lax.div(seq, 2)
    sibling = seq + 1 - 2 * core
    beside = seq + 2 - 4 * chip
    pair = place + 1 - 2 * lax.rem(place, 2)
    across = 3 - place
    is_mid = (place == 1) | (place == 2)
    is_end = (place == 0) | (place == 3)

    def columns_of(c):
        return pl.ds(pl.multiple_of(c * width, width), width)

    def weight(at, group, c):
        here = columns_of(c - group * chunks)
        source = w_refs[at].at[here, :] if weights[at][2] == "nt" else w_refs[at].at[:, here]
        slot = lax.rem(c, 3)
        return pltpu.make_async_copy(source, w_bufs[at].at[slot], w_sem.at[at, slot])

    members = []
    for group, items in enumerate(sums):
        for _ in items:
            members.append(group)

    def load_weights(c):
        for group in range(len(sums)):

            @pl.when((c >= group * chunks) & (c < (group + 1) * chunks))
            def _():
                for at in range(len(weights)):
                    if members[at] == group:
                        weight(at, group, c).start()

    def remote(source, target, send, recv, device):
        return pltpu.make_async_remote_copy(
            src_ref=source, dst_ref=target, send_sem=send, recv_sem=recv, device_id=device, device_id_type=MESH
        )

    def slot_of(c):
        return lax.rem(c, chunks)

    high = part.shape[1] // HALVES

    def rows_of(h):
        return slice(h * high, (h + 1) * high)

    def up(c, h):
        slot = slot_of(c)
        source, target = part.at[slot, rows_of(h)], first.at[slot, rows_of(h)]
        return remote(source, target, ar_send.at[0, h, c], ar_recv.at[0, h, c], {"mp": pair})

    def over(c, h):
        slot = slot_of(c)
        source, target = part.at[slot, rows_of(h)], second.at[slot, rows_of(h)]
        return remote(source, target, ar_send.at[1, h, c], ar_recv.at[1, h, c], {"mp": across})

    def down(c, h):
        here = out_ref.at[rows_of(h), columns_of(c)]
        return remote(here, here, ar_send.at[2, h, c], ar_recv.at[2, h, c], {"mp": pair})

    def to_core(u):
        return remote(away.at[lax.rem(u, 2)], come_one.at[u], core_send.at[u], core_recv.at[u], {"seq": sibling})

    def chip_first(u):
        return 1 - lax.rem(u, 2)

    def sent_at(u, k):
        x_first = chip_first(u)
        return x_first * (2 * k + 1 - chip) + (1 - x_first) * (2 * (1 - batch) + k)

    def kept_at(u, k):
        x_first = chip_first(u)
        return x_first * (2 * k + chip) + (1 - x_first) * (2 * batch + k)

    def own_at(u):
        x_first = chip_first(u)
        return x_first * batch + (1 - x_first) * chip

    def device_of(x_way):
        return {
            "seq": x_way * beside + (1 - x_way) * seq,
            "batch": x_way * batch + (1 - x_way) * (1 - batch),
        }

    def second_hop(u, k):
        return remote(
            come_one.at[u, sent_at(u, k)], come_two.at[u, k], two_send.at[k, u], two_recv.at[k, u], device_of(chip_first(u))
        )

    def third_hop(u):
        return remote(
            come_two.at[u, 1 - own_at(u)], come_three.at[u], three_send.at[u], three_recv.at[u], device_of(1 - chip_first(u))
        )

    def left_copy(at):
        return pltpu.make_async_copy(left_refs[at], stage, in_sem.at[at])

    def right_copy(at):
        offset, source, size = rights[at]
        return pltpu.make_async_copy(
            right_refs[at].at[:, source : source + size], right_all.at[:, offset : offset + size], right_sem.at[at]
        )

    def out_copy(at, u):
        kind, index, offset, start, size = spans[at]
        slot = lax.rem(u, 2)
        if size < block:
            source = result.at[slot, :, start % block : start % block + size]
            target = grad_refs[index].at[:, offset : offset + size]
        else:
            source = result.at[slot]
            here = pl.ds(pl.multiple_of((u - start // block) * block + offset, block), block)
            target = grad_refs[index].at[here, :] if kind == "turned" else grad_refs[index].at[:, here]
        return pltpu.make_async_copy(source, target, out_sem.at[at, slot])

    def units_of(at):
        _, _, _, start, size = spans[at]
        return start // block, max((start + size) // block, start // block + 1)

    seq_count = lax.axis_size("seq")
    peers = lax.axis_size("batch") * seq_count
    me = batch * seq_count + seq

    def peer(k):
        there = lax.rem(me + k, peers)
        return there, {"batch": lax.div(there, seq_count), "seq": lax.rem(there, seq_count)}

    def gain_copy(k):
        there, device = peer(k)
        return remote(gain_parts.at[there], gain_come.at[k], gain_send.at[k], gain_recv.at[k], device)

    def given_copy(at):
        return pltpu.make_async_copy(given_refs[at], given_bufs[at], given_sem.at[at])

    def made_copy(at):
        source = out_ref.at[:, columns // 2 :] if ending == "branch" and at == made - 1 else made_bufs[at]
        return pltpu.make_async_copy(source, made_refs[at], made_sem.at[at])

    columns = out_ref.shape[1]
    rows = out_ref.shape[0]
    tile = rows // TILES

    def tile_of(i):
        return pl.ds(pl.multiple_of(i * tile, tile), tile)

    def branch_rows(i):
        here = tile_of(i)
        gm_buf, gb_buf, _ = made_bufs[:3]
        x_buf, b_buf, gain_buf, _ = given_bufs
        grad = out_ref[here, : columns // 2].astype(F32)
        middle = x_buf[here, :].astype(F32) + b_buf[here, :].astype(F32)
        scale = lax.rsqrt(jnp.mean(middle * middle, axis=-1, keepdims=True) + epsilon)
        scaled = grad * gain_buf[...]
        mean = jnp.mean(middle * scaled, axis=-1, keepdims=True)
        value = stage[here, :].astype(F32) + scale * scaled - middle * (scale * scale * scale) * mean
        gm_buf[here, :] = value
        gb_buf[here, :] = value.astype(BF16)
        acc[...] += jnp.sum(grad * middle * scale, axis=0, keepdims=True)

    def branch_end():
        made_bufs[2][...] = dot_nt(made_bufs[1][...], given_bufs[3][...]).astype(BF16)
        made_bufs[3][...] = acc[...]
        for at in range(4):
            made_copy(at).start()

    def token_columns(c):
        here = columns_of(c)
        x_buf, _, gain_buf = given_bufs[:3]
        value = out_ref[:, here].astype(F32) * x_buf[:, here].astype(F32)
        dots[...] += value * gain_buf[:, here]
        acc[:, here] = jnp.sum(value * scales[...], axis=0, keepdims=True)

    def token_rows(i, carry):
        here = tile_of(i)
        x_buf, gm_buf, gain_buf = given_bufs[:3]
        scale = scales[here, :1]
        mean = jnp.sum(dots[here, :], axis=-1, keepdims=True) * (1.0 / columns)
        wide = x_buf[here, :].astype(F32)
        scaled = out_ref[here, :].astype(F32) * gain_buf[...]
        value = gm_buf[here, :] + scale * scaled - wide * ((scale * scale * scale) * mean)
        made_bufs[0][here, :] = value.astype(BF16)
        return carry

    def output_rows(i):
        here = tile_of(i)
        x_buf, b_buf, m_buf = given_bufs[0], given_bufs[4], given_bufs[5]
        wide = x_buf[here, :].astype(F32)
        scale = lax.rsqrt(jnp.mean(wide * wide, axis=-1, keepdims=True) + epsilon)
        scales[here, :] = jnp.broadcast_to(scale, (tile, width))
        value = wide + b_buf[here, :].astype(F32) + m_buf[here, :].astype(F32)
        made_bufs[2][here, :] = value.astype(BF16)

    acc[...] = jnp.zeros_like(acc)
    dots[...] = jnp.zeros_like(dots)
    load_weights(0)
    load_weights(1)
    for at in range(len(rights)):
        right_copy(at).start()
    left_copy(0).start()
    for at in range(given):
        given_copy(at).start()

    barrier = pltpu.get_barrier_semaphore()
    if ending == "tokens":
        greeted = [{"mp": pair}] + [peer(k)[1] for k in range(1, peers)]
    else:
        greeted = [{"mp": pair}, {"seq": sibling}, {"seq": beside}, {"batch": 1 - batch}]
    for device in greeted:
        pl.semaphore_signal(barrier, inc=1, device_id=device, device_id_type=MESH)

    @pl.when(is_mid)
    def _():
        pl.semaphore_signal(barrier, inc=1, device_id={"mp": across}, device_id_type=MESH)
        pl.semaphore_wait(barrier, len(greeted) + 1)

    @pl.when(is_end)
    def _():
        pl.semaphore_wait(barrier, len(greeted))

    for at in range(len(rights)):
        right_copy(at).wait()

    def left_of(u):
        index = 0
        for at in range(1, left_count):
            index = index + (u >= flips_before[at]).astype(jnp.int32)
        return index

    def product(u, at, side):
        row = pl.multiple_of((2 * at + side) * block, block)
        column = pl.multiple_of(u * block, block)
        return dot_nn(flip[left_of(u), pl.ds(row, block), :], right_all[:, pl.ds(column, block)])

    def step_of(u):
        return (u // active) * period + u % active

    def on_unit(t, body):
        u = lax.div(t, period) * active + lax.rem(t, period)

        @pl.when((t >= 0) & (lax.rem(t, period) < active) & (u < units))
        def _():
            body(u)

    def first_stage(u):
        @pl.when(u >= 2)
        def _():
            to_core(u - 2).wait_send()

        for at in range(4):
            away[lax.rem(u, 2), at] = product(u, at, 1 - core).astype(BF16)
        to_core(u).start()

    def second_stage(u):
        to_core(u).wait_recv()
        for at in range(4):
            come_one[u, at] = (product(u, at, core) + come_one[u, at].astype(F32)).astype(BF16)
        for k in range(2):
            second_hop(u, k).start()

    def third_stage(u):
        for k in range(2):
            second_hop(u, k).wait_recv()
        sent = 1 - own_at(u)
        come_two[u, sent] = (come_two[u, sent].astype(F32) + come_one[u, kept_at(u, sent)].astype(F32)).astype(BF16)
        third_hop(u).start()

    def last_stage(u):
        third_hop(u).wait_recv()
        own = own_at(u)
        value = come_three[u].astype(F32) + come_two[u, own].astype(F32) + come_one[u, kept_at(u, own)].astype(F32)
        for at in range(len(spans)):
            low, high = units_of(at)

            @pl.when((u - 2 >= low) & (u - 2 < high))
            def _():
                out_copy(at, u - 2).wait()

        for kind in ("turned", "plain"):
            mine = [units_of(at) for at in range(len(spans)) if spans[at][0] == kind]
            if mine:
                low, high = min(m[0] for m in mine), max(m[1] for m in mine)

                @pl.when((u >= low) & (u < high))
                def _():
                    result[lax.rem(u, 2)] = value.T if kind == "turned" else value

        for at in range(len(spans)):
            low, high = units_of(at)

            @pl.when((u >= low) & (u < high))
            def _():
                out_copy(at, u).start()

    def step(t, carry):
        @pl.when((t >= chunks) & (t < all_chunks))
        def _():
            @pl.when(is_end)
            def _():
                for h in range(HALVES):
                    up(t - chunks, h).wait_send()

            @pl.when(is_mid)
            def _():
                for h in range(HALVES):
                    over(t - chunks, h).wait_send()

        for group, items in enumerate(sums):

            @pl.when((t >= group * chunks) & (t < (group + 1) * chunks))
            def _():
                value = None
                for at, (start, size, mode) in enumerate(weights):
                    if members[at] == group:
                        weight(at, group, t).wait()
                        dot = dot_nt if mode == "nt" else dot_nn
                        term = dot(right_all[:, start : start + size], w_bufs[at][lax.rem(t, 3)])
                        value = term if value is None else value + term
                part[slot_of(t)] = value.astype(BF16)

        @pl.when(t < all_chunks)
        def _():
            @pl.when(is_end)
            def _():
                for h in range(HALVES):
                    up(t, h).start()

            load_weights(t + 2)

        @pl.when(is_mid & (t >= UP_LAG) & (t < all_chunks + UP_LAG))
        def _():
            c = t - UP_LAG
            slot = slot_of(c)
            for h in range(HALVES):
                here = rows_of(h)
                up(c, h).wait_recv()
                part[slot, here] = (part[slot, here].astype(F32) + first[slot, here].astype(F32)).astype(BF16)
                over(c, h).start()

        @pl.when(is_mid & (t >= OVER_LAG) & (t < all_chunks + OVER_LAG))
        def _():
            c = t - OVER_LAG
            slot = slot_of(c)
            for h in range(HALVES):
                here = rows_of(h)
                over(c, h).wait_recv()
                value = part[slot, here].astype(F32) + second[slot, here].astype(F32)
                out_ref[here, columns_of(c)] = value.astype(BF16)
                down(c, h).start()

        @pl.when(is_end & (t >= DOWN_LAG) & (t < all_chunks + DOWN_LAG))
        def _():
            for h in range(HALVES):
                down(t - DOWN_LAG, h).wait_recv()

        for at in range(left_count):

            @pl.when(t == max(step_of(flips_before[at]) - 2, at))
            def _():
                left_copy(at).wait()

                def turn(k, carry):
                    here = pl.ds(pl.multiple_of(k * block, block), block)
                    flip[at, here, :] = stage[:, here].T
                    return carry

                lax.fori_loop(0, flip.shape[1] // block, turn, 0)
                if at + 1 < left_count:
                    left_copy(at + 1).start()

        on_unit(t, first_stage)
        on_unit(t - 1, second_stage)
        on_unit(t - 1 - LAG, third_stage)
        on_unit(t - 1 - 2 * LAG, last_stage)
        if ending == "branch":

            @pl.when(t == chunks + DOWN_LAG)
            def _():
                for at in range(given):
                    given_copy(at).wait()

            @pl.when((t >= chunks + DOWN_LAG) & (t < chunks + DOWN_LAG + TILES))
            def _():
                branch_rows(t - chunks - DOWN_LAG)

            @pl.when(t == chunks + DOWN_LAG + TILES)
            def _():
                branch_end()

        else:

            @pl.when(t == TILES // 2)
            def _():
                for at in range(given):
                    given_copy(at).wait()

            @pl.when((t >= TILES // 2) & (t < TILES // 2 + TILES))
            def _():
                output_rows(t - TILES // 2)

            @pl.when(t == TILES // 2 + TILES)
            def _():
                made_copy(2).start()

            @pl.when((t >= LAST_LAG) & (t < all_chunks + LAST_LAG))
            def _():
                token_columns(t - LAST_LAG)

        return carry

    last = all_chunks + (DOWN_LAG if ending == "branch" else LAST_LAG)
    lax.fori_loop(0, max(step_of(units - 1) + 2 + 2 * LAG, last), step, 0)
    if ending == "branch":
        made_copy(made - 1).start()
    else:
        part_width = columns // peers
        for k in range(peers):
            here = slice(k * part_width, (k + 1) * part_width)
            gain_parts[k, 0:1, :] = acc[:, here]
            gain_parts[k, 1:2, :] = given_bufs[3][:, here]
        for k in range(1, peers):
            gain_copy(k).start()
        lax.fori_loop(0, TILES, token_rows, 0)
        made_copy(0).start()

    def finish(c, carry):
        @pl.when(is_mid)
        def _():
            for h in range(HALVES):
                down(c, h).wait_send()

        return carry

    lax.fori_loop(0, all_chunks, finish, 0)

    def finish_last(c, carry):
        @pl.when(is_end)
        def _():
            for h in range(HALVES):
                up(c, h).wait_send()

        @pl.when(is_mid)
        def _():
            for h in range(HALVES):
                over(c, h).wait_send()

        return carry

    lax.fori_loop(all_chunks - chunks, all_chunks, finish_last, 0)

    def settle(u, carry):
        for k in range(2):
            second_hop(u, k).wait_send()
        third_hop(u).wait_send()
        return carry

    lax.fori_loop(0, units, settle, 0)
    for u in (units - 2, units - 1):
        to_core(u).wait_send()
        for at in range(len(spans)):
            low, high = units_of(at)
            if low <= u < high:
                out_copy(at, u).wait()
    if ending == "tokens":
        gains = gain_parts[me]
        for k in range(1, peers):
            gain_copy(k).wait_recv()
            gains = gains + gain_come[k]
        made_bufs[1][...] = gains
        made_copy(1).start()
        for k in range(1, peers):
            gain_copy(k).wait_send()
    for at in range(made):
        made_copy(at).wait()


def exchange(lefts, rights, sums, flips_before, outs, spans, units, call_id, pace, ending, given, made, chunks=16):
    rows, depth = lefts[0].shape
    block = depth // 8
    placed, at = [], 0
    for _, source, size in rights:
        placed.append((at, source, size))
        at += size
    weights = [item[0] for group in sums for item in group]
    columns = weights[0].shape[0] if sums[0][0][3] == "nt" else weights[0].shape[1]
    width = columns // chunks
    sum_plan = [[item[1:] for item in group] for group in sums]
    plan = (len(lefts), placed, sum_plan, flips_before, spans, len(outs), units, chunks, *pace, ending, len(given), len(made))
    any_space = pl.BlockSpec(memory_space=pl.ANY)
    line_block = pltpu.VMEM((chunks, rows, width), BF16)
    peers = lax.axis_size("batch") * lax.axis_size("seq")
    kept = made[:-1] if ending == "branch" else made
    dma = pltpu.SemaphoreType.DMA
    all_chunks = chunks * len(sums)
    flops = sum(2 * rows * columns * size for group in sum_plan for _, size, _ in group) + 2 * rows * depth * at
    return pl.pallas_call(
        functools.partial(exchange_kernel, plan),
        out_shape=[jax.ShapeDtypeStruct(shape, F32) for shape in outs]
        + [jax.ShapeDtypeStruct(shape, kind) for shape, kind in made],
        in_specs=[any_space] * (len(lefts) + len(rights) + len(weights) + len(given)),
        out_specs=[any_space] * (len(outs) + len(made)),
        scratch_shapes=[
            pltpu.VMEM((rows, depth), BF16),
            pltpu.VMEM((len(lefts), depth, rows), BF16),
            pltpu.VMEM((rows, at), BF16),
            pltpu.VMEM((rows, columns * len(sums)), BF16),
        ]
        + [
            pltpu.VMEM((3, width, size) if mode == "nt" else (3, size, width), BF16)
            for group in sum_plan
            for _, size, mode in group
        ]
        + [
            line_block,
            line_block,
            line_block,
            pltpu.VMEM((2, 4, block, block), BF16),
            pltpu.VMEM((units, 4, block, block), BF16),
            pltpu.VMEM((units, 2, block, block), BF16),
            pltpu.VMEM((units, block, block), BF16),
            pltpu.VMEM((2, block, block), F32),
        ]
        + [pltpu.VMEM(value.shape, value.dtype) for value in given]
        + [pltpu.VMEM(shape, kind) for shape, kind in kept]
        + [
            pltpu.VMEM((1, depth), F32),
            pltpu.VMEM((rows, width), F32),
            pltpu.VMEM((rows, width), F32),
            pltpu.VMEM((peers, 2, depth // peers), F32),
            pltpu.VMEM((peers, 2, depth // peers), F32),
            dma((len(given),)),
            dma((len(made),)),
            dma((peers,)),
            dma((peers,)),
            dma((len(lefts),)),
            dma((len(rights),)),
            dma((len(weights), 3)),
            dma((3, HALVES, all_chunks)),
            dma((3, HALVES, all_chunks)),
            dma((units,)),
            dma((units,)),
            dma((2, units)),
            dma((2, units)),
            dma((units,)),
            dma((units,)),
            dma((len(spans), 2)),
        ],
        compiler_params=pltpu.CompilerParams(
            collective_id=call_id, has_side_effects=True, vmem_limit_bytes=62 << 20
        ),
        cost_estimate=pl.CostEstimate(flops=flops + (50 << 30), bytes_accessed=20 << 20, transcendentals=0),
        name=f"exchange_{call_id}",
    )(*lefts, *[right[0] for right in rights], *weights, *given)


def forward_kernel(
    mixed_ref, x_ref, gain_ref, wo_hbm, wg_hbm, wu_hbm, ga_hbm,
    branch_hbm, n_hbm, act_hbm, gg_hbm, gu_hbm,
    branch, n_ref, act_ref, gg_ref, gu_ref, ga_ref, gate_acc, up_acc, squares, wo_buf, w_buf, part, first, second,
    ga_sem, wo_sem, w_sem, ar_send, ar_recv, out_sem,
):
    chunks, rows, width = part.shape
    total_columns = branch.shape[1]
    place = lax.axis_index("mp")
    pair = place + 1 - 2 * lax.rem(place, 2)
    across = 3 - place
    is_mid = (place == 1) | (place == 2)
    is_end = (place == 0) | (place == 3)
    high = rows // HALVES
    deep = w_buf.shape[2]

    def columns_of(c):
        return pl.ds(pl.multiple_of(c * width, width), width)

    def rows_of(h):
        return slice(h * high, (h + 1) * high)

    def remote(source, target, kind, h, c, device):
        return pltpu.make_async_remote_copy(
            src_ref=source,
            dst_ref=target,
            send_sem=ar_send.at[kind, h, c],
            recv_sem=ar_recv.at[kind, h, c],
            device_id={"mp": device},
            device_id_type=MESH,
        )

    def up(c, h):
        return remote(part.at[c, rows_of(h)], first.at[c, rows_of(h)], 0, h, c, pair)

    def over(c, h):
        return remote(part.at[c, rows_of(h)], second.at[c, rows_of(h)], 1, h, c, across)

    def down(c, h):
        here = branch.at[rows_of(h), columns_of(c)]
        return remote(here, here, 2, h, c, pair)

    def out_weight(c):
        slot = lax.rem(c, 3)
        return pltpu.make_async_copy(wo_hbm.at[:, columns_of(c)], wo_buf.at[slot], wo_sem.at[slot])

    def deep_of(p):
        return pl.ds(pl.multiple_of(p * deep, deep), deep)

    def weight(at, p):
        slot = lax.rem(p, 3)
        source = (wg_hbm, wu_hbm)[at].at[deep_of(p), :]
        return pltpu.make_async_copy(source, w_buf.at[at, slot], w_sem.at[at, slot])

    ga_copy = pltpu.make_async_copy(ga_hbm, ga_ref, ga_sem.at[0])
    out_weight(0).start()
    out_weight(1).start()
    for p in range(2):
        for at in range(2):
            weight(at, p).start()
    ga_copy.start()
    barrier = pltpu.get_barrier_semaphore()
    pl.semaphore_signal(barrier, inc=1, device_id={"mp": pair}, device_id_type=MESH)

    @pl.when(is_mid)
    def _():
        pl.semaphore_signal(barrier, inc=1, device_id={"mp": across}, device_id_type=MESH)
        pl.semaphore_wait(barrier, 2)

    @pl.when(is_end)
    def _():
        pl.semaphore_wait(barrier, 1)

    squares[...] = jnp.zeros_like(squares)
    per_deep = deep // width

    def step(t, carry):
        @pl.when(t < chunks)
        def _():
            out_weight(t).wait()
            part[t] = dot_nn(mixed_ref[...], wo_buf[lax.rem(t, 3)]).astype(BF16)

            @pl.when(is_end)
            def _():
                for h in range(HALVES):
                    up(t, h).start()

            @pl.when(t + 2 < chunks)
            def _():
                out_weight(t + 2).start()

        @pl.when(is_mid & (t >= UP_LAG) & (t < chunks + UP_LAG))
        def _():
            c = t - UP_LAG
            for h in range(HALVES):
                here = rows_of(h)
                up(c, h).wait_recv()
                part[c, here] = (part[c, here].astype(F32) + first[c, here].astype(F32)).astype(BF16)
                over(c, h).start()

        @pl.when(is_mid & (t >= OVER_LAG) & (t < chunks + OVER_LAG))
        def _():
            c = t - OVER_LAG
            for h in range(HALVES):
                here = rows_of(h)
                over(c, h).wait_recv()
                value = part[c, here].astype(F32) + second[c, here].astype(F32)
                branch[here, columns_of(c)] = value.astype(BF16)
                down(c, h).start()

        @pl.when(is_end & (t >= DOWN_LAG))
        def _():
            for h in range(HALVES):
                down(t - DOWN_LAG, h).wait_recv()

        @pl.when((t >= DOWN_LAG) & (lax.rem(t - DOWN_LAG, per_deep) == per_deep - 1))
        def _():
            p = lax.div(t - DOWN_LAG, per_deep)
            here = deep_of(p)
            middle = x_ref[:, here].astype(F32) + branch[:, here].astype(F32)
            squares[...] += jnp.sum(middle * middle, axis=-1, keepdims=True)
            scaled = (middle * gain_ref[:, here]).astype(BF16)
            for at, acc in enumerate((gate_acc, up_acc)):
                weight(at, p).wait()
                value = dot_nn(scaled, w_buf[at, lax.rem(p, 3)])

                @pl.when(p == 0)
                def _():
                    acc[...] = value

                @pl.when(p > 0)
                def _():
                    acc[...] += value

            @pl.when((p + 2) * deep < total_columns)
            def _():
                for at in range(2):
                    weight(at, p + 2).start()

        return carry

    lax.fori_loop(0, chunks + DOWN_LAG, step, 0)
    ga_copy.wait()
    tile = rows // TILES
    outs = [(n_ref, n_hbm), (act_ref, act_hbm), (gg_ref, gg_hbm), (gu_ref, gu_hbm)]

    def out_copy(at, i):
        here = pl.ds(pl.multiple_of(i * tile, tile), tile)
        return pltpu.make_async_copy(outs[at][0].at[here, :], outs[at][1].at[here, :], out_sem.at[at, i])

    branch_copy = pltpu.make_async_copy(branch, branch_hbm, ga_sem.at[1])
    branch_copy.start()

    def rows_step(i, carry):
        here = pl.ds(pl.multiple_of(i * tile, tile), tile)
        scale = lax.rsqrt(squares[here, :1] * (1.0 / total_columns) + epsilon)
        middle = x_ref[here, :].astype(F32) + branch[here, :].astype(F32)
        n_ref[here, :] = (middle * scale * gain_ref[...]).astype(BF16)
        gate = gate_acc[here, :] * scale
        up_pre = up_acc[here, :] * scale
        grad = ga_ref[here, :].astype(F32)
        sigmoid = jax.nn.sigmoid(gate)
        swish = gate * sigmoid
        act_ref[here, :] = (swish * up_pre).astype(BF16)
        gu_ref[here, :] = (grad * swish).astype(BF16)
        gg_ref[here, :] = (grad * up_pre * sigmoid * (1.0 + gate * (1.0 - sigmoid))).astype(BF16)
        for at in range(4):
            out_copy(at, i).start()
        return carry

    lax.fori_loop(0, TILES, rows_step, 0)

    def finish(c, carry):
        @pl.when(is_end)
        def _():
            for h in range(HALVES):
                up(c, h).wait_send()

        @pl.when(is_mid)
        def _():
            for h in range(HALVES):
                over(c, h).wait_send()
                down(c, h).wait_send()

        return carry

    lax.fori_loop(0, chunks, finish, 0)

    def drain(i, carry):
        for at in range(4):
            out_copy(at, i).wait()
        return carry

    lax.fori_loop(0, TILES, drain, 0)
    branch_copy.wait()


def forward(mixed, tokens, gain, w_output, w_gate, w_up, grad_active, call_id, chunks=16, deep=256):
    rows, columns = tokens.shape
    hidden = w_gate.shape[1]
    width = columns // chunks
    vmem, any_space = pl.BlockSpec(memory_space=pltpu.VMEM), pl.BlockSpec(memory_space=pl.ANY)
    dma = pltpu.SemaphoreType.DMA
    shapes = [(rows, columns), (rows, columns), (rows, hidden), (rows, hidden), (rows, hidden)]
    line_block = pltpu.VMEM((chunks, rows, width), BF16)
    return pl.pallas_call(
        forward_kernel,
        in_specs=[vmem] * 3 + [any_space] * 4,
        out_specs=[any_space] * 5,
        out_shape=[jax.ShapeDtypeStruct(shape, BF16) for shape in shapes],
        scratch_shapes=[pltpu.VMEM(shape, BF16) for shape in shapes]
        + [
            pltpu.VMEM((rows, hidden), BF16),
            pltpu.VMEM((rows, hidden), F32),
            pltpu.VMEM((rows, hidden), F32),
            pltpu.VMEM((rows, PAIR), F32),
            pltpu.VMEM((3, mixed.shape[1], width), BF16),
            pltpu.VMEM((2, 3, deep, hidden), BF16),
            line_block,
            line_block,
            line_block,
            dma((2,)),
            dma((3,)),
            dma((2, 3)),
            dma((3, HALVES, chunks)),
            dma((3, HALVES, chunks)),
            dma((4, TILES)),
        ],
        compiler_params=pltpu.CompilerParams(
            collective_id=call_id, has_side_effects=True, vmem_limit_bytes=62 << 20
        ),
        name="forward",
    )(mixed, tokens, gain, w_output, w_gate, w_up, grad_active)


def final_kernel(gn_ref, x_ref, gm_ref, gain_ref, mlp_ref, out_ref, gains_ref, acc, parts, come, send_sem, recv_sem):
    seq, batch = lax.axis_index("seq"), lax.axis_index("batch")
    seq_count = lax.axis_size("seq")
    peers = parts.shape[0]
    block = parts.shape[2]
    me = batch * seq_count + seq

    def peer(k):
        there = lax.rem(me + k, peers)
        return there, {"batch": lax.div(there, seq_count), "seq": lax.rem(there, seq_count)}

    def copy(k):
        there, device = peer(k)
        return pltpu.make_async_remote_copy(
            src_ref=parts.at[there],
            dst_ref=come.at[k],
            send_sem=send_sem.at[k],
            recv_sem=recv_sem.at[k],
            device_id=device,
            device_id_type=MESH,
        )

    barrier = pltpu.get_barrier_semaphore()
    for k in range(1, peers):
        pl.semaphore_signal(barrier, inc=1, device_id=peer(k)[1], device_id_type=MESH)
    rows = x_ref.shape[0]
    tile = rows // 8
    gain = gain_ref[...]
    acc[...] = jnp.zeros_like(acc)

    def rows_step(i, carry):
        here = pl.ds(pl.multiple_of(i * tile, tile), tile)
        wide = x_ref[here, :].astype(F32)
        grad = gn_ref[here, :].astype(F32)
        scale = lax.rsqrt(jnp.mean(wide * wide, axis=-1, keepdims=True) + epsilon)
        scaled = grad * gain
        mean = jnp.mean(wide * scaled, axis=-1, keepdims=True)
        result = gm_ref[here, :] + scale * scaled - wide * (scale * scale * scale) * mean
        out_ref[here, :] = result.astype(BF16)
        acc[...] += jnp.sum(grad * wide * scale, axis=0, keepdims=True)
        return carry

    lax.fori_loop(0, 8, rows_step, 0)
    for k in range(peers):
        here = slice(k * block, (k + 1) * block)
        parts[k, 0:1, :] = acc[:, here]
        parts[k, 1:2, :] = mlp_ref[:, here]
    pl.semaphore_wait(barrier, peers - 1)
    for k in range(1, peers):
        copy(k).start()
    total = parts[me]
    for k in range(1, peers):
        copy(k).wait_recv()
        total = total + come[k]
    gains_ref[...] = total
    for k in range(1, peers):
        copy(k).wait_send()


def final(grad_normed, tokens, grad_middle, gain, mlp_part, call_id):
    rows, width = tokens.shape
    peers = lax.axis_size("batch") * lax.axis_size("seq")
    block = width // peers
    vmem = pl.BlockSpec(memory_space=pltpu.VMEM)
    return pl.pallas_call(
        final_kernel,
        out_shape=[jax.ShapeDtypeStruct((rows, width), BF16), jax.ShapeDtypeStruct((2, block), F32)],
        in_specs=[vmem] * 5,
        out_specs=[vmem, vmem],
        scratch_shapes=[
            pltpu.VMEM((1, width), F32),
            pltpu.VMEM((peers, 2, block), F32),
            pltpu.VMEM((peers, 2, block), F32),
            pltpu.SemaphoreType.DMA((peers,)),
            pltpu.SemaphoreType.DMA((peers,)),
        ],
        compiler_params=pltpu.CompilerParams(collective_id=call_id, has_side_effects=True),
        name="final",
    )(grad_normed, tokens, grad_middle, gain, mlp_part)


def settle_kernel(places, *refs):
    count = len(places)
    sources, targets = refs[:count], refs[count : -count - 2]
    bufs, load_sem, store_sem = refs[-count - 2 : -2], refs[-2], refs[-1]

    def load(at):
        return pltpu.make_async_copy(sources[at], bufs[at], load_sem.at[at])

    def store(at):
        index, row = places[at]
        target = targets[index].at[row : row + bufs[at].shape[0], :]
        return pltpu.make_async_copy(bufs[at], target, store_sem.at[at])

    for at in range(count):
        load(at).start()
    for at in range(count):
        load(at).wait()
        store(at).start()
    for at in range(count):
        store(at).wait()


def settle(groups):
    places, shapes, arrays = [], [], []
    for index, group in enumerate(groups):
        row = 0
        for array in group:
            places.append((index, row))
            arrays.append(array)
            row += array.shape[0]
        shapes.append(jax.ShapeDtypeStruct((row, group[0].shape[1]), group[0].dtype))
    any_space = pl.BlockSpec(memory_space=pl.ANY)
    dma = pltpu.SemaphoreType.DMA
    return pl.pallas_call(
        functools.partial(settle_kernel, places),
        in_specs=[any_space] * len(arrays),
        out_specs=[any_space] * len(groups),
        out_shape=shapes,
        scratch_shapes=[pltpu.VMEM(array.shape, array.dtype) for array in arrays]
        + [dma((len(arrays),)), dma((len(arrays),))],
        compiler_params=pltpu.CompilerParams(vmem_limit_bytes=62 << 20),
        name="settle",
    )(*arrays)


def scatter_sum(left, right):
    rows, depth = left.shape
    columns = right.shape[1]
    batch_count = lax.axis_size("batch")
    seq_index = lax.axis_index("seq")
    core, chip = seq_index % 2, seq_index // 2
    block = depth // (4 * batch_count)
    split = left.reshape(rows, batch_count, 2, 2, block)
    size = lax.axis_size("seq")

    def product(at):
        taken = lax.dynamic_index_in_dim(split, at, 3, keepdims=False).reshape(rows, depth // 2)
        return dot_tn(taken, right)

    away = product(1 - core).astype(BF16)
    arrived = lax.ppermute(away, "seq", [(s, s ^ 1) for s in range(size)])
    kept = (product(core) + arrived.astype(F32)).astype(BF16)
    kept = kept.reshape(batch_count, 2, block, columns)
    half = columns // 2

    def over_chip(values, axis):
        sent = lax.dynamic_index_in_dim(values, 1 - chip, axis, keepdims=False)
        stay = lax.dynamic_index_in_dim(values, chip, axis, keepdims=False)
        came = lax.ppermute(sent, "seq", [(s, s ^ 2) for s in range(size)])
        return stay.astype(F32) + came.astype(F32)

    def over_batch(values):
        if batch_count == 2:
            here = lax.axis_index("batch")
            sent = lax.dynamic_index_in_dim(values, 1 - here, 0, keepdims=False)
            stay = lax.dynamic_index_in_dim(values, here, 0, keepdims=False)
            came = lax.ppermute(sent, "batch", [(0, 1), (1, 0)])
            return stay.astype(F32) + came.astype(F32)
        return lax.psum_scatter(values, "batch", scatter_dimension=0, tiled=False).astype(F32)

    one = over_batch(over_chip(kept[..., :half], 1).astype(BF16))
    two = over_chip(over_batch(kept[..., half:]).astype(BF16), 0)
    return jnp.concatenate([one, two], axis=1)


def local(
    tokens, segment_ids, attn_gain, w_query, w_key, w_value, w_output, mlp_gain, w_gate, w_up, w_down, cotangent
):
    rows, width = tokens.shape
    cos, sin, normed, queries, key_value, grad_active = project(
        tokens, attn_gain[None, :], w_query, w_key, w_value, segment_ids, cotangent, w_down, 5
    )
    key_value = key_value.reshape(3 * rows, 2 * PAIR)
    mixed, logs = attend(queries, key_value, segment_ids)
    branch_low, normed_two, active, grad_gate_low, grad_up_low = forward(
        mixed, tokens, mlp_gain[None, :], w_output, w_gate, w_up, grad_active, 1
    )
    wide = tokens.astype(F32)
    middle = wide + branch_low.astype(F32)
    fused = lax.axis_size("batch") == 2
    hidden = w_gate.shape[1]
    unit = width // 8
    early = hidden * 5 // 8 // unit * unit
    if fused:
        grad_gate, grad_up, grad_down_one, grad_middle, grad_branch, grad_mixed, grad_mlp_gain, mlp_out = exchange(
            [normed_two, cotangent],
            [(grad_gate_low, 0, hidden), (grad_up_low, 0, hidden), (active, 0, hidden)],
            [
                [(w_gate, 0, hidden, "nt"), (w_up, hidden, hidden, "nt")],
                [(w_down, 2 * hidden, hidden, "nn")],
            ],
            (0, 2 * hidden // unit),
            [(unit, hidden), (unit, hidden), (early, unit)],
            [
                ("plain", 0, 0, 0, hidden),
                ("plain", 1, 0, hidden, hidden),
                ("turned", 2, 0, 2 * hidden, early),
            ],
            (2 * hidden + early) // unit,
            2,
            (3, 2),
            "branch",
            [tokens, branch_low, mlp_gain[None, :], w_output],
            [
                ((rows, width), F32),
                ((rows, width), BF16),
                ((rows, mixed.shape[1]), BF16),
                ((1, width), F32),
                ((rows, width), BF16),
            ],
        )
    else:
        grad_normed_two = line_sum([(grad_gate_low, w_gate, "nt"), (grad_up_low, w_up, "nt")], 2)
        grad_gate = scatter_sum(normed_two, grad_gate_low)
        grad_up = scatter_sum(normed_two, grad_up_low)
        mlp_out = lax.psum(dot_nn(active, w_down).astype(BF16), "mp")
        grad_normed_two = grad_normed_two.astype(F32)
        scaled_two = grad_normed_two * mlp_gain
        scale_two = lax.rsqrt(jnp.mean(middle * middle, axis=-1, keepdims=True) + epsilon)
        grad_middle = (
            cotangent.astype(F32)
            + scale_two * scaled_two
            - middle
            * (scale_two * scale_two * scale_two)
            * jnp.mean(middle * scaled_two, axis=-1, keepdims=True)
        )
        grad_mlp_gain = jnp.sum(grad_normed_two * middle * scale_two, axis=0)[None, :]
        grad_branch = grad_middle.astype(BF16)
        grad_mixed = dot_nt(grad_branch, w_output).astype(BF16)

    grad_query_pre, grad_key_pre, grad_value_pre = attend_back(
        queries, key_value, segment_ids, mixed, grad_mixed, logs, cos, sin, 6
    )
    query_width = grad_query_pre.shape[1]
    if fused:
        late, mixed_width = hidden - early, mixed.shape[1]
        query_at = late + mixed_width
        key_at = query_at + query_width
        grad_down_two, grad_output, grad_query, grad_key, grad_value, grad_tokens, gains, output = exchange(
            [cotangent, grad_branch, normed],
            [
                (active, early, late),
                (mixed, 0, mixed_width),
                (grad_query_pre, 0, query_width),
                (grad_key_pre, 0, PAIR),
                (grad_value_pre, 0, PAIR),
            ],
            [
                [
                    (w_query, query_at, query_width, "nt"),
                    (w_key, key_at, PAIR, "nt"),
                    (w_value, key_at + PAIR, PAIR, "nt"),
                ]
            ],
            (0, late // unit, query_at // unit),
            [(late, unit), (mixed_width, unit), (unit, query_width), (unit, PAIR), (unit, PAIR)],
            [
                ("turned", 0, 0, 0, late),
                ("turned", 1, 0, late, mixed_width),
                ("plain", 2, 0, query_at, query_width),
                ("plain", 3, 0, key_at, PAIR),
                ("plain", 4, 0, key_at + PAIR, PAIR),
            ],
            (key_at + 2 * PAIR) // unit,
            3,
            (3, 2),
            "tokens",
            [tokens, grad_middle, attn_gain[None, :], grad_mlp_gain, branch_low, mlp_out],
            [((rows, width), BF16), ((2, unit), F32), ((rows, width), BF16)],
        )
        grad_gate, grad_up, grad_down, grad_output, grad_query, grad_key, grad_value, grad_tokens, output = settle(
            [
                [grad_gate],
                [grad_up],
                [grad_down_one, grad_down_two],
                [grad_output],
                [grad_query],
                [grad_key],
                [grad_value],
                [grad_tokens],
                [output],
            ]
        )
    else:
        output = (middle + mlp_out.astype(F32)).astype(BF16)
        grad_down = scatter_sum(cotangent, active).T
        grad_output = scatter_sum(grad_branch, mixed).T
        grad_qkv = scatter_sum(normed, jnp.concatenate([grad_query_pre, grad_key_pre, grad_value_pre], axis=1))
        grad_query = grad_qkv[:, :query_width]
        grad_key = grad_qkv[:, query_width : query_width + PAIR]
        grad_value = grad_qkv[:, query_width + PAIR :]
        grad_normed = line_sum(
            [(grad_query_pre, w_query, "nt"), (grad_key_pre, w_key, "nt"), (grad_value_pre, w_value, "nt")], 3
        )
        grad_tokens, gains = final(grad_normed, tokens, grad_middle, attn_gain[None, :], grad_mlp_gain, 4)
    return (
        output,
        grad_tokens,
        gains[0],
        grad_query,
        grad_key,
        grad_value,
        grad_output,
        gains[1],
        grad_gate,
        grad_up,
        grad_down,
    )


def solution(mesh):
    tokens_spec = P(("batch", "seq"), None)
    in_specs = (
        tokens_spec,
        P("batch", None),
        P(),
        P(None, "mp"),
        P(None, "mp"),
        P(None, "mp"),
        P("mp", None),
        P(),
        P(None, "mp"),
        P(None, "mp"),
        P("mp", None),
        tokens_spec,
    )
    row_split = P(("batch", "seq"), "mp")
    column_split = P("mp", ("batch", "seq"))
    out_specs = (
        tokens_spec,
        tokens_spec,
        P(("batch", "seq")),
        row_split,
        row_split,
        row_split,
        column_split,
        P(("batch", "seq")),
        row_split,
        row_split,
        column_split,
    )
    return jax.shard_map(local, mesh=mesh, in_specs=in_specs, out_specs=out_specs, check_vma=False)
```

```python
import functools
import math

import jax
import jax.numpy as jnp
from jax import lax
from jax.experimental import pallas as pl
from jax.experimental.pallas import tpu as pltpu
from jax.sharding import PartitionSpec as P

HS = 64
PAIR = 2 * HS
LONGEST = 1024
FORWARD_ROWS = 256
BACKWARD_ROWS = 128
rope_base = 500000.0
epsilon = 1e-05
masked_score = -1e30
MESH = pl.DeviceIdType.MESH
F32 = jnp.float32
BF16 = jnp.bfloat16


def dot_nn(left, right):
    return lax.dot_general(left, right, (((1,), (0,)), ((), ())), preferred_element_type=F32)


def dot_nt(left, right):
    return lax.dot_general(left, right, (((1,), (1,)), ((), ())), preferred_element_type=F32)


def dot_tn(left, right):
    return lax.dot_general(left, right, (((0,), (0,)), ((), ())), preferred_element_type=F32)


def lanes_of(values):
    return lax.broadcasted_iota(jnp.int32, values.shape, 1)


def swap_halves(values):
    ahead = pltpu.roll(values, PAIR - HS // 2, 1)
    behind = pltpu.roll(values, HS // 2, 1)
    return jnp.where(lanes_of(values) % HS < HS // 2, ahead, behind)


def write_tables(seg_ref, cos_ref, sin_ref):
    rows = cos_ref.shape[0]
    first_row = lax.axis_index("seq") * rows
    every = seg_ref[...]
    mine = seg_ref[:, pl.ds(pl.multiple_of(first_row, rows), rows)]
    start = jnp.zeros(mine.shape, F32)
    for number in range(ID_COUNT - 1):
        size = jnp.sum((every == number).astype(F32), axis=1, keepdims=True)
        start = start + jnp.where(mine > number, size, 0.0)
    place = (first_row + lax.broadcasted_iota(jnp.int32, mine.shape, 1)).astype(F32) - start
    lane = lax.broadcasted_iota(jnp.int32, (1, PAIR), 1)
    frequency = jnp.exp((lane % (HS // 2)).astype(F32) * (-2.0 * math.log(rope_base) / HS))
    angles = jnp.broadcast_to(place, (PAIR, rows)).T * frequency
    cos_ref[...] = jnp.cos(angles)
    sin_ref[...] = jnp.sin(angles) * jnp.where(lane % HS < HS // 2, -1.0, 1.0)


def project_kernel(
    x_ref, gain_ref, wk_ref, wv_ref, seg_ref, cot_hbm, wq_hbm, wd_hbm,
    cos_ref, sin_ref, n_hbm, q_hbm, kv_hbm, ga_hbm,
    n_ref, q_ref, kv_ref, ga_ref, cot_ref, wq_ref, wd_ref, load_sem, wd_sem, send_sem, recv_sem, out_sem,
):
    rows = x_ref.shape[0]
    seq, seq_count = lax.axis_index("seq"), lax.axis_size("seq")
    hidden = wd_hbm.shape[0]
    width = wd_ref.shape[1]
    chunks = hidden // width
    block = rows // 2
    loads = [
        pltpu.make_async_copy(wq_hbm, wq_ref, load_sem.at[0]),
        pltpu.make_async_copy(cot_hbm, cot_ref, load_sem.at[1]),
    ]

    def weight(c):
        slot = lax.rem(c, 3)
        here = pl.ds(pl.multiple_of(c * width, width), width)
        return pltpu.make_async_copy(wd_hbm.at[here, :], wd_ref.at[slot], wd_sem.at[slot])

    def out_copy(at):
        source = (n_ref, q_ref, kv_ref, ga_ref)[at]
        return pltpu.make_async_copy(source, (n_hbm, q_hbm, kv_hbm, ga_hbm)[at], out_sem.at[at])

    def send(away):
        return pltpu.make_async_remote_copy(
            src_ref=kv_ref.at[2],
            dst_ref=kv_ref.at[2 - away],
            send_sem=send_sem.at[away],
            recv_sem=recv_sem.at[away],
            device_id={"seq": lax.rem(seq + away, seq_count)},
            device_id_type=MESH,
        )

    for load in loads:
        load.start()
    weight(0).start()
    weight(1).start()
    for away in (1, 2):

        @pl.when(seq < away)
        def _():
            kv_ref[2 - away] = jnp.zeros(kv_ref.shape[1:], BF16)

    barrier = pltpu.get_barrier_semaphore()
    for away in range(1, seq_count):
        there = lax.rem(seq + away, seq_count)
        pl.semaphore_signal(barrier, inc=1, device_id={"seq": there}, device_id_type=MESH)

    write_tables(seg_ref, cos_ref, sin_ref)
    for half in range(2):
        here = slice(half * block, (half + 1) * block)
        cos, sin = cos_ref[here, :], sin_ref[here, :]
        wide = x_ref[here, :].astype(F32)
        scale = lax.rsqrt(jnp.mean(wide * wide, axis=-1, keepdims=True) + epsilon)
        normed = (wide * scale * gain_ref[...]).astype(BF16)
        n_ref[here, :] = normed
        keys = dot_nn(normed, wk_ref[...])
        keys = keys * cos + swap_halves(keys) * sin
        values = dot_nn(normed, wv_ref[...])
        low_half = lanes_of(keys) < HS
        kv_ref[2, here, :PAIR] = jnp.where(low_half, keys, pltpu.roll(values, HS, 1)).astype(BF16)
        kv_ref[2, here, PAIR:] = jnp.where(low_half, pltpu.roll(keys, HS, 1), values).astype(BF16)
    pl.semaphore_wait(barrier, seq_count - 1)
    for away in (1, 2):

        @pl.when(seq + away < seq_count)
        def _():
            send(away).start()

    out_copy(0).start()
    for load in loads:
        load.wait()
    for half in range(2):
        here = slice(half * block, (half + 1) * block)
        cos, sin = cos_ref[here, :], sin_ref[here, :]
        queries = dot_nn(n_ref[here, :], wq_ref[...])
        for start in range(0, queries.shape[1], PAIR):
            part = queries[:, start : start + PAIR]
            q_ref[here, start : start + PAIR] = (part * cos + swap_halves(part) * sin).astype(BF16)
    out_copy(1).start()

    def step(c, carry):
        weight(c).wait()

        @pl.when(c + 2 < chunks)
        def _():
            weight(c + 2).start()

        here = pl.ds(pl.multiple_of(c * width, width), width)
        ga_ref[:, here] = dot_nt(cot_ref[...], wd_ref[lax.rem(c, 3)]).astype(BF16)
        return carry

    lax.fori_loop(0, chunks, step, 0)
    out_copy(3).start()
    for away in (1, 2):

        @pl.when(seq >= away)
        def _():
            send(away).wait_recv()

    out_copy(2).start()
    for away in (1, 2):

        @pl.when(seq + away < seq_count)
        def _():
            send(away).wait_send()

    for at in range(4):
        out_copy(at).wait()


def project(tokens, gain, w_query, w_key, w_value, segment_ids, cotangent, w_down, call_id):
    rows, width = tokens.shape
    columns, hidden = w_query.shape[1], w_down.shape[0]
    chunk = PROJECT_CHUNK
    vmem, any_space = pl.BlockSpec(memory_space=pltpu.VMEM), pl.BlockSpec(memory_space=pl.ANY)
    shapes = [(rows, width), (rows, columns), (3, rows, 2 * PAIR), (rows, hidden)]
    dma = pltpu.SemaphoreType.DMA
    return pl.pallas_call(
        project_kernel,
        in_specs=[vmem] * 5 + [any_space] * 3,
        out_specs=[vmem] * 2 + [any_space] * 4,
        out_shape=[jax.ShapeDtypeStruct((rows, PAIR), F32)] * 2
        + [jax.ShapeDtypeStruct(shape, BF16) for shape in shapes],
        scratch_shapes=[pltpu.VMEM(shape, BF16) for shape in shapes]
        + [
            pltpu.VMEM((rows, width), BF16),
            pltpu.VMEM(w_query.shape, BF16),
            pltpu.VMEM((3, chunk, width), BF16),
            dma((2,)),
            dma((3,)),
            dma((3,)),
            dma((3,)),
            dma((4,)),
        ],
        compiler_params=pltpu.CompilerParams(
            collective_id=call_id, has_side_effects=True, vmem_limit_bytes=62 << 20
        ),
        name="project",
    )(tokens, gain, w_key, w_value, segment_ids, cotangent, w_query, w_down)


def write_bias(bias_ref, seg_ref, padded_ref):
    tiles, span, both = bias_ref.shape
    size = both // 2
    rows = tiles * size
    padded_ref[:, :LONGEST] = jnp.full((1, LONGEST), -1, jnp.int32)
    padded_ref[:, LONGEST:] = seg_ref[...]
    first_row = pl.multiple_of(lax.axis_index("seq") * rows, rows)
    window = padded_ref[:, pl.ds(first_row, LONGEST + rows)].astype(F32)
    beside = jnp.broadcast_to(window, (PAIR, LONGEST + rows)).T
    beside = jnp.concatenate([beside] * (size // PAIR), axis=1)
    key_place = lax.broadcasted_iota(jnp.int32, (span, size), 0) - LONGEST
    row_place = lax.broadcasted_iota(jnp.int32, (span, size), 1)
    for tile in range(tiles):
        start = tile * size
        same = beside[start : start + span, :] == window[:, LONGEST + start : LONGEST + start + size]
        bias = jnp.where(same & (key_place <= row_place), 0.0, masked_score)
        bias_ref[tile] = jnp.concatenate([bias, bias], axis=1)


def bias_scratch(rows, size):
    assert LONGEST + rows == 3 * rows
    return pltpu.VMEM((rows // size, LONGEST + size, 2 * size), F32)


def heads_beside(values, here):
    return jnp.concatenate([values[:HS, here], values[HS:, here]], axis=1)


def heads_below(values, here):
    return jnp.concatenate([values[here, :HS], values[here, HS:]], axis=0)


def heads_stacked(values):
    size = values.shape[1] // 2
    return jnp.concatenate([values[:, :size], values[:, size:]], axis=0)


def attend_kernel(q_ref, kv_ref, seg_ref, out_ref, log_ref, bias_ref, padded_ref):
    @pl.when(pl.program_id(0) == 0)
    def _():
        write_bias(bias_ref, seg_ref, padded_ref)

    key_value = kv_ref[...]
    flipped = key_value.T
    q_flipped = (q_ref[...].astype(F32) * HS ** (-0.5)).astype(BF16).T
    tiles, span, both = bias_ref.shape
    size = both // 2
    for tile in range(tiles):
        here = slice(tile * size, (tile + 1) * size)
        keys = slice(tile * size, tile * size + span)
        scores = dot_nn(key_value[keys, :HS], heads_beside(q_flipped, here)) + bias_ref[tile]
        top = jnp.max(scores, axis=0, keepdims=True)
        powers = jnp.exp(scores - top)
        total = jnp.sum(powers, axis=0, keepdims=True)
        mixed = dot_nn(flipped[HS:, keys], powers.astype(BF16)) / total
        logs = top + jnp.log(total)
        log_ref[0, 0:1, here] = logs[:, :size]
        log_ref[0, 1:2, here] = logs[:, size:]
        out_ref[here, :] = heads_stacked(mixed).T.astype(BF16)


def attend(queries, key_value, segment_ids):
    rows, width = queries.shape
    pairs = width // PAIR
    per_group = pairs // 2
    pair_tile = pl.BlockSpec((rows, PAIR), lambda p: (0, p))
    kv_tile = pl.BlockSpec((3 * rows, PAIR), lambda p: (0, p // per_group))
    return pl.pallas_call(
        attend_kernel,
        grid=(pairs,),
        in_specs=[
            pair_tile,
            kv_tile,
            pl.BlockSpec(segment_ids.shape, lambda p: (0, 0)),
        ],
        out_specs=[pair_tile, pl.BlockSpec((1, 2, rows), lambda p: (p, 0, 0))],
        out_shape=[
            jax.ShapeDtypeStruct((rows, width), BF16),
            jax.ShapeDtypeStruct((pairs, 2, rows), F32),
        ],
        scratch_shapes=[
            bias_scratch(rows, FORWARD_ROWS),
            pltpu.VMEM((1, LONGEST + segment_ids.shape[1]), jnp.int32),
        ],
        cost_estimate=pl.CostEstimate(
            flops=16 << 30, bytes_accessed=4 << 20, transcendentals=3 * rows * rows * 2 * pairs
        ),
        name="attend",
    )(queries, key_value, segment_ids)


def attend_back_kernel(
    q_ref, kv_ref, seg_ref, out_ref, grad_ref, log_ref, cos_ref, sin_ref,
    dq_ref, dk_ref, dv_ref, bias_ref, padded_ref, dkv_ref, own_ref, sent_ref, come_ref, send_sem, recv_sem, per_group,
):
    step = pl.program_id(0)
    seq, seq_count = lax.axis_index("seq"), lax.axis_size("seq")
    barrier = pltpu.get_barrier_semaphore()

    def back(group, away):
        return pltpu.make_async_remote_copy(
            src_ref=sent_ref.at[group, 2 - away],
            dst_ref=come_ref.at[group, 2 - away],
            send_sem=send_sem.at[group, 2 - away],
            recv_sem=recv_sem.at[group, 2 - away],
            device_id={"seq": lax.rem(seq + seq_count - away, seq_count)},
            device_id_type=MESH,
        )

    @pl.when(step == 0)
    def _():
        for away in range(1, seq_count):
            there = lax.rem(seq + away, seq_count)
            pl.semaphore_signal(barrier, inc=1, device_id={"seq": there}, device_id_type=MESH)
        write_bias(bias_ref, seg_ref, padded_ref)

    rows = q_ref.shape[0]
    key_value = kv_ref[...]
    flipped = key_value[:, :].T
    scaled = (q_ref[...].astype(F32) * HS ** (-0.5)).astype(BF16)
    q_flipped = scaled.T
    grad = grad_ref[...]
    grad_flipped = grad.T
    product = (out_ref[...].astype(F32) * grad.astype(F32)).T
    tiles, span, both = bias_ref.shape
    size = both // 2

    @pl.when(step % per_group == 0)
    def _():
        dkv_ref[...] = jnp.zeros_like(dkv_ref)

    for tile in range(tiles):
        here = slice(tile * size, (tile + 1) * size)
        keys = slice(tile * size, tile * size + span)
        logs = jnp.concatenate([log_ref[0, 0:1, here], log_ref[0, 1:2, here]], axis=1)
        delta = jnp.sum(heads_beside(product, here), axis=0, keepdims=True)
        scores = dot_nn(key_value[keys, :HS], heads_beside(q_flipped, here)) + bias_ref[tile]
        shares = jnp.exp(scores - logs)
        grad_shares = dot_nn(key_value[keys, HS:], heads_beside(grad_flipped, here))
        grad_scores = (shares * (grad_shares - delta)).astype(BF16)
        dvalue = dot_nn(shares.astype(BF16), heads_below(grad, here))
        dkey = dot_nn(grad_scores, heads_below(scaled, here))
        dkv_ref[keys, :] += jnp.concatenate([dkey, dvalue], axis=1)
        dq = heads_stacked(dot_nn(flipped[:HS, keys], grad_scores)).T * HS ** (-0.5)
        dq_ref[here, :] = (dq * cos_ref[here, :] - swap_halves(dq) * sin_ref[here, :]).astype(BF16)

    for group in range(2):

        @pl.when(step == (group + 1) * per_group - 1)
        def _():
            sent_ref[group, 0] = dkv_ref[:rows, :].astype(BF16)
            sent_ref[group, 1] = dkv_ref[rows : 2 * rows, :].astype(BF16)
            own_ref[group] = dkv_ref[2 * rows :, :]
            if group == 0:
                pl.semaphore_wait(barrier, seq_count - 1)
            for away in (1, 2):

                @pl.when(seq >= away)
                def _():
                    back(group, away).start()

    @pl.when(step == 2 * per_group - 1)
    def _():
        for group in range(2):
            for away in (1, 2):

                @pl.when(seq + away < seq_count)
                def _():
                    back(group, away).wait_recv()
                    own_ref[group] += come_ref[group, 2 - away].astype(F32)

        one, two = own_ref[0], own_ref[1]
        low_half = lanes_of(one) < HS
        keys = jnp.where(low_half, one, pltpu.roll(two, HS, 1))
        dk_ref[...] = (keys * cos_ref[...] - swap_halves(keys) * sin_ref[...]).astype(BF16)
        dv_ref[...] = jnp.where(low_half, pltpu.roll(one, HS, 1), two).astype(BF16)
        for group in range(2):
            for away in (1, 2):

                @pl.when(seq >= away)
                def _():
                    back(group, away).wait_send()


def attend_back(queries, key_value, segment_ids, mixed, grad, logs, cos, sin, call_id):
    rows, width = queries.shape
    pairs = width // PAIR
    per_group = pairs // 2
    pair_tile = pl.BlockSpec((rows, PAIR), lambda p: (0, p))
    whole = pl.BlockSpec((rows, PAIR), lambda p: (0, 0))
    wide_tile = pl.BlockSpec((3 * rows, PAIR), lambda p: (0, p // per_group))
    full = lambda array: pl.BlockSpec(array.shape, lambda p: (0, 0))
    return pl.pallas_call(
        functools.partial(attend_back_kernel, per_group=per_group),
        grid=(pairs,),
        in_specs=[
            pair_tile,
            wide_tile,
            full(segment_ids),
            pair_tile,
            pair_tile,
            pl.BlockSpec((1, 2, rows), lambda p: (p, 0, 0)),
            full(cos),
            full(sin),
        ],
        out_specs=[pair_tile, whole, whole],
        out_shape=[
            jax.ShapeDtypeStruct((rows, width), BF16),
            jax.ShapeDtypeStruct((rows, PAIR), BF16),
            jax.ShapeDtypeStruct((rows, PAIR), BF16),
        ],
        scratch_shapes=[
            bias_scratch(rows, BACKWARD_ROWS),
            pltpu.VMEM((1, LONGEST + segment_ids.shape[1]), jnp.int32),
            pltpu.VMEM((3 * rows, PAIR), F32),
            pltpu.VMEM((2, rows, PAIR), F32),
            pltpu.VMEM((2, 2, rows, PAIR), BF16),
            pltpu.VMEM((2, 2, rows, PAIR), BF16),
            pltpu.SemaphoreType.DMA((2, 2)),
            pltpu.SemaphoreType.DMA((2, 2)),
        ],
        compiler_params=pltpu.CompilerParams(collective_id=call_id, has_side_effects=True),
        cost_estimate=pl.CostEstimate(
            flops=40 << 30, bytes_accessed=6 << 20, transcendentals=3 * rows * rows * 2 * pairs
        ),
        name="attend_back",
    )(queries, key_value, segment_ids, mixed, grad, logs, cos, sin)


def line_sum_kernel(modes, chunks, *refs):
    count = len(modes)
    a_refs, w_refs, out_ref = refs[:count], refs[count : 2 * count], refs[2 * count]
    rest = refs[2 * count + 1 :]
    w_bufs = rest[:count]
    part, first, second, total, w_sem, send_sem, recv_sem = rest[count:]
    width = part.shape[2]
    place = lax.axis_index("mp")
    pair = place + 1 - 2 * lax.rem(place, 2)
    across = 3 - place
    is_mid = (place == 1) | (place == 2)
    is_end = (place == 0) | (place == 3)

    def weight(at, c):
        if modes[at] == "nt":
            source = w_refs[at].at[pl.ds(pl.multiple_of(c * width, width), width), :]
        else:
            source = w_refs[at].at[:, pl.ds(pl.multiple_of(c * width, width), width)]
        return pltpu.make_async_copy(source, w_bufs[at].at[c], w_sem.at[at, c])

    def remote(kind, source, target, c, device):
        return pltpu.make_async_remote_copy(
            src_ref=source.at[c],
            dst_ref=target.at[c],
            send_sem=send_sem.at[kind, c],
            recv_sem=recv_sem.at[kind, c],
            device_id={"mp": device},
            device_id_type=MESH,
        )

    def up(c):
        return remote(0, part, first, c, pair)

    def over(c):
        return remote(1, part, second, c, across)

    def down(c):
        return remote(2, total, total, c, pair)

    def start_weights(c, carry):
        for at in range(count):
            weight(at, c).start()
        return carry

    lax.fori_loop(0, chunks, start_weights, 0)
    barrier = pltpu.get_barrier_semaphore()
    pl.semaphore_signal(barrier, inc=1, device_id={"mp": pair}, device_id_type=MESH)

    @pl.when(is_mid)
    def _():
        pl.semaphore_signal(barrier, inc=1, device_id={"mp": across}, device_id_type=MESH)
        pl.semaphore_wait(barrier, 2)

    @pl.when(is_end)
    def _():
        pl.semaphore_wait(barrier, 1)

    def step(t, carry):
        @pl.when(t < chunks)
        def _():
            value = None
            for at in range(count):
                weight(at, t).wait()
                dot = dot_nt if modes[at] == "nt" else dot_nn
                term = dot(a_refs[at][...], w_bufs[at][t])
                value = term if value is None else value + term
            part[t] = value.astype(BF16)

            @pl.when(is_end)
            def _():
                up(t).start()

        @pl.when(is_mid & (t >= 1) & (t < chunks + 1))
        def _():
            c = t - 1
            up(c).wait_recv()
            part[c] = (part[c].astype(F32) + first[c].astype(F32)).astype(BF16)
            over(c).start()

        @pl.when(is_mid & (t >= OVER_LAG))
        def _():
            c = t - OVER_LAG
            over(c).wait_recv()
            total[c] = (part[c].astype(F32) + second[c].astype(F32)).astype(BF16)
            down(c).start()

        return carry

    lax.fori_loop(0, chunks + OVER_LAG, step, 0)

    def finish(c, carry):
        @pl.when(is_end)
        def _():
            up(c).wait_send()
            down(c).wait_recv()

        @pl.when(is_mid)
        def _():
            over(c).wait_send()
            down(c).wait_send()

        out_ref[:, pl.ds(pl.multiple_of(c * width, width), width)] = total[c]
        return carry

    lax.fori_loop(0, chunks, finish, 0)


def line_sum(pairs, call_id, chunks=16):
    lefts = [left for left, _, _ in pairs]
    rights = [right for _, right, _ in pairs]
    modes = tuple(mode for _, _, mode in pairs)
    rows = lefts[0].shape[0]
    columns = rights[0].shape[0] if modes[0] == "nt" else rights[0].shape[1]
    width = columns // chunks
    count = len(pairs)
    bufs = [
        pltpu.VMEM((chunks, width, left.shape[1]) if mode == "nt" else (chunks, left.shape[1], width), BF16)
        for left, _, mode in pairs
    ]
    flops = sum(2 * rows * columns * left.shape[1] for left in lefts)
    moved = sum(right.size * 2 for right in rights)
    block = pltpu.VMEM((chunks, rows, width), BF16)
    return pl.pallas_call(
        functools.partial(line_sum_kernel, modes, chunks),
        out_shape=jax.ShapeDtypeStruct((rows, columns), BF16),
        in_specs=[pl.BlockSpec(memory_space=pltpu.VMEM)] * count
        + [pl.BlockSpec(memory_space=pl.ANY)] * count,
        out_specs=pl.BlockSpec(memory_space=pltpu.VMEM),
        scratch_shapes=bufs
        + [
            block,
            block,
            block,
            block,
            pltpu.SemaphoreType.DMA((count, chunks)),
            pltpu.SemaphoreType.DMA((3, chunks)),
            pltpu.SemaphoreType.DMA((3, chunks)),
        ],
        compiler_params=pltpu.CompilerParams(collective_id=call_id, has_side_effects=True),
        cost_estimate=pl.CostEstimate(
            flops=flops + (40 << 30), bytes_accessed=moved, transcendentals=0
        ),
        name=f"line_sum_{call_id}",
    )(*lefts, *rights)

LAG = 3
UP_LAG = 1
OVER_LAG = 3
DOWN_LAG = 8
HALVES = 1
ID_COUNT = 4
LAST_LAG = 12
TILES = 8
PROJECT_CHUNK = 512


def exchange_kernel(plan, *refs):
    left_count, rights, sums, flips_before, spans, out_count, units, chunks, period, active, ending, given, made = plan
    refs = list(refs)

    def take(n):
        got = refs[:n]
        del refs[:n]
        return got

    weights = [item for group in sums for item in group]
    left_refs, right_refs, w_refs = take(left_count), take(len(rights)), take(len(weights))
    given_refs = take(given)
    grad_refs, made_refs = take(out_count), take(made)
    stage, flip, right_all, out_ref = take(4)
    w_bufs = take(len(weights))
    part, first, second, away, come_one, come_two, come_three, result = take(8)
    given_bufs, made_bufs = take(given), take(made - (ending == "branch"))
    acc, dots, scales, gain_parts, gain_come, given_sem, made_sem, gain_send, gain_recv = take(9)
    in_sem, right_sem, w_sem, ar_send, ar_recv, core_send, core_recv, two_send, two_recv, three_send, three_recv, out_sem = refs
    width = part.shape[2]
    block = come_three.shape[1]
    all_chunks = chunks * len(sums)
    place = lax.axis_index("mp")
    seq, batch = lax.axis_index("seq"), lax.axis_index("batch")
    core, chip = lax.rem(seq, 2), lax.div(seq, 2)
    sibling = seq + 1 - 2 * core
    beside = seq + 2 - 4 * chip
    pair = place + 1 - 2 * lax.rem(place, 2)
    across = 3 - place
    is_mid = (place == 1) | (place == 2)
    is_end = (place == 0) | (place == 3)

    def columns_of(c):
        return pl.ds(pl.multiple_of(c * width, width), width)

    def weight(at, group, c):
        here = columns_of(c - group * chunks)
        source = w_refs[at].at[here, :] if weights[at][2] == "nt" else w_refs[at].at[:, here]
        slot = lax.rem(c, 3)
        return pltpu.make_async_copy(source, w_bufs[at].at[slot], w_sem.at[at, slot])

    members = []
    for group, items in enumerate(sums):
        for _ in items:
            members.append(group)

    def load_weights(c):
        for group in range(len(sums)):

            @pl.when((c >= group * chunks) & (c < (group + 1) * chunks))
            def _():
                for at in range(len(weights)):
                    if members[at] == group:
                        weight(at, group, c).start()

    def remote(source, target, send, recv, device):
        return pltpu.make_async_remote_copy(
            src_ref=source, dst_ref=target, send_sem=send, recv_sem=recv, device_id=device, device_id_type=MESH
        )

    def slot_of(c):
        return lax.rem(c, chunks)

    high = part.shape[1] // HALVES

    def rows_of(h):
        return slice(h * high, (h + 1) * high)

    def up(c, h):
        slot = slot_of(c)
        source, target = part.at[slot, rows_of(h)], first.at[slot, rows_of(h)]
        return remote(source, target, ar_send.at[0, h, c], ar_recv.at[0, h, c], {"mp": pair})

    def over(c, h):
        slot = slot_of(c)
        source, target = part.at[slot, rows_of(h)], second.at[slot, rows_of(h)]
        return remote(source, target, ar_send.at[1, h, c], ar_recv.at[1, h, c], {"mp": across})

    def down(c, h):
        here = out_ref.at[rows_of(h), columns_of(c)]
        return remote(here, here, ar_send.at[2, h, c], ar_recv.at[2, h, c], {"mp": pair})

    def to_core(u):
        return remote(away.at[lax.rem(u, 2)], come_one.at[u], core_send.at[u], core_recv.at[u], {"seq": sibling})

    def chip_first(u):
        return 1 - lax.rem(u, 2)

    def sent_at(u, k):
        x_first = chip_first(u)
        return x_first * (2 * k + 1 - chip) + (1 - x_first) * (2 * (1 - batch) + k)

    def kept_at(u, k):
        x_first = chip_first(u)
        return x_first * (2 * k + chip) + (1 - x_first) * (2 * batch + k)

    def own_at(u):
        x_first = chip_first(u)
        return x_first * batch + (1 - x_first) * chip

    def device_of(x_way):
        return {
            "seq": x_way * beside + (1 - x_way) * seq,
            "batch": x_way * batch + (1 - x_way) * (1 - batch),
        }

    def second_hop(u, k):
        return remote(
            come_one.at[u, sent_at(u, k)], come_two.at[u, k], two_send.at[k, u], two_recv.at[k, u], device_of(chip_first(u))
        )

    def third_hop(u):
        return remote(
            come_two.at[u, 1 - own_at(u)], come_three.at[u], three_send.at[u], three_recv.at[u], device_of(1 - chip_first(u))
        )

    def left_copy(at):
        return pltpu.make_async_copy(left_refs[at], stage, in_sem.at[at])

    def right_copy(at):
        offset, source, size = rights[at]
        return pltpu.make_async_copy(
            right_refs[at].at[:, source : source + size], right_all.at[:, offset : offset + size], right_sem.at[at]
        )

    def out_copy(at, u):
        kind, index, offset, start, size = spans[at]
        slot = lax.rem(u, 2)
        if size < block:
            source = result.at[slot, :, start % block : start % block + size]
            target = grad_refs[index].at[:, offset : offset + size]
        else:
            source = result.at[slot]
            here = pl.ds(pl.multiple_of((u - start // block) * block + offset, block), block)
            target = grad_refs[index].at[here, :] if kind == "turned" else grad_refs[index].at[:, here]
        return pltpu.make_async_copy(source, target, out_sem.at[at, slot])

    def units_of(at):
        _, _, _, start, size = spans[at]
        return start // block, max((start + size) // block, start // block + 1)

    seq_count = lax.axis_size("seq")
    peers = lax.axis_size("batch") * seq_count
    me = batch * seq_count + seq

    def peer(k):
        there = lax.rem(me + k, peers)
        return there, {"batch": lax.div(there, seq_count), "seq": lax.rem(there, seq_count)}

    def gain_copy(k):
        there, device = peer(k)
        return remote(gain_parts.at[there], gain_come.at[k], gain_send.at[k], gain_recv.at[k], device)

    def given_copy(at):
        return pltpu.make_async_copy(given_refs[at], given_bufs[at], given_sem.at[at])

    def made_copy(at):
        source = out_ref.at[:, columns // 2 :] if ending == "branch" and at == made - 1 else made_bufs[at]
        return pltpu.make_async_copy(source, made_refs[at], made_sem.at[at])

    columns = out_ref.shape[1]
    rows = out_ref.shape[0]
    tile = rows // TILES

    def tile_of(i):
        return pl.ds(pl.multiple_of(i * tile, tile), tile)

    def branch_rows(i):
        here = tile_of(i)
        gm_buf, gb_buf, _ = made_bufs[:3]
        x_buf, b_buf, gain_buf, _ = given_bufs
        grad = out_ref[here, : columns // 2].astype(F32)
        middle = x_buf[here, :].astype(F32) + b_buf[here, :].astype(F32)
        scale = lax.rsqrt(jnp.mean(middle * middle, axis=-1, keepdims=True) + epsilon)
        scaled = grad * gain_buf[...]
        mean = jnp.mean(middle * scaled, axis=-1, keepdims=True)
        value = stage[here, :].astype(F32) + scale * scaled - middle * (scale * scale * scale) * mean
        gm_buf[here, :] = value
        gb_buf[here, :] = value.astype(BF16)
        acc[...] += jnp.sum(grad * middle * scale, axis=0, keepdims=True)

    def branch_end():
        made_bufs[2][...] = dot_nt(made_bufs[1][...], given_bufs[3][...]).astype(BF16)
        made_bufs[3][...] = acc[...]
        for at in range(4):
            made_copy(at).start()

    def token_columns(c):
        here = columns_of(c)
        x_buf, _, gain_buf = given_bufs[:3]
        value = out_ref[:, here].astype(F32) * x_buf[:, here].astype(F32)
        dots[...] += value * gain_buf[:, here]
        acc[:, here] = jnp.sum(value * scales[...], axis=0, keepdims=True)

    def token_rows(i, carry):
        here = tile_of(i)
        x_buf, gm_buf, gain_buf = given_bufs[:3]
        scale = scales[here, :1]
        mean = jnp.sum(dots[here, :], axis=-1, keepdims=True) * (1.0 / columns)
        wide = x_buf[here, :].astype(F32)
        scaled = out_ref[here, :].astype(F32) * gain_buf[...]
        value = gm_buf[here, :] + scale * scaled - wide * ((scale * scale * scale) * mean)
        made_bufs[0][here, :] = value.astype(BF16)
        return carry

    def output_rows(i):
        here = tile_of(i)
        x_buf, b_buf, m_buf = given_bufs[0], given_bufs[4], given_bufs[5]
        wide = x_buf[here, :].astype(F32)
        scale = lax.rsqrt(jnp.mean(wide * wide, axis=-1, keepdims=True) + epsilon)
        scales[here, :] = jnp.broadcast_to(scale, (tile, width))
        value = wide + b_buf[here, :].astype(F32) + m_buf[here, :].astype(F32)
        made_bufs[2][here, :] = value.astype(BF16)

    acc[...] = jnp.zeros_like(acc)
    dots[...] = jnp.zeros_like(dots)
    load_weights(0)
    load_weights(1)
    for at in range(len(rights)):
        right_copy(at).start()
    left_copy(0).start()
    for at in range(given):
        given_copy(at).start()

    barrier = pltpu.get_barrier_semaphore()
    if ending == "tokens":
        greeted = [{"mp": pair}] + [peer(k)[1] for k in range(1, peers)]
    else:
        greeted = [{"mp": pair}, {"seq": sibling}, {"seq": beside}, {"batch": 1 - batch}]
    for device in greeted:
        pl.semaphore_signal(barrier, inc=1, device_id=device, device_id_type=MESH)

    @pl.when(is_mid)
    def _():
        pl.semaphore_signal(barrier, inc=1, device_id={"mp": across}, device_id_type=MESH)
        pl.semaphore_wait(barrier, len(greeted) + 1)

    @pl.when(is_end)
    def _():
        pl.semaphore_wait(barrier, len(greeted))

    for at in range(len(rights)):
        right_copy(at).wait()

    def left_of(u):
        index = 0
        for at in range(1, left_count):
            index = index + (u >= flips_before[at]).astype(jnp.int32)
        return index

    def product(u, at, side):
        row = pl.multiple_of((2 * at + side) * block, block)
        column = pl.multiple_of(u * block, block)
        return dot_nn(flip[left_of(u), pl.ds(row, block), :], right_all[:, pl.ds(column, block)])

    def step_of(u):
        return (u // active) * period + u % active

    def on_unit(t, body):
        u = lax.div(t, period) * active + lax.rem(t, period)

        @pl.when((t >= 0) & (lax.rem(t, period) < active) & (u < units))
        def _():
            body(u)

    def first_stage(u):
        @pl.when(u >= 2)
        def _():
            to_core(u - 2).wait_send()

        for at in range(4):
            away[lax.rem(u, 2), at] = product(u, at, 1 - core).astype(BF16)
        to_core(u).start()

    def second_stage(u):
        to_core(u).wait_recv()
        for at in range(4):
            come_one[u, at] = (product(u, at, core) + come_one[u, at].astype(F32)).astype(BF16)
        for k in range(2):
            second_hop(u, k).start()

    def third_stage(u):
        for k in range(2):
            second_hop(u, k).wait_recv()
        sent = 1 - own_at(u)
        come_two[u, sent] = (come_two[u, sent].astype(F32) + come_one[u, kept_at(u, sent)].astype(F32)).astype(BF16)
        third_hop(u).start()

    def last_stage(u):
        third_hop(u).wait_recv()
        own = own_at(u)
        value = come_three[u].astype(F32) + come_two[u, own].astype(F32) + come_one[u, kept_at(u, own)].astype(F32)
        for at in range(len(spans)):
            low, high = units_of(at)

            @pl.when((u - 2 >= low) & (u - 2 < high))
            def _():
                out_copy(at, u - 2).wait()

        for kind in ("turned", "plain"):
            mine = [units_of(at) for at in range(len(spans)) if spans[at][0] == kind]
            if mine:
                low, high = min(m[0] for m in mine), max(m[1] for m in mine)

                @pl.when((u >= low) & (u < high))
                def _():
                    result[lax.rem(u, 2)] = value.T if kind == "turned" else value

        for at in range(len(spans)):
            low, high = units_of(at)

            @pl.when((u >= low) & (u < high))
            def _():
                out_copy(at, u).start()

    def step(t, carry):
        @pl.when((t >= chunks) & (t < all_chunks))
        def _():
            @pl.when(is_end)
            def _():
                for h in range(HALVES):
                    up(t - chunks, h).wait_send()

            @pl.when(is_mid)
            def _():
                for h in range(HALVES):
                    over(t - chunks, h).wait_send()

        for group, items in enumerate(sums):

            @pl.when((t >= group * chunks) & (t < (group + 1) * chunks))
            def _():
                value = None
                for at, (start, size, mode) in enumerate(weights):
                    if members[at] == group:
                        weight(at, group, t).wait()
                        dot = dot_nt if mode == "nt" else dot_nn
                        term = dot(right_all[:, start : start + size], w_bufs[at][lax.rem(t, 3)])
                        value = term if value is None else value + term
                part[slot_of(t)] = value.astype(BF16)

        @pl.when(t < all_chunks)
        def _():
            @pl.when(is_end)
            def _():
                for h in range(HALVES):
                    up(t, h).start()

            load_weights(t + 2)

        @pl.when(is_mid & (t >= UP_LAG) & (t < all_chunks + UP_LAG))
        def _():
            c = t - UP_LAG
            slot = slot_of(c)
            for h in range(HALVES):
                here = rows_of(h)
                up(c, h).wait_recv()
                part[slot, here] = (part[slot, here].astype(F32) + first[slot, here].astype(F32)).astype(BF16)
                over(c, h).start()

        @pl.when(is_mid & (t >= OVER_LAG) & (t < all_chunks + OVER_LAG))
        def _():
            c = t - OVER_LAG
            slot = slot_of(c)
            for h in range(HALVES):
                here = rows_of(h)
                over(c, h).wait_recv()
                value = part[slot, here].astype(F32) + second[slot, here].astype(F32)
                out_ref[here, columns_of(c)] = value.astype(BF16)
                down(c, h).start()

        @pl.when(is_end & (t >= DOWN_LAG) & (t < all_chunks + DOWN_LAG))
        def _():
            for h in range(HALVES):
                down(t - DOWN_LAG, h).wait_recv()

        for at in range(left_count):

            @pl.when(t == max(step_of(flips_before[at]) - 2, at))
            def _():
                left_copy(at).wait()

                def turn(k, carry):
                    here = pl.ds(pl.multiple_of(k * block, block), block)
                    flip[at, here, :] = stage[:, here].T
                    return carry

                lax.fori_loop(0, flip.shape[1] // block, turn, 0)
                if at + 1 < left_count:
                    left_copy(at + 1).start()

        on_unit(t, first_stage)
        on_unit(t - 1, second_stage)
        on_unit(t - 1 - LAG, third_stage)
        on_unit(t - 1 - 2 * LAG, last_stage)
        if ending == "branch":

            @pl.when(t == chunks + DOWN_LAG)
            def _():
                for at in range(given):
                    given_copy(at).wait()

            @pl.when((t >= chunks + DOWN_LAG) & (t < chunks + DOWN_LAG + TILES))
            def _():
                branch_rows(t - chunks - DOWN_LAG)

            @pl.when(t == chunks + DOWN_LAG + TILES)
            def _():
                branch_end()

        else:

            @pl.when(t == TILES // 2)
            def _():
                for at in range(given):
                    given_copy(at).wait()

            @pl.when((t >= TILES // 2) & (t < TILES // 2 + TILES))
            def _():
                output_rows(t - TILES // 2)

            @pl.when(t == TILES // 2 + TILES)
            def _():
                made_copy(2).start()

            @pl.when((t >= LAST_LAG) & (t < all_chunks + LAST_LAG))
            def _():
                token_columns(t - LAST_LAG)

        return carry

    last = all_chunks + (DOWN_LAG if ending == "branch" else LAST_LAG)
    lax.fori_loop(0, max(step_of(units - 1) + 2 + 2 * LAG, last), step, 0)
    if ending == "branch":
        made_copy(made - 1).start()
    else:
        part_width = columns // peers
        for k in range(peers):
            here = slice(k * part_width, (k + 1) * part_width)
            gain_parts[k, 0:1, :] = acc[:, here]
            gain_parts[k, 1:2, :] = given_bufs[3][:, here]
        for k in range(1, peers):
            gain_copy(k).start()
        lax.fori_loop(0, TILES, token_rows, 0)
        made_copy(0).start()

    def finish(c, carry):
        @pl.when(is_mid)
        def _():
            for h in range(HALVES):
                down(c, h).wait_send()

        return carry

    lax.fori_loop(0, all_chunks, finish, 0)

    def finish_last(c, carry):
        @pl.when(is_end)
        def _():
            for h in range(HALVES):
                up(c, h).wait_send()

        @pl.when(is_mid)
        def _():
            for h in range(HALVES):
                over(c, h).wait_send()

        return carry

    lax.fori_loop(all_chunks - chunks, all_chunks, finish_last, 0)

    def settle(u, carry):
        for k in range(2):
            second_hop(u, k).wait_send()
        third_hop(u).wait_send()
        return carry

    lax.fori_loop(0, units, settle, 0)
    for u in (units - 2, units - 1):
        to_core(u).wait_send()
        for at in range(len(spans)):
            low, high = units_of(at)
            if low <= u < high:
                out_copy(at, u).wait()
    if ending == "tokens":
        gains = gain_parts[me]
        for k in range(1, peers):
            gain_copy(k).wait_recv()
            gains = gains + gain_come[k]
        made_bufs[1][...] = gains
        made_copy(1).start()
        for k in range(1, peers):
            gain_copy(k).wait_send()
    for at in range(made):
        made_copy(at).wait()


def exchange(lefts, rights, sums, flips_before, outs, spans, units, call_id, pace, ending, given, made, chunks=16):
    rows, depth = lefts[0].shape
    block = depth // 8
    placed, at = [], 0
    for _, source, size in rights:
        placed.append((at, source, size))
        at += size
    weights = [item[0] for group in sums for item in group]
    columns = weights[0].shape[0] if sums[0][0][3] == "nt" else weights[0].shape[1]
    width = columns // chunks
    sum_plan = [[item[1:] for item in group] for group in sums]
    plan = (len(lefts), placed, sum_plan, flips_before, spans, len(outs), units, chunks, *pace, ending, len(given), len(made))
    any_space = pl.BlockSpec(memory_space=pl.ANY)
    line_block = pltpu.VMEM((chunks, rows, width), BF16)
    peers = lax.axis_size("batch") * lax.axis_size("seq")
    kept = made[:-1] if ending == "branch" else made
    dma = pltpu.SemaphoreType.DMA
    all_chunks = chunks * len(sums)
    flops = sum(2 * rows * columns * size for group in sum_plan for _, size, _ in group) + 2 * rows * depth * at
    return pl.pallas_call(
        functools.partial(exchange_kernel, plan),
        out_shape=[jax.ShapeDtypeStruct(shape, F32) for shape in outs]
        + [jax.ShapeDtypeStruct(shape, kind) for shape, kind in made],
        in_specs=[any_space] * (len(lefts) + len(rights) + len(weights) + len(given)),
        out_specs=[any_space] * (len(outs) + len(made)),
        scratch_shapes=[
            pltpu.VMEM((rows, depth), BF16),
            pltpu.VMEM((len(lefts), depth, rows), BF16),
            pltpu.VMEM((rows, at), BF16),
            pltpu.VMEM((rows, columns * len(sums)), BF16),
        ]
        + [
            pltpu.VMEM((3, width, size) if mode == "nt" else (3, size, width), BF16)
            for group in sum_plan
            for _, size, mode in group
        ]
        + [
            line_block,
            line_block,
            line_block,
            pltpu.VMEM((2, 4, block, block), BF16),
            pltpu.VMEM((units, 4, block, block), BF16),
            pltpu.VMEM((units, 2, block, block), BF16),
            pltpu.VMEM((units, block, block), BF16),
            pltpu.VMEM((2, block, block), F32),
        ]
        + [pltpu.VMEM(value.shape, value.dtype) for value in given]
        + [pltpu.VMEM(shape, kind) for shape, kind in kept]
        + [
            pltpu.VMEM((1, depth), F32),
            pltpu.VMEM((rows, width), F32),
            pltpu.VMEM((rows, width), F32),
            pltpu.VMEM((peers, 2, depth // peers), F32),
            pltpu.VMEM((peers, 2, depth // peers), F32),
            dma((len(given),)),
            dma((len(made),)),
            dma((peers,)),
            dma((peers,)),
            dma((len(lefts),)),
            dma((len(rights),)),
            dma((len(weights), 3)),
            dma((3, HALVES, all_chunks)),
            dma((3, HALVES, all_chunks)),
            dma((units,)),
            dma((units,)),
            dma((2, units)),
            dma((2, units)),
            dma((units,)),
            dma((units,)),
            dma((len(spans), 2)),
        ],
        compiler_params=pltpu.CompilerParams(
            collective_id=call_id, has_side_effects=True, vmem_limit_bytes=62 << 20
        ),
        cost_estimate=pl.CostEstimate(flops=flops + (50 << 30), bytes_accessed=20 << 20, transcendentals=0),
        name=f"exchange_{call_id}",
    )(*lefts, *[right[0] for right in rights], *weights, *given)


def forward_kernel(
    mixed_ref, gain_ref, x_hbm, wo_hbm, wg_hbm, wu_hbm, ga_hbm,
    branch_hbm, n_hbm, act_hbm, gg_hbm, gu_hbm,
    branch, n_ref, act_ref, gg_ref, gu_ref, ga_ref, gate_acc, up_acc, squares, wo_buf, w_buf, part, first, second,
    ga_sem, wo_sem, w_sem, ar_send, ar_recv, out_sem, x_ref,
):
    chunks, rows, width = part.shape
    total_columns = branch.shape[1]
    place = lax.axis_index("mp")
    pair = place + 1 - 2 * lax.rem(place, 2)
    across = 3 - place
    is_mid = (place == 1) | (place == 2)
    is_end = (place == 0) | (place == 3)
    high = rows // HALVES
    deep = w_buf.shape[2]

    def columns_of(c):
        return pl.ds(pl.multiple_of(c * width, width), width)

    def rows_of(h):
        return slice(h * high, (h + 1) * high)

    def remote(source, target, kind, h, c, device):
        return pltpu.make_async_remote_copy(
            src_ref=source,
            dst_ref=target,
            send_sem=ar_send.at[kind, h, c],
            recv_sem=ar_recv.at[kind, h, c],
            device_id={"mp": device},
            device_id_type=MESH,
        )

    def up(c, h):
        return remote(part.at[c, rows_of(h)], first.at[c, rows_of(h)], 0, h, c, pair)

    def over(c, h):
        return remote(part.at[c, rows_of(h)], second.at[c, rows_of(h)], 1, h, c, across)

    def down(c, h):
        here = branch.at[rows_of(h), columns_of(c)]
        return remote(here, here, 2, h, c, pair)

    def out_weight(c):
        slot = lax.rem(c, 3)
        return pltpu.make_async_copy(wo_hbm.at[:, columns_of(c)], wo_buf.at[slot], wo_sem.at[slot])

    def deep_of(p):
        return pl.ds(pl.multiple_of(p * deep, deep), deep)

    def weight(at, p):
        slot = lax.rem(p, 3)
        source = (wg_hbm, wu_hbm)[at].at[deep_of(p), :]
        return pltpu.make_async_copy(source, w_buf.at[at, slot], w_sem.at[at, slot])

    ga_copy = pltpu.make_async_copy(ga_hbm, ga_ref, ga_sem.at[0])
    out_weight(0).start()
    out_weight(1).start()
    for p in range(2):
        for at in range(2):
            weight(at, p).start()
    ga_copy.start()
    x_copy = pltpu.make_async_copy(x_hbm, x_ref, ga_sem.at[2])
    x_copy.start()
    barrier = pltpu.get_barrier_semaphore()
    pl.semaphore_signal(barrier, inc=1, device_id={"mp": pair}, device_id_type=MESH)

    @pl.when(is_mid)
    def _():
        pl.semaphore_signal(barrier, inc=1, device_id={"mp": across}, device_id_type=MESH)
        pl.semaphore_wait(barrier, 2)

    @pl.when(is_end)
    def _():
        pl.semaphore_wait(barrier, 1)

    squares[...] = jnp.zeros_like(squares)
    per_deep = deep // width

    def step(t, carry):
        @pl.when(t < chunks)
        def _():
            out_weight(t).wait()
            part[t] = dot_nn(mixed_ref[...], wo_buf[lax.rem(t, 3)]).astype(BF16)

            @pl.when(is_end)
            def _():
                for h in range(HALVES):
                    up(t, h).start()

            @pl.when(t + 2 < chunks)
            def _():
                out_weight(t + 2).start()

        @pl.when(is_mid & (t >= UP_LAG) & (t < chunks + UP_LAG))
        def _():
            c = t - UP_LAG
            for h in range(HALVES):
                here = rows_of(h)
                up(c, h).wait_recv()
                part[c, here] = (part[c, here].astype(F32) + first[c, here].astype(F32)).astype(BF16)
                over(c, h).start()

        @pl.when(is_mid & (t >= OVER_LAG) & (t < chunks + OVER_LAG))
        def _():
            c = t - OVER_LAG
            for h in range(HALVES):
                here = rows_of(h)
                over(c, h).wait_recv()
                value = part[c, here].astype(F32) + second[c, here].astype(F32)
                branch[here, columns_of(c)] = value.astype(BF16)
                down(c, h).start()

        @pl.when(is_end & (t >= DOWN_LAG))
        def _():
            for h in range(HALVES):
                down(t - DOWN_LAG, h).wait_recv()

        @pl.when(t == DOWN_LAG)
        def _():
            x_copy.wait()

        @pl.when((t >= DOWN_LAG) & (lax.rem(t - DOWN_LAG, per_deep) == per_deep - 1))
        def _():
            p = lax.div(t - DOWN_LAG, per_deep)
            here = deep_of(p)
            middle = x_ref[:, here].astype(F32) + branch[:, here].astype(F32)
            squares[...] += jnp.sum(middle * middle, axis=-1, keepdims=True)
            scaled = (middle * gain_ref[:, here]).astype(BF16)
            for at, acc in enumerate((gate_acc, up_acc)):
                weight(at, p).wait()
                value = dot_nn(scaled, w_buf[at, lax.rem(p, 3)])

                @pl.when(p == 0)
                def _():
                    acc[...] = value

                @pl.when(p > 0)
                def _():
                    acc[...] += value

            @pl.when((p + 2) * deep < total_columns)
            def _():
                for at in range(2):
                    weight(at, p + 2).start()

        return carry

    lax.fori_loop(0, chunks + DOWN_LAG, step, 0)
    ga_copy.wait()
    tile = rows // TILES
    outs = [(n_ref, n_hbm), (act_ref, act_hbm), (gg_ref, gg_hbm), (gu_ref, gu_hbm)]

    def out_copy(at, i):
        here = pl.ds(pl.multiple_of(i * tile, tile), tile)
        return pltpu.make_async_copy(outs[at][0].at[here, :], outs[at][1].at[here, :], out_sem.at[at, i])

    branch_copy = pltpu.make_async_copy(branch, branch_hbm, ga_sem.at[1])
    branch_copy.start()

    def rows_step(i, carry):
        here = pl.ds(pl.multiple_of(i * tile, tile), tile)
        scale = lax.rsqrt(squares[here, :1] * (1.0 / total_columns) + epsilon)
        middle = x_ref[here, :].astype(F32) + branch[here, :].astype(F32)
        n_ref[here, :] = (middle * scale * gain_ref[...]).astype(BF16)
        gate = gate_acc[here, :] * scale
        up_pre = up_acc[here, :] * scale
        grad = ga_ref[here, :].astype(F32)
        sigmoid = jax.nn.sigmoid(gate)
        swish = gate * sigmoid
        act_ref[here, :] = (swish * up_pre).astype(BF16)
        gu_ref[here, :] = (grad * swish).astype(BF16)
        gg_ref[here, :] = (grad * up_pre * sigmoid * (1.0 + gate * (1.0 - sigmoid))).astype(BF16)
        for at in range(4):
            out_copy(at, i).start()
        return carry

    lax.fori_loop(0, TILES, rows_step, 0)

    def finish(c, carry):
        @pl.when(is_end)
        def _():
            for h in range(HALVES):
                up(c, h).wait_send()

        @pl.when(is_mid)
        def _():
            for h in range(HALVES):
                over(c, h).wait_send()
                down(c, h).wait_send()

        return carry

    lax.fori_loop(0, chunks, finish, 0)

    def drain(i, carry):
        for at in range(4):
            out_copy(at, i).wait()
        return carry

    lax.fori_loop(0, TILES, drain, 0)
    branch_copy.wait()


def forward(mixed, tokens, gain, w_output, w_gate, w_up, grad_active, call_id, chunks=16, deep=256):
    rows, columns = tokens.shape
    hidden = w_gate.shape[1]
    width = columns // chunks
    vmem, any_space = pl.BlockSpec(memory_space=pltpu.VMEM), pl.BlockSpec(memory_space=pl.ANY)
    dma = pltpu.SemaphoreType.DMA
    shapes = [(rows, columns), (rows, columns), (rows, hidden), (rows, hidden), (rows, hidden)]
    line_block = pltpu.VMEM((chunks, rows, width), BF16)
    return pl.pallas_call(
        forward_kernel,
        in_specs=[vmem] * 2 + [any_space] * 5,
        out_specs=[any_space] * 5,
        out_shape=[jax.ShapeDtypeStruct(shape, BF16) for shape in shapes],
        scratch_shapes=[pltpu.VMEM(shape, BF16) for shape in shapes]
        + [
            pltpu.VMEM((rows, hidden), BF16),
            pltpu.VMEM((rows, hidden), F32),
            pltpu.VMEM((rows, hidden), F32),
            pltpu.VMEM((rows, PAIR), F32),
            pltpu.VMEM((3, mixed.shape[1], width), BF16),
            pltpu.VMEM((2, 3, deep, hidden), BF16),
            line_block,
            line_block,
            line_block,
            dma((3,)),
            dma((3,)),
            dma((2, 3)),
            dma((3, HALVES, chunks)),
            dma((3, HALVES, chunks)),
            dma((4, TILES)),
            pltpu.VMEM((rows, columns), BF16),
        ],
        compiler_params=pltpu.CompilerParams(
            collective_id=call_id, has_side_effects=True, vmem_limit_bytes=62 << 20
        ),
        name="forward",
    )(mixed, gain, tokens, w_output, w_gate, w_up, grad_active)


def final_kernel(gn_ref, x_ref, gm_ref, gain_ref, mlp_ref, out_ref, gains_ref, acc, parts, come, send_sem, recv_sem):
    seq, batch = lax.axis_index("seq"), lax.axis_index("batch")
    seq_count = lax.axis_size("seq")
    peers = parts.shape[0]
    block = parts.shape[2]
    me = batch * seq_count + seq

    def peer(k):
        there = lax.rem(me + k, peers)
        return there, {"batch": lax.div(there, seq_count), "seq": lax.rem(there, seq_count)}

    def copy(k):
        there, device = peer(k)
        return pltpu.make_async_remote_copy(
            src_ref=parts.at[there],
            dst_ref=come.at[k],
            send_sem=send_sem.at[k],
            recv_sem=recv_sem.at[k],
            device_id=device,
            device_id_type=MESH,
        )

    barrier = pltpu.get_barrier_semaphore()
    for k in range(1, peers):
        pl.semaphore_signal(barrier, inc=1, device_id=peer(k)[1], device_id_type=MESH)
    rows = x_ref.shape[0]
    tile = rows // 8
    gain = gain_ref[...]
    acc[...] = jnp.zeros_like(acc)

    def rows_step(i, carry):
        here = pl.ds(pl.multiple_of(i * tile, tile), tile)
        wide = x_ref[here, :].astype(F32)
        grad = gn_ref[here, :].astype(F32)
        scale = lax.rsqrt(jnp.mean(wide * wide, axis=-1, keepdims=True) + epsilon)
        scaled = grad * gain
        mean = jnp.mean(wide * scaled, axis=-1, keepdims=True)
        result = gm_ref[here, :] + scale * scaled - wide * (scale * scale * scale) * mean
        out_ref[here, :] = result.astype(BF16)
        acc[...] += jnp.sum(grad * wide * scale, axis=0, keepdims=True)
        return carry

    lax.fori_loop(0, 8, rows_step, 0)
    for k in range(peers):
        here = slice(k * block, (k + 1) * block)
        parts[k, 0:1, :] = acc[:, here]
        parts[k, 1:2, :] = mlp_ref[:, here]
    pl.semaphore_wait(barrier, peers - 1)
    for k in range(1, peers):
        copy(k).start()
    total = parts[me]
    for k in range(1, peers):
        copy(k).wait_recv()
        total = total + come[k]
    gains_ref[...] = total
    for k in range(1, peers):
        copy(k).wait_send()


def final(grad_normed, tokens, grad_middle, gain, mlp_part, call_id):
    rows, width = tokens.shape
    peers = lax.axis_size("batch") * lax.axis_size("seq")
    block = width // peers
    vmem = pl.BlockSpec(memory_space=pltpu.VMEM)
    return pl.pallas_call(
        final_kernel,
        out_shape=[jax.ShapeDtypeStruct((rows, width), BF16), jax.ShapeDtypeStruct((2, block), F32)],
        in_specs=[vmem] * 5,
        out_specs=[vmem, vmem],
        scratch_shapes=[
            pltpu.VMEM((1, width), F32),
            pltpu.VMEM((peers, 2, block), F32),
            pltpu.VMEM((peers, 2, block), F32),
            pltpu.SemaphoreType.DMA((peers,)),
            pltpu.SemaphoreType.DMA((peers,)),
        ],
        compiler_params=pltpu.CompilerParams(collective_id=call_id, has_side_effects=True),
        name="final",
    )(grad_normed, tokens, grad_middle, gain, mlp_part)


def settle_kernel(pieces, count, *refs):
    sources, targets = refs[:count], refs[count : -count - 2]
    bufs, load_sem, store_sem = refs[-count - 2 : -2], refs[-2], refs[-1]

    def load(at):
        array, start, size, _, _ = pieces[at]
        here = slice(start, start + size)
        return pltpu.make_async_copy(sources[array].at[here, :], bufs[array].at[here, :], load_sem.at[at])

    def store(at):
        array, start, size, index, row = pieces[at]
        here, there = slice(start, start + size), slice(row, row + size)
        return pltpu.make_async_copy(bufs[array].at[here, :], targets[index].at[there, :], store_sem.at[at])

    for at in range(len(pieces)):
        load(at).start()
    for at in range(len(pieces)):
        load(at).wait()
        store(at).start()
    for at in range(len(pieces)):
        store(at).wait()


def settle(groups):
    pieces, shapes, arrays = [], [], []
    for index, group in enumerate(groups):
        row = 0
        for array in group:
            parts = 4 if array.size >= 1 << 18 and array.shape[0] % 64 == 0 else 1
            size = array.shape[0] // parts
            for part in range(parts):
                pieces.append((len(arrays), part * size, size, index, row + part * size))
            arrays.append(array)
            row += array.shape[0]
        shapes.append(jax.ShapeDtypeStruct((row, group[0].shape[1]), group[0].dtype))
    any_space = pl.BlockSpec(memory_space=pl.ANY)
    dma = pltpu.SemaphoreType.DMA
    return pl.pallas_call(
        functools.partial(settle_kernel, pieces, len(arrays)),
        in_specs=[any_space] * len(arrays),
        out_specs=[any_space] * len(groups),
        out_shape=shapes,
        scratch_shapes=[pltpu.VMEM(array.shape, array.dtype) for array in arrays]
        + [dma((len(pieces),)), dma((len(pieces),))],
        compiler_params=pltpu.CompilerParams(vmem_limit_bytes=62 << 20),
        name="settle",
    )(*arrays)


def scatter_sum(left, right):
    rows, depth = left.shape
    columns = right.shape[1]
    batch_count = lax.axis_size("batch")
    seq_index = lax.axis_index("seq")
    core, chip = seq_index % 2, seq_index // 2
    block = depth // (4 * batch_count)
    split = left.reshape(rows, batch_count, 2, 2, block)
    size = lax.axis_size("seq")

    def product(at):
        taken = lax.dynamic_index_in_dim(split, at, 3, keepdims=False).reshape(rows, depth // 2)
        return dot_tn(taken, right)

    away = product(1 - core).astype(BF16)
    arrived = lax.ppermute(away, "seq", [(s, s ^ 1) for s in range(size)])
    kept = (product(core) + arrived.astype(F32)).astype(BF16)
    kept = kept.reshape(batch_count, 2, block, columns)
    half = columns // 2

    def over_chip(values, axis):
        sent = lax.dynamic_index_in_dim(values, 1 - chip, axis, keepdims=False)
        stay = lax.dynamic_index_in_dim(values, chip, axis, keepdims=False)
        came = lax.ppermute(sent, "seq", [(s, s ^ 2) for s in range(size)])
        return stay.astype(F32) + came.astype(F32)

    def over_batch(values):
        if batch_count == 2:
            here = lax.axis_index("batch")
            sent = lax.dynamic_index_in_dim(values, 1 - here, 0, keepdims=False)
            stay = lax.dynamic_index_in_dim(values, here, 0, keepdims=False)
            came = lax.ppermute(sent, "batch", [(0, 1), (1, 0)])
            return stay.astype(F32) + came.astype(F32)
        return lax.psum_scatter(values, "batch", scatter_dimension=0, tiled=False).astype(F32)

    one = over_batch(over_chip(kept[..., :half], 1).astype(BF16))
    two = over_chip(over_batch(kept[..., half:]).astype(BF16), 0)
    return jnp.concatenate([one, two], axis=1)


def local(
    tokens, segment_ids, attn_gain, w_query, w_key, w_value, w_output, mlp_gain, w_gate, w_up, w_down, cotangent
):
    rows, width = tokens.shape
    cos, sin, normed, queries, key_value, grad_active = project(
        tokens, attn_gain[None, :], w_query, w_key, w_value, segment_ids, cotangent, w_down, 5
    )
    key_value = key_value.reshape(3 * rows, 2 * PAIR)
    mixed, logs = attend(queries, key_value, segment_ids)
    branch_low, normed_two, active, grad_gate_low, grad_up_low = forward(
        mixed, tokens, mlp_gain[None, :], w_output, w_gate, w_up, grad_active, 1
    )
    wide = tokens.astype(F32)
    middle = wide + branch_low.astype(F32)
    fused = lax.axis_size("batch") == 2
    hidden = w_gate.shape[1]
    unit = width // 8
    early = hidden * 5 // 8 // unit * unit
    if fused:
        grad_gate, grad_up, grad_down_one, grad_middle, grad_branch, grad_mixed, grad_mlp_gain, mlp_out = exchange(
            [normed_two, cotangent],
            [(grad_gate_low, 0, hidden), (grad_up_low, 0, hidden), (active, 0, hidden)],
            [
                [(w_gate, 0, hidden, "nt"), (w_up, hidden, hidden, "nt")],
                [(w_down, 2 * hidden, hidden, "nn")],
            ],
            (0, 2 * hidden // unit),
            [(unit, hidden), (unit, hidden), (early, unit)],
            [
                ("plain", 0, 0, 0, hidden),
                ("plain", 1, 0, hidden, hidden),
                ("turned", 2, 0, 2 * hidden, early),
            ],
            (2 * hidden + early) // unit,
            2,
            (3, 2),
            "branch",
            [tokens, branch_low, mlp_gain[None, :], w_output],
            [
                ((rows, width), F32),
                ((rows, width), BF16),
                ((rows, mixed.shape[1]), BF16),
                ((1, width), F32),
                ((rows, width), BF16),
            ],
        )
    else:
        grad_normed_two = line_sum([(grad_gate_low, w_gate, "nt"), (grad_up_low, w_up, "nt")], 2)
        grad_gate = scatter_sum(normed_two, grad_gate_low)
        grad_up = scatter_sum(normed_two, grad_up_low)
        mlp_out = lax.psum(dot_nn(active, w_down).astype(BF16), "mp")
        grad_normed_two = grad_normed_two.astype(F32)
        scaled_two = grad_normed_two * mlp_gain
        scale_two = lax.rsqrt(jnp.mean(middle * middle, axis=-1, keepdims=True) + epsilon)
        grad_middle = (
            cotangent.astype(F32)
            + scale_two * scaled_two
            - middle
            * (scale_two * scale_two * scale_two)
            * jnp.mean(middle * scaled_two, axis=-1, keepdims=True)
        )
        grad_mlp_gain = jnp.sum(grad_normed_two * middle * scale_two, axis=0)[None, :]
        grad_branch = grad_middle.astype(BF16)
        grad_mixed = dot_nt(grad_branch, w_output).astype(BF16)

    grad_query_pre, grad_key_pre, grad_value_pre = attend_back(
        queries, key_value, segment_ids, mixed, grad_mixed, logs, cos, sin, 6
    )
    query_width = grad_query_pre.shape[1]
    if fused:
        late, mixed_width = hidden - early, mixed.shape[1]
        query_at = late + mixed_width
        key_at = query_at + query_width
        grad_down_two, grad_output, grad_query, grad_key, grad_value, grad_tokens, gains, output = exchange(
            [cotangent, grad_branch, normed],
            [
                (active, early, late),
                (mixed, 0, mixed_width),
                (grad_query_pre, 0, query_width),
                (grad_key_pre, 0, PAIR),
                (grad_value_pre, 0, PAIR),
            ],
            [
                [
                    (w_query, query_at, query_width, "nt"),
                    (w_key, key_at, PAIR, "nt"),
                    (w_value, key_at + PAIR, PAIR, "nt"),
                ]
            ],
            (0, late // unit, query_at // unit),
            [(late, unit), (mixed_width, unit), (unit, query_width), (unit, PAIR), (unit, PAIR)],
            [
                ("turned", 0, 0, 0, late),
                ("turned", 1, 0, late, mixed_width),
                ("plain", 2, 0, query_at, query_width),
                ("plain", 3, 0, key_at, PAIR),
                ("plain", 4, 0, key_at + PAIR, PAIR),
            ],
            (key_at + 2 * PAIR) // unit,
            3,
            (3, 2),
            "tokens",
            [tokens, grad_middle, attn_gain[None, :], grad_mlp_gain, branch_low, mlp_out],
            [((rows, width), BF16), ((2, unit), F32), ((rows, width), BF16)],
        )
        grad_gate, grad_up, grad_down, grad_output, grad_query, grad_key, grad_value, grad_tokens, output = settle(
            [
                [grad_gate],
                [grad_up],
                [grad_down_one, grad_down_two],
                [grad_output],
                [grad_query],
                [grad_key],
                [grad_value],
                [grad_tokens],
                [output],
            ]
        )
    else:
        output = (middle + mlp_out.astype(F32)).astype(BF16)
        grad_down = scatter_sum(cotangent, active).T
        grad_output = scatter_sum(grad_branch, mixed).T
        grad_qkv = scatter_sum(normed, jnp.concatenate([grad_query_pre, grad_key_pre, grad_value_pre], axis=1))
        grad_query = grad_qkv[:, :query_width]
        grad_key = grad_qkv[:, query_width : query_width + PAIR]
        grad_value = grad_qkv[:, query_width + PAIR :]
        grad_normed = line_sum(
            [(grad_query_pre, w_query, "nt"), (grad_key_pre, w_key, "nt"), (grad_value_pre, w_value, "nt")], 3
        )
        grad_tokens, gains = final(grad_normed, tokens, grad_middle, attn_gain[None, :], grad_mlp_gain, 4)
    return (
        output,
        grad_tokens,
        gains[0],
        grad_query,
        grad_key,
        grad_value,
        grad_output,
        gains[1],
        grad_gate,
        grad_up,
        grad_down,
    )


def solution(mesh):
    tokens_spec = P(("batch", "seq"), None)
    in_specs = (
        tokens_spec,
        P("batch", None),
        P(),
        P(None, "mp"),
        P(None, "mp"),
        P(None, "mp"),
        P("mp", None),
        P(),
        P(None, "mp"),
        P(None, "mp"),
        P("mp", None),
        tokens_spec,
    )
    row_split = P(("batch", "seq"), "mp")
    column_split = P("mp", ("batch", "seq"))
    out_specs = (
        tokens_spec,
        tokens_spec,
        P(("batch", "seq")),
        row_split,
        row_split,
        row_split,
        column_split,
        P(("batch", "seq")),
        row_split,
        row_split,
        column_split,
    )
    return jax.shard_map(local, mesh=mesh, in_specs=in_specs, out_specs=out_specs, check_vma=False)
```
